32 devices in a mesh: part: 1 (over z), data: 4 (over y), seq: 8 (over x, core).
Axes of the slice: x: 4, y: 4, z: 1, core: 2. Of those that a mesh axis runs over, the one named last changes fastest.
The devices are a block of a 4x4x8 slice.
Arguments:
- enc_out: bfloat16 [128, 64, 512], P(('part', 'data'), 'seq')
- pred_out: bfloat16 [128, 32, 512], P(('part', 'data'))
- w_enc: bfloat16 [512, 640], replicated
- w_pred: bfloat16 [512, 640], replicated
- w_out: bfloat16 [640, 1024], replicated
- labels: int32 [128, 31], P(('part', 'data'))
- frame_len: int32 [128], P(('part', 'data'))
- label_len: int32 [128], P(('part', 'data'))
Outputs:
- output 1: float32 [128], P(('part', 'data'))
- output 2: bfloat16 [128, 64, 512], P(('part', 'data'), 'seq')
- output 3: float32 [128, 32, 512], P(('part', 'data'))
- output 4: float32 [512, 640], P('part')
- output 5: float32 [512, 640], P('part')
- output 6: float32 [640, 1024], P('part')
All inputs are finite; a program needn't handle non-finite values.
Results may differ from the reference program's by a relative error of at most 0.0127134.
Values are sent between devices in bfloat16 or wider.
A program may use at most 768 MiB of HBM per device.

```python
import jax
import jax.numpy as jnp
from jax import lax

H = 512
J = 640
V = 1024
UPOS = 32
B = 128
T = 64
T_BLK = 8
LABELS = UPOS - 1
NEG_FILL = -1e30


def setup_inputs(seed: int = 0, part: int = 0) -> dict:
    key = jax.random.key(seed)
    shared = jax.random.split(key, 3)
    own = jax.random.split(jax.random.fold_in(key, part), 5)
    enc_out = jax.random.normal(own[0], (B, T, H), jnp.float32)
    pred_out = jax.random.normal(own[1], (B, UPOS, H), jnp.float32)
    w_enc = jax.random.normal(shared[0], (H, J), jnp.float32) * H ** -0.5
    w_pred = jax.random.normal(shared[1], (H, J), jnp.float32) * H ** -0.5
    w_out = jax.random.normal(shared[2], (J, V), jnp.float32) * J ** -0.5
    labels = jax.random.randint(own[2], (B, LABELS), 1, V, jnp.int32)
    frame_len = jax.random.randint(own[3], (B,), T // 4 + 1, T + 1, jnp.int32).at[0].set(T)
    label_len = jax.random.randint(own[4], (B,), max(1, LABELS // 4), LABELS + 1, jnp.int32).at[B - 1].set(LABELS)
    return {"enc_out": enc_out.astype(jnp.bfloat16), "pred_out": pred_out.astype(jnp.bfloat16), "w_enc": w_enc.astype(jnp.bfloat16), "w_pred": w_pred.astype(jnp.bfloat16), "w_out": w_out.astype(jnp.bfloat16), "labels": labels, "frame_len": frame_len, "label_len": label_len}


def joint_block(enc_blk, pred_utt, w_enc, w_pred, w_out):
    act_enc = jnp.dot(enc_blk, w_enc, preferred_element_type=jnp.float32).astype(jnp.bfloat16)
    act_pred = jnp.dot(pred_utt, w_pred, preferred_element_type=jnp.float32).astype(jnp.bfloat16)
    hidden = jnp.tanh(act_enc.astype(jnp.float32)[:, None, :] + act_pred.astype(jnp.float32)[None, :, :]).astype(jnp.bfloat16).reshape(T_BLK * UPOS, J)
    logits = jnp.dot(hidden, w_out, preferred_element_type=jnp.float32)
    return hidden, logits


def lattice_terms(enc_utt, pred_utt, lab_ids, w_enc, w_pred, w_out):
    flat_ids = jnp.tile(lab_ids, T_BLK)

    def per_blk(enc_blk):
        _, logits = joint_block(enc_blk, pred_utt, w_enc, w_pred, w_out)
        log_probs = jax.nn.log_softmax(logits, axis=-1)
        picked = jnp.take_along_axis(log_probs, flat_ids[:, None], axis=1)[:, 0]
        return log_probs[:, 0].reshape(T_BLK, UPOS), picked.reshape(T_BLK, UPOS)

    blank, label_lp = lax.map(per_blk, enc_utt)
    return blank.reshape(T, UPOS), label_lp.reshape(T, UPOS)


def lattice_loss(blank, label_lp, frame_len, label_len):
    label_pos = jnp.arange(UPOS)
    lab_cum = jnp.concatenate([jnp.zeros((B, T, 1), jnp.float32), jnp.cumsum(label_lp[:, :, :-1], axis=2)], axis=2)
    start_row = jnp.broadcast_to(jnp.where(label_pos == 0, 0.0, NEG_FILL), (B, UPOS)).astype(jnp.float32)

    def frame_step(carry, frame_in):
        blank_t, cum_t = frame_in
        alpha_t = cum_t + lax.cumlogsumexp(carry - cum_t, axis=1)
        return alpha_t + blank_t, alpha_t

    blank_tm = jnp.swapaxes(blank, 0, 1)
    _, alpha = lax.scan(frame_step, start_row, (blank_tm, jnp.swapaxes(lab_cum, 0, 1)))
    last_cell = (jnp.arange(T)[:, None, None] == frame_len[None, :, None] - 1) & (label_pos[None, None, :] == label_len[None, :, None])
    return -jnp.sum(jnp.where(last_cell, alpha + blank_tm, 0.0), axis=(0, 2))


def reference(enc_out, pred_out, w_enc, w_pred, w_out, labels, frame_len, label_len):
    lab_ids = jnp.concatenate([labels, jnp.zeros((B, 1), jnp.int32)], axis=1)
    n_blocks = T // T_BLK
    enc_blocks = enc_out.reshape(B, n_blocks, T_BLK, H)
    blank, label_lp = lax.map(lambda utt_in: lattice_terms(utt_in[0], utt_in[1], utt_in[2], w_enc, w_pred, w_out), (enc_blocks, pred_out, lab_ids))
    loss, loss_vjp = jax.vjp(lambda blank_in, label_in: lattice_loss(blank_in, label_in, frame_len, label_len), blank, label_lp)
    d_blank, d_label = loss_vjp(jnp.ones_like(loss))
    vocab_idx = jnp.arange(V)

    def per_utt(carry, utt_in):
        enc_utt, pred_utt, utt_ids, d_blank_utt, d_label_utt = utt_in
        flat_ids = jnp.tile(utt_ids, T_BLK)

        def per_blk(inner, blk_in):
            pred_acc, enc_acc, out_acc = inner
            enc_blk, d_blank_blk, d_label_blk = blk_in
            hidden, logits = joint_block(enc_blk, pred_utt, w_enc, w_pred, w_out)
            softmax_p = jax.nn.softmax(logits, axis=-1)
            blank_col = d_blank_blk.reshape(T_BLK * UPOS, 1)
            label_col = d_label_blk.reshape(T_BLK * UPOS, 1)
            grad_logits = (jnp.where(vocab_idx[None, :] == 0, blank_col, 0.0) + jnp.where(vocab_idx[None, :] == flat_ids[:, None], label_col, 0.0) - softmax_p * (blank_col + label_col)).astype(jnp.bfloat16)
            grad_hidden = jnp.dot(grad_logits, w_out.T, preferred_element_type=jnp.float32)
            grad_pre = (grad_hidden * (1.0 - jnp.square(hidden.astype(jnp.float32)))).reshape(T_BLK, UPOS, J)
            grad_act_enc = jnp.sum(grad_pre, axis=1).astype(jnp.bfloat16)
            grad_enc_blk = jnp.dot(grad_act_enc, w_enc.T, preferred_element_type=jnp.float32).astype(jnp.bfloat16)
            pred_acc = pred_acc + jnp.sum(grad_pre, axis=0)
            enc_acc = enc_acc + jnp.dot(enc_blk.T, grad_act_enc, preferred_element_type=jnp.float32)
            out_acc = out_acc + jnp.dot(hidden.T, grad_logits, preferred_element_type=jnp.float32)
            return (pred_acc, enc_acc, out_acc), grad_enc_blk

        start_acc = (jnp.zeros((UPOS, J), jnp.float32), carry[0], carry[1])
        (pred_acc, enc_acc, out_acc), grad_enc_utt = lax.scan(per_blk, start_acc, (enc_utt, d_blank_utt, d_label_utt))
        return (enc_acc, out_acc), (grad_enc_utt, pred_acc)

    acc_init = (jnp.zeros((H, J), jnp.float32), jnp.zeros((J, V), jnp.float32))
    scan_in = (enc_blocks, pred_out, lab_ids, d_blank.reshape(B, n_blocks, T_BLK, UPOS), d_label.reshape(B, n_blocks, T_BLK, UPOS))
    (grad_w_enc, grad_w_out), (grad_enc, grad_act_pred) = lax.scan(per_utt, acc_init, scan_in)
    act_pred_grad = grad_act_pred.astype(jnp.bfloat16).reshape(B * UPOS, J)
    grad_pred = jnp.dot(act_pred_grad, w_pred.T, preferred_element_type=jnp.float32).reshape(B, UPOS, H)
    grad_w_pred = jnp.dot(pred_out.reshape(B * UPOS, H).T, act_pred_grad, preferred_element_type=jnp.float32)
    return loss, grad_enc.reshape(B, T, H), grad_pred, grad_w_enc, grad_w_pred, grad_w_out
```

```python
import functools

import jax
import jax.numpy as jnp
from jax import lax
from jax.experimental import pallas as pl
from jax.experimental.pallas import tpu as pltpu
from jax.sharding import PartitionSpec as P

NEG = -1e30
MESH = pl.DeviceIdType.MESH
VMEM = pltpu.VMEM
F32 = jnp.float32
BF16 = jnp.bfloat16
VMEM_LIMIT = 67_000_000
SUB = 8
LANES = 128
GROUPS = 8
CORES = 2
RING = 4


def vspec():
    return pl.BlockSpec(memory_space=pltpu.VMEM)


def sspec():
    return pl.BlockSpec(memory_space=pltpu.SMEM)


def exchange_kernel(n_seq, enc_ref, pred_ref, w_enc_ref, w_pred_ref, frames_ref, a_ref, c_ref, send_sem, recv_sem):
    seq = lax.axis_index("seq")
    n_own = frames_ref.shape[1]
    barrier = pltpu.get_barrier_semaphore()
    for hop in range(1, n_seq):
        pl.semaphore_signal(barrier, inc=1, device_id={"seq": lax.rem(seq + hop, n_seq)}, device_id_type=MESH)
    frames_ref[pl.ds(seq, 1)] = enc_ref[pl.ds(seq * n_own, n_own)][None]
    own_pred = pred_ref[pl.ds(seq * n_own, n_own)]
    c_ref[...] = jnp.dot(own_pred.reshape(-1, own_pred.shape[-1]), w_pred_ref[...], preferred_element_type=F32).astype(BF16).astype(F32)
    pl.semaphore_wait(barrier, n_seq - 1)
    copies = []
    for hop in range(1, n_seq):
        peer = lax.rem(seq + hop, n_seq)
        copy = pltpu.make_async_remote_copy(
            src_ref=enc_ref.at[pl.ds(peer * n_own, n_own)],
            dst_ref=frames_ref.at[seq],
            send_sem=send_sem.at[hop - 1],
            recv_sem=recv_sem.at[hop - 1],
            device_id={"seq": peer},
            device_id_type=MESH,
        )
        copy.start()
        copies.append(copy)
    for copy in copies:
        copy.wait()
    frames = frames_ref[...]
    a_ref[...] = jnp.dot(frames.reshape(-1, frames.shape[-1]), w_enc_ref[...], preferred_element_type=F32).astype(BF16).astype(F32)


def exchange(n_seq, enc_loc, pred_loc, w_enc, w_pred):
    n_utt, t_loc, width = enc_loc.shape
    n_own = n_utt // n_seq
    n_upos = pred_loc.shape[1]
    joint = w_enc.shape[1]
    return pl.pallas_call(
        functools.partial(exchange_kernel, n_seq),
        out_shape=(
            jax.ShapeDtypeStruct((n_seq, n_own, t_loc, width), BF16),
            jax.ShapeDtypeStruct((n_seq * n_own * t_loc, joint), F32),
            jax.ShapeDtypeStruct((n_own * n_upos, joint), F32),
        ),
        in_specs=[vspec()] * 4,
        out_specs=(vspec(), vspec(), vspec()),
        scratch_shapes=[pltpu.SemaphoreType.DMA((n_seq - 1,)), pltpu.SemaphoreType.DMA((n_seq - 1,))],
        compiler_params=pltpu.CompilerParams(collective_id=0, has_side_effects=True, vmem_limit_bytes=VMEM_LIMIT),
        name="exchange",
    )(enc_loc, pred_loc, w_enc, w_pred)


def logaddexp(x, y):
    top = jnp.maximum(x, y)
    return top + jnp.log(1.0 + jnp.exp(-jnp.abs(x - y)))


def lattice_kernel(n_own, n_frames, n_upos, seq_ref, flen_ref, llen_ref, labels_ref, a_ref, c_ref, w_ref, wt_ref,
                   da_ref, dc_ref, gw_ref, loss_ref,
                   p_ref, h_ref, blank_ref, label_ref, alpha_ref, beta_ref, ids_ref, dact_ref, dpred_ref):
    vocab = w_ref.shape[1]
    joint = w_ref.shape[0]
    n_vt = vocab // LANES
    rows_g = SUB * SUB
    rows_t = GROUPS * rows_g
    n_diag = n_frames + n_upos - 1
    first = seq_ref[0] * n_own
    lens_t = [flen_ref[first + b] for b in range(n_own)]
    lens_u = [llen_ref[first + b] for b in range(n_own)]
    blocks_t = [lax.div(n + SUB - 1, SUB) for n in lens_t]
    blocks_u = [lax.div(n + SUB, SUB) for n in lens_u]
    starts = [jnp.int32(0)]
    for b in range(n_own):
        starts.append(starts[-1] + blocks_t[b] * blocks_u[b])
    total = starts[-1]
    n_tiles = lax.div(total + GROUPS - 1, GROUPS)

    def decode(n):
        n = jnp.minimum(n, total - 1)
        b = jnp.int32(0)
        base, width = starts[0], blocks_u[0]
        for k in range(1, n_own):
            past = n >= starts[k]
            b = jnp.where(past, k, b)
            base = jnp.where(past, starts[k], base)
            width = jnp.where(past, blocks_u[k], width)
        ti = lax.div(n - base, width)
        return n, b, ti, n - base - ti * width

    pos_col = lax.broadcasted_iota(jnp.int32, (n_upos, n_upos - 1), 0)
    pos_row = lax.broadcasted_iota(jnp.int32, (n_upos, n_upos - 1), 1)
    for b in range(n_own):
        row = labels_ref[pl.ds(first + b, 1), :].astype(F32)
        col = jnp.sum(jnp.where(pos_col == pos_row, row, 0.0), axis=1, keepdims=True)
        ids_ref[pl.ds(b * n_upos, n_upos), :] = jnp.broadcast_to(col, (n_upos, LANES)).astype(jnp.int32)

    blank_ref[...] = jnp.zeros_like(blank_ref)
    label_ref[...] = jnp.zeros_like(label_ref)
    gw_ref[...] = jnp.zeros_like(gw_ref)
    dact_ref[...] = jnp.zeros_like(dact_ref)
    dpred_ref[...] = jnp.zeros_like(dpred_ref)

    lane = lax.broadcasted_iota(jnp.int32, (SUB, LANES), 1)
    vocab_lane = lax.broadcasted_iota(jnp.int32, (rows_t, LANES), 1)

    def tile_ids(groups):
        parts = []
        for _, b, ti, ui in groups:
            ids = ids_ref[pl.ds(pl.multiple_of(b * n_upos + ui * SUB, SUB), SUB), :]
            parts.append(jnp.broadcast_to(ids[None], (SUB, SUB, LANES)).reshape(rows_g, LANES))
        return jnp.concatenate(parts, axis=0)

    def cell_row(ti, k, ui):
        return pl.multiple_of((n_diag - 1 - ti * SUB - k) * n_upos + ui * SUB, SUB)

    def forward(i, carry):
        groups = [decode(i * GROUPS + g) for g in range(GROUPS)]
        parts = []
        for g, (n, b, ti, ui) in enumerate(groups):
            a8 = a_ref[pl.ds(pl.multiple_of((ti * n_own + b) * SUB, SUB), SUB), :]
            c8 = c_ref[pl.ds(pl.multiple_of(b * n_upos + ui * SUB, SUB), SUB), :]
            parts.append(jnp.tanh(a8[:, None, :] + c8[None, :, :]).reshape(rows_g, joint).astype(BF16))
        h = jnp.concatenate(parts, axis=0)
        row0 = pl.multiple_of(i * rows_t, rows_t)
        h_ref[pl.ds(row0, rows_t), :] = h
        z = jnp.dot(h, w_ref[...], preferred_element_type=F32)
        top = jnp.max(z, axis=1, keepdims=True)
        e = jnp.exp(z - top)
        norm = jnp.sum(e, axis=1, keepdims=True)
        p_ref[pl.ds(row0, rows_t), :] = e * (1.0 / norm)
        log_norm = top + jnp.log(norm)
        ids = tile_ids(groups)
        picked = jnp.zeros((rows_t, LANES), F32)
        for v in range(n_vt):
            picked = picked + jnp.where(vocab_lane + v * LANES == ids, z[:, v * LANES:(v + 1) * LANES], 0.0)
        label = jnp.sum(picked, axis=1, keepdims=True) - log_norm
        blank = z[:, 0:1] - log_norm
        for g, (n, b, ti, ui) in enumerate(groups):
            for k in range(SUB):
                at = cell_row(ti, k, ui)
                lo = g * rows_g + k * SUB
                blank_ref[pl.ds(at, SUB), :] = jnp.where(lane == b, blank[lo:lo + SUB], blank_ref[pl.ds(at, SUB), :])
                label_ref[pl.ds(at, SUB), :] = jnp.where(lane == b, label[lo:lo + SUB], label_ref[pl.ds(at, SUB), :])
        return carry

    lax.fori_loop(0, n_tiles, forward, 0)

    upos = lax.broadcasted_iota(jnp.int32, (n_upos, LANES), 0)
    utt = lax.broadcasted_iota(jnp.int32, (n_upos, LANES), 1)
    t_end = jnp.ones((n_upos, LANES), jnp.int32)
    u_end = jnp.zeros((n_upos, LANES), jnp.int32)
    for b in range(n_own):
        t_end = jnp.where(utt == b, lens_t[b], t_end)
        u_end = jnp.where(utt == b, lens_u[b], u_end)

    def diagonal(d):
        return pl.ds((n_diag - 1 - d) * n_upos, n_upos, stride=n_upos + 1)

    def down(x):
        return jnp.where(upos == 0, NEG, pltpu.roll(x, 1, 0))

    def up(x):
        return jnp.where(upos == n_upos - 1, NEG, pltpu.roll(x, n_upos - 1, 0))

    def edge(d):
        return jnp.where((d - upos == t_end) & (upos == u_end), 0.0, NEG)

    alpha0 = jnp.where(upos == 0, 0.0, NEG).astype(F32)
    beta0 = edge(n_diag)
    alpha_ref[0] = alpha0
    beta_ref[n_diag] = beta0

    def sweep(k, carry):
        alpha, beta = carry
        d = k + 1
        alpha = logaddexp(alpha + blank_ref[diagonal(k), :], down(alpha + label_ref[diagonal(k), :]))
        alpha = jnp.where(upos <= d, alpha, NEG)
        alpha_ref[d] = alpha
        d = n_diag - 1 - k
        inside = (d - upos < t_end) & (upos <= u_end)
        beta = logaddexp(beta + blank_ref[diagonal(d), :], up(beta) + label_ref[diagonal(d), :])
        beta = jnp.where(inside, beta, edge(d))
        beta_ref[d] = beta
        return alpha, beta

    lax.fori_loop(0, n_diag, sweep, (alpha0, beta0))
    log_prob = beta_ref[0][0:1, :]
    loss_ref[...] = jnp.broadcast_to(-log_prob, (SUB, LANES))

    def occupancy(d, carry):
        t = d - upos
        alpha = alpha_ref[d]
        after = beta_ref[d + 1]
        cell_ok = (t >= 0) & (t < t_end) & (upos <= u_end)
        q0 = jnp.where(cell_ok, jnp.exp(alpha + blank_ref[diagonal(d), :] + after - log_prob), 0.0)
        q1 = jnp.where(cell_ok & (upos < u_end), jnp.exp(alpha + label_ref[diagonal(d), :] + up(after) - log_prob), 0.0)
        blank_ref[diagonal(d), :] = q0
        label_ref[diagonal(d), :] = q1
        return carry

    lax.fori_loop(0, n_diag, occupancy, 0)

    def backward(i, carry):
        groups = [decode(i * GROUPS + g) for g in range(GROUPS)]
        row0 = pl.multiple_of(i * rows_t, rows_t)
        q0s, q1s = [], []
        for g, (n, b, ti, ui) in enumerate(groups):
            keep = (lane == b) & (i * GROUPS + g < total)
            for k in range(SUB):
                at = cell_row(ti, k, ui)
                q0s.append(jnp.where(keep, blank_ref[pl.ds(at, SUB), :], 0.0))
                q1s.append(jnp.where(keep, label_ref[pl.ds(at, SUB), :], 0.0))
        q0 = jnp.sum(jnp.concatenate(q0s, axis=0), axis=1, keepdims=True)
        q1 = jnp.sum(jnp.concatenate(q1s, axis=0), axis=1, keepdims=True)
        both = q0 + q1
        ids = tile_ids(groups)
        cols = []
        for v in range(n_vt):
            at_v = vocab_lane + v * LANES
            dz = p_ref[pl.ds(row0, rows_t), v * LANES:(v + 1) * LANES] * both
            if v == 0:
                dz = dz - jnp.where(at_v == 0, q0, 0.0)
            dz = dz - jnp.where(at_v == ids, q1, 0.0)
            cols.append(dz.astype(BF16))
        dz = jnp.concatenate(cols, axis=1)
        h = h_ref[pl.ds(row0, rows_t), :]
        dh = jnp.dot(dz, wt_ref[...], preferred_element_type=F32)
        hf = h.astype(F32)
        ds = dh * (1.0 - hf * hf)
        for g, (n, b, ti, ui) in enumerate(groups):
            cube = ds[g * rows_g:(g + 1) * rows_g].reshape(SUB, SUB, joint)
            at = pl.multiple_of((ti * n_own + b) * SUB, SUB)
            dact_ref[pl.ds(at, SUB), :] += jnp.sum(cube, axis=1)
            at = pl.multiple_of(b * n_upos + ui * SUB, SUB)
            dpred_ref[pl.ds(at, SUB), :] += jnp.sum(cube, axis=0)
        for y in range(gw_ref.shape[0]):
            part = dz[:, y * gw_ref.shape[2]:(y + 1) * gw_ref.shape[2]]
            gw_ref[y] += lax.dot_general(h, part, (((0,), (0,)), ((), ())), preferred_element_type=F32)
        return carry

    lax.fori_loop(0, n_tiles, backward, 0)
    da_ref[...] = dact_ref[...].astype(BF16)
    dc_ref[...] = dpred_ref[...].astype(BF16)


def lattice(n_seq, n_data, seq_idx, frame_len, label_len, labels, act, pred, w_out, w_out_t, n_upos, t_loc):
    n_own = frame_len.shape[0] // n_seq
    n_frames = n_seq * t_loc
    joint, vocab = w_out.shape
    cells = n_own * n_frames * n_upos
    n_diag = n_frames + n_upos - 1
    lat_rows = (n_diag + n_upos - 1) * n_upos
    return pl.pallas_call(
        functools.partial(lattice_kernel, n_own, n_frames, n_upos),
        out_shape=(
            jax.ShapeDtypeStruct(act.shape, BF16),
            jax.ShapeDtypeStruct(pred.shape, BF16),
            jax.ShapeDtypeStruct((n_data, joint, vocab // n_data), F32),
            jax.ShapeDtypeStruct((SUB, LANES), F32),
        ),
        in_specs=[sspec(), sspec(), sspec()] + [vspec()] * 5,
        out_specs=(vspec(),) * 4,
        scratch_shapes=[
            VMEM((cells, vocab), F32),
            VMEM((cells, joint), BF16),
            VMEM((lat_rows, LANES), F32),
            VMEM((lat_rows, LANES), F32),
            VMEM((n_diag + 1, n_upos, LANES), F32),
            VMEM((n_diag + 1, n_upos, LANES), F32),
            VMEM((n_own * n_upos, LANES), jnp.int32),
            VMEM(act.shape, F32),
            VMEM(pred.shape, F32),
        ],
        compiler_params=pltpu.CompilerParams(vmem_limit_bytes=VMEM_LIMIT),
        name="lattice",
    )(seq_idx, frame_len, label_len, labels, act, pred, w_out, w_out_t)


class Copies:
    def __init__(self, send_sem, recv_sem):
        self.sems = (send_sem, recv_sem)
        self.all = []

    def start(self, src, dst, device):
        k = len(self.all)
        copy = pltpu.make_async_remote_copy(src_ref=src, dst_ref=dst, send_sem=self.sems[0].at[k], recv_sem=self.sems[1].at[k], device_id=device, device_id_type=MESH)
        copy.start()
        self.all.append(copy)
        return copy

    def drain(self):
        for copy in self.all:
            copy.wait_send()


class Reduce:
    def __init__(self, copies, axis, me, acc, pair, left, right):
        self.copies, self.acc, self.pair, self.left, self.right = copies, acc, pair, left, right
        self.me, self.nxt, self.prv, self.opp = me, lax.rem(me + 1, RING), lax.rem(me + RING - 1, RING), lax.rem(me + 2, RING)
        self.to_right = {axis: self.nxt}
        self.to_left = {axis: self.prv}

    def begin(self, right_dev, left_dev):
        c, acc = self.copies, self.acc
        self.devs = (right_dev, left_dev)
        self.a1 = c.start(acc(self.opp, 0), self.pair(0), right_dev)
        self.b1 = c.start(acc(self.opp, 1), self.pair(1), left_dev)
        self.b2 = c.start(acc(self.nxt, 1), self.left(1), right_dev)
        self.a2 = c.start(acc(self.prv, 0), self.right(0), left_dev)

    def middle(self):
        c, acc = self.copies, self.acc
        self.a1.wait_recv()
        add = acc(self.nxt, 0)
        add[...] = add[...] + self.pair(0)[...]
        self.a3 = c.start(add, self.left(0), self.devs[0])
        self.b1.wait_recv()
        add = acc(self.prv, 1)
        add[...] = add[...] + self.pair(1)[...]
        self.b3 = c.start(add, self.right(1), self.devs[1])

    def end(self, store):
        self.b2.wait_recv()
        self.a3.wait_recv()
        self.a2.wait_recv()
        self.b3.wait_recv()
        for half in range(2):
            store(half, self.acc(self.me, half)[...] + self.left(half)[...] + self.right(half)[...])


class Gather:
    def __init__(self, copies, me, out, right_dev, left_dev):
        self.copies, self.out, self.devs = copies, out, (right_dev, left_dev)
        self.me, self.nxt, self.prv, self.opp = me, lax.rem(me + 1, RING), lax.rem(me + RING - 1, RING), lax.rem(me + 2, RING)

    def begin(self):
        c, out, (right_dev, left_dev) = self.copies, self.out, self.devs
        self.ra = c.start(out(self.me, 0), out(self.me, 0), right_dev)
        self.lb = c.start(out(self.me, 1), out(self.me, 1), left_dev)
        self.rb = c.start(out(self.me, 1), out(self.me, 1), right_dev)
        self.la = c.start(out(self.me, 0), out(self.me, 0), left_dev)

    def relay(self):
        c, out, (right_dev, left_dev) = self.copies, self.out, self.devs
        self.ra.wait_recv()
        self.ra2 = c.start(out(self.prv, 0), out(self.prv, 0), right_dev)
        self.lb.wait_recv()
        self.lb2 = c.start(out(self.nxt, 1), out(self.nxt, 1), left_dev)
        self.rb.wait_recv()
        self.la.wait_recv()

    def finish(self):
        self.ra2.wait_recv()
        self.lb2.wait_recv()


def combine_kernel(n_seq, n_data, frames_ref, pred_ref, da_ref, dc_ref, gw_ref, loss_ref,
                   da_out, dc_out, gj_out, gw_out, loss_out,
                   gj_acc, gw_acc, gj_pair, gw_pair, gj_py, gj_ly, gj_ry, gj_px, gj_lx, gj_rx, gw_px, gw_lx, gw_rx, gw_py, gw_ly, gw_ry, gj_mid, gw_mid,
                   send_sem, recv_sem):
    seq = lax.axis_index("seq")
    y = lax.axis_index("data")
    x = lax.div(seq, CORES)
    core = lax.rem(seq, CORES)
    n_own = frames_ref.shape[1]
    x_right = {"seq": lax.rem(x + 1, RING) * CORES + core}
    x_left = {"seq": lax.rem(x + RING - 1, RING) * CORES + core}
    y_right = {"data": lax.rem(y + 1, RING)}
    y_left = {"data": lax.rem(y + RING - 1, RING)}
    mate = {"seq": x * CORES + 1 - core}
    barrier = pltpu.get_barrier_semaphore()
    for hop in range(1, n_seq):
        pl.semaphore_signal(barrier, inc=1, device_id={"seq": lax.rem(seq + hop, n_seq)}, device_id_type=MESH)
    for dev in (y_right, y_left):
        pl.semaphore_signal(barrier, inc=1, device_id=dev, device_id_type=MESH)

    frames = frames_ref[...]
    contract_rows = (((0,), (0,)), ((), ()))
    gj_acc[0] = lax.dot_general(frames.reshape(-1, frames.shape[-1]), da_ref[...].reshape(-1, da_ref.shape[-1]), contract_rows, preferred_element_type=F32)
    own_pred = pred_ref[pl.ds(seq * n_own, n_own)]
    gj_acc[1] = lax.dot_general(own_pred.reshape(-1, own_pred.shape[-1]), dc_ref[...], contract_rows, preferred_element_type=F32)
    da_out[pl.ds(seq, 1)] = da_ref[pl.ds(seq, 1)]
    dc_out[pl.ds(seq, 1)] = dc_ref[...][None]
    loss_out[pl.ds(seq, 1)] = loss_ref[...][None]
    pl.semaphore_wait(barrier, n_seq - 1 + 2)

    copies = Copies(send_sem, recv_sem)
    gj_half = gj_acc.shape[1] // CORES
    gw_half = gw_ref.shape[1] // CORES
    gj_y, gw_x = gj_half // RING, gw_half // RING
    gj_x = gj_y // RING

    mate_gj = copies.start(gj_acc.at[:, pl.ds((1 - core) * gj_half, gj_half), :], gj_pair, mate)
    mate_gw = copies.start(gw_ref.at[:, pl.ds((1 - core) * gw_half, gw_half), :], gw_pair, mate)

    dc_half = dc_out.shape[1] // 2

    def dc_at(k, half):
        return dc_out.at[k * CORES + core, pl.ds(half * dc_half, dc_half), :]

    dc_gather = Gather(copies, x, dc_at, x_right, x_left)
    dc_gather.begin()
    dc_mate = [copies.start(dc_out.at[seq], dc_out.at[seq], mate)]
    small = []
    for hop in range(1, n_seq):
        peer = lax.rem(seq + hop, n_seq)
        small.append(copies.start(da_ref.at[peer], da_out.at[seq], {"seq": peer}))
        small.append(copies.start(loss_ref, loss_out.at[seq], {"seq": peer}))

    gj_row = pl.multiple_of(core * gj_half, gj_half)
    gw_row = pl.multiple_of(core * gw_half, gw_half)

    def gj_shard_y(k, half):
        return gj_acc.at[:, pl.ds(pl.multiple_of(gj_row + k * gj_y + half * (gj_y // 2), SUB), gj_y // 2), :]

    def gw_shard_x(k, half):
        return gw_acc.at[:, pl.ds(pl.multiple_of(k * gw_x + half * (gw_x // 2), SUB), gw_x // 2), :]

    def halves(ref):
        return lambda half: ref.at[half]

    mate_gj.wait_recv()
    gj_acc[:, pl.ds(gj_row, gj_half), :] = gj_acc[:, pl.ds(gj_row, gj_half), :] + gj_pair[...]
    gj_r1 = Reduce(copies, "data", y, gj_shard_y, halves(gj_py), halves(gj_ly), halves(gj_ry))
    gj_r1.begin(y_right, y_left)
    mate_gw.wait_recv()
    gw_acc[...] = gw_ref[:, pl.ds(gw_row, gw_half), :] + gw_pair[...]
    gw_r1 = Reduce(copies, "seq", x, gw_shard_x, halves(gw_px), halves(gw_lx), halves(gw_rx))
    gw_r1.begin(x_right, x_left)

    dc_gather.relay()
    dc_mate.append(copies.start(dc_out.at[dc_gather.prv * CORES + core], dc_out.at[dc_gather.prv * CORES + core], mate))
    dc_mate.append(copies.start(dc_out.at[dc_gather.nxt * CORES + core], dc_out.at[dc_gather.nxt * CORES + core], mate))
    gj_r1.middle()
    gw_r1.middle()

    def keep_gj(half, value):
        gj_mid[:, pl.ds(half * (gj_y // 2), gj_y // 2), :] = value

    gj_r1.end(keep_gj)

    def gj_shard_x(k, half):
        return gj_mid.at[:, pl.ds(pl.multiple_of(k * gj_x + half * (gj_x // 2), SUB), gj_x // 2), :]

    gj_r2 = Reduce(copies, "seq", x, gj_shard_x, halves(gj_px), halves(gj_lx), halves(gj_rx))
    gj_r2.begin(x_right, x_left)

    def keep_gw(half, value):
        gw_mid[:, pl.ds(half * (gw_x // 2), gw_x // 2), :] = value

    gw_r1.end(keep_gw)

    def gw_shard_y(k, half):
        return gw_mid.at[k, pl.ds(half * (gw_x // 2), gw_x // 2), :]

    gw_r2 = Reduce(copies, "data", y, gw_shard_y, halves(gw_py), halves(gw_ly), halves(gw_ry))
    gw_r2.begin(y_right, y_left)
    gj_r2.middle()
    gw_r2.middle()

    def gj_out_x(k, half):
        return gj_out.at[:, pl.ds(pl.multiple_of(gj_row + y * gj_y + k * gj_x + half * (gj_x // 2), SUB), gj_x // 2), :]

    def gw_out_y(k, half):
        return gw_out.at[k, pl.ds(pl.multiple_of(gw_row + x * gw_x + half * (gw_x // 2), SUB), gw_x // 2), :]

    def put_gj(half, value):
        gj_out_x(x, half)[...] = value

    def put_gw(half, value):
        gw_out_y(y, half)[...] = value

    gj_r2.end(put_gj)
    gj_g1 = Gather(copies, x, gj_out_x, x_right, x_left)
    gj_g1.begin()
    gw_r2.end(put_gw)
    gw_g1 = Gather(copies, y, gw_out_y, y_right, y_left)
    gw_g1.begin()
    gj_g1.relay()
    gw_g1.relay()
    gj_g1.finish()

    def gj_out_y(k, half):
        return gj_out.at[:, pl.ds(pl.multiple_of(gj_row + k * gj_y + half * (gj_y // 2), SUB), gj_y // 2), :]

    def gw_out_x(k, half):
        return gw_out.at[:, pl.ds(pl.multiple_of(gw_row + k * gw_x + half * (gw_x // 2), SUB), gw_x // 2), :]

    gj_g2 = Gather(copies, y, gj_out_y, y_right, y_left)
    gj_g2.begin()
    gw_g1.finish()
    gw_g2 = Gather(copies, x, gw_out_x, x_right, x_left)
    gw_g2.begin()

    def gj_whole(k):
        return gj_out.at[:, pl.ds(pl.multiple_of(gj_row + k * gj_y, SUB), gj_y), :]

    def gw_whole(k):
        return gw_out.at[:, pl.ds(pl.multiple_of(gw_row + k * gw_x, SUB), gw_x), :]

    last = [copies.start(gj_whole(y), gj_whole(y), mate), copies.start(gw_whole(x), gw_whole(x), mate)]
    dc_gather.finish()
    dc_mate.append(copies.start(dc_out.at[dc_gather.opp * CORES + core], dc_out.at[dc_gather.opp * CORES + core], mate))
    gj_g2.relay()
    for k in (gj_g2.prv, gj_g2.nxt):
        last.append(copies.start(gj_whole(k), gj_whole(k), mate))
    gw_g2.relay()
    for k in (gw_g2.prv, gw_g2.nxt):
        last.append(copies.start(gw_whole(k), gw_whole(k), mate))
    gj_g2.finish()
    last.append(copies.start(gj_whole(gj_g2.opp), gj_whole(gj_g2.opp), mate))
    gw_g2.finish()
    last.append(copies.start(gw_whole(gw_g2.opp), gw_whole(gw_g2.opp), mate))
    for copy in small + dc_mate + last:
        copy.wait_recv()
    copies.drain()


N_COPIES = 6 + 2 + 4 + 14 + 4 * 6 + 4 * 6 + 8


def combine(n_seq, n_data, frames, pred_loc, da, dc, gw, loss):
    _, n_own, t_loc, width = frames.shape
    joint = da.shape[-1]
    n_cols, _, col = gw.shape
    gj_half, gw_half = width // CORES, joint // CORES
    gj_y, gw_x = gj_half // RING, gw_half // RING
    gj_x = gj_y // RING
    return pl.pallas_call(
        functools.partial(combine_kernel, n_seq, n_data),
        out_shape=(
            jax.ShapeDtypeStruct((n_seq, n_own, t_loc, joint), BF16),
            jax.ShapeDtypeStruct((n_seq,) + dc.shape, BF16),
            jax.ShapeDtypeStruct((2, width, joint), F32),
            jax.ShapeDtypeStruct(gw.shape, F32),
            jax.ShapeDtypeStruct((n_seq,) + loss.shape, F32),
        ),
        in_specs=[vspec()] * 6,
        out_specs=(vspec(),) * 5,
        scratch_shapes=[
            VMEM((2, width, joint), F32),
            VMEM((n_cols, gw_half, col), F32),
            VMEM((2, gj_half, joint), F32),
            VMEM((n_cols, gw_half, col), F32),
        ]
        + [VMEM((2, 2, gj_y // 2, joint), F32)] * 3
        + [VMEM((2, 2, gj_x // 2, joint), F32)] * 3
        + [VMEM((2, n_cols, gw_x // 2, col), F32)] * 3
        + [VMEM((2, gw_x // 2, col), F32)] * 3
        + [
            VMEM((2, gj_y, joint), F32),
            VMEM((n_cols, gw_x, col), F32),
            pltpu.SemaphoreType.DMA((N_COPIES,)),
            pltpu.SemaphoreType.DMA((N_COPIES,)),
        ],
        compiler_params=pltpu.CompilerParams(collective_id=1, has_side_effects=True, vmem_limit_bytes=VMEM_LIMIT),
        name="combine",
    )(frames, pred_loc, da.reshape(n_seq, n_own, t_loc, joint), dc, gw, loss)


def solution(mesh):
    n_seq = mesh.shape["seq"]
    n_data = mesh.shape["data"]
    utt_rows = P(("part", "data"))
    utt_mats = P(("part", "data"), None)
    utt_cube = P(("part", "data"), None, None)
    enc_spec = P(("part", "data"), "seq", None)
    weight_in = P(None, None)
    weight_out = P("part", None)

    def body(enc_loc, pred_loc, w_enc, w_pred, w_out, labels, frame_len, label_len):
        n_utt, t_loc, width = enc_loc.shape
        n_own = n_utt // n_seq
        n_upos = pred_loc.shape[1]
        joint, vocab = w_out.shape
        seq_idx = lax.axis_index("seq").astype(jnp.int32).reshape(1)
        frames, act, pred = exchange(n_seq, enc_loc, pred_loc, w_enc, w_pred)
        da, dc, gw, loss = lattice(n_seq, n_data, seq_idx, frame_len, label_len, labels, act, pred, w_out, w_out.T, n_upos, t_loc)
        da_loc, dc_all, gj, gw, loss_all = combine(n_seq, n_data, frames, pred_loc, da, dc, gw, loss)
        grad_enc = jnp.einsum("btj,hj->bth", da_loc.reshape(n_utt, t_loc, joint), w_enc, preferred_element_type=F32).astype(BF16)
        grad_pred = jnp.einsum("buj,hj->buh", dc_all.reshape(n_utt, n_upos, joint), w_pred, preferred_element_type=F32)
        grad_w_out = jnp.swapaxes(gw, 0, 1).reshape(joint, vocab)
        return loss_all[:, 0, :n_own].reshape(n_utt), grad_enc, grad_pred, gj[0], gj[1], grad_w_out

    return jax.shard_map(body, mesh=mesh, in_specs=(enc_spec, utt_cube, weight_in, weight_in, weight_in, utt_mats, utt_rows, utt_rows), out_specs=(utt_rows, enc_spec, utt_cube, weight_out, weight_out, weight_out), check_vma=False)
```

```python
import functools

import jax
import jax.numpy as jnp
from jax import lax
from jax.experimental import pallas as pl
from jax.experimental.pallas import tpu as pltpu
from jax.sharding import PartitionSpec as P

NEG = -1e30
MESH = pl.DeviceIdType.MESH
VMEM = pltpu.VMEM
F32 = jnp.float32
BF16 = jnp.bfloat16
VMEM_LIMIT = 67_000_000
SUB = 8
LANES = 128
GROUPS = 8
CORES = 2
RING = 4


def vspec():
    return pl.BlockSpec(memory_space=pltpu.VMEM)


def sspec():
    return pl.BlockSpec(memory_space=pltpu.SMEM)


def exchange_kernel(n_seq, flen_ref, llen_ref, enc_ref, pred_ref, w_enc_ref, w_pred_ref, w_out_ref,
                    order_ref, place_ref, frames_ref, own_pred_ref, a_ref, c_ref, w_out_t_ref,
                    key_ref, sorted_ref, send_sem, recv_sem):
    seq = lax.axis_index("seq")
    n_utt = enc_ref.shape[0]
    n_own = n_utt // n_seq
    barrier = pltpu.get_barrier_semaphore()
    for hop in range(1, n_seq):
        pl.semaphore_signal(barrier, inc=1, device_id={"seq": lax.rem(seq + hop, n_seq)}, device_id_type=MESH)

    def set_key(i, carry):
        key_ref[i] = ((flen_ref[i] + SUB - 1) // SUB) * ((llen_ref[i] + SUB) // SUB) * n_utt + i
        return carry

    def set_place(i, carry):
        key = key_ref[i]
        rank = jnp.int32(0)
        for j in range(n_utt):
            rank = rank + jnp.where(key_ref[j] > key, 1, 0)
        deal = rank // n_seq
        at = rank - deal * n_seq
        at = jnp.where(deal % 2 == 0, at, n_seq - 1 - at)
        place_ref[i] = at * n_own + deal
        return carry

    def set_order(k, carry):
        utt = jnp.int32(0)
        for j in range(n_utt):
            utt = utt + jnp.where(place_ref[j] == k, j, 0)
        order_ref[k] = utt
        return carry

    lax.fori_loop(0, n_utt, set_key, 0)
    lax.fori_loop(0, n_utt, set_place, 0)
    lax.fori_loop(0, n_utt, set_order, 0)
    for k in range(n_utt):
        sorted_ref[k] = enc_ref[order_ref[k]]
    pl.semaphore_wait(barrier, n_seq - 1)
    copies = []
    for hop in range(1, n_seq):
        peer = lax.rem(seq + hop, n_seq)
        copy = pltpu.make_async_remote_copy(
            src_ref=sorted_ref.at[pl.ds(peer * n_own, n_own)],
            dst_ref=frames_ref.at[seq],
            send_sem=send_sem.at[hop - 1],
            recv_sem=recv_sem.at[hop - 1],
            device_id={"seq": peer},
            device_id_type=MESH,
        )
        copy.start()
        copies.append(copy)
    frames_ref[pl.ds(seq, 1)] = sorted_ref[pl.ds(seq * n_own, n_own)][None]
    for j in range(n_own):
        own_pred_ref[j] = pred_ref[order_ref[seq * n_own + j]]
    own_pred = own_pred_ref[...]
    c_ref[...] = jnp.dot(own_pred.reshape(-1, own_pred.shape[-1]), w_pred_ref[...], preferred_element_type=F32).astype(BF16).astype(F32)
    w_out_t_ref[...] = w_out_ref[...].T
    for copy in copies:
        copy.wait()
    frames = frames_ref[...]
    a_ref[...] = jnp.dot(frames.reshape(-1, frames.shape[-1]), w_enc_ref[...], preferred_element_type=F32).astype(BF16).astype(F32)


def exchange(n_seq, frame_len, label_len, enc_loc, pred_loc, w_enc, w_pred, w_out):
    n_utt, t_loc, width = enc_loc.shape
    n_own = n_utt // n_seq
    n_upos = pred_loc.shape[1]
    joint, vocab = w_out.shape
    return pl.pallas_call(
        functools.partial(exchange_kernel, n_seq),
        out_shape=(
            jax.ShapeDtypeStruct((n_utt,), jnp.int32),
            jax.ShapeDtypeStruct((n_utt,), jnp.int32),
            jax.ShapeDtypeStruct((n_seq, n_own, t_loc, width), BF16),
            jax.ShapeDtypeStruct((n_own, n_upos, width), BF16),
            jax.ShapeDtypeStruct((n_seq * n_own * t_loc, joint), F32),
            jax.ShapeDtypeStruct((n_own * n_upos, joint), F32),
            jax.ShapeDtypeStruct((vocab, joint), BF16),
        ),
        in_specs=[sspec()] * 2 + [vspec()] * 5,
        out_specs=(sspec(),) * 2 + (vspec(),) * 5,
        scratch_shapes=[
            pltpu.SMEM((n_utt,), jnp.int32),
            VMEM(enc_loc.shape, BF16),
            pltpu.SemaphoreType.DMA((n_seq - 1,)),
            pltpu.SemaphoreType.DMA((n_seq - 1,)),
        ],
        compiler_params=pltpu.CompilerParams(collective_id=0, has_side_effects=True, vmem_limit_bytes=20_000_000),
        name="exchange",
    )(frame_len, label_len, enc_loc, pred_loc, w_enc, w_pred, w_out)


def logaddexp(x, y):
    top = jnp.maximum(x, y)
    return top + jnp.log(1.0 + jnp.exp(-jnp.abs(x - y)))


def lattice_kernel(n_own, n_frames, n_upos, seq_ref, order_ref, flen_ref, llen_ref, labels_ref, a_ref, c_ref, w_ref, wt_ref,
                   da_ref, dc_ref, gw_ref, loss_ref,
                   p_ref, h_ref, blank_ref, label_ref, alpha_ref, beta_ref, ids_ref, dact_ref, dpred_ref):
    vocab = w_ref.shape[1]
    joint = w_ref.shape[0]
    n_vt = vocab // LANES
    rows_g = SUB * SUB
    rows_t = GROUPS * rows_g
    n_diag = n_frames + n_upos - 1
    first = seq_ref[0] * n_own
    utts = [order_ref[first + b] for b in range(n_own)]
    lens_t = [flen_ref[utt] for utt in utts]
    lens_u = [llen_ref[utt] for utt in utts]
    blocks_t = [lax.div(n + SUB - 1, SUB) for n in lens_t]
    blocks_u = [lax.div(n + SUB, SUB) for n in lens_u]
    starts = [jnp.int32(0)]
    for b in range(n_own):
        starts.append(starts[-1] + blocks_t[b] * blocks_u[b])
    total = starts[-1]
    n_tiles = lax.div(total + GROUPS - 1, GROUPS)

    def decode(n):
        n = jnp.minimum(n, total - 1)
        b = jnp.int32(0)
        base, width = starts[0], blocks_u[0]
        for k in range(1, n_own):
            past = n >= starts[k]
            b = jnp.where(past, k, b)
            base = jnp.where(past, starts[k], base)
            width = jnp.where(past, blocks_u[k], width)
        ti = lax.div(n - base, width)
        return n, b, ti, n - base - ti * width

    pos_col = lax.broadcasted_iota(jnp.int32, (n_upos, n_upos - 1), 0)
    pos_row = lax.broadcasted_iota(jnp.int32, (n_upos, n_upos - 1), 1)
    for b in range(n_own):
        row = labels_ref[pl.ds(utts[b], 1), :].astype(F32)
        col = jnp.sum(jnp.where(pos_col == pos_row, row, 0.0), axis=1, keepdims=True)
        ids_ref[pl.ds(b * n_upos, n_upos), :] = jnp.broadcast_to(col, (n_upos, LANES)).astype(jnp.int32)

    blank_ref[...] = jnp.zeros_like(blank_ref)
    label_ref[...] = jnp.zeros_like(label_ref)
    gw_ref[...] = jnp.zeros_like(gw_ref)
    dact_ref[...] = jnp.zeros_like(dact_ref)
    dpred_ref[...] = jnp.zeros_like(dpred_ref)

    lane = lax.broadcasted_iota(jnp.int32, (SUB, LANES), 1)
    vocab_lane = lax.broadcasted_iota(jnp.int32, (rows_t, LANES), 1)

    def tile_ids(groups):
        parts = []
        for _, b, ti, ui in groups:
            ids = ids_ref[pl.ds(pl.multiple_of(b * n_upos + ui * SUB, SUB), SUB), :]
            parts.append(jnp.broadcast_to(ids[None], (SUB, SUB, LANES)).reshape(rows_g, LANES))
        return jnp.concatenate(parts, axis=0)

    def cell_row(ti, k, ui):
        return pl.multiple_of((n_diag - 1 - ti * SUB - k) * n_upos + ui * SUB, SUB)

    def forward(i, carry):
        groups = [decode(i * GROUPS + g) for g in range(GROUPS)]
        parts = []
        for g, (n, b, ti, ui) in enumerate(groups):
            a8 = a_ref[pl.ds(pl.multiple_of((ti * n_own + b) * SUB, SUB), SUB), :]
            c8 = c_ref[pl.ds(pl.multiple_of(b * n_upos + ui * SUB, SUB), SUB), :]
            parts.append(jnp.tanh(a8[:, None, :] + c8[None, :, :]).reshape(rows_g, joint).astype(BF16))
        h = jnp.concatenate(parts, axis=0)
        row0 = pl.multiple_of(i * rows_t, rows_t)
        h_ref[pl.ds(row0, rows_t), :] = h
        z = jnp.dot(h, w_ref[...], preferred_element_type=F32)
        top = jnp.max(z, axis=1, keepdims=True)
        e = jnp.exp(z - top)
        norm = jnp.sum(e, axis=1, keepdims=True)
        p_ref[pl.ds(row0, rows_t), :] = e * (1.0 / norm)
        log_norm = top + jnp.log(norm)
        ids = tile_ids(groups)
        picked = jnp.zeros((rows_t, LANES), F32)
        for v in range(n_vt):
            picked = picked + jnp.where(vocab_lane + v * LANES == ids, z[:, v * LANES:(v + 1) * LANES], 0.0)
        label = jnp.sum(picked, axis=1, keepdims=True) - log_norm
        blank = z[:, 0:1] - log_norm
        for g, (n, b, ti, ui) in enumerate(groups):
            for k in range(SUB):
                at = cell_row(ti, k, ui)
                lo = g * rows_g + k * SUB
                blank_ref[pl.ds(at, SUB), :] = jnp.where(lane == b, blank[lo:lo + SUB], blank_ref[pl.ds(at, SUB), :])
                label_ref[pl.ds(at, SUB), :] = jnp.where(lane == b, label[lo:lo + SUB], label_ref[pl.ds(at, SUB), :])
        return carry

    lax.fori_loop(0, n_tiles, forward, 0)

    upos = lax.broadcasted_iota(jnp.int32, (n_upos, LANES), 0)
    utt = lax.broadcasted_iota(jnp.int32, (n_upos, LANES), 1)
    t_end = jnp.ones((n_upos, LANES), jnp.int32)
    u_end = jnp.zeros((n_upos, LANES), jnp.int32)
    for b in range(n_own):
        t_end = jnp.where(utt == b, lens_t[b], t_end)
        u_end = jnp.where(utt == b, lens_u[b], u_end)

    def diagonal(d):
        return pl.ds((n_diag - 1 - d) * n_upos, n_upos, stride=n_upos + 1)

    def down(x):
        return jnp.where(upos == 0, NEG, pltpu.roll(x, 1, 0))

    def up(x):
        return jnp.where(upos == n_upos - 1, NEG, pltpu.roll(x, n_upos - 1, 0))

    def edge(d):
        return jnp.where((d - upos == t_end) & (upos == u_end), 0.0, NEG)

    alpha0 = jnp.where(upos == 0, 0.0, NEG).astype(F32)
    beta0 = edge(n_diag)
    alpha_ref[0] = alpha0
    beta_ref[n_diag] = beta0

    def sweep(k, carry):
        alpha, beta = carry
        d = k + 1
        alpha = logaddexp(alpha + blank_ref[diagonal(k), :], down(alpha + label_ref[diagonal(k), :]))
        alpha = jnp.where(upos <= d, alpha, NEG)
        alpha_ref[d] = alpha
        d = n_diag - 1 - k
        inside = (d - upos < t_end) & (upos <= u_end)
        beta = logaddexp(beta + blank_ref[diagonal(d), :], up(beta) + label_ref[diagonal(d), :])
        beta = jnp.where(inside, beta, edge(d))
        beta_ref[d] = beta
        return alpha, beta

    lax.fori_loop(0, n_diag, sweep, (alpha0, beta0))
    log_prob = beta_ref[0][0:1, :]
    loss_ref[...] = jnp.broadcast_to(-log_prob, (SUB, LANES))

    def occupancy(d, carry):
        t = d - upos
        alpha = alpha_ref[d]
        after = beta_ref[d + 1]
        cell_ok = (t >= 0) & (t < t_end) & (upos <= u_end)
        q0 = jnp.where(cell_ok, jnp.exp(alpha + blank_ref[diagonal(d), :] + after - log_prob), 0.0)
        q1 = jnp.where(cell_ok & (upos < u_end), jnp.exp(alpha + label_ref[diagonal(d), :] + up(after) - log_prob), 0.0)
        blank_ref[diagonal(d), :] = q0
        label_ref[diagonal(d), :] = q1
        return carry

    lax.fori_loop(0, n_diag, occupancy, 0)

    def backward(i, carry):
        groups = [decode(i * GROUPS + g) for g in range(GROUPS)]
        row0 = pl.multiple_of(i * rows_t, rows_t)
        q0s, q1s = [], []
        for g, (n, b, ti, ui) in enumerate(groups):
            keep = (lane == b) & (i * GROUPS + g < total)
            for k in range(SUB):
                at = cell_row(ti, k, ui)
                q0s.append(jnp.where(keep, blank_ref[pl.ds(at, SUB), :], 0.0))
                q1s.append(jnp.where(keep, label_ref[pl.ds(at, SUB), :], 0.0))
        q0 = jnp.sum(jnp.concatenate(q0s, axis=0), axis=1, keepdims=True)
        q1 = jnp.sum(jnp.concatenate(q1s, axis=0), axis=1, keepdims=True)
        both = q0 + q1
        ids = tile_ids(groups)
        cols = []
        for v in range(n_vt):
            at_v = vocab_lane + v * LANES
            dz = p_ref[pl.ds(row0, rows_t), v * LANES:(v + 1) * LANES] * both
            if v == 0:
                dz = dz - jnp.where(at_v == 0, q0, 0.0)
            dz = dz - jnp.where(at_v == ids, q1, 0.0)
            cols.append(dz.astype(BF16))
        dz = jnp.concatenate(cols, axis=1)
        h = h_ref[pl.ds(row0, rows_t), :]
        dh = jnp.dot(dz, wt_ref[...], preferred_element_type=F32)
        hf = h.astype(F32)
        ds = dh * (1.0 - hf * hf)
        for g, (n, b, ti, ui) in enumerate(groups):
            cube = ds[g * rows_g:(g + 1) * rows_g].reshape(SUB, SUB, joint)
            at = pl.multiple_of((ti * n_own + b) * SUB, SUB)
            dact_ref[pl.ds(at, SUB), :] += jnp.sum(cube, axis=1)
            at = pl.multiple_of(b * n_upos + ui * SUB, SUB)
            dpred_ref[pl.ds(at, SUB), :] += jnp.sum(cube, axis=0)
        for y in range(gw_ref.shape[0]):
            part = dz[:, y * gw_ref.shape[2]:(y + 1) * gw_ref.shape[2]]
            gw_ref[y] += lax.dot_general(h, part, (((0,), (0,)), ((), ())), preferred_element_type=F32)
        return carry

    lax.fori_loop(0, n_tiles, backward, 0)
    da_ref[...] = dact_ref[...].astype(BF16)
    dc_ref[...] = dpred_ref[...].astype(BF16)


def lattice(n_seq, n_data, seq_idx, order, frame_len, label_len, labels, act, pred, w_out, w_out_t, n_upos, t_loc):
    n_own = frame_len.shape[0] // n_seq
    n_frames = n_seq * t_loc
    joint, vocab = w_out.shape
    cells = n_own * n_frames * n_upos
    n_diag = n_frames + n_upos - 1
    lat_rows = (n_diag + n_upos - 1) * n_upos
    return pl.pallas_call(
        functools.partial(lattice_kernel, n_own, n_frames, n_upos),
        out_shape=(
            jax.ShapeDtypeStruct(act.shape, BF16),
            jax.ShapeDtypeStruct(pred.shape, BF16),
            jax.ShapeDtypeStruct((n_data, joint, vocab // n_data), F32),
            jax.ShapeDtypeStruct((SUB, LANES), F32),
        ),
        in_specs=[sspec()] * 4 + [vspec()] * 5,
        out_specs=(vspec(),) * 4,
        scratch_shapes=[
            VMEM((cells, vocab), F32),
            VMEM((cells, joint), BF16),
            VMEM((lat_rows, LANES), F32),
            VMEM((lat_rows, LANES), F32),
            VMEM((n_diag + 1, n_upos, LANES), F32),
            VMEM((n_diag + 1, n_upos, LANES), F32),
            VMEM((n_own * n_upos, LANES), jnp.int32),
            VMEM(act.shape, F32),
            VMEM(pred.shape, F32),
        ],
        compiler_params=pltpu.CompilerParams(vmem_limit_bytes=VMEM_LIMIT),
        name="lattice",
    )(seq_idx, order, frame_len, label_len, labels, act, pred, w_out, w_out_t)


class Copies:
    def __init__(self, send_sem, recv_sem):
        self.sems = (send_sem, recv_sem)
        self.all = []

    def start(self, src, dst, device):
        k = len(self.all)
        copy = pltpu.make_async_remote_copy(src_ref=src, dst_ref=dst, send_sem=self.sems[0].at[k], recv_sem=self.sems[1].at[k], device_id=device, device_id_type=MESH)
        copy.start()
        self.all.append(copy)
        return copy

    def drain(self):
        for copy in self.all:
            copy.wait_send()


class Reduce:
    def __init__(self, copies, axis, me, acc, pair, left, right):
        self.copies, self.acc, self.pair, self.left, self.right = copies, acc, pair, left, right
        self.me, self.nxt, self.prv, self.opp = me, lax.rem(me + 1, RING), lax.rem(me + RING - 1, RING), lax.rem(me + 2, RING)
        self.to_right = {axis: self.nxt}
        self.to_left = {axis: self.prv}

    def begin(self, right_dev, left_dev):
        c, acc = self.copies, self.acc
        self.devs = (right_dev, left_dev)
        self.a1 = c.start(acc(self.opp, 0), self.pair(0), right_dev)
        self.b1 = c.start(acc(self.opp, 1), self.pair(1), left_dev)
        self.b2 = c.start(acc(self.nxt, 1), self.left(1), right_dev)
        self.a2 = c.start(acc(self.prv, 0), self.right(0), left_dev)

    def middle(self):
        c, acc = self.copies, self.acc
        self.a1.wait_recv()
        add = acc(self.nxt, 0)
        add[...] = add[...] + self.pair(0)[...]
        self.a3 = c.start(add, self.left(0), self.devs[0])
        self.b1.wait_recv()
        add = acc(self.prv, 1)
        add[...] = add[...] + self.pair(1)[...]
        self.b3 = c.start(add, self.right(1), self.devs[1])

    def end(self, store):
        self.b2.wait_recv()
        self.a3.wait_recv()
        self.a2.wait_recv()
        self.b3.wait_recv()
        for half in range(2):
            store(half, self.acc(self.me, half)[...] + self.left(half)[...] + self.right(half)[...])


class Gather:
    def __init__(self, copies, me, out, right_dev, left_dev):
        self.copies, self.out, self.devs = copies, out, (right_dev, left_dev)
        self.me, self.nxt, self.prv, self.opp = me, lax.rem(me + 1, RING), lax.rem(me + RING - 1, RING), lax.rem(me + 2, RING)

    def begin(self):
        c, out, (right_dev, left_dev) = self.copies, self.out, self.devs
        self.ra = c.start(out(self.me, 0), out(self.me, 0), right_dev)
        self.lb = c.start(out(self.me, 1), out(self.me, 1), left_dev)
        self.rb = c.start(out(self.me, 1), out(self.me, 1), right_dev)
        self.la = c.start(out(self.me, 0), out(self.me, 0), left_dev)

    def relay(self):
        c, out, (right_dev, left_dev) = self.copies, self.out, self.devs
        self.ra.wait_recv()
        self.ra2 = c.start(out(self.prv, 0), out(self.prv, 0), right_dev)
        self.lb.wait_recv()
        self.lb2 = c.start(out(self.nxt, 1), out(self.nxt, 1), left_dev)
        self.rb.wait_recv()
        self.la.wait_recv()

    def finish(self):
        self.ra2.wait_recv()
        self.lb2.wait_recv()


def combine_kernel(n_seq, n_data, frames_ref, pred_ref, w_enc_ref, da_ref, dc_ref, gw_ref, loss_ref,
                   ge_out, dc_out, gj_out, gw_out, loss_out,
                   gj_acc, gw_acc, gj_pair, gw_pair, gj_py, gj_ly, gj_ry, gj_px, gj_lx, gj_rx, gw_px, gw_lx, gw_rx, gw_py, gw_ly, gw_ry, gj_mid, gw_mid, ge_ref,
                   send_sem, recv_sem):
    seq = lax.axis_index("seq")
    y = lax.axis_index("data")
    x = lax.div(seq, CORES)
    core = lax.rem(seq, CORES)
    x_right = {"seq": lax.rem(x + 1, RING) * CORES + core}
    x_left = {"seq": lax.rem(x + RING - 1, RING) * CORES + core}
    y_right = {"data": lax.rem(y + 1, RING)}
    y_left = {"data": lax.rem(y + RING - 1, RING)}
    mate = {"seq": x * CORES + 1 - core}
    barrier = pltpu.get_barrier_semaphore()
    for hop in range(1, n_seq):
        pl.semaphore_signal(barrier, inc=1, device_id={"seq": lax.rem(seq + hop, n_seq)}, device_id_type=MESH)
    for dev in (y_right, y_left):
        pl.semaphore_signal(barrier, inc=1, device_id=dev, device_id_type=MESH)

    frames = frames_ref[...]
    contract_rows = (((0,), (0,)), ((), ()))
    gj_acc[0] = lax.dot_general(frames.reshape(-1, frames.shape[-1]), da_ref[...], contract_rows, preferred_element_type=F32)
    own_pred = pred_ref[...]
    gj_acc[1] = lax.dot_general(own_pred.reshape(-1, own_pred.shape[-1]), dc_ref[...], contract_rows, preferred_element_type=F32)
    ge = lax.dot_general(da_ref[...], w_enc_ref[...], (((1,), (1,)), ((), ())), preferred_element_type=F32)
    ge_ref[...] = ge.astype(BF16).reshape(ge_ref.shape)
    ge_out[pl.ds(seq, 1)] = ge_ref[pl.ds(seq, 1)]
    dc_out[pl.ds(seq, 1)] = dc_ref[...][None]
    loss_out[pl.ds(seq, 1)] = loss_ref[...][None]
    pl.semaphore_wait(barrier, n_seq - 1 + 2)

    copies = Copies(send_sem, recv_sem)
    gj_half = gj_acc.shape[1] // CORES
    gw_half = gw_ref.shape[1] // CORES
    gj_y, gw_x = gj_half // RING, gw_half // RING
    gj_x = gj_y // RING

    mate_gj = copies.start(gj_acc.at[:, pl.ds((1 - core) * gj_half, gj_half), :], gj_pair, mate)
    mate_gw = copies.start(gw_ref.at[:, pl.ds((1 - core) * gw_half, gw_half), :], gw_pair, mate)

    dc_half = dc_out.shape[1] // 2

    def dc_at(k, half):
        return dc_out.at[k * CORES + core, pl.ds(half * dc_half, dc_half), :]

    dc_gather = Gather(copies, x, dc_at, x_right, x_left)
    dc_gather.begin()
    dc_mate = [copies.start(dc_out.at[seq], dc_out.at[seq], mate)]
    small = []
    for hop in range(1, n_seq):
        peer = lax.rem(seq + hop, n_seq)
        small.append(copies.start(ge_ref.at[peer], ge_out.at[seq], {"seq": peer}))
        small.append(copies.start(loss_ref, loss_out.at[seq], {"seq": peer}))

    gj_row = pl.multiple_of(core * gj_half, gj_half)
    gw_row = pl.multiple_of(core * gw_half, gw_half)

    def gj_shard_y(k, half):
        return gj_acc.at[:, pl.ds(pl.multiple_of(gj_row + k * gj_y + half * (gj_y // 2), SUB), gj_y // 2), :]

    def gw_shard_x(k, half):
        return gw_acc.at[:, pl.ds(pl.multiple_of(k * gw_x + half * (gw_x // 2), SUB), gw_x // 2), :]

    def halves(ref):
        return lambda half: ref.at[half]

    mate_gj.wait_recv()
    gj_acc[:, pl.ds(gj_row, gj_half), :] = gj_acc[:, pl.ds(gj_row, gj_half), :] + gj_pair[...]
    gj_r1 = Reduce(copies, "data", y, gj_shard_y, halves(gj_py), halves(gj_ly), halves(gj_ry))
    gj_r1.begin(y_right, y_left)
    mate_gw.wait_recv()
    gw_acc[...] = gw_ref[:, pl.ds(gw_row, gw_half), :] + gw_pair[...]
    gw_r1 = Reduce(copies, "seq", x, gw_shard_x, halves(gw_px), halves(gw_lx), halves(gw_rx))
    gw_r1.begin(x_right, x_left)

    dc_gather.relay()
    dc_mate.append(copies.start(dc_out.at[dc_gather.prv * CORES + core], dc_out.at[dc_gather.prv * CORES + core], mate))
    dc_mate.append(copies.start(dc_out.at[dc_gather.nxt * CORES + core], dc_out.at[dc_gather.nxt * CORES + core], mate))
    gj_r1.middle()
    gw_r1.middle()

    def keep_gj(half, value):
        gj_mid[:, pl.ds(half * (gj_y // 2), gj_y // 2), :] = value

    gj_r1.end(keep_gj)

    def gj_shard_x(k, half):
        return gj_mid.at[:, pl.ds(pl.multiple_of(k * gj_x + half * (gj_x // 2), SUB), gj_x // 2), :]

    gj_r2 = Reduce(copies, "seq", x, gj_shard_x, halves(gj_px), halves(gj_lx), halves(gj_rx))
    gj_r2.begin(x_right, x_left)

    def keep_gw(half, value):
        gw_mid[:, pl.ds(half * (gw_x // 2), gw_x // 2), :] = value

    gw_r1.end(keep_gw)

    def gw_shard_y(k, half):
        return gw_mid.at[k, pl.ds(half * (gw_x // 2), gw_x // 2), :]

    gw_r2 = Reduce(copies, "data", y, gw_shard_y, halves(gw_py), halves(gw_ly), halves(gw_ry))
    gw_r2.begin(y_right, y_left)
    gj_r2.middle()
    gw_r2.middle()

    def gj_out_x(k, half):
        return gj_out.at[:, pl.ds(pl.multiple_of(gj_row + y * gj_y + k * gj_x + half * (gj_x // 2), SUB), gj_x // 2), :]

    def gw_out_y(k, half):
        return gw_out.at[k, pl.ds(pl.multiple_of(gw_row + x * gw_x + half * (gw_x // 2), SUB), gw_x // 2), :]

    def put_gj(half, value):
        gj_out_x(x, half)[...] = value

    def put_gw(half, value):
        gw_out_y(y, half)[...] = value

    gj_r2.end(put_gj)
    gj_g1 = Gather(copies, x, gj_out_x, x_right, x_left)
    gj_g1.begin()
    gw_r2.end(put_gw)
    gw_g1 = Gather(copies, y, gw_out_y, y_right, y_left)
    gw_g1.begin()
    gj_g1.relay()
    gw_g1.relay()
    gj_g1.finish()

    def gj_out_y(k, half):
        return gj_out.at[:, pl.ds(pl.multiple_of(gj_row + k * gj_y + half * (gj_y // 2), SUB), gj_y // 2), :]

    def gw_out_x(k, half):
        return gw_out.at[:, pl.ds(pl.multiple_of(gw_row + k * gw_x + half * (gw_x // 2), SUB), gw_x // 2), :]

    gj_g2 = Gather(copies, y, gj_out_y, y_right, y_left)
    gj_g2.begin()
    gw_g1.finish()
    gw_g2 = Gather(copies, x, gw_out_x, x_right, x_left)
    gw_g2.begin()

    def gj_whole(k):
        return gj_out.at[:, pl.ds(pl.multiple_of(gj_row + k * gj_y, SUB), gj_y), :]

    def gw_whole(k):
        return gw_out.at[:, pl.ds(pl.multiple_of(gw_row + k * gw_x, SUB), gw_x), :]

    last = [copies.start(gj_whole(y), gj_whole(y), mate), copies.start(gw_whole(x), gw_whole(x), mate)]
    dc_gather.finish()
    dc_mate.append(copies.start(dc_out.at[dc_gather.opp * CORES + core], dc_out.at[dc_gather.opp * CORES + core], mate))
    gj_g2.relay()
    for k in (gj_g2.prv, gj_g2.nxt):
        last.append(copies.start(gj_whole(k), gj_whole(k), mate))
    gw_g2.relay()
    for k in (gw_g2.prv, gw_g2.nxt):
        last.append(copies.start(gw_whole(k), gw_whole(k), mate))
    gj_g2.finish()
    last.append(copies.start(gj_whole(gj_g2.opp), gj_whole(gj_g2.opp), mate))
    gw_g2.finish()
    last.append(copies.start(gw_whole(gw_g2.opp), gw_whole(gw_g2.opp), mate))
    for copy in small + dc_mate + last:
        copy.wait_recv()
    copies.drain()


N_COPIES = 6 + 2 + 4 + 14 + 4 * 6 + 4 * 6 + 8


def combine(n_seq, n_data, frames, own_pred, w_enc, da, dc, gw, loss):
    width = frames.shape[-1]
    joint = da.shape[-1]
    n_cols, _, col = gw.shape
    gj_half, gw_half = width // CORES, joint // CORES
    gj_y, gw_x = gj_half // RING, gw_half // RING
    gj_x = gj_y // RING
    return pl.pallas_call(
        functools.partial(combine_kernel, n_seq, n_data),
        out_shape=(
            jax.ShapeDtypeStruct(frames.shape, BF16),
            jax.ShapeDtypeStruct((n_seq,) + dc.shape, BF16),
            jax.ShapeDtypeStruct((2, width, joint), F32),
            jax.ShapeDtypeStruct(gw.shape, F32),
            jax.ShapeDtypeStruct((n_seq,) + loss.shape, F32),
        ),
        in_specs=[vspec()] * 7,
        out_specs=(vspec(),) * 5,
        scratch_shapes=[
            VMEM((2, width, joint), F32),
            VMEM((n_cols, gw_half, col), F32),
            VMEM((2, gj_half, joint), F32),
            VMEM((n_cols, gw_half, col), F32),
        ]
        + [VMEM((2, 2, gj_y // 2, joint), F32)] * 3
        + [VMEM((2, 2, gj_x // 2, joint), F32)] * 3
        + [VMEM((2, n_cols, gw_x // 2, col), F32)] * 3
        + [VMEM((2, gw_x // 2, col), F32)] * 3
        + [
            VMEM((2, gj_y, joint), F32),
            VMEM((n_cols, gw_x, col), F32),
            VMEM(frames.shape, BF16),
            pltpu.SemaphoreType.DMA((N_COPIES,)),
            pltpu.SemaphoreType.DMA((N_COPIES,)),
        ],
        compiler_params=pltpu.CompilerParams(collective_id=1, has_side_effects=True, vmem_limit_bytes=40_000_000),
        name="combine",
    )(frames, own_pred, w_enc, da, dc, gw, loss)


def output_kernel(place_ref, losses_ref, ge_ref, dc_ref, w_pred_ref, gj_ref, gw_ref,
                  loss_out, ge_out, gp_out, gwe_out, gwp_out, gwo_out, rows_ref, gp_ref, sem):
    n_utt, n_upos, width = gp_out.shape
    n_own = ge_ref.shape[1]
    n_cols, _, col = gw_ref.shape
    copies = [pltpu.make_async_copy(gj_ref.at[0], gwe_out, sem.at[0]), pltpu.make_async_copy(gj_ref.at[1], gwp_out, sem.at[1])]
    for k in range(n_cols):
        copies.append(pltpu.make_async_copy(gw_ref.at[k], gwo_out.at[:, pl.ds(k * col, col)], sem.at[2 + k]))
    for copy in copies:
        copy.start()
    n_parts = 4
    part = n_utt // n_parts
    for p in range(n_parts):
        for i in range(p * part, (p + 1) * part):
            place = place_ref[i]
            dev = place // n_own
            own = place - dev * n_own
            loss_out[i] = losses_ref[dev, 0, own]
            ge_out[i] = ge_ref[dev, own]
            rows_ref[i] = dc_ref[dev, pl.ds(pl.multiple_of(own * n_upos, n_upos), n_upos), :]
        rows = rows_ref[p * part:(p + 1) * part]
        grads = lax.dot_general(rows.reshape(part * n_upos, -1), w_pred_ref[...], (((1,), (1,)), ((), ())), preferred_element_type=F32)
        gp_ref[p * part:(p + 1) * part] = grads.reshape(part, n_upos, width)
        copy = pltpu.make_async_copy(gp_ref.at[pl.ds(p * part, part)], gp_out.at[pl.ds(p * part, part)], sem.at[2 + n_cols + p])
        copy.start()
        copies.append(copy)
    for copy in copies:
        copy.wait()


def outputs(place, losses, ge, dc, w_pred, gj, gw, n_upos):
    n_seq, n_own, t_loc, width = ge.shape
    n_utt = n_seq * n_own
    n_cols, joint, col = gw.shape
    hbm = pl.BlockSpec(memory_space=pl.ANY)
    return pl.pallas_call(
        output_kernel,
        out_shape=(
            jax.ShapeDtypeStruct((n_utt,), F32),
            jax.ShapeDtypeStruct((n_utt, t_loc, width), BF16),
            jax.ShapeDtypeStruct((n_utt, n_upos, width), F32),
            jax.ShapeDtypeStruct((width, joint), F32),
            jax.ShapeDtypeStruct((width, joint), F32),
            jax.ShapeDtypeStruct((joint, n_cols * col), F32),
        ),
        in_specs=[sspec()] * 2 + [vspec()] * 5,
        out_specs=(sspec(), vspec()) + (hbm,) * 4,
        scratch_shapes=[
            VMEM((n_utt, n_upos, joint), BF16),
            VMEM((n_utt, n_upos, width), F32),
            pltpu.SemaphoreType.DMA((2 + n_cols + 4,)),
        ],
        compiler_params=pltpu.CompilerParams(vmem_limit_bytes=20_000_000),
        name="outputs",
    )(place, losses, ge, dc, w_pred, gj, gw)


def solution(mesh):
    n_seq = mesh.shape["seq"]
    n_data = mesh.shape["data"]
    utt_rows = P(("part", "data"))
    utt_mats = P(("part", "data"), None)
    utt_cube = P(("part", "data"), None, None)
    enc_spec = P(("part", "data"), "seq", None)
    weight_in = P(None, None)
    weight_out = P("part", None)

    def body(enc_loc, pred_loc, w_enc, w_pred, w_out, labels, frame_len, label_len):
        t_loc = enc_loc.shape[1]
        n_upos = pred_loc.shape[1]
        seq_idx = lax.axis_index("seq").astype(jnp.int32).reshape(1)
        order, place, frames, own_pred, act, pred, w_out_t = exchange(n_seq, frame_len, label_len, enc_loc, pred_loc, w_enc, w_pred, w_out)
        da, dc, gw, loss = lattice(n_seq, n_data, seq_idx, order, frame_len, label_len, labels, act, pred, w_out, w_out_t, n_upos, t_loc)
        ge, dc_all, gj, gw, losses = combine(n_seq, n_data, frames, own_pred, w_enc, da, dc, gw, loss)
        loss, grad_enc, grad_pred, gw_enc, gw_pred, gw_out = outputs(place, losses, ge, dc_all, w_pred, gj, gw, n_upos)
        return loss, grad_enc, grad_pred, gw_enc, gw_pred, gw_out

    return jax.shard_map(body, mesh=mesh, in_specs=(enc_spec, utt_cube, weight_in, weight_in, weight_in, utt_mats, utt_rows, utt_rows), out_specs=(utt_rows, enc_spec, utt_cube, weight_out, weight_out, weight_out), check_vma=False)
```

```python
import functools

import jax
import jax.numpy as jnp
from jax import lax
from jax.experimental import pallas as pl
from jax.experimental.pallas import tpu as pltpu
from jax.sharding import PartitionSpec as P

NEG = -1e30
MESH = pl.DeviceIdType.MESH
VMEM = pltpu.VMEM
F32 = jnp.float32
BF16 = jnp.bfloat16
VMEM_LIMIT = 67_000_000
SUB = 8
LANES = 128
GROUPS = 4
BLOCK = 32
CORES = 2
RING = 4


def vspec():
    return pl.BlockSpec(memory_space=pltpu.VMEM)


def sspec():
    return pl.BlockSpec(memory_space=pltpu.SMEM)


def exchange_kernel(n_seq, flen_ref, llen_ref, enc_ref, pred_ref, w_enc_ref, w_pred_ref, w_out_ref,
                    order_ref, place_ref, frames_ref, own_pred_ref, a_ref, c_ref, w_out_t_ref,
                    key_ref, sorted_ref, send_sem, recv_sem):
    seq = lax.axis_index("seq")
    n_utt = enc_ref.shape[0]
    n_own = n_utt // n_seq
    barrier = pltpu.get_barrier_semaphore()
    for hop in range(1, n_seq):
        pl.semaphore_signal(barrier, inc=1, device_id={"seq": lax.rem(seq + hop, n_seq)}, device_id_type=MESH)

    def set_key(i, carry):
        key_ref[i] = ((flen_ref[i] + SUB - 1) // SUB) * ((llen_ref[i] + SUB) // SUB) * n_utt + i
        return carry

    def set_place(i, carry):
        key = key_ref[i]
        rank = jnp.int32(0)
        for j in range(n_utt):
            rank = rank + jnp.where(key_ref[j] > key, 1, 0)
        deal = rank // n_seq
        at = rank - deal * n_seq
        at = jnp.where(deal % 2 == 0, at, n_seq - 1 - at)
        place_ref[i] = at * n_own + deal
        return carry

    def set_order(k, carry):
        utt = jnp.int32(0)
        for j in range(n_utt):
            utt = utt + jnp.where(place_ref[j] == k, j, 0)
        order_ref[k] = utt
        return carry

    lax.fori_loop(0, n_utt, set_key, 0)
    lax.fori_loop(0, n_utt, set_place, 0)
    lax.fori_loop(0, n_utt, set_order, 0)
    for k in range(n_utt):
        sorted_ref[k] = enc_ref[order_ref[k]]
    pl.semaphore_wait(barrier, n_seq - 1)
    copies = []
    for hop in range(1, n_seq):
        peer = lax.rem(seq + hop, n_seq)
        copy = pltpu.make_async_remote_copy(
            src_ref=sorted_ref.at[pl.ds(peer * n_own, n_own)],
            dst_ref=frames_ref.at[seq],
            send_sem=send_sem.at[hop - 1],
            recv_sem=recv_sem.at[hop - 1],
            device_id={"seq": peer},
            device_id_type=MESH,
        )
        copy.start()
        copies.append(copy)
    frames_ref[pl.ds(seq, 1)] = sorted_ref[pl.ds(seq * n_own, n_own)][None]
    for j in range(n_own):
        own_pred_ref[j] = pred_ref[order_ref[seq * n_own + j]]
    own_pred = own_pred_ref[...]
    c_ref[...] = jnp.dot(own_pred.reshape(-1, own_pred.shape[-1]), w_pred_ref[...], preferred_element_type=F32).astype(BF16).astype(F32)
    w_out_t_ref[...] = w_out_ref[...].T
    for copy in copies:
        copy.wait()
    frames = frames_ref[...]
    a_ref[...] = jnp.dot(frames.reshape(-1, frames.shape[-1]), w_enc_ref[...], preferred_element_type=F32).astype(BF16).astype(F32)


def exchange(n_seq, frame_len, label_len, enc_loc, pred_loc, w_enc, w_pred, w_out):
    n_utt, t_loc, width = enc_loc.shape
    n_own = n_utt // n_seq
    n_upos = pred_loc.shape[1]
    joint, vocab = w_out.shape
    return pl.pallas_call(
        functools.partial(exchange_kernel, n_seq),
        out_shape=(
            jax.ShapeDtypeStruct((n_utt,), jnp.int32),
            jax.ShapeDtypeStruct((n_utt,), jnp.int32),
            jax.ShapeDtypeStruct((n_seq, n_own, t_loc, width), BF16),
            jax.ShapeDtypeStruct((n_own, n_upos, width), BF16),
            jax.ShapeDtypeStruct((n_seq * n_own * t_loc, joint), F32),
            jax.ShapeDtypeStruct((n_own * n_upos, joint), F32),
            jax.ShapeDtypeStruct((vocab, joint), BF16),
        ),
        in_specs=[sspec()] * 2 + [vspec()] * 5,
        out_specs=(sspec(),) * 2 + (vspec(),) * 5,
        scratch_shapes=[
            pltpu.SMEM((n_utt,), jnp.int32),
            VMEM(enc_loc.shape, BF16),
            pltpu.SemaphoreType.DMA((n_seq - 1,)),
            pltpu.SemaphoreType.DMA((n_seq - 1,)),
        ],
        compiler_params=pltpu.CompilerParams(collective_id=0, has_side_effects=True, vmem_limit_bytes=VMEM_LIMIT),
        name="exchange",
    )(frame_len, label_len, enc_loc, pred_loc, w_enc, w_pred, w_out)


def logaddexp(x, y):
    top = jnp.maximum(x, y)
    return top + jnp.log(1.0 + jnp.exp(-jnp.abs(x - y)))


def lattice_kernel(n_own, n_frames, n_upos, seq_ref, order_ref, flen_ref, llen_ref, labels_ref, a_ref, c_ref, w_ref, wt_ref,
                   da_ref, dc_ref, gw_ref, loss_ref,
                   e_ref, h_ref, blank_ref, label_ref, alpha_ref, beta_ref, ids_ref, dact_ref, dpred_ref, work0, work1, dz0, dz1):
    vocab = w_ref.shape[1]
    joint = w_ref.shape[0]
    n_vt = vocab // LANES
    rows_g = SUB * SUB
    rows_t = GROUPS * rows_g
    n_diag = n_frames + n_upos - 1
    first = seq_ref[0] * n_own
    utts = [order_ref[first + b] for b in range(n_own)]
    lens_t = [flen_ref[utt] for utt in utts]
    lens_u = [llen_ref[utt] for utt in utts]
    blocks_t = [lax.div(n + SUB - 1, SUB) for n in lens_t]
    blocks_u = [lax.div(n + SUB, SUB) for n in lens_u]
    starts = [jnp.int32(0)]
    for b in range(n_own):
        starts.append(starts[-1] + blocks_t[b] * blocks_u[b])
    total = starts[-1]
    n_tiles = lax.div(total + GROUPS - 1, GROUPS)

    def decode(n):
        n = jnp.minimum(n, total - 1)
        b = jnp.int32(0)
        base, width = starts[0], blocks_u[0]
        for k in range(1, n_own):
            past = n >= starts[k]
            b = jnp.where(past, k, b)
            base = jnp.where(past, starts[k], base)
            width = jnp.where(past, blocks_u[k], width)
        ti = lax.div(n - base, width)
        return n, b, ti, n - base - ti * width

    pos_col = lax.broadcasted_iota(jnp.int32, (n_upos, n_upos - 1), 0)
    pos_row = lax.broadcasted_iota(jnp.int32, (n_upos, n_upos - 1), 1)
    for b in range(n_own):
        row = labels_ref[pl.ds(utts[b], 1), :].astype(F32)
        col = jnp.sum(jnp.where(pos_col == pos_row, row, 0.0), axis=1, keepdims=True)
        ids_ref[pl.ds(b * n_upos, n_upos), :] = jnp.broadcast_to(col, (n_upos, LANES)).astype(jnp.int32)

    blank_ref[...] = jnp.zeros_like(blank_ref)
    label_ref[...] = jnp.zeros_like(label_ref)
    gw_ref[...] = jnp.zeros_like(gw_ref)
    dact_ref[...] = jnp.zeros_like(dact_ref)
    dpred_ref[...] = jnp.zeros_like(dpred_ref)

    lane = lax.broadcasted_iota(jnp.int32, (SUB, LANES), 1)
    block_lane = lax.broadcasted_iota(jnp.int32, (BLOCK, LANES), 1)
    t_block = BLOCK // SUB
    works, dzs = (work0, work1), (dz0, dz1)

    def tile_rows(i):
        return pl.ds(pl.multiple_of(jnp.clip(i, 0, n_tiles - 1) * rows_t, rows_t), rows_t)

    def tile_groups(i):
        return [decode(jnp.clip(i, 0, n_tiles - 1) * GROUPS + g) for g in range(GROUPS)]

    def pred_row(b, ui):
        return pl.ds(pl.multiple_of(b * n_upos + ui * SUB, SUB), SUB)

    def act_row(b, ti):
        return pl.ds(pl.multiple_of((ti * n_own + b) * SUB, SUB), SUB)

    def block_ids(b, ui):
        ids = ids_ref[pred_row(b, ui), :]
        return jnp.broadcast_to(ids[None], (t_block, SUB, LANES)).reshape(BLOCK, LANES)

    def cell_rows(ti, k, ui):
        return pl.ds(pl.multiple_of((n_diag - 1 - ti * SUB - k) * n_upos + ui * SUB, SUB), SUB)

    def make_hidden(i):
        first_row = jnp.clip(i, 0, n_tiles - 1) * rows_t
        for g, (n, b, ti, ui) in enumerate(tile_groups(i)):
            a8 = a_ref[act_row(b, ti), :]
            c8 = c_ref[pred_row(b, ui), :]
            h = jnp.tanh(a8[:, None, :] + c8[None, :, :]).reshape(rows_g, joint).astype(BF16)
            h_ref[pl.ds(pl.multiple_of(first_row + g * rows_g, rows_g), rows_g), :] = h

    def make_logits(i, z_ref):
        z_ref[...] = jnp.dot(h_ref[tile_rows(i), :], w_ref[...], preferred_element_type=F32)

    def make_softmax(i, z_ref):
        first_row = jnp.clip(i, 0, n_tiles - 1) * rows_t
        for g, (n, b, ti, ui) in enumerate(tile_groups(i)):
            ids = block_ids(b, ui)
            for r in range(0, rows_g, BLOCK):
                z = z_ref[g * rows_g + r:g * rows_g + r + BLOCK, :]
                top = jnp.max(z, axis=1, keepdims=True)
                e = jnp.exp(z - top)
                norm = jnp.sum(e, axis=1, keepdims=True)
                e_ref[pl.ds(pl.multiple_of(first_row + g * rows_g + r, BLOCK), BLOCK), :] = e
                log_norm = top + jnp.log(norm)
                picked = jnp.zeros((BLOCK, LANES), F32)
                for v in range(n_vt):
                    picked = picked + jnp.where(block_lane + v * LANES == ids, z[:, v * LANES:(v + 1) * LANES], 0.0)
                label = jnp.sum(picked, axis=1, keepdims=True) - log_norm
                blank = z[:, 0:1] - log_norm
                scale = 1.0 / norm
                rows = [cell_rows(ti, r // SUB + k, ui) for k in range(t_block)]
                old_blank = [blank_ref[at, :] for at in rows]
                old_label = [label_ref[at, :] for at in rows]
                for k, at in enumerate(rows):
                    sl = slice(k * SUB, (k + 1) * SUB)
                    blank_ref[at, :] = jnp.where(lane == b, blank[sl], jnp.where(lane == b + n_own, scale[sl], old_blank[k]))
                    label_ref[at, :] = jnp.where(lane == b, label[sl], old_label[k])

    make_hidden(0)
    make_logits(0, work0)
    make_hidden(1)

    def forward(j, carry):
        for half in range(2):
            i = 2 * j + half
            make_logits(i + 1, works[1 - half])
            make_softmax(i, works[half])
            make_hidden(i + 2)
        return carry

    lax.fori_loop(0, lax.div(n_tiles + 1, 2), forward, 0)

    upos = lax.broadcasted_iota(jnp.int32, (n_upos, LANES), 0)
    utt = lax.broadcasted_iota(jnp.int32, (n_upos, LANES), 1)
    t_end = jnp.ones((n_upos, LANES), jnp.int32)
    u_end = jnp.zeros((n_upos, LANES), jnp.int32)
    for b in range(n_own):
        t_end = jnp.where(utt == b, lens_t[b], t_end)
        u_end = jnp.where(utt == b, lens_u[b], u_end)

    def diagonal(d):
        return pl.ds((n_diag - 1 - d) * n_upos, n_upos, stride=n_upos + 1)

    def down(x):
        return jnp.where(upos == 0, NEG, pltpu.roll(x, 1, 0))

    def up(x):
        return jnp.where(upos == n_upos - 1, NEG, pltpu.roll(x, n_upos - 1, 0))

    def edge(d):
        return jnp.where((d - upos == t_end) & (upos == u_end), 0.0, NEG)

    alpha0 = jnp.where(upos == 0, 0.0, NEG).astype(F32)
    beta0 = edge(n_diag)
    alpha_ref[0] = alpha0
    beta_ref[n_diag] = beta0

    def sweep(k, carry):
        alpha, beta = carry
        d = k + 1
        alpha = logaddexp(alpha + blank_ref[diagonal(k), :], down(alpha + label_ref[diagonal(k), :]))
        alpha = jnp.where(upos <= d, alpha, NEG)
        alpha_ref[d] = alpha
        d = n_diag - 1 - k
        inside = (d - upos < t_end) & (upos <= u_end)
        beta = logaddexp(beta + blank_ref[diagonal(d), :], up(beta) + label_ref[diagonal(d), :])
        beta = jnp.where(inside, beta, edge(d))
        beta_ref[d] = beta
        return alpha, beta

    lax.fori_loop(0, n_diag, sweep, (alpha0, beta0))
    log_prob = beta_ref[0][0:1, :]
    loss_ref[...] = jnp.broadcast_to(-log_prob, (SUB, LANES))

    def occupancy(d, carry):
        t = d - upos
        alpha = alpha_ref[d]
        after = beta_ref[d + 1]
        cell_ok = (t >= 0) & (t < t_end) & (upos <= u_end)
        blank = blank_ref[diagonal(d), :]
        q0 = jnp.where(cell_ok, jnp.exp(alpha + blank + after - log_prob), 0.0)
        q1 = jnp.where(cell_ok & (upos < u_end), jnp.exp(alpha + label_ref[diagonal(d), :] + up(after) - log_prob), 0.0)
        blank_ref[diagonal(d), :] = jnp.where(utt < n_own, q0, blank)
        label_ref[diagonal(d), :] = q1
        return carry

    lax.fori_loop(0, n_diag, occupancy, 0)

    def make_dz(i, dz_ref):
        first_row = jnp.clip(i, 0, n_tiles - 1) * rows_t
        for g, (n, b, ti, ui) in enumerate(tile_groups(i)):
            keep = (lane == b) & (i * GROUPS + g < total)
            ids = block_ids(b, ui)
            for r in range(0, rows_g, BLOCK):
                q0s, q1s, scales = [], [], []
                for k in range(t_block):
                    at = cell_rows(ti, r // SUB + k, ui)
                    blank = blank_ref[at, :]
                    q0s.append(jnp.where(keep, blank, 0.0))
                    scales.append(jnp.where(lane == b + n_own, blank, 0.0))
                    q1s.append(jnp.where(keep, label_ref[at, :], 0.0))
                q0 = jnp.sum(jnp.concatenate(q0s, axis=0), axis=1, keepdims=True)
                q1 = jnp.sum(jnp.concatenate(q1s, axis=0), axis=1, keepdims=True)
                scale = jnp.sum(jnp.concatenate(scales, axis=0), axis=1, keepdims=True) * (q0 + q1)
                rows = pl.ds(pl.multiple_of(first_row + g * rows_g + r, BLOCK), BLOCK)
                for v in range(n_vt):
                    at_v = block_lane + v * LANES
                    dz = e_ref[rows, v * LANES:(v + 1) * LANES] * scale
                    if v == 0:
                        dz = dz - jnp.where(at_v == 0, q0, 0.0)
                    dz = dz - jnp.where(at_v == ids, q1, 0.0)
                    dz_ref[g * rows_g + r:g * rows_g + r + BLOCK, v * LANES:(v + 1) * LANES] = dz.astype(BF16)

    def make_products(i, dz_ref, dh_ref):
        dz = dz_ref[...]
        dh_ref[:, :joint] = jnp.dot(dz, wt_ref[...], preferred_element_type=F32)
        h = h_ref[tile_rows(i), :]
        for y in range(gw_ref.shape[0]):
            part = dz[:, y * gw_ref.shape[2]:(y + 1) * gw_ref.shape[2]]
            gw_ref[y] += lax.dot_general(h, part, (((0,), (0,)), ((), ())), preferred_element_type=F32)

    def make_sums(i, dh_ref):
        first_row = jnp.clip(i, 0, n_tiles - 1) * rows_t
        for g, (n, b, ti, ui) in enumerate(tile_groups(i)):
            rows = pl.ds(pl.multiple_of(first_row + g * rows_g, rows_g), rows_g)
            for v in range(joint // LANES):
                cols = slice(v * LANES, (v + 1) * LANES)
                h = h_ref[rows, cols].astype(F32)
                ds = dh_ref[g * rows_g:(g + 1) * rows_g, cols] * (1.0 - h * h)
                cube = ds.reshape(SUB, SUB, LANES)
                dact_ref[act_row(b, ti), cols] += jnp.sum(cube, axis=1)
                dpred_ref[pred_row(b, ui), cols] += jnp.sum(cube, axis=0)

    work1[...] = jnp.zeros_like(work1)
    make_dz(0, dz0)

    def backward(j, carry):
        for half in range(2):
            i = 2 * j + half
            make_products(i, dzs[half], works[half])
            make_dz(i + 1, dzs[1 - half])
            make_sums(i - 1, works[1 - half])
        return carry

    lax.fori_loop(0, lax.div(n_tiles + 2, 2), backward, 0)
    da_ref[...] = dact_ref[...].astype(BF16)
    dc_ref[...] = dpred_ref[...].astype(BF16)


def lattice(n_seq, n_data, seq_idx, order, frame_len, label_len, labels, act, pred, w_out, w_out_t, n_upos, t_loc):
    n_own = frame_len.shape[0] // n_seq
    n_frames = n_seq * t_loc
    joint, vocab = w_out.shape
    cells = n_own * n_frames * n_upos
    n_diag = n_frames + n_upos - 1
    lat_rows = (n_diag + n_upos - 1) * n_upos
    return pl.pallas_call(
        functools.partial(lattice_kernel, n_own, n_frames, n_upos),
        out_shape=(
            jax.ShapeDtypeStruct(act.shape, BF16),
            jax.ShapeDtypeStruct(pred.shape, BF16),
            jax.ShapeDtypeStruct((n_data, joint, vocab // n_data), F32),
            jax.ShapeDtypeStruct((SUB, LANES), F32),
        ),
        in_specs=[sspec()] * 4 + [vspec()] * 5,
        out_specs=(vspec(),) * 4,
        scratch_shapes=[
            VMEM((cells, vocab), F32),
            VMEM((cells, joint), BF16),
            VMEM((lat_rows, LANES), F32),
            VMEM((lat_rows, LANES), F32),
            VMEM((n_diag + 1, n_upos, LANES), F32),
            VMEM((n_diag + 1, n_upos, LANES), F32),
            VMEM((n_own * n_upos, LANES), jnp.int32),
            VMEM(act.shape, F32),
            VMEM(pred.shape, F32),
            VMEM((GROUPS * SUB * SUB, vocab), F32),
            VMEM((GROUPS * SUB * SUB, vocab), F32),
            VMEM((GROUPS * SUB * SUB, vocab), BF16),
            VMEM((GROUPS * SUB * SUB, vocab), BF16),
        ],
        compiler_params=pltpu.CompilerParams(vmem_limit_bytes=VMEM_LIMIT),
        name="lattice",
    )(seq_idx, order, frame_len, label_len, labels, act, pred, w_out, w_out_t)


class Copies:
    def __init__(self, send_sem, recv_sem):
        self.sems = (send_sem, recv_sem)
        self.all = []

    def start(self, src, dst, device):
        k = len(self.all)
        copy = pltpu.make_async_remote_copy(src_ref=src, dst_ref=dst, send_sem=self.sems[0].at[k], recv_sem=self.sems[1].at[k], device_id=device, device_id_type=MESH)
        copy.start()
        self.all.append(copy)
        return copy

    def drain(self):
        for copy in self.all:
            copy.wait_send()


class Reduce:
    def __init__(self, copies, axis, me, acc, pair, left, right):
        self.copies, self.acc, self.pair, self.left, self.right = copies, acc, pair, left, right
        self.me, self.nxt, self.prv, self.opp = me, lax.rem(me + 1, RING), lax.rem(me + RING - 1, RING), lax.rem(me + 2, RING)
        self.to_right = {axis: self.nxt}
        self.to_left = {axis: self.prv}

    def begin(self, right_dev, left_dev):
        c, acc = self.copies, self.acc
        self.devs = (right_dev, left_dev)
        self.a1 = c.start(acc(self.opp, 0), self.pair(0), right_dev)
        self.b1 = c.start(acc(self.opp, 1), self.pair(1), left_dev)
        self.b2 = c.start(acc(self.nxt, 1), self.left(1), right_dev)
        self.a2 = c.start(acc(self.prv, 0), self.right(0), left_dev)

    def middle(self):
        c, acc = self.copies, self.acc
        self.a1.wait_recv()
        add = acc(self.nxt, 0)
        add[...] = add[...] + self.pair(0)[...]
        self.a3 = c.start(add, self.left(0), self.devs[0])
        self.b1.wait_recv()
        add = acc(self.prv, 1)
        add[...] = add[...] + self.pair(1)[...]
        self.b3 = c.start(add, self.right(1), self.devs[1])

    def end(self, store):
        self.b2.wait_recv()
        self.a3.wait_recv()
        self.a2.wait_recv()
        self.b3.wait_recv()
        for half in range(2):
            store(half, self.acc(self.me, half)[...] + self.left(half)[...] + self.right(half)[...])


class Gather:
    def __init__(self, copies, me, out, right_dev, left_dev):
        self.copies, self.out, self.devs = copies, out, (right_dev, left_dev)
        self.me, self.nxt, self.prv, self.opp = me, lax.rem(me + 1, RING), lax.rem(me + RING - 1, RING), lax.rem(me + 2, RING)

    def begin(self):
        c, out, (right_dev, left_dev) = self.copies, self.out, self.devs
        self.ra = c.start(out(self.me, 0), out(self.me, 0), right_dev)
        self.lb = c.start(out(self.me, 1), out(self.me, 1), left_dev)
        self.rb = c.start(out(self.me, 1), out(self.me, 1), right_dev)
        self.la = c.start(out(self.me, 0), out(self.me, 0), left_dev)

    def relay(self):
        c, out, (right_dev, left_dev) = self.copies, self.out, self.devs
        self.ra.wait_recv()
        self.ra2 = c.start(out(self.prv, 0), out(self.prv, 0), right_dev)
        self.lb.wait_recv()
        self.lb2 = c.start(out(self.nxt, 1), out(self.nxt, 1), left_dev)
        self.rb.wait_recv()
        self.la.wait_recv()

    def finish(self):
        self.ra2.wait_recv()
        self.lb2.wait_recv()


def combine_kernel(n_seq, n_data, frames_ref, pred_ref, w_enc_ref, da_ref, dc_ref, gw_ref, loss_ref,
                   ge_out, dc_out, gj_out, gw_out, loss_out,
                   gj_acc, gw_acc, gj_pair, gw_pair, gj_py, gj_ly, gj_ry, gj_px, gj_lx, gj_rx, gw_px, gw_lx, gw_rx, gw_py, gw_ly, gw_ry, gj_mid, gw_mid, ge_ref,
                   send_sem, recv_sem):
    seq = lax.axis_index("seq")
    y = lax.axis_index("data")
    x = lax.div(seq, CORES)
    core = lax.rem(seq, CORES)
    x_right = {"seq": lax.rem(x + 1, RING) * CORES + core}
    x_left = {"seq": lax.rem(x + RING - 1, RING) * CORES + core}
    y_right = {"data": lax.rem(y + 1, RING)}
    y_left = {"data": lax.rem(y + RING - 1, RING)}
    mate = {"seq": x * CORES + 1 - core}
    barrier = pltpu.get_barrier_semaphore()
    for hop in range(1, n_seq):
        pl.semaphore_signal(barrier, inc=1, device_id={"seq": lax.rem(seq + hop, n_seq)}, device_id_type=MESH)
    for dev in (y_right, y_left):
        pl.semaphore_signal(barrier, inc=1, device_id=dev, device_id_type=MESH)

    frames = frames_ref[...]
    contract_rows = (((0,), (0,)), ((), ()))
    gj_acc[0] = lax.dot_general(frames.reshape(-1, frames.shape[-1]), da_ref[...], contract_rows, preferred_element_type=F32)
    own_pred = pred_ref[...]
    gj_acc[1] = lax.dot_general(own_pred.reshape(-1, own_pred.shape[-1]), dc_ref[...], contract_rows, preferred_element_type=F32)
    ge = lax.dot_general(da_ref[...], w_enc_ref[...], (((1,), (1,)), ((), ())), preferred_element_type=F32)
    ge_ref[...] = ge.astype(BF16).reshape(ge_ref.shape)
    ge_out[pl.ds(seq, 1)] = ge_ref[pl.ds(seq, 1)]
    dc_out[pl.ds(seq, 1)] = dc_ref[...][None]
    loss_out[pl.ds(seq, 1)] = loss_ref[...][None]
    pl.semaphore_wait(barrier, n_seq - 1 + 2)

    copies = Copies(send_sem, recv_sem)
    gj_half = gj_acc.shape[1] // CORES
    gw_half = gw_ref.shape[1] // CORES
    gj_y, gw_x = gj_half // RING, gw_half // RING
    gj_x = gj_y // RING

    mate_gj = copies.start(gj_acc.at[:, pl.ds((1 - core) * gj_half, gj_half), :], gj_pair, mate)
    mate_gw = copies.start(gw_ref.at[:, pl.ds((1 - core) * gw_half, gw_half), :], gw_pair, mate)

    dc_half = dc_out.shape[1] // 2

    def dc_at(k, half):
        return dc_out.at[k * CORES + core, pl.ds(half * dc_half, dc_half), :]

    dc_gather = Gather(copies, x, dc_at, x_right, x_left)
    dc_gather.begin()
    dc_mate = [copies.start(dc_out.at[seq], dc_out.at[seq], mate)]
    small = []
    for hop in range(1, n_seq):
        peer = lax.rem(seq + hop, n_seq)
        small.append(copies.start(ge_ref.at[peer], ge_out.at[seq], {"seq": peer}))
        small.append(copies.start(loss_ref, loss_out.at[seq], {"seq": peer}))

    gj_row = pl.multiple_of(core * gj_half, gj_half)
    gw_row = pl.multiple_of(core * gw_half, gw_half)

    def gj_shard_y(k, half):
        return gj_acc.at[:, pl.ds(pl.multiple_of(gj_row + k * gj_y + half * (gj_y // 2), SUB), gj_y // 2), :]

    def gw_shard_x(k, half):
        return gw_acc.at[:, pl.ds(pl.multiple_of(k * gw_x + half * (gw_x // 2), SUB), gw_x // 2), :]

    def halves(ref):
        return lambda half: ref.at[half]

    mate_gj.wait_recv()
    gj_acc[:, pl.ds(gj_row, gj_half), :] = gj_acc[:, pl.ds(gj_row, gj_half), :] + gj_pair[...]
    gj_r1 = Reduce(copies, "data", y, gj_shard_y, halves(gj_py), halves(gj_ly), halves(gj_ry))
    gj_r1.begin(y_right, y_left)
    mate_gw.wait_recv()
    gw_acc[...] = gw_ref[:, pl.ds(gw_row, gw_half), :] + gw_pair[...]
    gw_r1 = Reduce(copies, "seq", x, gw_shard_x, halves(gw_px), halves(gw_lx), halves(gw_rx))
    gw_r1.begin(x_right, x_left)

    dc_gather.relay()
    dc_mate.append(copies.start(dc_out.at[dc_gather.prv * CORES + core], dc_out.at[dc_gather.prv * CORES + core], mate))
    dc_mate.append(copies.start(dc_out.at[dc_gather.nxt * CORES + core], dc_out.at[dc_gather.nxt * CORES + core], mate))
    gj_r1.middle()
    gw_r1.middle()

    def keep_gj(half, value):
        gj_mid[:, pl.ds(half * (gj_y // 2), gj_y // 2), :] = value

    gj_r1.end(keep_gj)

    def gj_shard_x(k, half):
        return gj_mid.at[:, pl.ds(pl.multiple_of(k * gj_x + half * (gj_x // 2), SUB), gj_x // 2), :]

    gj_r2 = Reduce(copies, "seq", x, gj_shard_x, halves(gj_px), halves(gj_lx), halves(gj_rx))
    gj_r2.begin(x_right, x_left)

    def keep_gw(half, value):
        gw_mid[:, pl.ds(half * (gw_x // 2), gw_x // 2), :] = value

    gw_r1.end(keep_gw)

    def gw_shard_y(k, half):
        return gw_mid.at[k, pl.ds(half * (gw_x // 2), gw_x // 2), :]

    gw_r2 = Reduce(copies, "data", y, gw_shard_y, halves(gw_py), halves(gw_ly), halves(gw_ry))
    gw_r2.begin(y_right, y_left)
    gj_r2.middle()
    gw_r2.middle()

    def gj_out_x(k, half):
        return gj_out.at[:, pl.ds(pl.multiple_of(gj_row + y * gj_y + k * gj_x + half * (gj_x // 2), SUB), gj_x // 2), :]

    def gw_out_y(k, half):
        return gw_out.at[k, pl.ds(pl.multiple_of(gw_row + x * gw_x + half * (gw_x // 2), SUB), gw_x // 2), :]

    def put_gj(half, value):
        gj_out_x(x, half)[...] = value

    def put_gw(half, value):
        gw_out_y(y, half)[...] = value

    gj_r2.end(put_gj)
    gj_g1 = Gather(copies, x, gj_out_x, x_right, x_left)
    gj_g1.begin()
    gw_r2.end(put_gw)
    gw_g1 = Gather(copies, y, gw_out_y, y_right, y_left)
    gw_g1.begin()
    gj_g1.relay()
    gw_g1.relay()
    gj_g1.finish()

    def gj_out_y(k, half):
        return gj_out.at[:, pl.ds(pl.multiple_of(gj_row + k * gj_y + half * (gj_y // 2), SUB), gj_y // 2), :]

    def gw_out_x(k, half):
        return gw_out.at[:, pl.ds(pl.multiple_of(gw_row + k * gw_x + half * (gw_x // 2), SUB), gw_x // 2), :]

    gj_g2 = Gather(copies, y, gj_out_y, y_right, y_left)
    gj_g2.begin()
    gw_g1.finish()
    gw_g2 = Gather(copies, x, gw_out_x, x_right, x_left)
    gw_g2.begin()

    def gj_whole(k):
        return gj_out.at[:, pl.ds(pl.multiple_of(gj_row + k * gj_y, SUB), gj_y), :]

    def gw_whole(k):
        return gw_out.at[:, pl.ds(pl.multiple_of(gw_row + k * gw_x, SUB), gw_x), :]

    last = [copies.start(gj_whole(y), gj_whole(y), mate), copies.start(gw_whole(x), gw_whole(x), mate)]
    dc_gather.finish()
    dc_mate.append(copies.start(dc_out.at[dc_gather.opp * CORES + core], dc_out.at[dc_gather.opp * CORES + core], mate))
    gj_g2.relay()
    for k in (gj_g2.prv, gj_g2.nxt):
        last.append(copies.start(gj_whole(k), gj_whole(k), mate))
    gw_g2.relay()
    for k in (gw_g2.prv, gw_g2.nxt):
        last.append(copies.start(gw_whole(k), gw_whole(k), mate))
    gj_g2.finish()
    last.append(copies.start(gj_whole(gj_g2.opp), gj_whole(gj_g2.opp), mate))
    gw_g2.finish()
    last.append(copies.start(gw_whole(gw_g2.opp), gw_whole(gw_g2.opp), mate))
    for copy in small + dc_mate + last:
        copy.wait_recv()
    copies.drain()


N_COPIES = 6 + 2 + 4 + 14 + 4 * 6 + 4 * 6 + 8


def combine(n_seq, n_data, frames, own_pred, w_enc, da, dc, gw, loss):
    width = frames.shape[-1]
    joint = da.shape[-1]
    n_cols, _, col = gw.shape
    gj_half, gw_half = width // CORES, joint // CORES
    gj_y, gw_x = gj_half // RING, gw_half // RING
    gj_x = gj_y // RING
    return pl.pallas_call(
        functools.partial(combine_kernel, n_seq, n_data),
        out_shape=(
            jax.ShapeDtypeStruct(frames.shape, BF16),
            jax.ShapeDtypeStruct((n_seq,) + dc.shape, BF16),
            jax.ShapeDtypeStruct((2, width, joint), F32),
            jax.ShapeDtypeStruct(gw.shape, F32),
            jax.ShapeDtypeStruct((n_seq,) + loss.shape, F32),
        ),
        in_specs=[vspec()] * 7,
        out_specs=(vspec(),) * 5,
        scratch_shapes=[
            VMEM((2, width, joint), F32),
            VMEM((n_cols, gw_half, col), F32),
            VMEM((2, gj_half, joint), F32),
            VMEM((n_cols, gw_half, col), F32),
        ]
        + [VMEM((2, 2, gj_y // 2, joint), F32)] * 3
        + [VMEM((2, 2, gj_x // 2, joint), F32)] * 3
        + [VMEM((2, n_cols, gw_x // 2, col), F32)] * 3
        + [VMEM((2, gw_x // 2, col), F32)] * 3
        + [
            VMEM((2, gj_y, joint), F32),
            VMEM((n_cols, gw_x, col), F32),
            VMEM(frames.shape, BF16),
            pltpu.SemaphoreType.DMA((N_COPIES,)),
            pltpu.SemaphoreType.DMA((N_COPIES,)),
        ],
        compiler_params=pltpu.CompilerParams(collective_id=1, has_side_effects=True, vmem_limit_bytes=VMEM_LIMIT),
        name="combine",
    )(frames, own_pred, w_enc, da, dc, gw, loss)


def output_kernel(place_ref, losses_ref, ge_ref, dc_ref, w_pred_ref, gj_ref, gw_ref,
                  loss_out, ge_out, gp_out, gwe_out, gwp_out, gwo_out, rows_ref, gp_ref, sem):
    n_utt, n_upos, width = gp_out.shape
    n_own = ge_ref.shape[1]
    n_cols, _, col = gw_ref.shape
    copies = [pltpu.make_async_copy(gj_ref.at[0], gwe_out, sem.at[0]), pltpu.make_async_copy(gj_ref.at[1], gwp_out, sem.at[1])]
    for k in range(n_cols):
        copies.append(pltpu.make_async_copy(gw_ref.at[k], gwo_out.at[:, pl.ds(k * col, col)], sem.at[2 + k]))
    for copy in copies:
        copy.start()
    n_parts = 4
    part = n_utt // n_parts
    for p in range(n_parts):
        for i in range(p * part, (p + 1) * part):
            place = place_ref[i]
            dev = place // n_own
            own = place - dev * n_own
            loss_out[i] = losses_ref[dev, 0, own]
            ge_out[i] = ge_ref[dev, own]
            rows_ref[i] = dc_ref[dev, pl.ds(pl.multiple_of(own * n_upos, n_upos), n_upos), :]
        rows = rows_ref[p * part:(p + 1) * part]
        grads = lax.dot_general(rows.reshape(part * n_upos, -1), w_pred_ref[...], (((1,), (1,)), ((), ())), preferred_element_type=F32)
        gp_ref[p * part:(p + 1) * part] = grads.reshape(part, n_upos, width)
        copy = pltpu.make_async_copy(gp_ref.at[pl.ds(p * part, part)], gp_out.at[pl.ds(p * part, part)], sem.at[2 + n_cols + p])
        copy.start()
        copies.append(copy)
    for copy in copies:
        copy.wait()


def outputs(place, losses, ge, dc, w_pred, gj, gw, n_upos):
    n_seq, n_own, t_loc, width = ge.shape
    n_utt = n_seq * n_own
    n_cols, joint, col = gw.shape
    hbm = pl.BlockSpec(memory_space=pl.ANY)
    return pl.pallas_call(
        output_kernel,
        out_shape=(
            jax.ShapeDtypeStruct((n_utt,), F32),
            jax.ShapeDtypeStruct((n_utt, t_loc, width), BF16),
            jax.ShapeDtypeStruct((n_utt, n_upos, width), F32),
            jax.ShapeDtypeStruct((width, joint), F32),
            jax.ShapeDtypeStruct((width, joint), F32),
            jax.ShapeDtypeStruct((joint, n_cols * col), F32),
        ),
        in_specs=[sspec()] * 2 + [vspec()] * 5,
        out_specs=(sspec(), vspec()) + (hbm,) * 4,
        scratch_shapes=[
            VMEM((n_utt, n_upos, joint), BF16),
            VMEM((n_utt, n_upos, width), F32),
            pltpu.SemaphoreType.DMA((2 + n_cols + 4,)),
        ],
        compiler_params=pltpu.CompilerParams(vmem_limit_bytes=VMEM_LIMIT),
        name="outputs",
    )(place, losses, ge, dc, w_pred, gj, gw)


def solution(mesh):
    n_seq = mesh.shape["seq"]
    n_data = mesh.shape["data"]
    utt_rows = P(("part", "data"))
    utt_mats = P(("part", "data"), None)
    utt_cube = P(("part", "data"), None, None)
    enc_spec = P(("part", "data"), "seq", None)
    weight_in = P(None, None)
    weight_out = P("part", None)

    def body(enc_loc, pred_loc, w_enc, w_pred, w_out, labels, frame_len, label_len):
        t_loc = enc_loc.shape[1]
        n_upos = pred_loc.shape[1]
        seq_idx = lax.axis_index("seq").astype(jnp.int32).reshape(1)
        order, place, frames, own_pred, act, pred, w_out_t = exchange(n_seq, frame_len, label_len, enc_loc, pred_loc, w_enc, w_pred, w_out)
        da, dc, gw, loss = lattice(n_seq, n_data, seq_idx, order, frame_len, label_len, labels, act, pred, w_out, w_out_t, n_upos, t_loc)
        ge, dc_all, gj, gw, losses = combine(n_seq, n_data, frames, own_pred, w_enc, da, dc, gw, loss)
        loss, grad_enc, grad_pred, gw_enc, gw_pred, gw_out = outputs(place, losses, ge, dc_all, w_pred, gj, gw, n_upos)
        return loss, grad_enc, grad_pred, gw_enc, gw_pred, gw_out

    return jax.shard_map(body, mesh=mesh, in_specs=(enc_spec, utt_cube, weight_in, weight_in, weight_in, utt_mats, utt_rows, utt_rows), out_specs=(utt_rows, enc_spec, utt_cube, weight_out, weight_out, weight_out), check_vma=False)
```

```python
import functools

import jax
import jax.numpy as jnp
from jax import lax
from jax.experimental import pallas as pl
from jax.experimental.pallas import tpu as pltpu
from jax.sharding import PartitionSpec as P

NEG = -1e30
MESH = pl.DeviceIdType.MESH
VMEM = pltpu.VMEM
F32 = jnp.float32
BF16 = jnp.bfloat16
VMEM_LIMIT = 67_000_000
SUB = 8
LANES = 128
GROUPS = 4
BLOCK = 32
CORES = 2
RING = 4


def vspec():
    return pl.BlockSpec(memory_space=pltpu.VMEM)


def sspec():
    return pl.BlockSpec(memory_space=pltpu.SMEM)


def exchange_kernel(n_seq, flen_ref, llen_ref, enc_ref, pred_ref, w_enc_ref, w_pred_ref, w_out_ref,
                    order_ref, place_ref, frames_ref, a_ref, c_ref, w_out_t_ref,
                    key_ref, sorted_ref, own_pred_ref, send_sem, recv_sem):
    seq = lax.axis_index("seq")
    n_utt = enc_ref.shape[0]
    n_own = n_utt // n_seq
    barrier = pltpu.get_barrier_semaphore()
    for hop in range(1, n_seq):
        pl.semaphore_signal(barrier, inc=1, device_id={"seq": lax.rem(seq + hop, n_seq)}, device_id_type=MESH)

    def set_key(i, carry):
        key_ref[i] = ((flen_ref[i] + SUB - 1) // SUB) * ((llen_ref[i] + SUB) // SUB) * n_utt + i
        return carry

    def set_place(i, carry):
        key = key_ref[i]
        rank = jnp.int32(0)
        for j in range(n_utt):
            rank = rank + jnp.where(key_ref[j] > key, 1, 0)
        deal = rank // n_seq
        at = rank - deal * n_seq
        at = jnp.where(deal % 2 == 0, at, n_seq - 1 - at)
        place_ref[i] = at * n_own + deal
        return carry

    def set_order(k, carry):
        utt = jnp.int32(0)
        for j in range(n_utt):
            utt = utt + jnp.where(place_ref[j] == k, j, 0)
        order_ref[k] = utt
        return carry

    lax.fori_loop(0, n_utt, set_key, 0)
    lax.fori_loop(0, n_utt, set_place, 0)
    lax.fori_loop(0, n_utt, set_order, 0)
    for k in range(n_utt):
        sorted_ref[k] = enc_ref[order_ref[k]]
    pl.semaphore_wait(barrier, n_seq - 1)
    copies = []
    for hop in range(1, n_seq):
        peer = lax.rem(seq + hop, n_seq)
        copy = pltpu.make_async_remote_copy(
            src_ref=sorted_ref.at[pl.ds(peer * n_own, n_own)],
            dst_ref=frames_ref.at[seq],
            send_sem=send_sem.at[hop - 1],
            recv_sem=recv_sem.at[hop - 1],
            device_id={"seq": peer},
            device_id_type=MESH,
        )
        copy.start()
        copies.append(copy)
    frames_ref[pl.ds(seq, 1)] = sorted_ref[pl.ds(seq * n_own, n_own)][None]
    for j in range(n_own):
        own_pred_ref[j] = pred_ref[order_ref[seq * n_own + j]]
    own_pred = own_pred_ref[...]
    c_ref[...] = jnp.dot(own_pred.reshape(-1, own_pred.shape[-1]), w_pred_ref[...], preferred_element_type=F32).astype(BF16).astype(F32)
    w_out_t_ref[...] = w_out_ref[...].T
    for copy in copies:
        copy.wait()
    frames = frames_ref[...]
    a_ref[...] = jnp.dot(frames.reshape(-1, frames.shape[-1]), w_enc_ref[...], preferred_element_type=F32).astype(BF16).astype(F32)


def exchange(n_seq, frame_len, label_len, enc_loc, pred_loc, w_enc, w_pred, w_out):
    n_utt, t_loc, width = enc_loc.shape
    n_own = n_utt // n_seq
    n_upos = pred_loc.shape[1]
    joint, vocab = w_out.shape
    return pl.pallas_call(
        functools.partial(exchange_kernel, n_seq),
        out_shape=(
            jax.ShapeDtypeStruct((n_utt,), jnp.int32),
            jax.ShapeDtypeStruct((n_utt,), jnp.int32),
            jax.ShapeDtypeStruct((n_seq, n_own, t_loc, width), BF16),
            jax.ShapeDtypeStruct((n_seq * n_own * t_loc, joint), F32),
            jax.ShapeDtypeStruct((n_own * n_upos, joint), F32),
            jax.ShapeDtypeStruct((vocab, joint), BF16),
        ),
        in_specs=[sspec()] * 2 + [vspec()] * 5,
        out_specs=(sspec(),) * 2 + (vspec(),) * 4,
        scratch_shapes=[
            pltpu.SMEM((n_utt,), jnp.int32),
            VMEM(enc_loc.shape, BF16),
            VMEM((n_own, n_upos, width), BF16),
            pltpu.SemaphoreType.DMA((n_seq - 1,)),
            pltpu.SemaphoreType.DMA((n_seq - 1,)),
        ],
        compiler_params=pltpu.CompilerParams(collective_id=0, has_side_effects=True, vmem_limit_bytes=VMEM_LIMIT),
        name="exchange",
    )(frame_len, label_len, enc_loc, pred_loc, w_enc, w_pred, w_out)


def logaddexp(x, y):
    top = jnp.maximum(x, y)
    return top + jnp.log(1.0 + jnp.exp(-jnp.abs(x - y)))


def lattice_kernel(n_own, n_frames, n_upos, seq_ref, order_ref, flen_ref, llen_ref, labels_ref, a_ref, c_ref, w_ref, wt_ref,
                   da_ref, dc_ref, gw_ref, loss_ref,
                   e_ref, h_ref, blank_ref, label_ref, alpha_ref, beta_ref, ids_ref, dact_ref, dpred_ref, work0, work1, dz0, dz1):
    vocab = w_ref.shape[1]
    joint = w_ref.shape[0]
    n_vt = vocab // LANES
    rows_g = SUB * SUB
    rows_t = GROUPS * rows_g
    n_diag = n_frames + n_upos - 1
    first = seq_ref[0] * n_own
    utts = [order_ref[first + b] for b in range(n_own)]
    lens_t = [flen_ref[utt] for utt in utts]
    lens_u = [llen_ref[utt] for utt in utts]
    blocks_t = [lax.div(n + SUB - 1, SUB) for n in lens_t]
    blocks_u = [lax.div(n + SUB, SUB) for n in lens_u]
    starts = [jnp.int32(0)]
    for b in range(n_own):
        starts.append(starts[-1] + blocks_t[b] * blocks_u[b])
    total = starts[-1]
    n_tiles = lax.div(total + GROUPS - 1, GROUPS)

    def decode(n):
        n = jnp.minimum(n, total - 1)
        b = jnp.int32(0)
        base, width = starts[0], blocks_u[0]
        for k in range(1, n_own):
            past = n >= starts[k]
            b = jnp.where(past, k, b)
            base = jnp.where(past, starts[k], base)
            width = jnp.where(past, blocks_u[k], width)
        ti = lax.div(n - base, width)
        return n, b, ti, n - base - ti * width

    pos_col = lax.broadcasted_iota(jnp.int32, (n_upos, n_upos - 1), 0)
    pos_row = lax.broadcasted_iota(jnp.int32, (n_upos, n_upos - 1), 1)
    for b in range(n_own):
        row = labels_ref[pl.ds(utts[b], 1), :].astype(F32)
        col = jnp.sum(jnp.where(pos_col == pos_row, row, 0.0), axis=1, keepdims=True)
        ids_ref[pl.ds(b * n_upos, n_upos), :] = jnp.broadcast_to(col, (n_upos, LANES)).astype(jnp.int32)

    blank_ref[...] = jnp.zeros_like(blank_ref)
    label_ref[...] = jnp.zeros_like(label_ref)
    gw_ref[...] = jnp.zeros_like(gw_ref)
    dact_ref[...] = jnp.zeros_like(dact_ref)
    dpred_ref[...] = jnp.zeros_like(dpred_ref)

    lane = lax.broadcasted_iota(jnp.int32, (SUB, LANES), 1)
    block_lane = lax.broadcasted_iota(jnp.int32, (BLOCK, LANES), 1)
    t_block = BLOCK // SUB
    works, dzs = (work0, work1), (dz0, dz1)

    def tile_rows(i):
        return pl.ds(pl.multiple_of(jnp.clip(i, 0, n_tiles - 1) * rows_t, rows_t), rows_t)

    def tile_groups(i):
        return [decode(jnp.clip(i, 0, n_tiles - 1) * GROUPS + g) for g in range(GROUPS)]

    def pred_row(b, ui):
        return pl.ds(pl.multiple_of(b * n_upos + ui * SUB, SUB), SUB)

    def act_row(b, ti):
        return pl.ds(pl.multiple_of((ti * n_own + b) * SUB, SUB), SUB)

    def block_ids(b, ui):
        ids = ids_ref[pred_row(b, ui), :]
        return jnp.broadcast_to(ids[None], (t_block, SUB, LANES)).reshape(BLOCK, LANES)

    def cell_rows(ti, k, ui):
        return pl.ds(pl.multiple_of((n_diag - 1 - ti * SUB - k) * n_upos + ui * SUB, SUB), SUB)

    def make_hidden(i):
        first_row = jnp.clip(i, 0, n_tiles - 1) * rows_t
        for g, (n, b, ti, ui) in enumerate(tile_groups(i)):
            a8 = a_ref[act_row(b, ti), :]
            c8 = c_ref[pred_row(b, ui), :]
            h = jnp.tanh(a8[:, None, :] + c8[None, :, :]).reshape(rows_g, joint).astype(BF16)
            h_ref[pl.ds(pl.multiple_of(first_row + g * rows_g, rows_g), rows_g), :] = h

    def make_logits(i, z_ref):
        z_ref[...] = jnp.dot(h_ref[tile_rows(i), :], w_ref[...], preferred_element_type=F32)

    def make_softmax(i, z_ref):
        first_row = jnp.clip(i, 0, n_tiles - 1) * rows_t
        for g, (n, b, ti, ui) in enumerate(tile_groups(i)):
            ids = block_ids(b, ui)
            for r in range(0, rows_g, BLOCK):
                z = z_ref[g * rows_g + r:g * rows_g + r + BLOCK, :]
                top = jnp.max(z, axis=1, keepdims=True)
                e = jnp.exp(z - top)
                norm = jnp.sum(e, axis=1, keepdims=True)
                e_ref[pl.ds(pl.multiple_of(first_row + g * rows_g + r, BLOCK), BLOCK), :] = e
                log_norm = top + jnp.log(norm)
                picked = jnp.zeros((BLOCK, LANES), F32)
                for v in range(n_vt):
                    picked = picked + jnp.where(block_lane + v * LANES == ids, z[:, v * LANES:(v + 1) * LANES], 0.0)
                label = jnp.sum(picked, axis=1, keepdims=True) - log_norm
                blank = z[:, 0:1] - log_norm
                scale = 1.0 / norm
                rows = [cell_rows(ti, r // SUB + k, ui) for k in range(t_block)]
                old_blank = [blank_ref[at, :] for at in rows]
                old_label = [label_ref[at, :] for at in rows]
                for k, at in enumerate(rows):
                    sl = slice(k * SUB, (k + 1) * SUB)
                    blank_ref[at, :] = jnp.where(lane == b, blank[sl], jnp.where(lane == b + n_own, scale[sl], old_blank[k]))
                    label_ref[at, :] = jnp.where(lane == b, label[sl], old_label[k])

    make_hidden(0)
    make_logits(0, work0)
    make_hidden(1)

    def forward(j, carry):
        for half in range(2):
            i = 2 * j + half
            make_logits(i + 1, works[1 - half])
            make_softmax(i, works[half])
            make_hidden(i + 2)
        return carry

    lax.fori_loop(0, lax.div(n_tiles + 1, 2), forward, 0)

    upos = lax.broadcasted_iota(jnp.int32, (n_upos, LANES), 0)
    utt = lax.broadcasted_iota(jnp.int32, (n_upos, LANES), 1)
    t_end = jnp.ones((n_upos, LANES), jnp.int32)
    u_end = jnp.zeros((n_upos, LANES), jnp.int32)
    for b in range(n_own):
        t_end = jnp.where(utt == b, lens_t[b], t_end)
        u_end = jnp.where(utt == b, lens_u[b], u_end)

    def diagonal(d):
        return pl.ds((n_diag - 1 - d) * n_upos, n_upos, stride=n_upos + 1)

    def down(x):
        return jnp.where(upos == 0, NEG, pltpu.roll(x, 1, 0))

    def up(x):
        return jnp.where(upos == n_upos - 1, NEG, pltpu.roll(x, n_upos - 1, 0))

    def edge(d):
        return jnp.where((d - upos == t_end) & (upos == u_end), 0.0, NEG)

    alpha0 = jnp.where(upos == 0, 0.0, NEG).astype(F32)
    beta0 = edge(n_diag)
    alpha_ref[0] = alpha0
    beta_ref[n_diag] = beta0

    def sweep(k, carry):
        alpha, beta = carry
        d = k + 1
        alpha = logaddexp(alpha + blank_ref[diagonal(k), :], down(alpha + label_ref[diagonal(k), :]))
        alpha = jnp.where(upos <= d, alpha, NEG)
        alpha_ref[d] = alpha
        d = n_diag - 1 - k
        inside = (d - upos < t_end) & (upos <= u_end)
        beta = logaddexp(beta + blank_ref[diagonal(d), :], up(beta) + label_ref[diagonal(d), :])
        beta = jnp.where(inside, beta, edge(d))
        beta_ref[d] = beta
        return alpha, beta

    lax.fori_loop(0, n_diag, sweep, (alpha0, beta0))
    log_prob = beta_ref[0][0:1, :]
    loss_ref[...] = jnp.broadcast_to(-log_prob, (SUB, LANES))

    def occupancy(d, carry):
        t = d - upos
        alpha = alpha_ref[d]
        after = beta_ref[d + 1]
        cell_ok = (t >= 0) & (t < t_end) & (upos <= u_end)
        blank = blank_ref[diagonal(d), :]
        q0 = jnp.where(cell_ok, jnp.exp(alpha + blank + after - log_prob), 0.0)
        q1 = jnp.where(cell_ok & (upos < u_end), jnp.exp(alpha + label_ref[diagonal(d), :] + up(after) - log_prob), 0.0)
        blank_ref[diagonal(d), :] = jnp.where(utt < n_own, q0, blank)
        label_ref[diagonal(d), :] = q1
        return carry

    lax.fori_loop(0, n_diag, occupancy, 0)

    def make_dz(i, dz_ref):
        first_row = jnp.clip(i, 0, n_tiles - 1) * rows_t
        for g, (n, b, ti, ui) in enumerate(tile_groups(i)):
            keep = (lane == b) & (i * GROUPS + g < total)
            ids = block_ids(b, ui)
            for r in range(0, rows_g, BLOCK):
                q0s, q1s, scales = [], [], []
                for k in range(t_block):
                    at = cell_rows(ti, r // SUB + k, ui)
                    blank = blank_ref[at, :]
                    q0s.append(jnp.where(keep, blank, 0.0))
                    scales.append(jnp.where(lane == b + n_own, blank, 0.0))
                    q1s.append(jnp.where(keep, label_ref[at, :], 0.0))
                q0 = jnp.sum(jnp.concatenate(q0s, axis=0), axis=1, keepdims=True)
                q1 = jnp.sum(jnp.concatenate(q1s, axis=0), axis=1, keepdims=True)
                scale = jnp.sum(jnp.concatenate(scales, axis=0), axis=1, keepdims=True) * (q0 + q1)
                rows = pl.ds(pl.multiple_of(first_row + g * rows_g + r, BLOCK), BLOCK)
                for v in range(n_vt):
                    at_v = block_lane + v * LANES
                    dz = e_ref[rows, v * LANES:(v + 1) * LANES] * scale
                    if v == 0:
                        dz = dz - jnp.where(at_v == 0, q0, 0.0)
                    dz = dz - jnp.where(at_v == ids, q1, 0.0)
                    dz_ref[g * rows_g + r:g * rows_g + r + BLOCK, v * LANES:(v + 1) * LANES] = dz.astype(BF16)

    def make_products(i, dz_ref, dh_ref):
        dz = dz_ref[...]
        dh_ref[:, :joint] = jnp.dot(dz, wt_ref[...], preferred_element_type=F32)
        h = h_ref[tile_rows(i), :]
        for v in range(0, n_vt, 2):
            part = lax.dot_general(h, dz[:, v * LANES:(v + 2) * LANES], (((0,), (0,)), ((), ())), preferred_element_type=F32)
            gw_ref[v] += part[:, :LANES]
            gw_ref[v + 1] += part[:, LANES:]

    def make_sums(i, dh_ref):
        first_row = jnp.clip(i, 0, n_tiles - 1) * rows_t
        for g, (n, b, ti, ui) in enumerate(tile_groups(i)):
            rows = pl.ds(pl.multiple_of(first_row + g * rows_g, rows_g), rows_g)
            for v in range(joint // LANES):
                cols = slice(v * LANES, (v + 1) * LANES)
                h = h_ref[rows, cols].astype(F32)
                ds = dh_ref[g * rows_g:(g + 1) * rows_g, cols] * (1.0 - h * h)
                cube = ds.reshape(SUB, SUB, LANES)
                dact_ref[act_row(b, ti), cols] += jnp.sum(cube, axis=1)
                dpred_ref[pred_row(b, ui), cols] += jnp.sum(cube, axis=0)

    work1[...] = jnp.zeros_like(work1)
    make_dz(0, dz0)

    def backward(j, carry):
        for half in range(2):
            i = 2 * j + half
            make_products(i, dzs[half], works[half])
            make_dz(i + 1, dzs[1 - half])
            make_sums(i - 1, works[1 - half])
        return carry

    lax.fori_loop(0, lax.div(n_tiles + 2, 2), backward, 0)
    da_ref[...] = dact_ref[...].astype(BF16)
    dc_ref[...] = dpred_ref[...].astype(BF16)


def lattice(n_seq, seq_idx, order, frame_len, label_len, labels, act, pred, w_out, w_out_t, n_upos, t_loc):
    n_own = frame_len.shape[0] // n_seq
    n_frames = n_seq * t_loc
    joint, vocab = w_out.shape
    cells = n_own * n_frames * n_upos
    n_diag = n_frames + n_upos - 1
    lat_rows = (n_diag + n_upos - 1) * n_upos
    return pl.pallas_call(
        functools.partial(lattice_kernel, n_own, n_frames, n_upos),
        out_shape=(
            jax.ShapeDtypeStruct(act.shape, BF16),
            jax.ShapeDtypeStruct(pred.shape, BF16),
            jax.ShapeDtypeStruct((vocab // LANES, joint, LANES), F32),
            jax.ShapeDtypeStruct((SUB, LANES), F32),
        ),
        in_specs=[sspec()] * 4 + [vspec()] * 5,
        out_specs=(vspec(),) * 4,
        scratch_shapes=[
            VMEM((cells, vocab), F32),
            VMEM((cells, joint), BF16),
            VMEM((lat_rows, LANES), F32),
            VMEM((lat_rows, LANES), F32),
            VMEM((n_diag + 1, n_upos, LANES), F32),
            VMEM((n_diag + 1, n_upos, LANES), F32),
            VMEM((n_own * n_upos, LANES), jnp.int32),
            VMEM(act.shape, F32),
            VMEM(pred.shape, F32),
            VMEM((GROUPS * SUB * SUB, vocab), F32),
            VMEM((GROUPS * SUB * SUB, vocab), F32),
            VMEM((GROUPS * SUB * SUB, vocab), BF16),
            VMEM((GROUPS * SUB * SUB, vocab), BF16),
        ],
        compiler_params=pltpu.CompilerParams(vmem_limit_bytes=VMEM_LIMIT),
        name="lattice",
    )(seq_idx, order, frame_len, label_len, labels, act, pred, w_out, w_out_t)


class Copies:
    def __init__(self, send_sem, recv_sem):
        self.sems = (send_sem, recv_sem)
        self.all = []

    def start(self, src, dst, device):
        k = len(self.all)
        copy = pltpu.make_async_remote_copy(src_ref=src, dst_ref=dst, send_sem=self.sems[0].at[k], recv_sem=self.sems[1].at[k], device_id=device, device_id_type=MESH)
        copy.start()
        self.all.append(copy)
        return copy

    def drain(self):
        for copy in self.all:
            copy.wait_send()


class Ring:
    def __init__(self, me, right, left):
        self.me, self.right, self.left = me, right, left
        self.nxt, self.prv, self.opp = lax.rem(me + 1, RING), lax.rem(me + RING - 1, RING), lax.rem(me + 2, RING)


class Reduce:
    def __init__(self, copies, ring, acc, bufs):
        self.copies, self.ring, self.acc = copies, ring, acc
        self.pair, self.from_left, self.from_right = bufs

    def begin(self):
        c, r, acc = self.copies, self.ring, self.acc
        self.a1 = c.start(acc(r.opp, 0), self.pair.at[0], r.right)
        self.b1 = c.start(acc(r.opp, 1), self.pair.at[1], r.left)
        self.b2 = c.start(acc(r.nxt, 1), self.from_left.at[1], r.right)
        self.a2 = c.start(acc(r.prv, 0), self.from_right.at[0], r.left)

    def middle(self):
        c, r, acc = self.copies, self.ring, self.acc
        self.a1.wait_recv()
        add = acc(r.nxt, 0)
        add[...] = add[...] + self.pair[0]
        self.a3 = c.start(add, self.from_left.at[0], r.right)
        self.b1.wait_recv()
        add = acc(r.prv, 1)
        add[...] = add[...] + self.pair[1]
        self.b3 = c.start(add, self.from_right.at[1], r.left)

    def end(self, target):
        for copy in (self.b2, self.a3, self.a2, self.b3):
            copy.wait_recv()
        for half in range(2):
            target(half)[...] = self.acc(self.ring.me, half)[...] + self.from_left[half] + self.from_right[half]


class Gather:
    def __init__(self, copies, ring, out):
        self.copies, self.ring, self.out = copies, ring, out

    def send(self, k, half, device):
        return self.copies.start(self.out(k, half), self.out(k, half), device)

    def begin(self):
        r = self.ring
        self.ra = self.send(r.me, 0, r.right)
        self.lb = self.send(r.me, 1, r.left)
        self.rb = self.send(r.me, 1, r.right)
        self.la = self.send(r.me, 0, r.left)

    def relay(self):
        r = self.ring
        self.ra.wait_recv()
        self.ra2 = self.send(r.prv, 0, r.right)
        self.lb.wait_recv()
        self.lb2 = self.send(r.nxt, 1, r.left)
        self.rb.wait_recv()
        self.la.wait_recv()

    def finish(self):
        self.ra2.wait_recv()
        self.lb2.wait_recv()


def rows_of(start, size):
    return pl.ds(pl.multiple_of(start, SUB), size)


def combine_kernel(n_seq, order_ref, frames_ref, pred_ref, w_enc_ref, da_ref, dc_ref, gw_ref, loss_ref,
                   ge_out, dc_out, gwe_out, gwp_out, gwo_out, loss_out, *scratch):
    (enc_acc, enc_pair, enc_mid, enc_y, enc_x, outs_acc, outs_pair, outs_mid, outs_1, outs_2, pred_acc, pred_y, rows_ref, ge_ref, send_sem, recv_sem) = unflatten(scratch)
    seq = lax.axis_index("seq")
    y = lax.axis_index("data")
    x = lax.div(seq, CORES)
    core = lax.rem(seq, CORES)
    mate = {"seq": x * CORES + 1 - core}
    ring_x = Ring(x, {"seq": lax.rem(x + 1, RING) * CORES + core}, {"seq": lax.rem(x + RING - 1, RING) * CORES + core})
    ring_y = Ring(y, {"data": lax.rem(y + 1, RING)}, {"data": lax.rem(y + RING - 1, RING)})
    barrier = pltpu.get_barrier_semaphore()
    for hop in range(1, n_seq):
        pl.semaphore_signal(barrier, inc=1, device_id={"seq": lax.rem(seq + hop, n_seq)}, device_id_type=MESH)
    for dev in (ring_y.right, ring_y.left):
        pl.semaphore_signal(barrier, inc=1, device_id=dev, device_id_type=MESH)

    n_blk = gw_ref.shape[0] // 2
    n_utt = n_seq * frames_ref.shape[1]
    n_upos = pred_ref.shape[1]
    enc_half = enc_acc.shape[0] // CORES
    out_half = gw_ref.shape[1] // CORES
    enc_q, out_q = enc_half // RING, out_half // RING
    enc_s = enc_q // RING
    enc_row, out_row = core * enc_half, core * out_half
    contract_rows = (((0,), (0,)), ((), ()))

    frames = frames_ref[...]
    enc_acc[...] = lax.dot_general(frames.reshape(-1, frames.shape[-1]), da_ref[...], contract_rows, preferred_element_type=F32)
    dc_out[pl.ds(seq, 1)] = dc_ref[...][None]
    loss_out[pl.ds(seq, 1)] = loss_ref[...][None]
    pl.semaphore_wait(barrier, n_seq - 1 + 2)

    copies = Copies(send_sem, recv_sem)

    def swap_out(part):
        blocks = pl.ds(part * n_blk, n_blk)
        return copies.start(gw_ref.at[blocks, rows_of((1 - core) * out_half, out_half), :], outs_pair[part], mate)

    dc_half = dc_out.shape[1] // 2
    dc_gather = Gather(copies, ring_x, lambda k, half: dc_out.at[k * CORES + core, pl.ds(half * dc_half, dc_half), :])
    swap_1 = swap_out(1)
    swap_enc = copies.start(enc_acc.at[rows_of((1 - core) * enc_half, enc_half), :], enc_pair, mate)
    dc_gather.begin()
    dc_mate = [copies.start(dc_out.at[seq], dc_out.at[seq], mate)]
    swap_0 = swap_out(0)

    def dc_pass(k):
        dc_mate.append(copies.start(dc_out.at[k * CORES + core], dc_out.at[k * CORES + core], mate))

    ge = lax.dot_general(da_ref[...], w_enc_ref[...], (((1,), (1,)), ((), ())), preferred_element_type=F32)
    ge_ref[...] = ge.astype(BF16).reshape(ge_ref.shape)
    ge_out[pl.ds(seq, 1)] = ge_ref[pl.ds(seq, 1)]

    def add_out(part):
        outs_acc[part][...] = gw_ref[pl.ds(part * n_blk, n_blk), rows_of(out_row, out_half), :] + outs_pair[part][...]

    def out_first(part):
        return lambda k, half: outs_acc[part].at[:, rows_of(k * out_q + half * (out_q // 2), out_q // 2), :]

    def out_second(part):
        return lambda k, half: outs_mid[part].at[k, pl.ds(half * (out_q // 2), out_q // 2), :]

    rings = ((ring_x, ring_y), (ring_y, ring_x))
    first = [Reduce(copies, rings[part][0], out_first(part), outs_1[part]) for part in range(2)]
    second = [Reduce(copies, rings[part][1], out_second(part), outs_2[part]) for part in range(2)]
    enc_first = Reduce(copies, ring_y, lambda k, half: enc_acc.at[rows_of(enc_row + k * enc_q + half * (enc_q // 2), enc_q // 2), :], enc_y)
    enc_second = Reduce(copies, ring_x, lambda k, half: enc_mid.at[rows_of(k * enc_s + half * (enc_s // 2), enc_s // 2), :], enc_x)
    pred_first = Reduce(copies, ring_y, lambda k, half: pred_acc.at[rows_of(k * enc_s + half * (enc_s // 2), enc_s // 2), :], pred_y)

    swap_1.wait_recv()
    add_out(1)
    first[1].begin()
    swap_enc.wait_recv()
    enc_acc[rows_of(enc_row, enc_half), :] = enc_acc[rows_of(enc_row, enc_half), :] + enc_pair[...]
    enc_first.begin()
    swap_0.wait_recv()
    add_out(0)
    first[0].begin()
    dc_gather.relay()
    dc_pass(ring_x.prv)
    dc_pass(ring_x.nxt)
    first[1].middle()
    enc_first.middle()
    small = []
    for hop in range(1, n_seq):
        peer = lax.rem(seq + hop, n_seq)
        small.append(copies.start(loss_ref, loss_out.at[seq], {"seq": peer}))
    for hop in range(1, n_seq):
        peer = lax.rem(seq + hop, n_seq)
        small.append(copies.start(ge_ref.at[peer], ge_out.at[seq], {"seq": peer}))
    first[0].middle()
    dc_gather.finish()
    dc_pass(ring_x.opp)

    def out_place(part, k1, k2, half, whole=False):
        start, size = out_row + k1 * out_q, out_q
        if not whole:
            start, size = start + half * (out_q // 2), out_q // 2
        return gwo_out.at[part * n_blk + k2 if k2 is not None else pl.ds(part * n_blk, n_blk), rows_of(start, size), :]

    first[1].end(lambda half: outs_mid[1].at[:, pl.ds(half * (out_q // 2), out_q // 2), :])
    second[1].begin()
    enc_first.end(lambda half: enc_mid.at[pl.ds(half * (enc_q // 2), enc_q // 2), :])
    enc_second.begin()

    for copy in dc_mate:
        copy.wait_recv()
    for k in range(n_utt):
        rows_ref[k * n_upos:(k + 1) * n_upos, :] = pred_ref[order_ref[k], :, pl.ds(pl.multiple_of(x * LANES, LANES), LANES)]
    pred_part = lax.dot_general(rows_ref[...], dc_out[...].reshape(n_utt * n_upos, -1), contract_rows, preferred_element_type=F32)
    pred_acc[...] = jnp.where(core == 0, pred_part[:enc_q], pred_part[enc_q:])
    pred_first.begin()

    first[0].end(lambda half: outs_mid[0].at[:, pl.ds(half * (out_q // 2), out_q // 2), :])
    second[0].begin()
    second[1].middle()
    enc_second.middle()
    pred_first.middle()
    second[0].middle()

    def pair_place(part):
        ring1, ring2 = rings[part]
        return (
            Gather(copies, ring2, lambda k, half: out_place(part, ring1.me, k, half)),
            Gather(copies, ring1, lambda k, half: out_place(part, k, None, half)),
        )

    gathers = [pair_place(0), pair_place(1)]
    enc_at = lambda ky, kx, half: gwe_out.at[rows_of(enc_row + ky * enc_q + kx * enc_s + half * (enc_s // 2), enc_s // 2), :]
    enc_g1 = Gather(copies, ring_x, lambda k, half: enc_at(y, k, half))
    enc_g2 = Gather(copies, ring_y, lambda k, half: gwe_out.at[rows_of(enc_row + k * enc_q + half * (enc_q // 2), enc_q // 2), :])
    pred_at = lambda ky, half: gwp_out.at[x, core, rows_of(ky * enc_s + half * (enc_s // 2), enc_s // 2), :]
    pred_g1 = Gather(copies, ring_y, pred_at)
    pred_g2 = Gather(copies, ring_x, lambda k, half: gwp_out.at[k, core, pl.ds(half * (enc_q // 2), enc_q // 2), :])

    second[1].end(lambda half: out_place(1, y, x, half))
    gathers[1][0].begin()
    enc_second.end(lambda half: enc_at(y, x, half))
    enc_g1.begin()
    pred_first.end(lambda half: pred_at(y, half))
    pred_g1.begin()
    second[0].end(lambda half: out_place(0, x, y, half))
    gathers[0][0].begin()
    gathers[1][0].relay()
    enc_g1.relay()
    pred_g1.relay()
    gathers[0][0].relay()

    last = []

    def pass_on(ref):
        last.append(copies.start(ref, ref, mate))

    enc_whole = lambda k: gwe_out.at[rows_of(enc_row + k * enc_q, enc_q), :]
    pred_whole = lambda k: gwp_out.at[k, core]
    out_whole = lambda part: lambda k: out_place(part, k, None, 0, True)
    finals = [(gathers[1], out_whole(1)), ((enc_g1, enc_g2), enc_whole), ((pred_g1, pred_g2), pred_whole), (gathers[0], out_whole(0))]
    for (g1, g2), whole in finals:
        g1.finish()
        g2.begin()
        pass_on(whole(g2.ring.me))
    for (g1, g2), whole in finals:
        g2.relay()
        pass_on(whole(g2.ring.prv))
        pass_on(whole(g2.ring.nxt))
    for (g1, g2), whole in finals:
        g2.finish()
        pass_on(whole(g2.ring.opp))
    for copy in small + last:
        copy.wait_recv()
    copies.drain()


N_COPIES = 3 + 10 + 14 + 6 * 7 + 6 * 8 + 16


def unflatten(refs):
    refs = list(refs)
    take = lambda n: [refs.pop(0) for _ in range(n)]
    enc_acc, enc_pair, enc_mid = take(3)
    enc_y, enc_x = take(3), take(3)
    outs = [(take(1)[0], take(1)[0], take(1)[0], take(3), take(3)) for _ in range(2)]
    outs_acc, outs_pair, outs_mid, outs_1, outs_2 = zip(*outs)
    pred_acc = refs.pop(0)
    pred_y = take(3)
    return (enc_acc, enc_pair, enc_mid, enc_y, enc_x, outs_acc, outs_pair, outs_mid, outs_1, outs_2, pred_acc, pred_y, *refs)


def combine(n_seq, order, frames, pred_loc, w_enc, da, dc, gw, loss):
    width = frames.shape[-1]
    n_utt, n_upos, _ = pred_loc.shape
    joint = da.shape[-1]
    n_blk = gw.shape[0] // 2
    enc_half, out_half = width // CORES, joint // CORES
    enc_q, out_q = enc_half // RING, out_half // RING
    enc_s = enc_q // RING
    ring = lambda *shape: [VMEM(shape, F32)] * 3
    outs = [VMEM((n_blk, out_half, LANES), F32)] * 2 + [VMEM((n_blk, out_q, LANES), F32)] + ring(2, n_blk, out_q // 2, LANES) + ring(2, out_q // 2, LANES)
    return pl.pallas_call(
        functools.partial(combine_kernel, n_seq),
        out_shape=(
            jax.ShapeDtypeStruct(frames.shape, BF16),
            jax.ShapeDtypeStruct((n_seq,) + dc.shape, BF16),
            jax.ShapeDtypeStruct((width, joint), F32),
            jax.ShapeDtypeStruct((RING, CORES, enc_q, joint), F32),
            jax.ShapeDtypeStruct(gw.shape, F32),
            jax.ShapeDtypeStruct((n_seq,) + loss.shape, F32),
        ),
        in_specs=[sspec()] + [vspec()] * 7,
        out_specs=(vspec(),) * 6,
        scratch_shapes=[VMEM((width, joint), F32), VMEM((enc_half, joint), F32), VMEM((enc_q, joint), F32)]
        + ring(2, enc_q // 2, joint)
        + ring(2, enc_s // 2, joint)
        + outs
        + outs
        + [VMEM((enc_q, joint), F32)]
        + ring(2, enc_s // 2, joint)
        + [
            VMEM((n_utt * n_upos, LANES), BF16),
            VMEM(frames.shape, BF16),
            pltpu.SemaphoreType.DMA((N_COPIES,)),
            pltpu.SemaphoreType.DMA((N_COPIES,)),
        ],
        compiler_params=pltpu.CompilerParams(collective_id=1, has_side_effects=True, vmem_limit_bytes=VMEM_LIMIT),
        name="combine",
    )(order, frames, pred_loc, w_enc, da, dc, gw, loss)


def output_kernel(place_ref, losses_ref, ge_ref, dc_ref, w_pred_ref, gwe_ref, gwp_ref, gw_ref,
                  loss_out, ge_out, gp_out, gwe_out, gwp_out, gwo_out, rows_ref, gp_ref, sem):
    n_utt, n_upos, width = gp_out.shape
    n_own = ge_ref.shape[1]
    n_cols, _, col = gw_ref.shape
    copies = [pltpu.make_async_copy(gwe_ref, gwe_out, sem.at[0]), pltpu.make_async_copy(gwp_ref, gwp_out, sem.at[1])]
    for k in range(n_cols):
        copies.append(pltpu.make_async_copy(gw_ref.at[k], gwo_out.at[:, pl.ds(k * col, col)], sem.at[2 + k]))
    for copy in copies:
        copy.start()
    n_parts = 4
    part = n_utt // n_parts
    for p in range(n_parts):
        for i in range(p * part, (p + 1) * part):
            place = place_ref[i]
            dev = place // n_own
            own = place - dev * n_own
            loss_out[i] = losses_ref[dev, 0, own]
            ge_out[i] = ge_ref[dev, own]
            rows_ref[i] = dc_ref[dev, pl.ds(pl.multiple_of(own * n_upos, n_upos), n_upos), :]
        rows = rows_ref[p * part:(p + 1) * part]
        grads = lax.dot_general(rows.reshape(part * n_upos, -1), w_pred_ref[...], (((1,), (1,)), ((), ())), preferred_element_type=F32)
        gp_ref[p * part:(p + 1) * part] = grads.reshape(part, n_upos, width)
        copy = pltpu.make_async_copy(gp_ref.at[pl.ds(p * part, part)], gp_out.at[pl.ds(p * part, part)], sem.at[2 + n_cols + p])
        copy.start()
        copies.append(copy)
    for copy in copies:
        copy.wait()


def outputs(place, losses, ge, dc, w_pred, gwe, gwp, gw, n_upos):
    n_seq, n_own, t_loc, width = ge.shape
    n_utt = n_seq * n_own
    n_cols, joint, col = gw.shape
    hbm = pl.BlockSpec(memory_space=pl.ANY)
    return pl.pallas_call(
        output_kernel,
        out_shape=(
            jax.ShapeDtypeStruct((n_utt,), F32),
            jax.ShapeDtypeStruct((n_utt, t_loc, width), BF16),
            jax.ShapeDtypeStruct((n_utt, n_upos, width), F32),
            jax.ShapeDtypeStruct((width, joint), F32),
            jax.ShapeDtypeStruct((width, joint), F32),
            jax.ShapeDtypeStruct((joint, n_cols * col), F32),
        ),
        in_specs=[sspec()] * 2 + [vspec()] * 6,
        out_specs=(sspec(), vspec()) + (hbm,) * 4,
        scratch_shapes=[
            VMEM((n_utt, n_upos, joint), BF16),
            VMEM((n_utt, n_upos, width), F32),
            pltpu.SemaphoreType.DMA((2 + n_cols + 4,)),
        ],
        compiler_params=pltpu.CompilerParams(vmem_limit_bytes=VMEM_LIMIT),
        name="outputs",
    )(place, losses, ge, dc, w_pred, gwe, gwp, gw)


def solution(mesh):
    n_seq = mesh.shape["seq"]
    utt_rows = P(("part", "data"))
    utt_mats = P(("part", "data"), None)
    utt_cube = P(("part", "data"), None, None)
    enc_spec = P(("part", "data"), "seq", None)
    weight_in = P(None, None)
    weight_out = P("part", None)

    def body(enc_loc, pred_loc, w_enc, w_pred, w_out, labels, frame_len, label_len):
        t_loc = enc_loc.shape[1]
        n_upos = pred_loc.shape[1]
        seq_idx = lax.axis_index("seq").astype(jnp.int32).reshape(1)
        order, place, frames, act, pred, w_out_t = exchange(n_seq, frame_len, label_len, enc_loc, pred_loc, w_enc, w_pred, w_out)
        da, dc, gw, loss = lattice(n_seq, seq_idx, order, frame_len, label_len, labels, act, pred, w_out, w_out_t, n_upos, t_loc)
        ge, dc_all, gwe, gwp, gw, losses = combine(n_seq, order, frames, pred_loc, w_enc, da, dc, gw, loss)
        loss, grad_enc, grad_pred, gw_enc, gw_pred, gw_out = outputs(place, losses, ge, dc_all, w_pred, gwe, gwp.reshape(gwe.shape), gw, n_upos)
        return loss, grad_enc, grad_pred, gw_enc, gw_pred, gw_out

    return jax.shard_map(body, mesh=mesh, in_specs=(enc_spec, utt_cube, weight_in, weight_in, weight_in, utt_mats, utt_rows, utt_rows), out_specs=(utt_rows, enc_spec, utt_cube, weight_out, weight_out, weight_out), check_vma=False)
```

```python
import functools

import jax
import jax.numpy as jnp
from jax import lax
from jax.experimental import pallas as pl
from jax.experimental.pallas import tpu as pltpu
from jax.sharding import PartitionSpec as P

NEG = -1e30
MESH = pl.DeviceIdType.MESH
VMEM = pltpu.VMEM
F32 = jnp.float32
BF16 = jnp.bfloat16
VMEM_LIMIT = 67_000_000
SUB = 8
LANES = 128
GROUPS = 4
BLOCK = 32
CORES = 2
RING = 4


def vspec():
    return pl.BlockSpec(memory_space=pltpu.VMEM)


def in_hbm(x):
    return pltpu.with_memory_space_constraint(x, pltpu.HBM)


def sspec():
    return pl.BlockSpec(memory_space=pltpu.SMEM)


def exchange_kernel(n_seq, flen_ref, llen_ref, enc_ref, pred_ref, w_enc_ref, w_pred_ref, w_out_ref,
                    order_ref, place_ref, frames_ref, a_ref, c_ref, w_out_t_ref,
                    key_ref, sorted_ref, own_pred_ref, send_sem, recv_sem):
    seq = lax.axis_index("seq")
    n_utt = enc_ref.shape[0]
    n_own = n_utt // n_seq
    barrier = pltpu.get_barrier_semaphore()
    for hop in range(1, n_seq):
        pl.semaphore_signal(barrier, inc=1, device_id={"seq": lax.rem(seq + hop, n_seq)}, device_id_type=MESH)

    def set_key(i, carry):
        key_ref[i] = ((flen_ref[i] + SUB - 1) // SUB) * ((llen_ref[i] + SUB) // SUB) * n_utt + i
        return carry

    def set_place(i, carry):
        key = key_ref[i]
        rank = jnp.int32(0)
        for j in range(n_utt):
            rank = rank + jnp.where(key_ref[j] > key, 1, 0)
        deal = rank // n_seq
        at = rank - deal * n_seq
        at = jnp.where(deal % 2 == 0, at, n_seq - 1 - at)
        place_ref[i] = at * n_own + deal
        return carry

    def set_order(k, carry):
        utt = jnp.int32(0)
        for j in range(n_utt):
            utt = utt + jnp.where(place_ref[j] == k, j, 0)
        order_ref[k] = utt
        return carry

    lax.fori_loop(0, n_utt, set_key, 0)
    lax.fori_loop(0, n_utt, set_place, 0)
    lax.fori_loop(0, n_utt, set_order, 0)
    for k in range(n_utt):
        sorted_ref[k] = enc_ref[order_ref[k]]
    pl.semaphore_wait(barrier, n_seq - 1)
    copies = []
    for hop in range(1, n_seq):
        peer = lax.rem(seq + hop, n_seq)
        copy = pltpu.make_async_remote_copy(
            src_ref=sorted_ref.at[pl.ds(peer * n_own, n_own)],
            dst_ref=frames_ref.at[seq],
            send_sem=send_sem.at[hop - 1],
            recv_sem=recv_sem.at[hop - 1],
            device_id={"seq": peer},
            device_id_type=MESH,
        )
        copy.start()
        copies.append(copy)
    frames_ref[pl.ds(seq, 1)] = sorted_ref[pl.ds(seq * n_own, n_own)][None]
    for j in range(n_own):
        own_pred_ref[j] = pred_ref[order_ref[seq * n_own + j]]
    own_pred = own_pred_ref[...]
    c_ref[...] = jnp.dot(own_pred.reshape(-1, own_pred.shape[-1]), w_pred_ref[...], preferred_element_type=F32).astype(BF16).astype(F32)
    w_out_t_ref[...] = w_out_ref[...].T
    for copy in copies:
        copy.wait()
    frames = frames_ref[...]
    a_ref[...] = jnp.dot(frames.reshape(-1, frames.shape[-1]), w_enc_ref[...], preferred_element_type=F32).astype(BF16).astype(F32)


def exchange(n_seq, frame_len, label_len, enc_loc, pred_loc, w_enc, w_pred, w_out):
    n_utt, t_loc, width = enc_loc.shape
    n_own = n_utt // n_seq
    n_upos = pred_loc.shape[1]
    joint, vocab = w_out.shape
    return pl.pallas_call(
        functools.partial(exchange_kernel, n_seq),
        out_shape=(
            jax.ShapeDtypeStruct((n_utt,), jnp.int32),
            jax.ShapeDtypeStruct((n_utt,), jnp.int32),
            jax.ShapeDtypeStruct((n_seq, n_own, t_loc, width), BF16),
            jax.ShapeDtypeStruct((n_seq * n_own * t_loc, joint), F32),
            jax.ShapeDtypeStruct((n_own * n_upos, joint), F32),
            jax.ShapeDtypeStruct((vocab, joint), BF16),
        ),
        in_specs=[sspec()] * 2 + [vspec()] * 5,
        out_specs=(sspec(),) * 2 + (vspec(),) * 4,
        scratch_shapes=[
            pltpu.SMEM((n_utt,), jnp.int32),
            VMEM(enc_loc.shape, BF16),
            VMEM((n_own, n_upos, width), BF16),
            pltpu.SemaphoreType.DMA((n_seq - 1,)),
            pltpu.SemaphoreType.DMA((n_seq - 1,)),
        ],
        compiler_params=pltpu.CompilerParams(collective_id=0, has_side_effects=True, vmem_limit_bytes=VMEM_LIMIT),
        name="exchange",
    )(frame_len, label_len, enc_loc, pred_loc, w_enc, w_pred, w_out)


def logaddexp(x, y):
    top = jnp.maximum(x, y)
    return top + jnp.log(1.0 + jnp.exp(-jnp.abs(x - y)))


def lattice_kernel(n_own, n_frames, n_upos, seq_ref, order_ref, flen_ref, llen_ref, labels_ref, a_ref, c_ref, w_ref, wt_ref,
                   da_ref, dc_ref, gw_ref, loss_ref,
                   e_ref, h_ref, blank_ref, label_ref, alpha_ref, beta_ref, ids_ref, dact_ref, dpred_ref, work0, work1, dz0, dz1):
    vocab = w_ref.shape[1]
    joint = w_ref.shape[0]
    n_vt = vocab // LANES
    rows_g = SUB * SUB
    rows_t = GROUPS * rows_g
    n_diag = n_frames + n_upos - 1
    first = seq_ref[0] * n_own
    utts = [order_ref[first + b] for b in range(n_own)]
    lens_t = [flen_ref[utt] for utt in utts]
    lens_u = [llen_ref[utt] for utt in utts]
    blocks_t = [lax.div(n + SUB - 1, SUB) for n in lens_t]
    blocks_u = [lax.div(n + SUB, SUB) for n in lens_u]
    starts = [jnp.int32(0)]
    for b in range(n_own):
        starts.append(starts[-1] + blocks_t[b] * blocks_u[b])
    total = starts[-1]
    n_tiles = lax.div(total + GROUPS - 1, GROUPS)

    def decode(n):
        n = jnp.minimum(n, total - 1)
        b = jnp.int32(0)
        base, width = starts[0], blocks_u[0]
        for k in range(1, n_own):
            past = n >= starts[k]
            b = jnp.where(past, k, b)
            base = jnp.where(past, starts[k], base)
            width = jnp.where(past, blocks_u[k], width)
        ti = lax.div(n - base, width)
        return n, b, ti, n - base - ti * width

    pos_col = lax.broadcasted_iota(jnp.int32, (n_upos, n_upos - 1), 0)
    pos_row = lax.broadcasted_iota(jnp.int32, (n_upos, n_upos - 1), 1)
    for b in range(n_own):
        row = labels_ref[pl.ds(utts[b], 1), :].astype(F32)
        col = jnp.sum(jnp.where(pos_col == pos_row, row, 0.0), axis=1, keepdims=True)
        ids_ref[pl.ds(b * n_upos, n_upos), :] = jnp.broadcast_to(col, (n_upos, LANES)).astype(jnp.int32)

    blank_ref[...] = jnp.zeros_like(blank_ref)
    label_ref[...] = jnp.zeros_like(label_ref)
    gw_ref[...] = jnp.zeros_like(gw_ref)
    dact_ref[...] = jnp.zeros_like(dact_ref)
    dpred_ref[...] = jnp.zeros_like(dpred_ref)

    lane = lax.broadcasted_iota(jnp.int32, (SUB, LANES), 1)
    block_lane = lax.broadcasted_iota(jnp.int32, (BLOCK, LANES), 1)
    t_block = BLOCK // SUB
    works, dzs = (work0, work1), (dz0, dz1)

    def tile_rows(i):
        return pl.ds(pl.multiple_of(jnp.clip(i, 0, n_tiles - 1) * rows_t, rows_t), rows_t)

    def tile_groups(i):
        return [decode(jnp.clip(i, 0, n_tiles - 1) * GROUPS + g) for g in range(GROUPS)]

    def pred_row(b, ui):
        return pl.ds(pl.multiple_of(b * n_upos + ui * SUB, SUB), SUB)

    def act_row(b, ti):
        return pl.ds(pl.multiple_of((ti * n_own + b) * SUB, SUB), SUB)

    def block_ids(b, ui):
        ids = ids_ref[pred_row(b, ui), :]
        return jnp.broadcast_to(ids[None], (t_block, SUB, LANES)).reshape(BLOCK, LANES)

    def cell_rows(ti, k, ui):
        return pl.ds(pl.multiple_of((n_diag - 1 - ti * SUB - k) * n_upos + ui * SUB, SUB), SUB)

    def make_hidden(i):
        first_row = jnp.clip(i, 0, n_tiles - 1) * rows_t
        for g, (n, b, ti, ui) in enumerate(tile_groups(i)):
            a8 = a_ref[act_row(b, ti), :]
            c8 = c_ref[pred_row(b, ui), :]
            h = jnp.tanh(a8[:, None, :] + c8[None, :, :]).reshape(rows_g, joint).astype(BF16)
            h_ref[pl.ds(pl.multiple_of(first_row + g * rows_g, rows_g), rows_g), :] = h

    def make_logits(i, z_ref):
        z_ref[...] = jnp.dot(h_ref[tile_rows(i), :], w_ref[...], preferred_element_type=F32)

    def make_softmax(i, z_ref):
        first_row = jnp.clip(i, 0, n_tiles - 1) * rows_t
        for g, (n, b, ti, ui) in enumerate(tile_groups(i)):
            ids = block_ids(b, ui)
            for r in range(0, rows_g, BLOCK):
                z = z_ref[g * rows_g + r:g * rows_g + r + BLOCK, :]
                top = jnp.max(z, axis=1, keepdims=True)
                e = jnp.exp(z - top)
                norm = jnp.sum(e, axis=1, keepdims=True)
                e_ref[pl.ds(pl.multiple_of(first_row + g * rows_g + r, BLOCK), BLOCK), :] = e
                log_norm = top + jnp.log(norm)
                picked = jnp.zeros((BLOCK, LANES), F32)
                for v in range(n_vt):
                    picked = picked + jnp.where(block_lane + v * LANES == ids, z[:, v * LANES:(v + 1) * LANES], 0.0)
                label = jnp.sum(picked, axis=1, keepdims=True) - log_norm
                blank = z[:, 0:1] - log_norm
                scale = 1.0 / norm
                rows = [cell_rows(ti, r // SUB + k, ui) for k in range(t_block)]
                old_blank = [blank_ref[at, :] for at in rows]
                old_label = [label_ref[at, :] for at in rows]
                for k, at in enumerate(rows):
                    sl = slice(k * SUB, (k + 1) * SUB)
                    blank_ref[at, :] = jnp.where(lane == b, blank[sl], jnp.where(lane == b + n_own, scale[sl], old_blank[k]))
                    label_ref[at, :] = jnp.where(lane == b, label[sl], old_label[k])

    make_hidden(0)
    make_logits(0, work0)
    make_hidden(1)

    def forward(j, carry):
        for half in range(2):
            i = 2 * j + half
            make_logits(i + 1, works[1 - half])
            make_softmax(i, works[half])
            make_hidden(i + 2)
        return carry

    lax.fori_loop(0, lax.div(n_tiles + 1, 2), forward, 0)

    upos = lax.broadcasted_iota(jnp.int32, (n_upos, LANES), 0)
    utt = lax.broadcasted_iota(jnp.int32, (n_upos, LANES), 1)
    t_end = jnp.ones((n_upos, LANES), jnp.int32)
    u_end = jnp.zeros((n_upos, LANES), jnp.int32)
    for b in range(n_own):
        t_end = jnp.where(utt == b, lens_t[b], t_end)
        u_end = jnp.where(utt == b, lens_u[b], u_end)

    def diagonal(d):
        return pl.ds((n_diag - 1 - d) * n_upos, n_upos, stride=n_upos + 1)

    def down(x):
        return jnp.where(upos == 0, NEG, pltpu.roll(x, 1, 0))

    def up(x):
        return jnp.where(upos == n_upos - 1, NEG, pltpu.roll(x, n_upos - 1, 0))

    def edge(d):
        return jnp.where((d - upos == t_end) & (upos == u_end), 0.0, NEG)

    alpha0 = jnp.where(upos == 0, 0.0, NEG).astype(F32)
    beta0 = edge(n_diag)
    alpha_ref[0] = alpha0
    beta_ref[n_diag] = beta0

    def sweep(k, carry):
        alpha, beta = carry
        d = k + 1
        alpha = logaddexp(alpha + blank_ref[diagonal(k), :], down(alpha + label_ref[diagonal(k), :]))
        alpha = jnp.where(upos <= d, alpha, NEG)
        alpha_ref[d] = alpha
        d = n_diag - 1 - k
        inside = (d - upos < t_end) & (upos <= u_end)
        beta = logaddexp(beta + blank_ref[diagonal(d), :], up(beta) + label_ref[diagonal(d), :])
        beta = jnp.where(inside, beta, edge(d))
        beta_ref[d] = beta
        return alpha, beta

    lax.fori_loop(0, n_diag, sweep, (alpha0, beta0))
    log_prob = beta_ref[0][0:1, :]
    loss_ref[...] = jnp.broadcast_to(-log_prob, (SUB, LANES))

    def occupancy(d, carry):
        t = d - upos
        alpha = alpha_ref[d]
        after = beta_ref[d + 1]
        cell_ok = (t >= 0) & (t < t_end) & (upos <= u_end)
        blank = blank_ref[diagonal(d), :]
        q0 = jnp.where(cell_ok, jnp.exp(alpha + blank + after - log_prob), 0.0)
        q1 = jnp.where(cell_ok & (upos < u_end), jnp.exp(alpha + label_ref[diagonal(d), :] + up(after) - log_prob), 0.0)
        blank_ref[diagonal(d), :] = jnp.where(utt < n_own, q0, blank)
        label_ref[diagonal(d), :] = q1
        return carry

    lax.fori_loop(0, n_diag, occupancy, 0)

    def make_dz(i, dz_ref):
        first_row = jnp.clip(i, 0, n_tiles - 1) * rows_t
        for g, (n, b, ti, ui) in enumerate(tile_groups(i)):
            keep = (lane == b) & (i * GROUPS + g < total)
            ids = block_ids(b, ui)
            for r in range(0, rows_g, BLOCK):
                q0s, q1s, scales = [], [], []
                for k in range(t_block):
                    at = cell_rows(ti, r // SUB + k, ui)
                    blank = blank_ref[at, :]
                    q0s.append(jnp.where(keep, blank, 0.0))
                    scales.append(jnp.where(lane == b + n_own, blank, 0.0))
                    q1s.append(jnp.where(keep, label_ref[at, :], 0.0))
                q0 = jnp.sum(jnp.concatenate(q0s, axis=0), axis=1, keepdims=True)
                q1 = jnp.sum(jnp.concatenate(q1s, axis=0), axis=1, keepdims=True)
                scale = jnp.sum(jnp.concatenate(scales, axis=0), axis=1, keepdims=True) * (q0 + q1)
                rows = pl.ds(pl.multiple_of(first_row + g * rows_g + r, BLOCK), BLOCK)
                for v in range(n_vt):
                    at_v = block_lane + v * LANES
                    dz = e_ref[rows, v * LANES:(v + 1) * LANES] * scale
                    if v == 0:
                        dz = dz - jnp.where(at_v == 0, q0, 0.0)
                    dz = dz - jnp.where(at_v == ids, q1, 0.0)
                    dz_ref[g * rows_g + r:g * rows_g + r + BLOCK, v * LANES:(v + 1) * LANES] = dz.astype(BF16)

    def make_products(i, dz_ref, dh_ref):
        dz = dz_ref[...]
        dh_ref[:, :joint] = jnp.dot(dz, wt_ref[...], preferred_element_type=F32)
        h = h_ref[tile_rows(i), :]
        for v in range(0, n_vt, 2):
            part = lax.dot_general(h, dz[:, v * LANES:(v + 2) * LANES], (((0,), (0,)), ((), ())), preferred_element_type=F32)
            gw_ref[v] += part[:, :LANES]
            gw_ref[v + 1] += part[:, LANES:]

    def make_sums(i, dh_ref):
        first_row = jnp.clip(i, 0, n_tiles - 1) * rows_t
        for g, (n, b, ti, ui) in enumerate(tile_groups(i)):
            rows = pl.ds(pl.multiple_of(first_row + g * rows_g, rows_g), rows_g)
            for v in range(joint // LANES):
                cols = slice(v * LANES, (v + 1) * LANES)
                h = h_ref[rows, cols].astype(F32)
                ds = dh_ref[g * rows_g:(g + 1) * rows_g, cols] * (1.0 - h * h)
                cube = ds.reshape(SUB, SUB, LANES)
                dact_ref[act_row(b, ti), cols] += jnp.sum(cube, axis=1)
                dpred_ref[pred_row(b, ui), cols] += jnp.sum(cube, axis=0)

    work1[...] = jnp.zeros_like(work1)
    make_dz(0, dz0)

    def backward(j, carry):
        for half in range(2):
            i = 2 * j + half
            make_products(i, dzs[half], works[half])
            make_dz(i + 1, dzs[1 - half])
            make_sums(i - 1, works[1 - half])
        return carry

    lax.fori_loop(0, lax.div(n_tiles + 2, 2), backward, 0)
    da_ref[...] = dact_ref[...].astype(BF16)
    dc_ref[...] = dpred_ref[...].astype(BF16)


def lattice(n_seq, seq_idx, order, frame_len, label_len, labels, act, pred, w_out, w_out_t, n_upos, t_loc):
    n_own = frame_len.shape[0] // n_seq
    n_frames = n_seq * t_loc
    joint, vocab = w_out.shape
    cells = n_own * n_frames * n_upos
    n_diag = n_frames + n_upos - 1
    lat_rows = (n_diag + n_upos - 1) * n_upos
    return pl.pallas_call(
        functools.partial(lattice_kernel, n_own, n_frames, n_upos),
        out_shape=(
            jax.ShapeDtypeStruct(act.shape, BF16),
            jax.ShapeDtypeStruct(pred.shape, BF16),
            jax.ShapeDtypeStruct((vocab // LANES, joint, LANES), F32),
            jax.ShapeDtypeStruct((SUB, LANES), F32),
        ),
        in_specs=[sspec()] * 4 + [vspec()] * 5,
        out_specs=(vspec(),) * 4,
        scratch_shapes=[
            VMEM((cells, vocab), F32),
            VMEM((cells, joint), BF16),
            VMEM((lat_rows, LANES), F32),
            VMEM((lat_rows, LANES), F32),
            VMEM((n_diag + 1, n_upos, LANES), F32),
            VMEM((n_diag + 1, n_upos, LANES), F32),
            VMEM((n_own * n_upos, LANES), jnp.int32),
            VMEM(act.shape, F32),
            VMEM(pred.shape, F32),
            VMEM((GROUPS * SUB * SUB, vocab), F32),
            VMEM((GROUPS * SUB * SUB, vocab), F32),
            VMEM((GROUPS * SUB * SUB, vocab), BF16),
            VMEM((GROUPS * SUB * SUB, vocab), BF16),
        ],
        compiler_params=pltpu.CompilerParams(vmem_limit_bytes=VMEM_LIMIT),
        name="lattice",
    )(seq_idx, order, frame_len, label_len, labels, act, pred, w_out, w_out_t)


class Copies:
    def __init__(self, send_sem, recv_sem):
        self.sems = (send_sem, recv_sem)
        self.all = []

    def start(self, src, dst, device):
        k = len(self.all)
        copy = pltpu.make_async_remote_copy(src_ref=src, dst_ref=dst, send_sem=self.sems[0].at[k], recv_sem=self.sems[1].at[k], device_id=device, device_id_type=MESH)
        copy.start()
        self.all.append(copy)
        return copy

    def drain(self):
        for copy in self.all:
            copy.wait_send()


class Ring:
    def __init__(self, me, right, left):
        self.me, self.right, self.left = me, right, left
        self.nxt, self.prv, self.opp = lax.rem(me + 1, RING), lax.rem(me + RING - 1, RING), lax.rem(me + 2, RING)


class Reduce:
    def __init__(self, copies, ring, acc, bufs):
        self.copies, self.ring, self.acc = copies, ring, acc
        self.pair, self.from_left, self.from_right = bufs

    def begin(self):
        c, r, acc = self.copies, self.ring, self.acc
        self.a1 = c.start(acc(r.opp, 0), self.pair.at[0], r.right)
        self.b1 = c.start(acc(r.opp, 1), self.pair.at[1], r.left)
        self.b2 = c.start(acc(r.nxt, 1), self.from_left.at[1], r.right)
        self.a2 = c.start(acc(r.prv, 0), self.from_right.at[0], r.left)

    def middle(self):
        c, r, acc = self.copies, self.ring, self.acc
        self.a1.wait_recv()
        add = acc(r.nxt, 0)
        add[...] = add[...] + self.pair[0]
        self.a3 = c.start(add, self.from_left.at[0], r.right)
        self.b1.wait_recv()
        add = acc(r.prv, 1)
        add[...] = add[...] + self.pair[1]
        self.b3 = c.start(add, self.from_right.at[1], r.left)

    def end(self, target):
        for copy in (self.b2, self.a3, self.a2, self.b3):
            copy.wait_recv()
        for half in range(2):
            target(half)[...] = self.acc(self.ring.me, half)[...] + self.from_left[half] + self.from_right[half]


class Gather:
    def __init__(self, copies, ring, out):
        self.copies, self.ring, self.out = copies, ring, out

    def send(self, k, half, device):
        return self.copies.start(self.out(k, half), self.out(k, half), device)

    def begin(self):
        r = self.ring
        self.ra = self.send(r.me, 0, r.right)
        self.lb = self.send(r.me, 1, r.left)
        self.rb = self.send(r.me, 1, r.right)
        self.la = self.send(r.me, 0, r.left)

    def relay(self):
        r = self.ring
        self.ra.wait_recv()
        self.ra2 = self.send(r.prv, 0, r.right)
        self.lb.wait_recv()
        self.lb2 = self.send(r.nxt, 1, r.left)
        self.rb.wait_recv()
        self.la.wait_recv()

    def finish(self):
        self.ra2.wait_recv()
        self.lb2.wait_recv()


def rows_of(start, size):
    return pl.ds(pl.multiple_of(start, SUB), size)


def combine_kernel(n_seq, *refs):
    sources, refs = refs[:8], refs[8:]
    outs, refs = refs[:6], refs[6:]
    landed, load_sem, scratch = refs[:8], refs[8], refs[9:]
    loads = [pltpu.make_async_copy(src, dst, load_sem.at[k]) for k, (src, dst) in enumerate(zip(sources, landed))]
    for k in (6, 4, 1, 5, 3, 2, 0, 7):
        loads[k].start()
    combine_body(n_seq, loads, *landed, *outs, *scratch)


def combine_body(n_seq, loads, order_ref, frames_ref, pred_ref, w_enc_ref, da_ref, dc_ref, gw_ref, loss_ref,
                   ge_out, dc_out, gwe_out, gwp_out, gwo_out, loss_out, *scratch):
    (enc_acc, enc_pair, enc_mid, enc_y, enc_x, outs_acc, outs_pair, outs_mid, outs_1, outs_2, pred_acc, pred_y, rows_ref, ge_ref, send_sem, recv_sem) = unflatten(scratch)
    seq = lax.axis_index("seq")
    y = lax.axis_index("data")
    x = lax.div(seq, CORES)
    core = lax.rem(seq, CORES)
    mate = {"seq": x * CORES + 1 - core}
    ring_x = Ring(x, {"seq": lax.rem(x + 1, RING) * CORES + core}, {"seq": lax.rem(x + RING - 1, RING) * CORES + core})
    ring_y = Ring(y, {"data": lax.rem(y + 1, RING)}, {"data": lax.rem(y + RING - 1, RING)})
    barrier = pltpu.get_barrier_semaphore()
    for hop in range(1, n_seq):
        pl.semaphore_signal(barrier, inc=1, device_id={"seq": lax.rem(seq + hop, n_seq)}, device_id_type=MESH)
    for dev in (ring_y.right, ring_y.left):
        pl.semaphore_signal(barrier, inc=1, device_id=dev, device_id_type=MESH)

    n_blk = gw_ref.shape[0] // 2
    n_utt = n_seq * frames_ref.shape[1]
    n_upos = pred_ref.shape[1]
    enc_half = enc_acc.shape[0] // CORES
    out_half = gw_ref.shape[1] // CORES
    enc_q, out_q = enc_half // RING, out_half // RING
    enc_s = enc_q // RING
    enc_row, out_row = core * enc_half, core * out_half
    contract_rows = (((0,), (0,)), ((), ()))

    for k in (6, 4, 1):
        loads[k].wait()
    frames = frames_ref[...]
    enc_acc[...] = lax.dot_general(frames.reshape(-1, frames.shape[-1]), da_ref[...], contract_rows, preferred_element_type=F32)
    loads[5].wait()
    dc_out[pl.ds(seq, 1)] = dc_ref[...][None]
    pl.semaphore_wait(barrier, n_seq - 1 + 2)

    copies = Copies(send_sem, recv_sem)

    def swap_out(part):
        blocks = pl.ds(part * n_blk, n_blk)
        return copies.start(gw_ref.at[blocks, rows_of((1 - core) * out_half, out_half), :], outs_pair[part], mate)

    dc_half = dc_out.shape[1] // 2
    dc_gather = Gather(copies, ring_x, lambda k, half: dc_out.at[k * CORES + core, pl.ds(half * dc_half, dc_half), :])
    swap_1 = swap_out(1)
    swap_enc = copies.start(enc_acc.at[rows_of((1 - core) * enc_half, enc_half), :], enc_pair, mate)
    dc_gather.begin()
    dc_mate = [copies.start(dc_out.at[seq], dc_out.at[seq], mate)]
    swap_0 = swap_out(0)

    def dc_pass(k):
        dc_mate.append(copies.start(dc_out.at[k * CORES + core], dc_out.at[k * CORES + core], mate))

    def add_out(part):
        outs_acc[part][...] = gw_ref[pl.ds(part * n_blk, n_blk), rows_of(out_row, out_half), :] + outs_pair[part][...]

    def out_first(part):
        return lambda k, half: outs_acc[part].at[:, rows_of(k * out_q + half * (out_q // 2), out_q // 2), :]

    def out_second(part):
        return lambda k, half: outs_mid[part].at[k, pl.ds(half * (out_q // 2), out_q // 2), :]

    rings = ((ring_x, ring_y), (ring_y, ring_x))
    first = [Reduce(copies, rings[part][0], out_first(part), outs_1[part]) for part in range(2)]
    second = [Reduce(copies, rings[part][1], out_second(part), outs_2[part]) for part in range(2)]
    enc_first = Reduce(copies, ring_y, lambda k, half: enc_acc.at[rows_of(enc_row + k * enc_q + half * (enc_q // 2), enc_q // 2), :], enc_y)
    enc_second = Reduce(copies, ring_x, lambda k, half: enc_mid.at[rows_of(k * enc_s + half * (enc_s // 2), enc_s // 2), :], enc_x)
    pred_first = Reduce(copies, ring_y, lambda k, half: pred_acc.at[rows_of(k * enc_s + half * (enc_s // 2), enc_s // 2), :], pred_y)

    def out_place(part, k1, k2, half, whole=False):
        start, size = out_row + k1 * out_q, out_q
        if not whole:
            start, size = start + half * (out_q // 2), out_q // 2
        return gwo_out.at[part * n_blk + k2 if k2 is not None else pl.ds(part * n_blk, n_blk), rows_of(start, size), :]

    def pair_place(part):
        ring1, ring2 = rings[part]
        return (
            Gather(copies, ring2, lambda k, half: out_place(part, ring1.me, k, half)),
            Gather(copies, ring1, lambda k, half: out_place(part, k, None, half)),
        )

    a_g1, a_g2 = pair_place(0)
    b_g1, b_g2 = pair_place(1)
    enc_at = lambda ky, kx, half: gwe_out.at[rows_of(enc_row + ky * enc_q + kx * enc_s + half * (enc_s // 2), enc_s // 2), :]
    enc_g1 = Gather(copies, ring_x, lambda k, half: enc_at(y, k, half))
    enc_g2 = Gather(copies, ring_y, lambda k, half: gwe_out.at[rows_of(enc_row + k * enc_q + half * (enc_q // 2), enc_q // 2), :])
    pred_at = lambda ky, half: gwp_out.at[x, core, rows_of(ky * enc_s + half * (enc_s // 2), enc_s // 2), :]
    pred_g1 = Gather(copies, ring_y, pred_at)
    pred_g2 = Gather(copies, ring_x, lambda k, half: gwp_out.at[k, core, pl.ds(half * (enc_q // 2), enc_q // 2), :])

    last = []

    def pass_on(ref):
        last.append(copies.start(ref, ref, mate))

    a_whole = lambda k: out_place(0, k, None, 0, True)
    b_whole = lambda k: out_place(1, k, None, 0, True)
    enc_whole = lambda k: gwe_out.at[rows_of(enc_row + k * enc_q, enc_q), :]
    pred_whole = lambda k: gwp_out.at[k, core]

    def widen(g1, g2, whole):
        g1.finish()
        g2.begin()
        pass_on(whole(g2.ring.me))

    def relay(g2, whole):
        g2.relay()
        pass_on(whole(g2.ring.prv))
        pass_on(whole(g2.ring.nxt))

    def close(g2, whole):
        g2.finish()
        pass_on(whole(g2.ring.opp))

    swap_1.wait_recv()
    add_out(1)
    first[1].begin()
    swap_enc.wait_recv()
    enc_acc[rows_of(enc_row, enc_half), :] = enc_acc[rows_of(enc_row, enc_half), :] + enc_pair[...]
    dc_gather.relay()
    swap_0.wait_recv()
    add_out(0)
    first[0].begin()
    first[1].middle()
    enc_first.begin()
    dc_pass(ring_x.prv)
    dc_pass(ring_x.nxt)

    loads[3].wait()
    ge = lax.dot_general(da_ref[...], w_enc_ref[...], (((1,), (1,)), ((), ())), preferred_element_type=F32)
    ge_ref[...] = ge.astype(BF16).reshape(ge_ref.shape)
    ge_out[pl.ds(seq, 1)] = ge_ref[pl.ds(seq, 1)]
    loads[2].wait()
    loads[0].wait()
    for k in range(n_utt):
        rows_ref[k * n_upos:(k + 1) * n_upos, :] = pred_ref[order_ref[k], :, pl.ds(pl.multiple_of(x * LANES, LANES), LANES)]
    dc_gather.finish()
    dc_pass(ring_x.opp)
    first[1].end(lambda half: outs_mid[1].at[:, pl.ds(half * (out_q // 2), out_q // 2), :])
    first[0].middle()
    second[1].begin()

    for copy in dc_mate:
        copy.wait_recv()
    pred_part = lax.dot_general(rows_ref[...], dc_out[...].reshape(n_utt * n_upos, -1), contract_rows, preferred_element_type=F32)
    pred_acc[...] = jnp.where(core == 0, pred_part[:enc_q], pred_part[enc_q:])
    enc_first.middle()
    pred_first.begin()
    second[1].middle()
    first[0].end(lambda half: outs_mid[0].at[:, pl.ds(half * (out_q // 2), out_q // 2), :])
    second[0].begin()
    second[1].end(lambda half: out_place(1, y, x, half))
    b_g1.begin()
    enc_first.end(lambda half: enc_mid.at[pl.ds(half * (enc_q // 2), enc_q // 2), :])
    enc_second.begin()
    pred_first.middle()
    second[0].middle()
    b_g1.relay()
    enc_second.middle()
    loads[7].wait()
    loss_out[pl.ds(seq, 1)] = loss_ref[...][None]
    small = []
    for hop in range(1, n_seq):
        peer = lax.rem(seq + hop, n_seq)
        small.append(copies.start(ge_ref.at[peer], ge_out.at[seq], {"seq": peer}))
    for hop in range(1, n_seq):
        peer = lax.rem(seq + hop, n_seq)
        small.append(copies.start(loss_ref, loss_out.at[seq], {"seq": peer}))
    widen(b_g1, b_g2, b_whole)
    second[0].end(lambda half: out_place(0, x, y, half))
    a_g1.begin()
    pred_first.end(lambda half: pred_at(y, half))
    pred_g1.begin()
    enc_second.end(lambda half: enc_at(y, x, half))
    enc_g1.begin()
    a_g1.relay()
    pred_g1.relay()
    enc_g1.relay()
    widen(a_g1, a_g2, a_whole)
    relay(b_g2, b_whole)
    widen(enc_g1, enc_g2, enc_whole)
    relay(a_g2, a_whole)
    widen(pred_g1, pred_g2, pred_whole)
    close(b_g2, b_whole)
    relay(enc_g2, enc_whole)
    relay(pred_g2, pred_whole)
    close(a_g2, a_whole)
    close(enc_g2, enc_whole)
    close(pred_g2, pred_whole)
    for copy in small + last:
        copy.wait_recv()
    copies.drain()


N_COPIES = 3 + 10 + 14 + 6 * 7 + 6 * 8 + 16


def unflatten(refs):
    refs = list(refs)
    take = lambda n: [refs.pop(0) for _ in range(n)]
    enc_acc, enc_pair, enc_mid = take(3)
    enc_y, enc_x = take(3), take(3)
    outs = [(take(1)[0], take(1)[0], take(1)[0], take(3), take(3)) for _ in range(2)]
    outs_acc, outs_pair, outs_mid, outs_1, outs_2 = zip(*outs)
    pred_acc = refs.pop(0)
    pred_y = take(3)
    return (enc_acc, enc_pair, enc_mid, enc_y, enc_x, outs_acc, outs_pair, outs_mid, outs_1, outs_2, pred_acc, pred_y, *refs)


def combine(n_seq, order, frames, pred_loc, w_enc, da, dc, gw, loss):
    width = frames.shape[-1]
    n_utt, n_upos, _ = pred_loc.shape
    joint = da.shape[-1]
    n_blk = gw.shape[0] // 2
    enc_half, out_half = width // CORES, joint // CORES
    enc_q, out_q = enc_half // RING, out_half // RING
    enc_s = enc_q // RING
    ring = lambda *shape: [VMEM(shape, F32)] * 3
    outs = [VMEM((n_blk, out_half, LANES), F32)] * 2 + [VMEM((n_blk, out_q, LANES), F32)] + ring(2, n_blk, out_q // 2, LANES) + ring(2, out_q // 2, LANES)
    return pl.pallas_call(
        functools.partial(combine_kernel, n_seq),
        out_shape=(
            VMEM(frames.shape, BF16),
            VMEM((n_seq,) + dc.shape, BF16),
            VMEM((width, joint), F32),
            VMEM((RING, CORES, enc_q, joint), F32),
            VMEM(gw.shape, F32),
            VMEM((n_seq,) + loss.shape, F32),
        ),
        in_specs=[pl.BlockSpec(memory_space=pltpu.HBM)] * 8,
        out_specs=(vspec(),) * 6,
        scratch_shapes=[pltpu.SMEM(order.shape, jnp.int32)]
        + [VMEM(v.shape, v.dtype) for v in (frames, pred_loc, w_enc, da, dc, gw, loss)]
        + [pltpu.SemaphoreType.DMA((8,))]
        + [VMEM((width, joint), F32), VMEM((enc_half, joint), F32), VMEM((enc_q, joint), F32)]
        + ring(2, enc_q // 2, joint)
        + ring(2, enc_s // 2, joint)
        + outs
        + outs
        + [VMEM((enc_q, joint), F32)]
        + ring(2, enc_s // 2, joint)
        + [
            VMEM((n_utt * n_upos, LANES), BF16),
            VMEM(frames.shape, BF16),
            pltpu.SemaphoreType.DMA((N_COPIES,)),
            pltpu.SemaphoreType.DMA((N_COPIES,)),
        ],
        compiler_params=pltpu.CompilerParams(collective_id=1, has_side_effects=True, vmem_limit_bytes=48_000_000),
        name="combine",
    )(*(in_hbm(v) for v in (order, frames, pred_loc, w_enc, da, dc, gw, loss)))


def output_kernel(place_hbm, w_pred_hbm, losses_ref, ge_ref, dc_ref, gwe_ref, gwp_ref, gw_ref,
                  loss_out, ge_out, gp_out, gwe_out, gwp_out, gwo_out, rows_ref, gp_ref, place_ref, w_pred_ref, sem, load_sem):
    n_utt, n_upos, width = gp_out.shape
    n_own = ge_ref.shape[1]
    n_cols, _, col = gw_ref.shape
    loads = [pltpu.make_async_copy(place_hbm, place_ref, load_sem.at[0]), pltpu.make_async_copy(w_pred_hbm, w_pred_ref, load_sem.at[1])]
    for copy in loads:
        copy.start()
    copies = [pltpu.make_async_copy(gwe_ref, gwe_out, sem.at[0])]
    blocks, cores, size, _ = gwp_ref.shape
    for k in range(blocks * cores):
        copies.append(pltpu.make_async_copy(gwp_ref.at[k // cores, k % cores], gwp_out.at[pl.ds(k * size, size), :], sem.at[2 + n_cols + 4 + k]))
    for k in range(n_cols):
        copies.append(pltpu.make_async_copy(gw_ref.at[k], gwo_out.at[:, pl.ds(k * col, col)], sem.at[2 + k]))
    for copy in copies:
        copy.start()
    for copy in loads:
        copy.wait()
    n_parts = 4
    part = n_utt // n_parts
    for p in range(n_parts):
        for i in range(p * part, (p + 1) * part):
            place = place_ref[i]
            dev = place // n_own
            own = place - dev * n_own
            loss_out[i] = losses_ref[dev, 0, own]
            ge_out[i] = ge_ref[dev, own]
            rows_ref[i] = dc_ref[dev, pl.ds(pl.multiple_of(own * n_upos, n_upos), n_upos), :]
        rows = rows_ref[p * part:(p + 1) * part]
        grads = lax.dot_general(rows.reshape(part * n_upos, -1), w_pred_ref[...], (((1,), (1,)), ((), ())), preferred_element_type=F32)
        gp_ref[p * part:(p + 1) * part] = grads.reshape(part, n_upos, width)
        copy = pltpu.make_async_copy(gp_ref.at[pl.ds(p * part, part)], gp_out.at[pl.ds(p * part, part)], sem.at[2 + n_cols + p])
        copy.start()
        copies.append(copy)
    for copy in copies:
        copy.wait()


def outputs(place, losses, ge, dc, w_pred, gwe, gwp, gw, n_upos):
    n_seq, n_own, t_loc, width = ge.shape
    n_utt = n_seq * n_own
    n_cols, joint, col = gw.shape
    return pl.pallas_call(
        output_kernel,
        out_shape=(
            jax.ShapeDtypeStruct((n_utt,), F32),
            jax.ShapeDtypeStruct((n_utt, t_loc, width), BF16),
            jax.ShapeDtypeStruct((n_utt, n_upos, width), F32),
            jax.ShapeDtypeStruct((width, joint), F32),
            jax.ShapeDtypeStruct((width, joint), F32),
            jax.ShapeDtypeStruct((joint, n_cols * col), F32),
        ),
        in_specs=[pl.BlockSpec(memory_space=pltpu.HBM)] * 2 + [sspec()] + [vspec()] * 5,
        out_specs=(sspec(), vspec()) + (pl.BlockSpec(memory_space=pltpu.HBM),) * 4,
        scratch_shapes=[
            VMEM((n_utt, n_upos, joint), BF16),
            VMEM((n_utt, n_upos, width), F32),
            pltpu.SMEM(place.shape, jnp.int32),
            VMEM(w_pred.shape, BF16),
            pltpu.SemaphoreType.DMA((2 + n_cols + 4 + RING * CORES,)),
            pltpu.SemaphoreType.DMA((2,)),
        ],
        compiler_params=pltpu.CompilerParams(vmem_limit_bytes=48_000_000),
        name="outputs",
    )(in_hbm(place), in_hbm(w_pred), losses, ge, dc, gwe, gwp, gw)


def solution(mesh):
    n_seq = mesh.shape["seq"]
    utt_rows = P(("part", "data"))
    utt_mats = P(("part", "data"), None)
    utt_cube = P(("part", "data"), None, None)
    enc_spec = P(("part", "data"), "seq", None)
    weight_in = P(None, None)
    weight_out = P("part", None)

    def body(enc_loc, pred_loc, w_enc, w_pred, w_out, labels, frame_len, label_len):
        t_loc = enc_loc.shape[1]
        n_upos = pred_loc.shape[1]
        seq_idx = lax.axis_index("seq").astype(jnp.int32).reshape(1)
        order, place, frames, act, pred, w_out_t = exchange(n_seq, frame_len, label_len, enc_loc, pred_loc, w_enc, w_pred, w_out)
        da, dc, gw, loss = lattice(n_seq, seq_idx, order, frame_len, label_len, labels, act, pred, w_out, w_out_t, n_upos, t_loc)
        ge, dc_all, gwe, gwp, gw, losses = combine(n_seq, order, frames, pred_loc, w_enc, da, dc, gw, loss)
        loss, grad_enc, grad_pred, gw_enc, gw_pred, gw_out = outputs(place, losses, ge, dc_all, w_pred, gwe, gwp, gw, n_upos)
        return loss, grad_enc, grad_pred, gw_enc, gw_pred, gw_out

    return jax.shard_map(body, mesh=mesh, in_specs=(enc_spec, utt_cube, weight_in, weight_in, weight_in, utt_mats, utt_rows, utt_rows), out_specs=(utt_rows, enc_spec, utt_cube, weight_out, weight_out, weight_out), check_vma=False)
```

```python
import functools

import jax
import jax.numpy as jnp
from jax import lax
from jax.experimental import pallas as pl
from jax.experimental.pallas import tpu as pltpu
from jax.sharding import PartitionSpec as P

NEG = -1e30
MESH = pl.DeviceIdType.MESH
VMEM = pltpu.VMEM
F32 = jnp.float32
BF16 = jnp.bfloat16
VMEM_LIMIT = 67_000_000
SUB = 8
LANES = 128
GROUPS = 4
BLOCK = 32
CORES = 2
RING = 4


def vspec():
    return pl.BlockSpec(memory_space=pltpu.VMEM)


def in_hbm(x):
    return pltpu.with_memory_space_constraint(x, pltpu.HBM)


def sspec():
    return pl.BlockSpec(memory_space=pltpu.SMEM)


def exchange_kernel(n_seq, flen_ref, llen_ref, enc_ref, pred_ref, w_enc_ref, w_pred_ref, w_out_ref,
                    order_ref, place_ref, frames_ref, a_ref, c_ref, w_out_t_ref,
                    key_ref, sorted_ref, own_pred_ref, send_sem, recv_sem):
    seq = lax.axis_index("seq")
    n_utt = enc_ref.shape[0]
    n_own = n_utt // n_seq
    barrier = pltpu.get_barrier_semaphore()
    for hop in range(1, n_seq):
        pl.semaphore_signal(barrier, inc=1, device_id={"seq": lax.rem(seq + hop, n_seq)}, device_id_type=MESH)

    def set_key(i, carry):
        key_ref[i] = ((flen_ref[i] + SUB - 1) // SUB) * ((llen_ref[i] + SUB) // SUB) * n_utt + i
        return carry

    def set_place(i, carry):
        key = key_ref[i]
        rank = jnp.int32(0)
        for j in range(n_utt):
            rank = rank + jnp.where(key_ref[j] > key, 1, 0)
        deal = rank // n_seq
        at = rank - deal * n_seq
        at = jnp.where(deal % 2 == 0, at, n_seq - 1 - at)
        place_ref[i] = at * n_own + deal
        return carry

    def set_order(k, carry):
        utt = jnp.int32(0)
        for j in range(n_utt):
            utt = utt + jnp.where(place_ref[j] == k, j, 0)
        order_ref[k] = utt
        return carry

    lax.fori_loop(0, n_utt, set_key, 0)
    lax.fori_loop(0, n_utt, set_place, 0)
    lax.fori_loop(0, n_utt, set_order, 0)
    for k in range(n_utt):
        sorted_ref[k] = enc_ref[order_ref[k]]
    pl.semaphore_wait(barrier, n_seq - 1)
    copies = []
    for hop in range(1, n_seq):
        peer = lax.rem(seq + hop, n_seq)
        copy = pltpu.make_async_remote_copy(
            src_ref=sorted_ref.at[pl.ds(peer * n_own, n_own)],
            dst_ref=frames_ref.at[seq],
            send_sem=send_sem.at[hop - 1],
            recv_sem=recv_sem.at[hop - 1],
            device_id={"seq": peer},
            device_id_type=MESH,
        )
        copy.start()
        copies.append(copy)
    frames_ref[pl.ds(seq, 1)] = sorted_ref[pl.ds(seq * n_own, n_own)][None]
    for j in range(n_own):
        own_pred_ref[j] = pred_ref[order_ref[seq * n_own + j]]
    own_pred = own_pred_ref[...]
    c_ref[...] = jnp.dot(own_pred.reshape(-1, own_pred.shape[-1]), w_pred_ref[...], preferred_element_type=F32).astype(BF16).astype(F32)
    w_out_t_ref[...] = w_out_ref[...].T
    for copy in copies:
        copy.wait()
    frames = frames_ref[...]
    a_ref[...] = jnp.dot(frames.reshape(-1, frames.shape[-1]), w_enc_ref[...], preferred_element_type=F32).astype(BF16).astype(F32)


def exchange(n_seq, frame_len, label_len, enc_loc, pred_loc, w_enc, w_pred, w_out):
    n_utt, t_loc, width = enc_loc.shape
    n_own = n_utt // n_seq
    n_upos = pred_loc.shape[1]
    joint, vocab = w_out.shape
    return pl.pallas_call(
        functools.partial(exchange_kernel, n_seq),
        out_shape=(
            jax.ShapeDtypeStruct((n_utt,), jnp.int32),
            jax.ShapeDtypeStruct((n_utt,), jnp.int32),
            jax.ShapeDtypeStruct((n_seq, n_own, t_loc, width), BF16),
            jax.ShapeDtypeStruct((n_seq * n_own * t_loc, joint), F32),
            jax.ShapeDtypeStruct((n_own * n_upos, joint), F32),
            jax.ShapeDtypeStruct((vocab, joint), BF16),
        ),
        in_specs=[sspec()] * 2 + [vspec()] * 5,
        out_specs=(sspec(),) * 2 + (vspec(),) * 4,
        scratch_shapes=[
            pltpu.SMEM((n_utt,), jnp.int32),
            VMEM(enc_loc.shape, BF16),
            VMEM((n_own, n_upos, width), BF16),
            pltpu.SemaphoreType.DMA((n_seq - 1,)),
            pltpu.SemaphoreType.DMA((n_seq - 1,)),
        ],
        compiler_params=pltpu.CompilerParams(collective_id=0, has_side_effects=True, vmem_limit_bytes=VMEM_LIMIT),
        name="exchange",
    )(frame_len, label_len, enc_loc, pred_loc, w_enc, w_pred, w_out)


def logaddexp(x, y):
    top = jnp.maximum(x, y)
    return top + jnp.log(1.0 + jnp.exp(-jnp.abs(x - y)))


def lattice_kernel(n_own, n_frames, n_upos, seq_ref, order_ref, flen_ref, llen_ref, labels_ref, a_ref, c_ref, w_ref, wt_ref,
                   da_ref, dc_ref, gw_ref, loss_ref,
                   e_ref, h_ref, blank_ref, label_ref, alpha_ref, beta_ref, ids_ref, dact_ref, dpred_ref, work0, work1, dz0, dz1):
    vocab = w_ref.shape[1]
    joint = w_ref.shape[0]
    n_vt = vocab // LANES
    rows_g = SUB * SUB
    rows_t = GROUPS * rows_g
    n_diag = n_frames + n_upos - 1
    first = seq_ref[0] * n_own
    utts = [order_ref[first + b] for b in range(n_own)]
    lens_t = [flen_ref[utt] for utt in utts]
    lens_u = [llen_ref[utt] for utt in utts]
    blocks_t = [lax.div(n + SUB - 1, SUB) for n in lens_t]
    blocks_u = [lax.div(n + SUB, SUB) for n in lens_u]
    starts = [jnp.int32(0)]
    for b in range(n_own):
        starts.append(starts[-1] + blocks_t[b] * blocks_u[b])
    total = starts[-1]
    n_tiles = lax.div(total + GROUPS - 1, GROUPS)

    def decode(n):
        n = jnp.minimum(n, total - 1)
        b = jnp.int32(0)
        base, width = starts[0], blocks_u[0]
        for k in range(1, n_own):
            past = n >= starts[k]
            b = jnp.where(past, k, b)
            base = jnp.where(past, starts[k], base)
            width = jnp.where(past, blocks_u[k], width)
        ti = lax.div(n - base, width)
        return n, b, ti, n - base - ti * width

    pos_col = lax.broadcasted_iota(jnp.int32, (n_upos, n_upos - 1), 0)
    pos_row = lax.broadcasted_iota(jnp.int32, (n_upos, n_upos - 1), 1)
    for b in range(n_own):
        row = labels_ref[pl.ds(utts[b], 1), :].astype(F32)
        col = jnp.sum(jnp.where(pos_col == pos_row, row, 0.0), axis=1, keepdims=True)
        ids_ref[pl.ds(b * n_upos, n_upos), :] = jnp.broadcast_to(col, (n_upos, LANES)).astype(jnp.int32)

    blank_ref[...] = jnp.zeros_like(blank_ref)
    label_ref[...] = jnp.zeros_like(label_ref)
    gw_ref[...] = jnp.zeros_like(gw_ref)
    dact_ref[...] = jnp.zeros_like(dact_ref)
    dpred_ref[...] = jnp.zeros_like(dpred_ref)

    lane = lax.broadcasted_iota(jnp.int32, (SUB, LANES), 1)
    block_lane = lax.broadcasted_iota(jnp.int32, (BLOCK, LANES), 1)
    t_block = BLOCK // SUB
    works, dzs = (work0, work1), (dz0, dz1)

    def tile_rows(i):
        return pl.ds(pl.multiple_of(jnp.clip(i, 0, n_tiles - 1) * rows_t, rows_t), rows_t)

    def tile_groups(i):
        return [decode(jnp.clip(i, 0, n_tiles - 1) * GROUPS + g) for g in range(GROUPS)]

    def pred_row(b, ui):
        return pl.ds(pl.multiple_of(b * n_upos + ui * SUB, SUB), SUB)

    def act_row(b, ti):
        return pl.ds(pl.multiple_of((ti * n_own + b) * SUB, SUB), SUB)

    def block_ids(b, ui):
        ids = ids_ref[pred_row(b, ui), :]
        return jnp.broadcast_to(ids[None], (t_block, SUB, LANES)).reshape(BLOCK, LANES)

    def cell_rows(ti, k, ui):
        return pl.ds(pl.multiple_of((n_diag - 1 - ti * SUB - k) * n_upos + ui * SUB, SUB), SUB)

    def make_hidden(i):
        first_row = jnp.clip(i, 0, n_tiles - 1) * rows_t
        for g, (n, b, ti, ui) in enumerate(tile_groups(i)):
            a8 = a_ref[act_row(b, ti), :]
            c8 = c_ref[pred_row(b, ui), :]
            h = jnp.tanh(a8[:, None, :] + c8[None, :, :]).reshape(rows_g, joint).astype(BF16)
            h_ref[pl.ds(pl.multiple_of(first_row + g * rows_g, rows_g), rows_g), :] = h

    def make_logits(i, z_ref):
        z_ref[...] = jnp.dot(h_ref[tile_rows(i), :], w_ref[...], preferred_element_type=F32)

    def make_softmax(i, z_ref):
        first_row = jnp.clip(i, 0, n_tiles - 1) * rows_t
        for g, (n, b, ti, ui) in enumerate(tile_groups(i)):
            ids = block_ids(b, ui)
            for r in range(0, rows_g, BLOCK):
                z = z_ref[g * rows_g + r:g * rows_g + r + BLOCK, :]
                top = jnp.max(z, axis=1, keepdims=True)
                e = jnp.exp(z - top)
                norm = jnp.sum(e, axis=1, keepdims=True)
                e_ref[pl.ds(pl.multiple_of(first_row + g * rows_g + r, BLOCK), BLOCK), :] = e
                log_norm = top + jnp.log(norm)
                picked = jnp.zeros((BLOCK, LANES), F32)
                for v in range(n_vt):
                    picked = picked + jnp.where(block_lane + v * LANES == ids, z[:, v * LANES:(v + 1) * LANES], 0.0)
                label = jnp.sum(picked, axis=1, keepdims=True) - log_norm
                blank = z[:, 0:1] - log_norm
                scale = 1.0 / norm
                rows = [cell_rows(ti, r // SUB + k, ui) for k in range(t_block)]
                old_blank = [blank_ref[at, :] for at in rows]
                old_label = [label_ref[at, :] for at in rows]
                for k, at in enumerate(rows):
                    sl = slice(k * SUB, (k + 1) * SUB)
                    blank_ref[at, :] = jnp.where(lane == b, blank[sl], jnp.where(lane == b + n_own, scale[sl], old_blank[k]))
                    label_ref[at, :] = jnp.where(lane == b, label[sl], old_label[k])

    make_hidden(0)
    make_logits(0, work0)
    make_hidden(1)

    def forward(j, carry):
        for half in range(2):
            i = 2 * j + half
            make_logits(i + 1, works[1 - half])
            make_softmax(i, works[half])
            make_hidden(i + 2)
        return carry

    lax.fori_loop(0, lax.div(n_tiles + 1, 2), forward, 0)

    upos = lax.broadcasted_iota(jnp.int32, (n_upos, LANES), 0)
    utt = lax.broadcasted_iota(jnp.int32, (n_upos, LANES), 1)
    t_end = jnp.ones((n_upos, LANES), jnp.int32)
    u_end = jnp.zeros((n_upos, LANES), jnp.int32)
    for b in range(n_own):
        t_end = jnp.where(utt == b, lens_t[b], t_end)
        u_end = jnp.where(utt == b, lens_u[b], u_end)

    def diagonal(d):
        return pl.ds((n_diag - 1 - d) * n_upos, n_upos, stride=n_upos + 1)

    def down(x):
        return jnp.where(upos == 0, NEG, pltpu.roll(x, 1, 0))

    def up(x):
        return jnp.where(upos == n_upos - 1, NEG, pltpu.roll(x, n_upos - 1, 0))

    def edge(d):
        return jnp.where((d - upos == t_end) & (upos == u_end), 0.0, NEG)

    alpha0 = jnp.where(upos == 0, 0.0, NEG).astype(F32)
    beta0 = edge(n_diag)
    alpha_ref[0] = alpha0
    beta_ref[n_diag] = beta0

    def sweep(k, carry):
        alpha, beta = carry
        d = k + 1
        alpha = logaddexp(alpha + blank_ref[diagonal(k), :], down(alpha + label_ref[diagonal(k), :]))
        alpha = jnp.where(upos <= d, alpha, NEG)
        alpha_ref[d] = alpha
        d = n_diag - 1 - k
        inside = (d - upos < t_end) & (upos <= u_end)
        beta = logaddexp(beta + blank_ref[diagonal(d), :], up(beta) + label_ref[diagonal(d), :])
        beta = jnp.where(inside, beta, edge(d))
        beta_ref[d] = beta
        return alpha, beta

    lax.fori_loop(0, n_diag, sweep, (alpha0, beta0))
    log_prob = beta_ref[0][0:1, :]
    loss_ref[...] = jnp.broadcast_to(-log_prob, (SUB, LANES))

    def occupancy(d, carry):
        t = d - upos
        alpha = alpha_ref[d]
        after = beta_ref[d + 1]
        cell_ok = (t >= 0) & (t < t_end) & (upos <= u_end)
        blank = blank_ref[diagonal(d), :]
        q0 = jnp.where(cell_ok, jnp.exp(alpha + blank + after - log_prob), 0.0)
        q1 = jnp.where(cell_ok & (upos < u_end), jnp.exp(alpha + label_ref[diagonal(d), :] + up(after) - log_prob), 0.0)
        blank_ref[diagonal(d), :] = jnp.where(utt < n_own, q0, blank)
        label_ref[diagonal(d), :] = q1
        return carry

    lax.fori_loop(0, n_diag, occupancy, 0)

    def make_dz(i, dz_ref):
        first_row = jnp.clip(i, 0, n_tiles - 1) * rows_t
        for g, (n, b, ti, ui) in enumerate(tile_groups(i)):
            keep = (lane == b) & (i * GROUPS + g < total)
            ids = block_ids(b, ui)
            for r in range(0, rows_g, BLOCK):
                q0s, q1s, scales = [], [], []
                for k in range(t_block):
                    at = cell_rows(ti, r // SUB + k, ui)
                    blank = blank_ref[at, :]
                    q0s.append(jnp.where(keep, blank, 0.0))
                    scales.append(jnp.where(lane == b + n_own, blank, 0.0))
                    q1s.append(jnp.where(keep, label_ref[at, :], 0.0))
                q0 = jnp.sum(jnp.concatenate(q0s, axis=0), axis=1, keepdims=True)
                q1 = jnp.sum(jnp.concatenate(q1s, axis=0), axis=1, keepdims=True)
                scale = jnp.sum(jnp.concatenate(scales, axis=0), axis=1, keepdims=True) * (q0 + q1)
                rows = pl.ds(pl.multiple_of(first_row + g * rows_g + r, BLOCK), BLOCK)
                for v in range(n_vt):
                    at_v = block_lane + v * LANES
                    dz = e_ref[rows, v * LANES:(v + 1) * LANES] * scale
                    if v == 0:
                        dz = dz - jnp.where(at_v == 0, q0, 0.0)
                    dz = dz - jnp.where(at_v == ids, q1, 0.0)
                    dz_ref[g * rows_g + r:g * rows_g + r + BLOCK, v * LANES:(v + 1) * LANES] = dz.astype(BF16)

    def make_products(i, dz_ref, dh_ref):
        dz = dz_ref[...]
        dh_ref[:, :joint] = jnp.dot(dz, wt_ref[...], preferred_element_type=F32)
        h = h_ref[tile_rows(i), :]
        for v in range(0, n_vt, 2):
            part = lax.dot_general(h, dz[:, v * LANES:(v + 2) * LANES], (((0,), (0,)), ((), ())), preferred_element_type=F32)
            gw_ref[v] += part[:, :LANES]
            gw_ref[v + 1] += part[:, LANES:]

    def make_sums(i, dh_ref):
        first_row = jnp.clip(i, 0, n_tiles - 1) * rows_t
        for g, (n, b, ti, ui) in enumerate(tile_groups(i)):
            rows = pl.ds(pl.multiple_of(first_row + g * rows_g, rows_g), rows_g)
            for v in range(joint // LANES):
                cols = slice(v * LANES, (v + 1) * LANES)
                h = h_ref[rows, cols].astype(F32)
                ds = dh_ref[g * rows_g:(g + 1) * rows_g, cols] * (1.0 - h * h)
                cube = ds.reshape(SUB, SUB, LANES)
                dact_ref[act_row(b, ti), cols] += jnp.sum(cube, axis=1)
                dpred_ref[pred_row(b, ui), cols] += jnp.sum(cube, axis=0)

    work1[...] = jnp.zeros_like(work1)
    make_dz(0, dz0)

    def backward(j, carry):
        for half in range(2):
            i = 2 * j + half
            make_products(i, dzs[half], works[half])
            make_dz(i + 1, dzs[1 - half])
            make_sums(i - 1, works[1 - half])
        return carry

    lax.fori_loop(0, lax.div(n_tiles + 2, 2), backward, 0)
    da_ref[...] = dact_ref[...].astype(BF16)
    dc_ref[...] = dpred_ref[...].astype(BF16)


def lattice(n_seq, seq_idx, order, frame_len, label_len, labels, act, pred, w_out, w_out_t, n_upos, t_loc):
    n_own = frame_len.shape[0] // n_seq
    n_frames = n_seq * t_loc
    joint, vocab = w_out.shape
    cells = n_own * n_frames * n_upos
    n_diag = n_frames + n_upos - 1
    lat_rows = (n_diag + n_upos - 1) * n_upos
    return pl.pallas_call(
        functools.partial(lattice_kernel, n_own, n_frames, n_upos),
        out_shape=(
            jax.ShapeDtypeStruct(act.shape, BF16),
            jax.ShapeDtypeStruct(pred.shape, BF16),
            jax.ShapeDtypeStruct((vocab // LANES, joint, LANES), F32),
            jax.ShapeDtypeStruct((SUB, LANES), F32),
        ),
        in_specs=[sspec()] * 4 + [vspec()] * 5,
        out_specs=(vspec(),) * 4,
        scratch_shapes=[
            VMEM((cells, vocab), F32),
            VMEM((cells, joint), BF16),
            VMEM((lat_rows, LANES), F32),
            VMEM((lat_rows, LANES), F32),
            VMEM((n_diag + 1, n_upos, LANES), F32),
            VMEM((n_diag + 1, n_upos, LANES), F32),
            VMEM((n_own * n_upos, LANES), jnp.int32),
            VMEM(act.shape, F32),
            VMEM(pred.shape, F32),
            VMEM((GROUPS * SUB * SUB, vocab), F32),
            VMEM((GROUPS * SUB * SUB, vocab), F32),
            VMEM((GROUPS * SUB * SUB, vocab), BF16),
            VMEM((GROUPS * SUB * SUB, vocab), BF16),
        ],
        compiler_params=pltpu.CompilerParams(vmem_limit_bytes=VMEM_LIMIT),
        name="lattice",
    )(seq_idx, order, frame_len, label_len, labels, act, pred, w_out, w_out_t)


class Copies:
    def __init__(self, send_sem, recv_sem):
        self.sems = (send_sem, recv_sem)
        self.all = []

    def start(self, src, dst, device):
        k = len(self.all)
        copy = pltpu.make_async_remote_copy(src_ref=src, dst_ref=dst, send_sem=self.sems[0].at[k], recv_sem=self.sems[1].at[k], device_id=device, device_id_type=MESH)
        copy.start()
        self.all.append(copy)
        return copy

    def drain(self):
        for copy in self.all:
            copy.wait_send()


class Ring:
    def __init__(self, me, device):
        self.me = me
        self.right, self.left, self.across = [device(lax.rem(me + hop, RING)) for hop in (1, RING - 1, 2)]
        self.nxt, self.prv, self.opp = lax.rem(me + 1, RING), lax.rem(me + RING - 1, RING), lax.rem(me + 2, RING)


class Reduce:
    def __init__(self, copies, ring, acc, bufs):
        self.copies, self.ring, self.acc = copies, ring, acc
        self.pair, self.from_left, self.from_right = bufs

    def begin(self):
        c, r, acc = self.copies, self.ring, self.acc
        self.a1 = c.start(acc(r.opp, 0), self.pair.at[0], r.right)
        self.b1 = c.start(acc(r.opp, 1), self.pair.at[1], r.left)
        self.b2 = c.start(acc(r.nxt, 1), self.from_left.at[1], r.right)
        self.a2 = c.start(acc(r.prv, 0), self.from_right.at[0], r.left)

    def middle(self):
        c, r, acc = self.copies, self.ring, self.acc
        self.a1.wait_recv()
        add = acc(r.nxt, 0)
        add[...] = add[...] + self.pair[0]
        self.a3 = c.start(add, self.from_left.at[0], r.right)
        self.b1.wait_recv()
        add = acc(r.prv, 1)
        add[...] = add[...] + self.pair[1]
        self.b3 = c.start(add, self.from_right.at[1], r.left)

    def end(self, target):
        for copy in (self.b2, self.a3, self.a2, self.b3):
            copy.wait_recv()
        for half in range(2):
            target(half)[...] = self.acc(self.ring.me, half)[...] + self.from_left[half] + self.from_right[half]


class Gather:
    def __init__(self, copies, ring, out):
        self.copies, self.ring, self.out = copies, ring, out

    def send(self, k, half, device):
        return self.copies.start(self.out(k, half), self.out(k, half), device)

    def begin(self):
        r = self.ring
        self.ra = self.send(r.me, 0, r.right)
        self.lb = self.send(r.me, 1, r.left)
        self.rb = self.send(r.me, 1, r.right)
        self.la = self.send(r.me, 0, r.left)

    def relay(self):
        r = self.ring
        self.ra.wait_recv()
        self.ra2 = self.send(r.prv, 0, r.right)
        self.lb.wait_recv()
        self.lb2 = self.send(r.nxt, 1, r.left)
        self.rb.wait_recv()
        self.la.wait_recv()

    def finish(self):
        self.ra2.wait_recv()
        self.lb2.wait_recv()


class Swap:
    def __init__(self, copies, ring, acc, bufs):
        self.copies, self.ring, self.acc, self.bufs = copies, ring, acc, bufs

    def begin(self):
        r = self.ring
        sends = ((r.nxt, r.right), (r.prv, r.left), (r.opp, r.across))
        self.sent = [self.copies.start(self.acc(k), buf, device) for (k, device), buf in zip(sends, self.bufs)]

    def end(self, target):
        for copy in self.sent:
            copy.wait_recv()
        target[...] = (self.acc(self.ring.me)[...] + self.bufs[0][...]) + (self.bufs[1][...] + self.bufs[2][...])


class Spread:
    def __init__(self, copies, ring, out):
        self.copies, self.ring, self.out = copies, ring, out

    def begin(self):
        r = self.ring
        self.sent = [self.copies.start(self.out(r.me), self.out(r.me), device) for device in (r.right, r.left, r.across)]

    def finish(self):
        for copy in self.sent:
            copy.wait_recv()


def rows_of(start, size):
    return pl.ds(pl.multiple_of(start, SUB), size)


def combine_kernel(n_seq, *refs):
    sources, refs = refs[:8], refs[8:]
    outs, refs = refs[:6], refs[6:]
    landed, load_sem, scratch = refs[:8], refs[8], refs[9:]
    loads = [pltpu.make_async_copy(src, dst, load_sem.at[k]) for k, (src, dst) in enumerate(zip(sources, landed))]
    for k in (6, 4, 1, 5, 3, 2, 0, 7):
        loads[k].start()
    combine_body(n_seq, loads, *landed, *outs, *scratch)


def combine_body(n_seq, loads, order_ref, frames_ref, pred_ref, w_enc_ref, da_ref, dc_ref, gw_ref, loss_ref,
                   ge_out, dc_out, gwe_out, gwp_out, gwo_out, loss_out, *scratch):
    (enc_acc, enc_pair, enc_mid, enc_y, enc_x, outs_acc, outs_pair, outs_mid, outs_1, outs_2, pred_acc, pred_y, rows_ref, ge_ref, send_sem, recv_sem) = unflatten(scratch)
    seq = lax.axis_index("seq")
    y = lax.axis_index("data")
    x = lax.div(seq, CORES)
    core = lax.rem(seq, CORES)
    mate = {"seq": x * CORES + 1 - core}
    ring_x = Ring(x, lambda k: {"seq": k * CORES + core})
    ring_y = Ring(y, lambda k: {"data": k})
    barrier = pltpu.get_barrier_semaphore()
    for hop in range(1, n_seq):
        pl.semaphore_signal(barrier, inc=1, device_id={"seq": lax.rem(seq + hop, n_seq)}, device_id_type=MESH)
    for dev in (ring_y.right, ring_y.left, ring_y.across):
        pl.semaphore_signal(barrier, inc=1, device_id=dev, device_id_type=MESH)

    n_blk = gw_ref.shape[0] // 2
    n_utt = n_seq * frames_ref.shape[1]
    n_upos = pred_ref.shape[1]
    enc_half = enc_acc.shape[0] // CORES
    out_half = gw_ref.shape[1] // CORES
    enc_q, out_q = enc_half // RING, out_half // RING
    enc_s = enc_q // RING
    enc_row, out_row = core * enc_half, core * out_half
    contract_rows = (((0,), (0,)), ((), ()))

    loads[6].wait()
    loads[5].wait()
    dc_out[pl.ds(seq, 1)] = dc_ref[...][None]
    pl.semaphore_wait(barrier, n_seq - 1 + RING - 1)

    copies = Copies(send_sem, recv_sem)

    def swap_out(part):
        blocks = pl.ds(part * n_blk, n_blk)
        return copies.start(gw_ref.at[blocks, rows_of((1 - core) * out_half, out_half), :], outs_pair[part], mate)

    dc_half = dc_out.shape[1] // 2
    dc_gather = Gather(copies, ring_x, lambda k, half: dc_out.at[k * CORES + core, pl.ds(half * dc_half, dc_half), :])
    swap_1 = swap_out(1)
    dc_gather.begin()
    dc_mate = [copies.start(dc_out.at[seq], dc_out.at[seq], mate)]
    loads[4].wait()
    loads[1].wait()
    frames = frames_ref[...]
    enc_acc[...] = lax.dot_general(frames.reshape(-1, frames.shape[-1]), da_ref[...], contract_rows, preferred_element_type=F32)
    swap_enc = copies.start(enc_acc.at[rows_of((1 - core) * enc_half, enc_half), :], enc_pair, mate)
    swap_0 = swap_out(0)

    def dc_pass(k):
        dc_mate.append(copies.start(dc_out.at[k * CORES + core], dc_out.at[k * CORES + core], mate))

    def add_out(part):
        outs_acc[part][...] = gw_ref[pl.ds(part * n_blk, n_blk), rows_of(out_row, out_half), :] + outs_pair[part][...]

    def out_first(part):
        return lambda k, half: outs_acc[part].at[:, rows_of(k * out_q + half * (out_q // 2), out_q // 2), :]

    def out_second(part):
        return lambda k: outs_mid[part].at[k]

    rings = ((ring_x, ring_y), (ring_y, ring_x))
    first = [Reduce(copies, rings[part][0], out_first(part), outs_1[part]) for part in range(2)]
    second = [Swap(copies, rings[part][1], out_second(part), outs_2[part]) for part in range(2)]
    enc_first = Reduce(copies, ring_y, lambda k, half: enc_acc.at[rows_of(enc_row + k * enc_q + half * (enc_q // 2), enc_q // 2), :], enc_y)
    enc_second = Swap(copies, ring_x, lambda k: enc_mid.at[rows_of(k * enc_s, enc_s), :], enc_x)
    pred_first = Swap(copies, ring_y, lambda k: pred_acc.at[rows_of(k * enc_s, enc_s), :], pred_y)

    def out_place(part, k1, k2, half, whole=False):
        start, size = out_row + k1 * out_q, out_q
        if not whole:
            start, size = start + half * (out_q // 2), out_q // 2
        return gwo_out.at[part * n_blk + k2 if k2 is not None else pl.ds(part * n_blk, n_blk), rows_of(start, size), :]

    def pair_place(part):
        ring1, ring2 = rings[part]
        return (
            Spread(copies, ring2, lambda k: out_place(part, ring1.me, k, 0, True)),
            Gather(copies, ring1, lambda k, half: out_place(part, k, None, half)),
        )

    a_g1, a_g2 = pair_place(0)
    b_g1, b_g2 = pair_place(1)
    enc_at = lambda k: gwe_out.at[rows_of(enc_row + y * enc_q + k * enc_s, enc_s), :]
    enc_g1 = Spread(copies, ring_x, enc_at)
    enc_g2 = Gather(copies, ring_y, lambda k, half: gwe_out.at[rows_of(enc_row + k * enc_q + half * (enc_q // 2), enc_q // 2), :])
    pred_at = lambda k: gwp_out.at[x, core, rows_of(k * enc_s, enc_s), :]
    pred_g1 = Spread(copies, ring_y, pred_at)
    pred_g2 = Gather(copies, ring_x, lambda k, half: gwp_out.at[k, core, pl.ds(half * (enc_q // 2), enc_q // 2), :])

    last = []

    def pass_on(ref):
        last.append(copies.start(ref, ref, mate))

    a_whole = lambda k: out_place(0, k, None, 0, True)
    b_whole = lambda k: out_place(1, k, None, 0, True)
    enc_whole = lambda k: gwe_out.at[rows_of(enc_row + k * enc_q, enc_q), :]
    pred_whole = lambda k: gwp_out.at[k, core]

    def widen(g1, g2, whole):
        g1.finish()
        g2.begin()
        pass_on(whole(g2.ring.me))

    def relay(g2, whole):
        g2.relay()
        pass_on(whole(g2.ring.prv))
        pass_on(whole(g2.ring.nxt))

    def close(g2, whole):
        g2.finish()
        pass_on(whole(g2.ring.opp))

    swap_1.wait_recv()
    add_out(1)
    first[1].begin()
    swap_enc.wait_recv()
    enc_acc[rows_of(enc_row, enc_half), :] = enc_acc[rows_of(enc_row, enc_half), :] + enc_pair[...]
    dc_gather.relay()
    dc_pass(ring_x.prv)
    dc_pass(ring_x.nxt)
    swap_0.wait_recv()
    add_out(0)
    first[0].begin()
    first[1].middle()
    enc_first.begin()

    loads[3].wait()
    ge = lax.dot_general(da_ref[...], w_enc_ref[...], (((1,), (1,)), ((), ())), preferred_element_type=F32)
    ge_ref[...] = ge.astype(BF16).reshape(ge_ref.shape)
    ge_out[pl.ds(seq, 1)] = ge_ref[pl.ds(seq, 1)]
    loads[7].wait()
    loss_out[pl.ds(seq, 1)] = loss_ref[...][None]
    loads[2].wait()
    loads[0].wait()
    for k in range(n_utt):
        rows_ref[k * n_upos:(k + 1) * n_upos, :] = pred_ref[order_ref[k], :, pl.ds(pl.multiple_of(x * LANES, LANES), LANES)]
    dc_gather.finish()
    dc_pass(ring_x.opp)
    first[0].middle()
    first[1].end(lambda half: outs_mid[1].at[:, pl.ds(half * (out_q // 2), out_q // 2), :])
    second[1].begin()

    for copy in dc_mate:
        copy.wait_recv()
    pred_part = lax.dot_general(rows_ref[...], dc_out[...].reshape(n_utt * n_upos, -1), contract_rows, preferred_element_type=F32)
    pred_acc[...] = jnp.where(core == 0, pred_part[:enc_q], pred_part[enc_q:])
    pred_first.begin()
    enc_first.middle()
    small = []
    for hop in range(1, n_seq):
        peer = lax.rem(seq + hop, n_seq)
        small.append(copies.start(ge_ref.at[peer], ge_out.at[seq], {"seq": peer}))
        small.append(copies.start(loss_ref, loss_out.at[seq], {"seq": peer}))
    first[0].end(lambda half: outs_mid[0].at[:, pl.ds(half * (out_q // 2), out_q // 2), :])
    second[0].begin()
    second[1].end(out_place(1, y, x, 0, True))
    b_g1.begin()
    enc_first.end(lambda half: enc_mid.at[pl.ds(half * (enc_q // 2), enc_q // 2), :])
    enc_second.begin()
    pred_first.end(pred_at(y))
    pred_g1.begin()
    second[0].end(out_place(0, x, y, 0, True))
    a_g1.begin()
    widen(b_g1, b_g2, b_whole)
    enc_second.end(enc_at(x))
    enc_g1.begin()
    widen(pred_g1, pred_g2, pred_whole)
    relay(b_g2, b_whole)
    widen(enc_g1, enc_g2, enc_whole)
    relay(pred_g2, pred_whole)
    widen(a_g1, a_g2, a_whole)
    close(b_g2, b_whole)
    relay(enc_g2, enc_whole)
    relay(a_g2, a_whole)
    close(pred_g2, pred_whole)
    close(enc_g2, enc_whole)
    close(a_g2, a_whole)
    for copy in small + last:
        copy.wait_recv()
    copies.drain()


N_COPIES = 3 + 10 + 14 + 3 * 6 + 4 * 6 + 4 * 6 + 16


def unflatten(refs):
    refs = list(refs)
    take = lambda n: [refs.pop(0) for _ in range(n)]
    enc_acc, enc_pair, enc_mid = take(3)
    enc_y, enc_x = take(3), take(3)
    outs = [(take(1)[0], take(1)[0], take(1)[0], take(3), take(3)) for _ in range(2)]
    outs_acc, outs_pair, outs_mid, outs_1, outs_2 = zip(*outs)
    pred_acc = refs.pop(0)
    pred_y = take(3)
    return (enc_acc, enc_pair, enc_mid, enc_y, enc_x, outs_acc, outs_pair, outs_mid, outs_1, outs_2, pred_acc, pred_y, *refs)


def combine(n_seq, order, frames, pred_loc, w_enc, da, dc, gw, loss):
    width = frames.shape[-1]
    n_utt, n_upos, _ = pred_loc.shape
    joint = da.shape[-1]
    n_blk = gw.shape[0] // 2
    enc_half, out_half = width // CORES, joint // CORES
    enc_q, out_q = enc_half // RING, out_half // RING
    enc_s = enc_q // RING
    ring = lambda *shape: [VMEM(shape, F32)] * 3
    outs = [VMEM((n_blk, out_half, LANES), F32)] * 2 + [VMEM((n_blk, out_q, LANES), F32)] + ring(2, n_blk, out_q // 2, LANES) + ring(out_q, LANES)
    return pl.pallas_call(
        functools.partial(combine_kernel, n_seq),
        out_shape=(
            VMEM(frames.shape, BF16),
            VMEM((n_seq,) + dc.shape, BF16),
            VMEM((width, joint), F32),
            VMEM((RING, CORES, enc_q, joint), F32),
            VMEM(gw.shape, F32),
            VMEM((n_seq,) + loss.shape, F32),
        ),
        in_specs=[pl.BlockSpec(memory_space=pltpu.HBM)] * 8,
        out_specs=(vspec(),) * 6,
        scratch_shapes=[pltpu.SMEM(order.shape, jnp.int32)]
        + [VMEM(v.shape, v.dtype) for v in (frames, pred_loc, w_enc, da, dc, gw, loss)]
        + [pltpu.SemaphoreType.DMA((8,))]
        + [VMEM((width, joint), F32), VMEM((enc_half, joint), F32), VMEM((enc_q, joint), F32)]
        + ring(2, enc_q // 2, joint)
        + ring(enc_s, joint)
        + outs
        + outs
        + [VMEM((enc_q, joint), F32)]
        + ring(enc_s, joint)
        + [
            VMEM((n_utt * n_upos, LANES), BF16),
            VMEM(frames.shape, BF16),
            pltpu.SemaphoreType.DMA((N_COPIES,)),
            pltpu.SemaphoreType.DMA((N_COPIES,)),
        ],
        compiler_params=pltpu.CompilerParams(collective_id=1, has_side_effects=True, vmem_limit_bytes=48_000_000),
        name="combine",
    )(*(in_hbm(v) for v in (order, frames, pred_loc, w_enc, da, dc, gw, loss)))


def output_kernel(place_hbm, w_pred_hbm, losses_ref, ge_ref, dc_ref, gwe_ref, gwp_ref, gw_ref,
                  loss_out, ge_out, gp_out, gwe_out, gwp_out, gwo_out, rows_ref, gp_ref, place_ref, w_pred_ref, sem, load_sem):
    n_utt, n_upos, width = gp_out.shape
    n_own = ge_ref.shape[1]
    n_cols, _, col = gw_ref.shape
    loads = [pltpu.make_async_copy(place_hbm, place_ref, load_sem.at[0]), pltpu.make_async_copy(w_pred_hbm, w_pred_ref, load_sem.at[1])]
    for copy in loads:
        copy.start()
    copies = [pltpu.make_async_copy(gwe_ref, gwe_out, sem.at[0])]
    blocks, cores, size, _ = gwp_ref.shape
    for k in range(blocks * cores):
        copies.append(pltpu.make_async_copy(gwp_ref.at[k // cores, k % cores], gwp_out.at[pl.ds(k * size, size), :], sem.at[2 + n_cols + 4 + k]))
    for k in range(n_cols):
        copies.append(pltpu.make_async_copy(gw_ref.at[k], gwo_out.at[:, pl.ds(k * col, col)], sem.at[2 + k]))
    for copy in copies:
        copy.start()
    for copy in loads:
        copy.wait()
    n_parts = 4
    part = n_utt // n_parts
    for p in range(n_parts):
        for i in range(p * part, (p + 1) * part):
            place = place_ref[i]
            dev = place // n_own
            own = place - dev * n_own
            loss_out[i] = losses_ref[dev, 0, own]
            ge_out[i] = ge_ref[dev, own]
            rows_ref[i] = dc_ref[dev, pl.ds(pl.multiple_of(own * n_upos, n_upos), n_upos), :]
        rows = rows_ref[p * part:(p + 1) * part]
        grads = lax.dot_general(rows.reshape(part * n_upos, -1), w_pred_ref[...], (((1,), (1,)), ((), ())), preferred_element_type=F32)
        gp_ref[p * part:(p + 1) * part] = grads.reshape(part, n_upos, width)
        copy = pltpu.make_async_copy(gp_ref.at[pl.ds(p * part, part)], gp_out.at[pl.ds(p * part, part)], sem.at[2 + n_cols + p])
        copy.start()
        copies.append(copy)
    for copy in copies:
        copy.wait()


def outputs(place, losses, ge, dc, w_pred, gwe, gwp, gw, n_upos):
    n_seq, n_own, t_loc, width = ge.shape
    n_utt = n_seq * n_own
    n_cols, joint, col = gw.shape
    return pl.pallas_call(
        output_kernel,
        out_shape=(
            jax.ShapeDtypeStruct((n_utt,), F32),
            jax.ShapeDtypeStruct((n_utt, t_loc, width), BF16),
            jax.ShapeDtypeStruct((n_utt, n_upos, width), F32),
            jax.ShapeDtypeStruct((width, joint), F32),
            jax.ShapeDtypeStruct((width, joint), F32),
            jax.ShapeDtypeStruct((joint, n_cols * col), F32),
        ),
        in_specs=[pl.BlockSpec(memory_space=pltpu.HBM)] * 2 + [sspec()] + [vspec()] * 5,
        out_specs=(sspec(), vspec()) + (pl.BlockSpec(memory_space=pltpu.HBM),) * 4,
        scratch_shapes=[
            VMEM((n_utt, n_upos, joint), BF16),
            VMEM((n_utt, n_upos, width), F32),
            pltpu.SMEM(place.shape, jnp.int32),
            VMEM(w_pred.shape, BF16),
            pltpu.SemaphoreType.DMA((2 + n_cols + 4 + RING * CORES,)),
            pltpu.SemaphoreType.DMA((2,)),
        ],
        compiler_params=pltpu.CompilerParams(vmem_limit_bytes=48_000_000),
        name="outputs",
    )(in_hbm(place), in_hbm(w_pred), losses, ge, dc, gwe, gwp, gw)


def solution(mesh):
    n_seq = mesh.shape["seq"]
    utt_rows = P(("part", "data"))
    utt_mats = P(("part", "data"), None)
    utt_cube = P(("part", "data"), None, None)
    enc_spec = P(("part", "data"), "seq", None)
    weight_in = P(None, None)
    weight_out = P("part", None)

    def body(enc_loc, pred_loc, w_enc, w_pred, w_out, labels, frame_len, label_len):
        t_loc = enc_loc.shape[1]
        n_upos = pred_loc.shape[1]
        seq_idx = lax.axis_index("seq").astype(jnp.int32).reshape(1)
        order, place, frames, act, pred, w_out_t = exchange(n_seq, frame_len, label_len, enc_loc, pred_loc, w_enc, w_pred, w_out)
        da, dc, gw, loss = lattice(n_seq, seq_idx, order, frame_len, label_len, labels, act, pred, w_out, w_out_t, n_upos, t_loc)
        ge, dc_all, gwe, gwp, gw, losses = combine(n_seq, order, frames, pred_loc, w_enc, da, dc, gw, loss)
        loss, grad_enc, grad_pred, gw_enc, gw_pred, gw_out = outputs(place, losses, ge, dc_all, w_pred, gwe, gwp, gw, n_upos)
        return loss, grad_enc, grad_pred, gw_enc, gw_pred, gw_out

    return jax.shard_map(body, mesh=mesh, in_specs=(enc_spec, utt_cube, weight_in, weight_in, weight_in, utt_mats, utt_rows, utt_rows), out_specs=(utt_rows, enc_spec, utt_cube, weight_out, weight_out, weight_out), check_vma=False)
```

```python
import functools

import jax
import jax.numpy as jnp
from jax import lax
from jax.experimental import pallas as pl
from jax.experimental.pallas import tpu as pltpu
from jax.sharding import PartitionSpec as P

NEG = -1e30
MESH = pl.DeviceIdType.MESH
VMEM = pltpu.VMEM
F32 = jnp.float32
BF16 = jnp.bfloat16
VMEM_LIMIT = 67_000_000
SUB = 8
LANES = 128
GROUPS = 4
BLOCK = 32
CORES = 2
RING = 4


def vspec():
    return pl.BlockSpec(memory_space=pltpu.VMEM)


def in_hbm(x):
    return pltpu.with_memory_space_constraint(x, pltpu.HBM)


def in_vmem(x):
    return pltpu.with_memory_space_constraint(x, pltpu.VMEM)


def sspec():
    return pl.BlockSpec(memory_space=pltpu.SMEM)


def exchange_kernel(n_seq, flen_hbm, llen_hbm, enc_hbm, pred_hbm, w_enc_hbm, w_pred_hbm, w_out_hbm,
                    order_ref, place_ref, frames_ref, a_ref, c_ref, w_out_t_ref,
                    key_ref, sorted_ref, own_pred_ref, flen_ref, llen_ref, enc_ref, pred_ref, w_enc_ref, w_pred_ref, w_out_ref, load_sem, send_sem, recv_sem):
    sources = (flen_hbm, llen_hbm, enc_hbm, pred_hbm, w_pred_hbm, w_out_hbm, w_enc_hbm)
    landed = (flen_ref, llen_ref, enc_ref, pred_ref, w_pred_ref, w_out_ref, w_enc_ref)
    loads = [pltpu.make_async_copy(src, dst, load_sem.at[k]) for k, (src, dst) in enumerate(zip(sources, landed))]
    for copy in loads:
        copy.start()
    seq = lax.axis_index("seq")
    n_utt = enc_ref.shape[0]
    n_own = n_utt // n_seq
    barrier = pltpu.get_barrier_semaphore()
    for hop in range(1, n_seq):
        pl.semaphore_signal(barrier, inc=1, device_id={"seq": lax.rem(seq + hop, n_seq)}, device_id_type=MESH)

    def set_key(i, carry):
        key_ref[i] = ((flen_ref[i] + SUB - 1) // SUB) * ((llen_ref[i] + SUB) // SUB) * n_utt + i
        return carry

    def set_place(i, carry):
        key = key_ref[i]
        rank = jnp.int32(0)
        for j in range(n_utt):
            rank = rank + jnp.where(key_ref[j] > key, 1, 0)
        deal = rank // n_seq
        at = rank - deal * n_seq
        at = jnp.where(deal % 2 == 0, at, n_seq - 1 - at)
        place_ref[i] = at * n_own + deal
        return carry

    def set_order(k, carry):
        utt = jnp.int32(0)
        for j in range(n_utt):
            utt = utt + jnp.where(place_ref[j] == k, j, 0)
        order_ref[k] = utt
        return carry

    loads[0].wait()
    loads[1].wait()
    lax.fori_loop(0, n_utt, set_key, 0)
    lax.fori_loop(0, n_utt, set_place, 0)
    lax.fori_loop(0, n_utt, set_order, 0)
    loads[2].wait()
    for k in range(n_utt):
        sorted_ref[k] = enc_ref[order_ref[k]]
    pl.semaphore_wait(barrier, n_seq - 1)
    copies = []
    for hop in range(1, n_seq):
        peer = lax.rem(seq + hop, n_seq)
        copy = pltpu.make_async_remote_copy(
            src_ref=sorted_ref.at[pl.ds(peer * n_own, n_own)],
            dst_ref=frames_ref.at[seq],
            send_sem=send_sem.at[hop - 1],
            recv_sem=recv_sem.at[hop - 1],
            device_id={"seq": peer},
            device_id_type=MESH,
        )
        copy.start()
        copies.append(copy)
    frames_ref[pl.ds(seq, 1)] = sorted_ref[pl.ds(seq * n_own, n_own)][None]
    loads[3].wait()
    loads[4].wait()
    for j in range(n_own):
        own_pred_ref[j] = pred_ref[order_ref[seq * n_own + j]]
    own_pred = own_pred_ref[...]
    c_ref[...] = jnp.dot(own_pred.reshape(-1, own_pred.shape[-1]), w_pred_ref[...], preferred_element_type=F32).astype(BF16).astype(F32)
    loads[5].wait()
    w_out_t_ref[...] = w_out_ref[...].T
    loads[6].wait()
    for copy in copies:
        copy.wait()
    frames = frames_ref[...]
    a_ref[...] = jnp.dot(frames.reshape(-1, frames.shape[-1]), w_enc_ref[...], preferred_element_type=F32).astype(BF16).astype(F32)


def exchange(n_seq, frame_len, label_len, enc_loc, pred_loc, w_enc, w_pred, w_out):
    n_utt, t_loc, width = enc_loc.shape
    n_own = n_utt // n_seq
    n_upos = pred_loc.shape[1]
    joint, vocab = w_out.shape
    return pl.pallas_call(
        functools.partial(exchange_kernel, n_seq),
        out_shape=(
            pltpu.HBM((n_utt,), jnp.int32),
            pltpu.HBM((n_utt,), jnp.int32),
            pltpu.HBM((n_seq, n_own, t_loc, width), BF16),
            VMEM((n_seq * n_own * t_loc, joint), F32),
            VMEM((n_own * n_upos, joint), F32),
            VMEM((vocab, joint), BF16),
        ),
        in_specs=[pl.BlockSpec(memory_space=pltpu.HBM)] * 7,
        out_specs=(sspec(),) * 2 + (vspec(),) * 4,
        scratch_shapes=[
            pltpu.SMEM((n_utt,), jnp.int32),
            VMEM(enc_loc.shape, BF16),
            VMEM((n_own, n_upos, width), BF16),
            pltpu.SMEM((n_utt,), jnp.int32),
            pltpu.SMEM((n_utt,), jnp.int32),
        ]
        + [VMEM(v.shape, BF16) for v in (enc_loc, pred_loc, w_enc, w_pred, w_out)]
        + [
            pltpu.SemaphoreType.DMA((7,)),
            pltpu.SemaphoreType.DMA((n_seq - 1,)),
            pltpu.SemaphoreType.DMA((n_seq - 1,)),
        ],
        compiler_params=pltpu.CompilerParams(collective_id=0, has_side_effects=True, vmem_limit_bytes=40_000_000),
        name="exchange",
    )(*(in_hbm(v) for v in (frame_len, label_len, enc_loc, pred_loc, w_enc, w_pred, w_out)))


def logaddexp(x, y):
    top = jnp.maximum(x, y)
    return top + jnp.log(1.0 + jnp.exp(-jnp.abs(x - y)))


def lattice_kernel(n_own, n_frames, n_upos, seq_ref, order_ref, flen_ref, llen_ref, labels_ref, a_ref, c_ref, w_ref, wt_ref,
                   da_ref, dc_ref, gw_ref, loss_ref,
                   e_ref, h_ref, blank_ref, label_ref, alpha_ref, beta_ref, ids_ref, dact_ref, dpred_ref, work0, work1, dz0, dz1):
    vocab = w_ref.shape[1]
    joint = w_ref.shape[0]
    n_vt = vocab // LANES
    rows_g = SUB * SUB
    rows_t = GROUPS * rows_g
    n_diag = n_frames + n_upos - 1
    first = seq_ref[0] * n_own
    utts = [order_ref[first + b] for b in range(n_own)]
    lens_t = [flen_ref[utt] for utt in utts]
    lens_u = [llen_ref[utt] for utt in utts]
    blocks_t = [lax.div(n + SUB - 1, SUB) for n in lens_t]
    blocks_u = [lax.div(n + SUB, SUB) for n in lens_u]
    starts = [jnp.int32(0)]
    for b in range(n_own):
        starts.append(starts[-1] + blocks_t[b] * blocks_u[b])
    total = starts[-1]
    n_tiles = lax.div(total + GROUPS - 1, GROUPS)

    def decode(n):
        n = jnp.minimum(n, total - 1)
        b = jnp.int32(0)
        base, width = starts[0], blocks_u[0]
        for k in range(1, n_own):
            past = n >= starts[k]
            b = jnp.where(past, k, b)
            base = jnp.where(past, starts[k], base)
            width = jnp.where(past, blocks_u[k], width)
        ti = lax.div(n - base, width)
        return n, b, ti, n - base - ti * width

    pos_col = lax.broadcasted_iota(jnp.int32, (n_upos, n_upos - 1), 0)
    pos_row = lax.broadcasted_iota(jnp.int32, (n_upos, n_upos - 1), 1)
    for b in range(n_own):
        row = labels_ref[pl.ds(utts[b], 1), :].astype(F32)
        col = jnp.sum(jnp.where(pos_col == pos_row, row, 0.0), axis=1, keepdims=True)
        ids_ref[pl.ds(b * n_upos, n_upos), :] = jnp.broadcast_to(col, (n_upos, LANES)).astype(jnp.int32)

    blank_ref[...] = jnp.zeros_like(blank_ref)
    label_ref[...] = jnp.zeros_like(label_ref)
    gw_ref[...] = jnp.zeros_like(gw_ref)
    dact_ref[...] = jnp.zeros_like(dact_ref)
    dpred_ref[...] = jnp.zeros_like(dpred_ref)

    lane = lax.broadcasted_iota(jnp.int32, (SUB, LANES), 1)
    block_lane = lax.broadcasted_iota(jnp.int32, (BLOCK, LANES), 1)
    t_block = BLOCK // SUB
    works, dzs = (work0, work1), (dz0, dz1)

    def tile_rows(i):
        return pl.ds(pl.multiple_of(jnp.clip(i, 0, n_tiles - 1) * rows_t, rows_t), rows_t)

    def tile_groups(i):
        return [decode(jnp.clip(i, 0, n_tiles - 1) * GROUPS + g) for g in range(GROUPS)]

    def pred_row(b, ui):
        return pl.ds(pl.multiple_of(b * n_upos + ui * SUB, SUB), SUB)

    def act_row(b, ti):
        return pl.ds(pl.multiple_of((ti * n_own + b) * SUB, SUB), SUB)

    def block_ids(b, ui):
        ids = ids_ref[pred_row(b, ui), :]
        return jnp.broadcast_to(ids[None], (t_block, SUB, LANES)).reshape(BLOCK, LANES)

    def cell_rows(ti, k, ui):
        return pl.ds(pl.multiple_of((n_diag - 1 - ti * SUB - k) * n_upos + ui * SUB, SUB), SUB)

    def make_hidden(i):
        first_row = jnp.clip(i, 0, n_tiles - 1) * rows_t
        for g, (n, b, ti, ui) in enumerate(tile_groups(i)):
            a8 = a_ref[act_row(b, ti), :]
            c8 = c_ref[pred_row(b, ui), :]
            h = jnp.tanh(a8[:, None, :] + c8[None, :, :]).reshape(rows_g, joint).astype(BF16)
            h_ref[pl.ds(pl.multiple_of(first_row + g * rows_g, rows_g), rows_g), :] = h

    def make_logits(i, z_ref):
        z_ref[...] = jnp.dot(h_ref[tile_rows(i), :], w_ref[...], preferred_element_type=F32)

    def make_softmax(i, z_ref):
        first_row = jnp.clip(i, 0, n_tiles - 1) * rows_t
        for g, (n, b, ti, ui) in enumerate(tile_groups(i)):
            ids = block_ids(b, ui)
            for r in range(0, rows_g, BLOCK):
                z = z_ref[g * rows_g + r:g * rows_g + r + BLOCK, :]
                top = jnp.max(z, axis=1, keepdims=True)
                e = jnp.exp(z - top)
                norm = jnp.sum(e, axis=1, keepdims=True)
                e_ref[pl.ds(pl.multiple_of(first_row + g * rows_g + r, BLOCK), BLOCK), :] = e
                log_norm = top + jnp.log(norm)
                picked = jnp.zeros((BLOCK, LANES), F32)
                for v in range(n_vt):
                    picked = picked + jnp.where(block_lane + v * LANES == ids, z[:, v * LANES:(v + 1) * LANES], 0.0)
                label = jnp.sum(picked, axis=1, keepdims=True) - log_norm
                blank = z[:, 0:1] - log_norm
                scale = 1.0 / norm
                rows = [cell_rows(ti, r // SUB + k, ui) for k in range(t_block)]
                old_blank = [blank_ref[at, :] for at in rows]
                old_label = [label_ref[at, :] for at in rows]
                for k, at in enumerate(rows):
                    sl = slice(k * SUB, (k + 1) * SUB)
                    blank_ref[at, :] = jnp.where(lane == b, blank[sl], jnp.where(lane == b + n_own, scale[sl], old_blank[k]))
                    label_ref[at, :] = jnp.where(lane == b, label[sl], old_label[k])

    make_hidden(0)
    make_logits(0, work0)
    make_hidden(1)

    def forward(j, carry):
        for half in range(2):
            i = 2 * j + half
            make_logits(i + 1, works[1 - half])
            make_softmax(i, works[half])
            make_hidden(i + 2)
        return carry

    lax.fori_loop(0, lax.div(n_tiles + 1, 2), forward, 0)

    upos = lax.broadcasted_iota(jnp.int32, (n_upos, LANES), 0)
    utt = lax.broadcasted_iota(jnp.int32, (n_upos, LANES), 1)
    t_end = jnp.ones((n_upos, LANES), jnp.int32)
    u_end = jnp.zeros((n_upos, LANES), jnp.int32)
    for b in range(n_own):
        t_end = jnp.where(utt == b, lens_t[b], t_end)
        u_end = jnp.where(utt == b, lens_u[b], u_end)

    def diagonal(d):
        return pl.ds((n_diag - 1 - d) * n_upos, n_upos, stride=n_upos + 1)

    def down(x):
        return jnp.where(upos == 0, NEG, pltpu.roll(x, 1, 0))

    def up(x):
        return jnp.where(upos == n_upos - 1, NEG, pltpu.roll(x, n_upos - 1, 0))

    def edge(d):
        return jnp.where((d - upos == t_end) & (upos == u_end), 0.0, NEG)

    alpha0 = jnp.where(upos == 0, 0.0, NEG).astype(F32)
    beta0 = edge(n_diag)
    alpha_ref[0] = alpha0
    beta_ref[n_diag] = beta0

    def sweep(k, carry):
        alpha, beta = carry
        d = k + 1
        alpha = logaddexp(alpha + blank_ref[diagonal(k), :], down(alpha + label_ref[diagonal(k), :]))
        alpha = jnp.where(upos <= d, alpha, NEG)
        alpha_ref[d] = alpha
        d = n_diag - 1 - k
        inside = (d - upos < t_end) & (upos <= u_end)
        beta = logaddexp(beta + blank_ref[diagonal(d), :], up(beta) + label_ref[diagonal(d), :])
        beta = jnp.where(inside, beta, edge(d))
        beta_ref[d] = beta
        return alpha, beta

    lax.fori_loop(0, n_diag, sweep, (alpha0, beta0))
    log_prob = beta_ref[0][0:1, :]
    loss_ref[...] = jnp.broadcast_to(-log_prob, (SUB, LANES))

    def occupancy(d, carry):
        t = d - upos
        alpha = alpha_ref[d]
        after = beta_ref[d + 1]
        cell_ok = (t >= 0) & (t < t_end) & (upos <= u_end)
        blank = blank_ref[diagonal(d), :]
        q0 = jnp.where(cell_ok, jnp.exp(alpha + blank + after - log_prob), 0.0)
        q1 = jnp.where(cell_ok & (upos < u_end), jnp.exp(alpha + label_ref[diagonal(d), :] + up(after) - log_prob), 0.0)
        blank_ref[diagonal(d), :] = jnp.where(utt < n_own, q0, blank)
        label_ref[diagonal(d), :] = q1
        return carry

    lax.fori_loop(0, n_diag, occupancy, 0)

    def make_dz(i, dz_ref):
        first_row = jnp.clip(i, 0, n_tiles - 1) * rows_t
        for g, (n, b, ti, ui) in enumerate(tile_groups(i)):
            keep = (lane == b) & (i * GROUPS + g < total)
            ids = block_ids(b, ui)
            for r in range(0, rows_g, BLOCK):
                q0s, q1s, scales = [], [], []
                for k in range(t_block):
                    at = cell_rows(ti, r // SUB + k, ui)
                    blank = blank_ref[at, :]
                    q0s.append(jnp.where(keep, blank, 0.0))
                    scales.append(jnp.where(lane == b + n_own, blank, 0.0))
                    q1s.append(jnp.where(keep, label_ref[at, :], 0.0))
                q0 = jnp.sum(jnp.concatenate(q0s, axis=0), axis=1, keepdims=True)
                q1 = jnp.sum(jnp.concatenate(q1s, axis=0), axis=1, keepdims=True)
                scale = jnp.sum(jnp.concatenate(scales, axis=0), axis=1, keepdims=True) * (q0 + q1)
                rows = pl.ds(pl.multiple_of(first_row + g * rows_g + r, BLOCK), BLOCK)
                for v in range(n_vt):
                    at_v = block_lane + v * LANES
                    dz = e_ref[rows, v * LANES:(v + 1) * LANES] * scale
                    if v == 0:
                        dz = dz - jnp.where(at_v == 0, q0, 0.0)
                    dz = dz - jnp.where(at_v == ids, q1, 0.0)
                    dz_ref[g * rows_g + r:g * rows_g + r + BLOCK, v * LANES:(v + 1) * LANES] = dz.astype(BF16)

    def make_products(i, dz_ref, dh_ref):
        dz = dz_ref[...]
        dh_ref[:, :joint] = jnp.dot(dz, wt_ref[...], preferred_element_type=F32)
        h = h_ref[tile_rows(i), :]
        for v in range(0, n_vt, 2):
            part = lax.dot_general(h, dz[:, v * LANES:(v + 2) * LANES], (((0,), (0,)), ((), ())), preferred_element_type=F32)
            gw_ref[v] += part[:, :LANES]
            gw_ref[v + 1] += part[:, LANES:]

    def make_sums(i, dh_ref):
        first_row = jnp.clip(i, 0, n_tiles - 1) * rows_t
        for g, (n, b, ti, ui) in enumerate(tile_groups(i)):
            rows = pl.ds(pl.multiple_of(first_row + g * rows_g, rows_g), rows_g)
            for v in range(joint // LANES):
                cols = slice(v * LANES, (v + 1) * LANES)
                h = h_ref[rows, cols].astype(F32)
                ds = dh_ref[g * rows_g:(g + 1) * rows_g, cols] * (1.0 - h * h)
                cube = ds.reshape(SUB, SUB, LANES)
                dact_ref[act_row(b, ti), cols] += jnp.sum(cube, axis=1)
                dpred_ref[pred_row(b, ui), cols] += jnp.sum(cube, axis=0)

    work1[...] = jnp.zeros_like(work1)
    make_dz(0, dz0)

    def backward(j, carry):
        for half in range(2):
            i = 2 * j + half
            make_products(i, dzs[half], works[half])
            make_dz(i + 1, dzs[1 - half])
            make_sums(i - 1, works[1 - half])
        return carry

    lax.fori_loop(0, lax.div(n_tiles + 2, 2), backward, 0)
    da_ref[...] = dact_ref[...].astype(BF16)
    dc_ref[...] = dpred_ref[...].astype(BF16)


def lattice(n_seq, seq_idx, order, frame_len, label_len, labels, act, pred, w_out, w_out_t, n_upos, t_loc):
    n_own = frame_len.shape[0] // n_seq
    n_frames = n_seq * t_loc
    joint, vocab = w_out.shape
    cells = n_own * n_frames * n_upos
    n_diag = n_frames + n_upos - 1
    lat_rows = (n_diag + n_upos - 1) * n_upos
    return pl.pallas_call(
        functools.partial(lattice_kernel, n_own, n_frames, n_upos),
        out_shape=(
            VMEM(act.shape, BF16),
            VMEM(pred.shape, BF16),
            VMEM((vocab // LANES, joint, LANES), F32),
            VMEM((SUB, LANES), F32),
        ),
        in_specs=[sspec()] * 4 + [vspec()] * 5,
        out_specs=(vspec(),) * 4,
        scratch_shapes=[
            VMEM((cells, vocab), F32),
            VMEM((cells, joint), BF16),
            VMEM((lat_rows, LANES), F32),
            VMEM((lat_rows, LANES), F32),
            VMEM((n_diag + 1, n_upos, LANES), F32),
            VMEM((n_diag + 1, n_upos, LANES), F32),
            VMEM((n_own * n_upos, LANES), jnp.int32),
            VMEM(act.shape, F32),
            VMEM(pred.shape, F32),
            VMEM((GROUPS * SUB * SUB, vocab), F32),
            VMEM((GROUPS * SUB * SUB, vocab), F32),
            VMEM((GROUPS * SUB * SUB, vocab), BF16),
            VMEM((GROUPS * SUB * SUB, vocab), BF16),
        ],
        compiler_params=pltpu.CompilerParams(vmem_limit_bytes=59_400_000),
        name="lattice",
    )(seq_idx, order, frame_len, label_len, labels, in_vmem(act), in_vmem(pred), w_out, in_vmem(w_out_t))


class Copies:
    def __init__(self, send_sem, recv_sem):
        self.sems = (send_sem, recv_sem)
        self.all = []

    def start(self, src, dst, device):
        k = len(self.all)
        copy = pltpu.make_async_remote_copy(src_ref=src, dst_ref=dst, send_sem=self.sems[0].at[k], recv_sem=self.sems[1].at[k], device_id=device, device_id_type=MESH)
        copy.start()
        self.all.append(copy)
        return copy

    def drain(self):
        for copy in self.all:
            copy.wait_send()


class Ring:
    def __init__(self, me, device):
        self.me = me
        self.right, self.left, self.across = [device(lax.rem(me + hop, RING)) for hop in (1, RING - 1, 2)]
        self.nxt, self.prv, self.opp = lax.rem(me + 1, RING), lax.rem(me + RING - 1, RING), lax.rem(me + 2, RING)


class Reduce:
    def __init__(self, copies, ring, acc, bufs):
        self.copies, self.ring, self.acc = copies, ring, acc
        self.pair, self.from_left, self.from_right = bufs

    def begin(self):
        c, r, acc = self.copies, self.ring, self.acc
        self.a1 = c.start(acc(r.opp, 0), self.pair.at[0], r.right)
        self.b1 = c.start(acc(r.opp, 1), self.pair.at[1], r.left)
        self.b2 = c.start(acc(r.nxt, 1), self.from_left.at[1], r.right)
        self.a2 = c.start(acc(r.prv, 0), self.from_right.at[0], r.left)

    def middle(self):
        c, r, acc = self.copies, self.ring, self.acc
        self.a1.wait_recv()
        add = acc(r.nxt, 0)
        add[...] = add[...] + self.pair[0]
        self.a3 = c.start(add, self.from_left.at[0], r.right)
        self.b1.wait_recv()
        add = acc(r.prv, 1)
        add[...] = add[...] + self.pair[1]
        self.b3 = c.start(add, self.from_right.at[1], r.left)

    def end(self, target):
        for copy in (self.b2, self.a3, self.a2, self.b3):
            copy.wait_recv()
        for half in range(2):
            target(half)[...] = self.acc(self.ring.me, half)[...] + self.from_left[half] + self.from_right[half]


class Gather:
    def __init__(self, copies, ring, out):
        self.copies, self.ring, self.out = copies, ring, out

    def send(self, k, half, device):
        return self.copies.start(self.out(k, half), self.out(k, half), device)

    def begin(self):
        r = self.ring
        self.ra = self.send(r.me, 0, r.right)
        self.lb = self.send(r.me, 1, r.left)
        self.rb = self.send(r.me, 1, r.right)
        self.la = self.send(r.me, 0, r.left)

    def relay(self):
        r = self.ring
        self.ra.wait_recv()
        self.ra2 = self.send(r.prv, 0, r.right)
        self.lb.wait_recv()
        self.lb2 = self.send(r.nxt, 1, r.left)
        self.rb.wait_recv()
        self.la.wait_recv()

    def finish(self):
        self.ra2.wait_recv()
        self.lb2.wait_recv()


class Swap:
    def __init__(self, copies, ring, acc, bufs):
        self.copies, self.ring, self.acc, self.bufs = copies, ring, acc, bufs

    def begin(self):
        r = self.ring
        sends = ((r.nxt, r.right), (r.prv, r.left), (r.opp, r.across))
        self.sent = [self.copies.start(self.acc(k), buf, device) for (k, device), buf in zip(sends, self.bufs)]

    def end(self, target):
        for copy in self.sent:
            copy.wait_recv()
        target[...] = (self.acc(self.ring.me)[...] + self.bufs[0][...]) + (self.bufs[1][...] + self.bufs[2][...])


class Spread:
    def __init__(self, copies, ring, out):
        self.copies, self.ring, self.out = copies, ring, out

    def begin(self):
        r = self.ring
        self.sent = [self.copies.start(self.out(r.me), self.out(r.me), device) for device in (r.right, r.left, r.across)]

    def finish(self):
        for copy in self.sent:
            copy.wait_recv()


def rows_of(start, size):
    return pl.ds(pl.multiple_of(start, SUB), size)


def combine_kernel(n_seq, order_hbm, place_hbm, frames_hbm, pred_hbm, w_enc_hbm, w_pred_hbm, da_ref, dc_ref, gw_ref, loss_ref,
                   ge_out, gp_out, gwe_out, gwp_out, gwo_out, loss_out,
                   order_ref, place_ref, frames_ref, pred_ref, w_enc_ref, w_pred_ref, load_sem, dc_out, grad_rows_ref, *scratch):
    sources = (frames_hbm, order_hbm, pred_hbm, w_enc_hbm, place_hbm, w_pred_hbm)
    landed = (frames_ref, order_ref, pred_ref, w_enc_ref, place_ref, w_pred_ref)
    loads = [pltpu.make_async_copy(src, dst, load_sem.at[k]) for k, (src, dst) in enumerate(zip(sources, landed))]
    for copy in loads:
        copy.start()
    (enc_acc, enc_pair, enc_mid, enc_y, enc_x, outs_acc, outs_pair, outs_mid, outs_1, outs_2, pred_acc, pred_y, rows_ref, ge_ref, send_sem, recv_sem) = unflatten(scratch)
    seq = lax.axis_index("seq")
    y = lax.axis_index("data")
    x = lax.div(seq, CORES)
    core = lax.rem(seq, CORES)
    mate = {"seq": x * CORES + 1 - core}
    ring_x = Ring(x, lambda k: {"seq": k * CORES + core})
    ring_y = Ring(y, lambda k: {"data": k})
    barrier = pltpu.get_barrier_semaphore()
    for hop in range(1, n_seq):
        pl.semaphore_signal(barrier, inc=1, device_id={"seq": lax.rem(seq + hop, n_seq)}, device_id_type=MESH)
    for dev in (ring_y.right, ring_y.left, ring_y.across):
        pl.semaphore_signal(barrier, inc=1, device_id=dev, device_id_type=MESH)

    n_blk = gw_ref.shape[0] // 2
    n_utt = n_seq * frames_ref.shape[1]
    n_upos = pred_ref.shape[1]
    enc_half = enc_acc.shape[0] // CORES
    out_half = gw_ref.shape[1] // CORES
    enc_q, out_q = enc_half // RING, out_half // RING
    enc_s = enc_q // RING
    enc_row, out_row = core * enc_half, core * out_half
    contract_rows = (((0,), (0,)), ((), ()))

    n_own = frames_ref.shape[1]
    dc_out[pl.ds(seq * n_own, n_own)] = dc_ref[...].reshape(n_own, n_upos, -1)
    pl.semaphore_wait(barrier, n_seq - 1 + RING - 1)

    copies = Copies(send_sem, recv_sem)

    def swap_out(part):
        blocks = pl.ds(part * n_blk, n_blk)
        return copies.start(gw_ref.at[blocks, rows_of((1 - core) * out_half, out_half), :], outs_pair[part], mate)

    dc_gather = Gather(copies, ring_x, lambda k, half: dc_out.at[pl.ds((k * CORES + core) * n_own + half * (n_own // 2), n_own // 2)])
    swap_1 = swap_out(1)
    dc_gather.begin()
    dc_whole = lambda dev: dc_out.at[pl.ds(dev * n_own, n_own)]
    dc_mate = [copies.start(dc_whole(seq), dc_whole(seq), mate)]
    loads[0].wait()
    frames = frames_ref[...]
    enc_acc[...] = lax.dot_general(frames.reshape(-1, frames.shape[-1]), da_ref[...], contract_rows, preferred_element_type=F32)
    swap_enc = copies.start(enc_acc.at[rows_of((1 - core) * enc_half, enc_half), :], enc_pair, mate)
    swap_0 = swap_out(0)

    def dc_pass(k):
        dc_mate.append(copies.start(dc_whole(k * CORES + core), dc_whole(k * CORES + core), mate))

    def add_out(part):
        outs_acc[part][...] = gw_ref[pl.ds(part * n_blk, n_blk), rows_of(out_row, out_half), :] + outs_pair[part][...]

    def out_first(part):
        return lambda k, half: outs_acc[part].at[:, rows_of(k * out_q + half * (out_q // 2), out_q // 2), :]

    def out_second(part):
        return lambda k: outs_mid[part].at[k]

    rings = ((ring_x, ring_y), (ring_y, ring_x))
    first = [Reduce(copies, rings[part][0], out_first(part), outs_1[part]) for part in range(2)]
    second = [Swap(copies, rings[part][1], out_second(part), outs_2[part]) for part in range(2)]
    enc_first = Reduce(copies, ring_y, lambda k, half: enc_acc.at[rows_of(enc_row + k * enc_q + half * (enc_q // 2), enc_q // 2), :], enc_y)
    enc_second = Swap(copies, ring_x, lambda k: enc_mid.at[rows_of(k * enc_s, enc_s), :], enc_x)
    pred_first = Swap(copies, ring_y, lambda k: pred_acc.at[rows_of(k * enc_s, enc_s), :], pred_y)

    def out_place(part, k1, k2, half, whole=False):
        start, size = out_row + k1 * out_q, out_q
        if not whole:
            start, size = start + half * (out_q // 2), out_q // 2
        return gwo_out.at[part * n_blk + k2 if k2 is not None else pl.ds(part * n_blk, n_blk), rows_of(start, size), :]

    def pair_place(part):
        ring1, ring2 = rings[part]
        return (
            Spread(copies, ring2, lambda k: out_place(part, ring1.me, k, 0, True)),
            Gather(copies, ring1, lambda k, half: out_place(part, k, None, half)),
        )

    a_g1, a_g2 = pair_place(0)
    b_g1, b_g2 = pair_place(1)
    enc_at = lambda k: gwe_out.at[rows_of(enc_row + y * enc_q + k * enc_s, enc_s), :]
    enc_g1 = Spread(copies, ring_x, enc_at)
    enc_g2 = Gather(copies, ring_y, lambda k, half: gwe_out.at[rows_of(enc_row + k * enc_q + half * (enc_q // 2), enc_q // 2), :])
    pred_at = lambda k: gwp_out.at[x, core, rows_of(k * enc_s, enc_s), :]
    pred_g1 = Spread(copies, ring_y, pred_at)
    pred_g2 = Gather(copies, ring_x, lambda k, half: gwp_out.at[k, core, pl.ds(half * (enc_q // 2), enc_q // 2), :])

    last = []

    def pass_on(ref):
        last.append(copies.start(ref, ref, mate))

    a_whole = lambda k: out_place(0, k, None, 0, True)
    b_whole = lambda k: out_place(1, k, None, 0, True)
    enc_whole = lambda k: gwe_out.at[rows_of(enc_row + k * enc_q, enc_q), :]
    pred_whole = lambda k: gwp_out.at[k, core]

    def widen(g1, g2, whole):
        g1.finish()
        g2.begin()
        pass_on(whole(g2.ring.me))

    def relay(g2, whole):
        g2.relay()
        pass_on(whole(g2.ring.prv))
        pass_on(whole(g2.ring.nxt))

    def close(g2, whole):
        g2.finish()
        pass_on(whole(g2.ring.opp))

    swap_1.wait_recv()
    add_out(1)
    first[1].begin()
    swap_enc.wait_recv()
    enc_acc[rows_of(enc_row, enc_half), :] = enc_acc[rows_of(enc_row, enc_half), :] + enc_pair[...]
    dc_gather.relay()
    dc_pass(ring_x.prv)
    dc_pass(ring_x.nxt)
    swap_0.wait_recv()
    add_out(0)
    first[0].begin()
    first[1].middle()
    enc_first.begin()

    loads[3].wait()
    ge = lax.dot_general(da_ref[...], w_enc_ref[...], (((1,), (1,)), ((), ())), preferred_element_type=F32)
    ge_ref[...] = ge.astype(BF16).reshape(ge_ref.shape)
    ge_out[pl.ds(seq, 1)] = ge_ref[pl.ds(seq, 1)]
    loss_out[pl.ds(seq, 1)] = loss_ref[...][None]
    loads[1].wait()
    loads[2].wait()
    for k in range(n_utt):
        rows_ref[k * n_upos:(k + 1) * n_upos, :] = pred_ref[order_ref[k], :, pl.ds(pl.multiple_of(x * LANES, LANES), LANES)]
    dc_gather.finish()
    dc_pass(ring_x.opp)
    first[0].middle()
    first[1].end(lambda half: outs_mid[1].at[:, pl.ds(half * (out_q // 2), out_q // 2), :])
    second[1].begin()

    for copy in dc_mate:
        copy.wait_recv()
    pred_part = lax.dot_general(rows_ref[...], dc_out[...].reshape(n_utt * n_upos, -1), contract_rows, preferred_element_type=F32)
    pred_acc[...] = jnp.where(core == 0, pred_part[:enc_q], pred_part[enc_q:])
    pred_first.begin()
    enc_first.middle()
    small = []
    for hop in range(1, n_seq):
        peer = lax.rem(seq + hop, n_seq)
        small.append(copies.start(ge_ref.at[peer], ge_out.at[seq], {"seq": peer}))
        small.append(copies.start(loss_ref, loss_out.at[seq], {"seq": peer}))
    first[0].end(lambda half: outs_mid[0].at[:, pl.ds(half * (out_q // 2), out_q // 2), :])
    second[0].begin()
    second[1].end(out_place(1, y, x, 0, True))
    b_g1.begin()
    enc_first.end(lambda half: enc_mid.at[pl.ds(half * (enc_q // 2), enc_q // 2), :])
    enc_second.begin()
    pred_first.end(pred_at(y))
    pred_g1.begin()
    second[0].end(out_place(0, x, y, 0, True))
    a_g1.begin()

    loads[4].wait()
    loads[5].wait()
    for i in range(n_utt):
        grad_rows_ref[i] = dc_out[place_ref[i]]
    widen(b_g1, b_g2, b_whole)
    enc_second.end(enc_at(x))
    enc_g1.begin()
    widen(pred_g1, pred_g2, pred_whole)
    half_utt = n_utt // 2

    def grad_rows(part):
        rows = grad_rows_ref[part * half_utt:(part + 1) * half_utt].reshape(half_utt * n_upos, -1)
        grads = lax.dot_general(rows, w_pred_ref[...], (((1,), (1,)), ((), ())), preferred_element_type=F32)
        gp_out[part * half_utt:(part + 1) * half_utt] = grads.reshape(half_utt, n_upos, -1)

    grad_rows(0)
    relay(b_g2, b_whole)
    widen(enc_g1, enc_g2, enc_whole)
    grad_rows(1)
    relay(pred_g2, pred_whole)
    widen(a_g1, a_g2, a_whole)
    close(b_g2, b_whole)
    relay(enc_g2, enc_whole)
    relay(a_g2, a_whole)
    close(pred_g2, pred_whole)
    close(enc_g2, enc_whole)
    close(a_g2, a_whole)
    for copy in small + last:
        copy.wait_recv()
    copies.drain()


N_COPIES = 3 + 10 + 14 + 3 * 6 + 4 * 6 + 4 * 6 + 16


def unflatten(refs):
    refs = list(refs)
    take = lambda n: [refs.pop(0) for _ in range(n)]
    enc_acc, enc_pair, enc_mid = take(3)
    enc_y, enc_x = take(3), take(3)
    outs = [(take(1)[0], take(1)[0], take(1)[0], take(3), take(3)) for _ in range(2)]
    outs_acc, outs_pair, outs_mid, outs_1, outs_2 = zip(*outs)
    pred_acc = refs.pop(0)
    pred_y = take(3)
    return (enc_acc, enc_pair, enc_mid, enc_y, enc_x, outs_acc, outs_pair, outs_mid, outs_1, outs_2, pred_acc, pred_y, *refs)


def combine(n_seq, order, place, frames, pred_loc, w_enc, w_pred, da, dc, gw, loss):
    width = frames.shape[-1]
    n_utt, n_upos, _ = pred_loc.shape
    joint = da.shape[-1]
    n_blk = gw.shape[0] // 2
    enc_half, out_half = width // CORES, joint // CORES
    enc_q, out_q = enc_half // RING, out_half // RING
    enc_s = enc_q // RING
    ring = lambda *shape: [VMEM(shape, F32)] * 3
    outs = [VMEM((n_blk, out_half, LANES), F32)] * 2 + [VMEM((n_blk, out_q, LANES), F32)] + ring(2, n_blk, out_q // 2, LANES) + ring(out_q, LANES)
    return pl.pallas_call(
        functools.partial(combine_kernel, n_seq),
        out_shape=(
            VMEM(frames.shape, BF16),
            VMEM((n_utt, n_upos, width), F32),
            VMEM((width, joint), F32),
            VMEM((RING, CORES, enc_q, joint), F32),
            VMEM(gw.shape, F32),
            VMEM((n_seq,) + loss.shape, F32),
        ),
        in_specs=[pl.BlockSpec(memory_space=pltpu.HBM)] * 6 + [vspec()] * 4,
        out_specs=(vspec(),) * 6,
        scratch_shapes=[pltpu.SMEM(order.shape, jnp.int32)] * 2
        + [VMEM(v.shape, v.dtype) for v in (frames, pred_loc, w_enc, w_pred)]
        + [pltpu.SemaphoreType.DMA((6,)), VMEM((n_utt, n_upos, joint), BF16), VMEM((n_utt, n_upos, joint), BF16)]
        + [VMEM((width, joint), F32), VMEM((enc_half, joint), F32), VMEM((enc_q, joint), F32)]
        + ring(2, enc_q // 2, joint)
        + ring(enc_s, joint)
        + outs
        + outs
        + [VMEM((enc_q, joint), F32)]
        + ring(enc_s, joint)
        + [
            VMEM((n_utt * n_upos, LANES), BF16),
            VMEM(frames.shape, BF16),
            pltpu.SemaphoreType.DMA((N_COPIES,)),
            pltpu.SemaphoreType.DMA((N_COPIES,)),
        ],
        compiler_params=pltpu.CompilerParams(collective_id=1, has_side_effects=True, vmem_limit_bytes=48_000_000),
        name="combine",
    )(*(in_hbm(v) for v in (order, place, frames, pred_loc, w_enc, w_pred)), *(in_vmem(v) for v in (da, dc, gw, loss)))


def output_kernel(place_hbm, losses_ref, ge_ref, gp_ref, gwe_ref, gwp_ref, gw_ref,
                  loss_out, ge_out, gp_out, gwe_out, gwp_out, gwo_out, place_ref, load_sem, sem):
    n_utt = gp_out.shape[0]
    n_own = ge_ref.shape[1]
    n_cols, _, col = gw_ref.shape
    load = pltpu.make_async_copy(place_hbm, place_ref, load_sem)
    load.start()
    pairs = [(gp_ref, gp_out), (gwe_ref, gwe_out)]
    pairs += [(gw_ref.at[k], gwo_out.at[:, pl.ds(k * col, col)]) for k in range(n_cols)]
    blocks, cores, size, _ = gwp_ref.shape
    pairs += [(gwp_ref.at[k // cores, k % cores], gwp_out.at[pl.ds(k * size, size), :]) for k in range(blocks * cores)]
    copies = [pltpu.make_async_copy(src, dst, sem.at[k]) for k, (src, dst) in enumerate(pairs)]
    for copy in copies:
        copy.start()
    load.wait()
    for i in range(n_utt):
        place = place_ref[i]
        dev = place // n_own
        own = place - dev * n_own
        loss_out[i] = losses_ref[dev, 0, own]
        ge_out[i] = ge_ref[dev, own]
    for copy in copies:
        copy.wait()


def outputs(place, losses, ge, gp, gwe, gwp, gw):
    n_seq, n_own, t_loc, width = ge.shape
    n_cols, joint, col = gw.shape
    hbm = pl.BlockSpec(memory_space=pltpu.HBM)
    return pl.pallas_call(
        output_kernel,
        out_shape=(
            jax.ShapeDtypeStruct((n_seq * n_own,), F32),
            jax.ShapeDtypeStruct((n_seq * n_own, t_loc, width), BF16),
            jax.ShapeDtypeStruct(gp.shape, F32),
            jax.ShapeDtypeStruct((width, joint), F32),
            jax.ShapeDtypeStruct((width, joint), F32),
            jax.ShapeDtypeStruct((joint, n_cols * col), F32),
        ),
        in_specs=[hbm, sspec()] + [vspec()] * 5,
        out_specs=(sspec(), vspec()) + (hbm,) * 4,
        scratch_shapes=[
            pltpu.SMEM(place.shape, jnp.int32),
            pltpu.SemaphoreType.DMA,
            pltpu.SemaphoreType.DMA((2 + n_cols + RING * CORES,)),
        ],
        compiler_params=pltpu.CompilerParams(vmem_limit_bytes=48_000_000),
        name="outputs",
    )(in_hbm(place), losses, ge, gp, gwe, gwp, gw)


def solution(mesh):
    n_seq = mesh.shape["seq"]
    utt_rows = P(("part", "data"))
    utt_mats = P(("part", "data"), None)
    utt_cube = P(("part", "data"), None, None)
    enc_spec = P(("part", "data"), "seq", None)
    weight_in = P(None, None)
    weight_out = P("part", None)

    def body(enc_loc, pred_loc, w_enc, w_pred, w_out, labels, frame_len, label_len):
        t_loc = enc_loc.shape[1]
        n_upos = pred_loc.shape[1]
        seq_idx = lax.axis_index("seq").astype(jnp.int32).reshape(1)
        order, place, frames, act, pred, w_out_t = exchange(n_seq, frame_len, label_len, enc_loc, pred_loc, w_enc, w_pred, w_out)
        da, dc, gw, loss = lattice(n_seq, seq_idx, order, frame_len, label_len, labels, act, pred, w_out, w_out_t, n_upos, t_loc)
        ge, gp, gwe, gwp, gw, losses = combine(n_seq, order, place, frames, pred_loc, w_enc, w_pred, da, dc, gw, loss)
        loss, grad_enc, grad_pred, gw_enc, gw_pred, gw_out = outputs(place, losses, ge, gp, gwe, gwp, gw)
        return loss, grad_enc, grad_pred, gw_enc, gw_pred, gw_out

    return jax.shard_map(body, mesh=mesh, in_specs=(enc_spec, utt_cube, weight_in, weight_in, weight_in, utt_mats, utt_rows, utt_rows), out_specs=(utt_rows, enc_spec, utt_cube, weight_out, weight_out, weight_out), check_vma=False)
```

```python
import functools

import jax
import jax.numpy as jnp
from jax import lax
from jax.experimental import pallas as pl
from jax.experimental.pallas import tpu as pltpu
from jax.sharding import PartitionSpec as P

NEG = -1e30
MESH = pl.DeviceIdType.MESH
VMEM = pltpu.VMEM
F32 = jnp.float32
BF16 = jnp.bfloat16
VMEM_LIMIT = 67_000_000
SUB = 8
LANES = 128
GROUPS = 4
WIDE = 8
BLOCK = 32
CORES = 2
RING = 4


def vspec():
    return pl.BlockSpec(memory_space=pltpu.VMEM)


def in_hbm(x):
    return pltpu.with_memory_space_constraint(x, pltpu.HBM)


def in_vmem(x):
    return pltpu.with_memory_space_constraint(x, pltpu.VMEM)


def sspec():
    return pl.BlockSpec(memory_space=pltpu.SMEM)


def exchange_kernel(n_seq, flen_hbm, llen_hbm, enc_hbm, pred_hbm, w_enc_hbm, w_pred_hbm, w_out_hbm,
                    order_ref, place_ref, frames_ref, a_ref, c_ref, w_out_t_ref,
                    key_ref, sorted_ref, own_pred_ref, flen_ref, llen_ref, enc_ref, pred_ref, w_enc_ref, w_pred_ref, w_out_ref, load_sem, send_sem, recv_sem):
    sources = (flen_hbm, llen_hbm, enc_hbm, pred_hbm, w_pred_hbm, w_out_hbm, w_enc_hbm)
    landed = (flen_ref, llen_ref, enc_ref, pred_ref, w_pred_ref, w_out_ref, w_enc_ref)
    loads = [pltpu.make_async_copy(src, dst, load_sem.at[k]) for k, (src, dst) in enumerate(zip(sources, landed))]
    for copy in loads:
        copy.start()
    seq = lax.axis_index("seq")
    n_utt = enc_ref.shape[0]
    n_own = n_utt // n_seq
    barrier = pltpu.get_barrier_semaphore()
    for hop in range(1, n_seq):
        pl.semaphore_signal(barrier, inc=1, device_id={"seq": lax.rem(seq + hop, n_seq)}, device_id_type=MESH)

    def set_key(i, carry):
        key_ref[i] = ((flen_ref[i] + SUB - 1) // SUB) * ((llen_ref[i] + SUB) // SUB) * n_utt + i
        return carry

    def set_place(i, carry):
        key = key_ref[i]
        rank = jnp.int32(0)
        for j in range(n_utt):
            rank = rank + jnp.where(key_ref[j] > key, 1, 0)
        deal = rank // n_seq
        at = rank - deal * n_seq
        at = jnp.where(deal % 2 == 0, at, n_seq - 1 - at)
        place_ref[i] = at * n_own + deal
        return carry

    def set_order(k, carry):
        utt = jnp.int32(0)
        for j in range(n_utt):
            utt = utt + jnp.where(place_ref[j] == k, j, 0)
        order_ref[k] = utt
        return carry

    loads[0].wait()
    loads[1].wait()
    lax.fori_loop(0, n_utt, set_key, 0)
    lax.fori_loop(0, n_utt, set_place, 0)
    lax.fori_loop(0, n_utt, set_order, 0)
    loads[2].wait()
    for k in range(n_utt):
        sorted_ref[k] = enc_ref[order_ref[k]]
    pl.semaphore_wait(barrier, n_seq - 1)
    copies = []
    for hop in range(1, n_seq):
        peer = lax.rem(seq + hop, n_seq)
        copy = pltpu.make_async_remote_copy(
            src_ref=sorted_ref.at[pl.ds(peer * n_own, n_own)],
            dst_ref=frames_ref.at[seq],
            send_sem=send_sem.at[hop - 1],
            recv_sem=recv_sem.at[hop - 1],
            device_id={"seq": peer},
            device_id_type=MESH,
        )
        copy.start()
        copies.append(copy)
    frames_ref[pl.ds(seq, 1)] = sorted_ref[pl.ds(seq * n_own, n_own)][None]
    loads[3].wait()
    loads[4].wait()
    for j in range(n_own):
        own_pred_ref[j] = pred_ref[order_ref[seq * n_own + j]]
    own_pred = own_pred_ref[...]
    c_ref[...] = jnp.dot(own_pred.reshape(-1, own_pred.shape[-1]), w_pred_ref[...], preferred_element_type=F32).astype(BF16).astype(F32)
    loads[5].wait()
    w_out_t_ref[...] = w_out_ref[...].T
    loads[6].wait()
    for copy in copies:
        copy.wait()
    frames = frames_ref[...]
    a_ref[...] = jnp.dot(frames.reshape(-1, frames.shape[-1]), w_enc_ref[...], preferred_element_type=F32).astype(BF16).astype(F32)


def exchange(n_seq, frame_len, label_len, enc_loc, pred_loc, w_enc, w_pred, w_out):
    n_utt, t_loc, width = enc_loc.shape
    n_own = n_utt // n_seq
    n_upos = pred_loc.shape[1]
    joint, vocab = w_out.shape
    return pl.pallas_call(
        functools.partial(exchange_kernel, n_seq),
        out_shape=(
            pltpu.HBM((n_utt,), jnp.int32),
            pltpu.HBM((n_utt,), jnp.int32),
            pltpu.HBM((n_seq, n_own, t_loc, width), BF16),
            VMEM((n_seq * n_own * t_loc, joint), F32),
            VMEM((n_own * n_upos, joint), F32),
            VMEM((vocab, joint), BF16),
        ),
        in_specs=[pl.BlockSpec(memory_space=pltpu.HBM)] * 7,
        out_specs=(sspec(),) * 2 + (vspec(),) * 4,
        scratch_shapes=[
            pltpu.SMEM((n_utt,), jnp.int32),
            VMEM(enc_loc.shape, BF16),
            VMEM((n_own, n_upos, width), BF16),
            pltpu.SMEM((n_utt,), jnp.int32),
            pltpu.SMEM((n_utt,), jnp.int32),
        ]
        + [VMEM(v.shape, BF16) for v in (enc_loc, pred_loc, w_enc, w_pred, w_out)]
        + [
            pltpu.SemaphoreType.DMA((7,)),
            pltpu.SemaphoreType.DMA((n_seq - 1,)),
            pltpu.SemaphoreType.DMA((n_seq - 1,)),
        ],
        compiler_params=pltpu.CompilerParams(collective_id=0, has_side_effects=True, vmem_limit_bytes=40_000_000),
        name="exchange",
    )(*(in_hbm(v) for v in (frame_len, label_len, enc_loc, pred_loc, w_enc, w_pred, w_out)))


def logaddexp(x, y):
    top = jnp.maximum(x, y)
    return top + jnp.log(1.0 + jnp.exp(-jnp.abs(x - y)))


def lattice_kernel(n_own, n_frames, n_upos, seq_ref, order_ref, flen_ref, llen_ref, labels_ref, a_ref, c_ref, w_ref, wt_ref,
                   da_ref, dc_ref, gw_ref, loss_ref,
                   e_ref, h_ref, blank_ref, label_ref, alpha_ref, beta_ref, ids_ref, dact_ref, dpred_ref, work0, work1, dz_ref, dh_ref):
    vocab = w_ref.shape[1]
    joint = w_ref.shape[0]
    n_vt = vocab // LANES
    rows_g = SUB * SUB
    rows_t = GROUPS * rows_g
    n_diag = n_frames + n_upos - 1
    first = seq_ref[0] * n_own
    utts = [order_ref[first + b] for b in range(n_own)]
    lens_t = [flen_ref[utt] for utt in utts]
    lens_u = [llen_ref[utt] for utt in utts]
    blocks_t = [lax.div(n + SUB - 1, SUB) for n in lens_t]
    blocks_u = [lax.div(n + SUB, SUB) for n in lens_u]
    starts = [jnp.int32(0)]
    for b in range(n_own):
        starts.append(starts[-1] + blocks_t[b] * blocks_u[b])
    total = starts[-1]
    n_tiles = lax.div(total + GROUPS - 1, GROUPS)

    def decode(n):
        n = jnp.minimum(n, total - 1)
        b = jnp.int32(0)
        base, width = starts[0], blocks_u[0]
        for k in range(1, n_own):
            past = n >= starts[k]
            b = jnp.where(past, k, b)
            base = jnp.where(past, starts[k], base)
            width = jnp.where(past, blocks_u[k], width)
        ti = lax.div(n - base, width)
        return n, b, ti, n - base - ti * width

    pos_col = lax.broadcasted_iota(jnp.int32, (n_upos, n_upos - 1), 0)
    pos_row = lax.broadcasted_iota(jnp.int32, (n_upos, n_upos - 1), 1)
    for b in range(n_own):
        row = labels_ref[pl.ds(utts[b], 1), :].astype(F32)
        col = jnp.sum(jnp.where(pos_col == pos_row, row, 0.0), axis=1, keepdims=True)
        ids_ref[pl.ds(b * n_upos, n_upos), :] = jnp.broadcast_to(col, (n_upos, LANES)).astype(jnp.int32)

    blank_ref[...] = jnp.zeros_like(blank_ref)
    label_ref[...] = jnp.zeros_like(label_ref)
    gw_ref[...] = jnp.zeros_like(gw_ref)
    dact_ref[...] = jnp.zeros_like(dact_ref)
    dpred_ref[...] = jnp.zeros_like(dpred_ref)

    lane = lax.broadcasted_iota(jnp.int32, (SUB, LANES), 1)
    block_lane = lax.broadcasted_iota(jnp.int32, (BLOCK, LANES), 1)
    t_block = BLOCK // SUB
    works = (work0, work1)

    def tile_rows(i):
        return pl.ds(pl.multiple_of(jnp.clip(i, 0, n_tiles - 1) * rows_t, rows_t), rows_t)

    def tile_groups(i):
        return [decode(jnp.clip(i, 0, n_tiles - 1) * GROUPS + g) for g in range(GROUPS)]

    def pred_row(b, ui):
        return pl.ds(pl.multiple_of(b * n_upos + ui * SUB, SUB), SUB)

    def act_row(b, ti):
        return pl.ds(pl.multiple_of((ti * n_own + b) * SUB, SUB), SUB)

    def block_ids(b, ui):
        ids = ids_ref[pred_row(b, ui), :]
        return jnp.broadcast_to(ids[None], (t_block, SUB, LANES)).reshape(BLOCK, LANES)

    def cell_rows(ti, k, ui):
        return pl.ds(pl.multiple_of((n_diag - 1 - ti * SUB - k) * n_upos + ui * SUB, SUB), SUB)

    def make_hidden(i):
        first_row = jnp.clip(i, 0, n_tiles - 1) * rows_t
        for g, (n, b, ti, ui) in enumerate(tile_groups(i)):
            a8 = a_ref[act_row(b, ti), :]
            c8 = c_ref[pred_row(b, ui), :]
            h = jnp.tanh(a8[:, None, :] + c8[None, :, :]).reshape(rows_g, joint).astype(BF16)
            h_ref[pl.ds(pl.multiple_of(first_row + g * rows_g, rows_g), rows_g), :] = h

    def make_logits(i, z_ref):
        z_ref[...] = jnp.dot(h_ref[tile_rows(i), :], w_ref[...], preferred_element_type=F32)

    def make_softmax(i, z_ref):
        first_row = jnp.clip(i, 0, n_tiles - 1) * rows_t
        for g, (n, b, ti, ui) in enumerate(tile_groups(i)):
            ids = block_ids(b, ui)
            for r in range(0, rows_g, BLOCK):
                z = z_ref[g * rows_g + r:g * rows_g + r + BLOCK, :]
                top = jnp.max(z, axis=1, keepdims=True)
                e = jnp.exp(z - top)
                norm = jnp.sum(e, axis=1, keepdims=True)
                e_ref[pl.ds(pl.multiple_of(first_row + g * rows_g + r, BLOCK), BLOCK), :] = e
                log_norm = top + jnp.log(norm)
                picked = jnp.zeros((BLOCK, LANES), F32)
                for v in range(n_vt):
                    picked = picked + jnp.where(block_lane + v * LANES == ids, z[:, v * LANES:(v + 1) * LANES], 0.0)
                label = jnp.sum(picked, axis=1, keepdims=True) - log_norm
                blank = z[:, 0:1] - log_norm
                scale = 1.0 / norm
                rows = [cell_rows(ti, r // SUB + k, ui) for k in range(t_block)]
                old_blank = [blank_ref[at, :] for at in rows]
                old_label = [label_ref[at, :] for at in rows]
                for k, at in enumerate(rows):
                    sl = slice(k * SUB, (k + 1) * SUB)
                    blank_ref[at, :] = jnp.where(lane == b, blank[sl], jnp.where(lane == b + n_own, scale[sl], old_blank[k]))
                    label_ref[at, :] = jnp.where(lane == b, label[sl], old_label[k])

    make_hidden(0)
    make_logits(0, work0)
    make_hidden(1)

    def forward(j, carry):
        for half in range(2):
            i = 2 * j + half
            make_logits(i + 1, works[1 - half])
            make_softmax(i, works[half])
            make_hidden(i + 2)
        return carry

    lax.fori_loop(0, lax.div(n_tiles + 1, 2), forward, 0)

    upos = lax.broadcasted_iota(jnp.int32, (n_upos, LANES), 0)
    utt = lax.broadcasted_iota(jnp.int32, (n_upos, LANES), 1)
    t_end = jnp.ones((n_upos, LANES), jnp.int32)
    u_end = jnp.zeros((n_upos, LANES), jnp.int32)
    for b in range(n_own):
        t_end = jnp.where(utt == b, lens_t[b], t_end)
        u_end = jnp.where(utt == b, lens_u[b], u_end)

    def diagonal(d):
        return pl.ds((n_diag - 1 - d) * n_upos, n_upos, stride=n_upos + 1)

    def down(x):
        return jnp.where(upos == 0, NEG, pltpu.roll(x, 1, 0))

    def up(x):
        return jnp.where(upos == n_upos - 1, NEG, pltpu.roll(x, n_upos - 1, 0))

    def edge(d):
        return jnp.where((d - upos == t_end) & (upos == u_end), 0.0, NEG)

    last = functools.reduce(jnp.maximum, [t + u for t, u in zip(lens_t, lens_u)])
    reach = functools.reduce(jnp.maximum, [(t + u) * SUB - 1 for t, u in zip(blocks_t, blocks_u)])
    alpha0 = jnp.where(upos == 0, 0.0, NEG).astype(F32)
    beta0 = edge(last)
    alpha_ref[0] = alpha0
    beta_ref[last] = beta0

    def sweep(k, carry):
        alpha, beta = carry
        d = k + 1
        alpha = logaddexp(alpha + blank_ref[diagonal(k), :], down(alpha + label_ref[diagonal(k), :]))
        alpha = jnp.where(upos <= d, alpha, NEG)
        alpha_ref[d] = alpha
        d = last - 1 - k
        inside = (d - upos < t_end) & (upos <= u_end)
        beta = logaddexp(beta + blank_ref[diagonal(d), :], up(beta) + label_ref[diagonal(d), :])
        beta = jnp.where(inside, beta, edge(d))
        beta_ref[d] = beta
        return alpha, beta

    lax.fori_loop(0, last, sweep, (alpha0, beta0))
    log_prob = beta_ref[0][0:1, :]
    loss_ref[...] = jnp.broadcast_to(-log_prob, (SUB, LANES))

    def occupancy(d, carry):
        t = d - upos
        alpha = alpha_ref[d]
        after = beta_ref[d + 1]
        cell_ok = (t >= 0) & (t < t_end) & (upos <= u_end)
        blank = blank_ref[diagonal(d), :]
        q0 = jnp.where(cell_ok, jnp.exp(alpha + blank + after - log_prob), 0.0)
        q1 = jnp.where(cell_ok & (upos < u_end), jnp.exp(alpha + label_ref[diagonal(d), :] + up(after) - log_prob), 0.0)
        blank_ref[diagonal(d), :] = jnp.where(utt < n_own, q0, blank)
        label_ref[diagonal(d), :] = q1
        return carry

    lax.fori_loop(0, jnp.minimum(reach, n_diag), occupancy, 0)

    sub_row = lax.broadcasted_iota(jnp.int32, (SUB, LANES), 0)

    def group_rows(n, r, size):
        return pl.ds(pl.multiple_of(n * rows_g + r, size), size)

    def make_dz(index, g, n, b, ti, ui):
        keep = (lane == b) & (index < total)
        ids = block_ids(b, ui)
        for r in range(0, rows_g, BLOCK):
            q0s, q1s, scales = [], [], []
            for k in range(t_block):
                at = cell_rows(ti, r // SUB + k, ui)
                blank = blank_ref[at, :]
                q0s.append(jnp.where(keep, blank, 0.0))
                scales.append(jnp.where(lane == b + n_own, blank, 0.0))
                q1s.append(jnp.where(keep, label_ref[at, :], 0.0))
            q0 = jnp.sum(jnp.concatenate(q0s, axis=0), axis=1, keepdims=True)
            q1 = jnp.sum(jnp.concatenate(q1s, axis=0), axis=1, keepdims=True)
            scale = jnp.sum(jnp.concatenate(scales, axis=0), axis=1, keepdims=True) * (q0 + q1)
            for v in range(n_vt):
                cols = slice(v * LANES, (v + 1) * LANES)
                dz = e_ref[group_rows(n, r, BLOCK), cols] * scale
                if v == 0:
                    dz = dz - jnp.where(block_lane == 0, q0, 0.0)
                dz = dz - jnp.where(block_lane + v * LANES == ids, q1, 0.0)
                dz_ref[g * rows_g + r:g * rows_g + r + BLOCK, cols] = dz.astype(BF16)

    def make_sums(g, n, b, ti, ui):
        for v in range(joint // LANES):
            cols = slice(v * LANES, (v + 1) * LANES)
            h = h_ref[group_rows(n, 0, rows_g), cols].astype(F32)
            ds = dh_ref[g * rows_g:(g + 1) * rows_g, cols] * (1.0 - h * h)
            cube = [ds[k * SUB:(k + 1) * SUB] for k in range(SUB)]
            dpred_ref[pred_row(b, ui), cols] += ((cube[0] + cube[1]) + (cube[2] + cube[3])) + ((cube[4] + cube[5]) + (cube[6] + cube[7]))
            for shift in (4, 2, 1):
                low = sub_row % (2 * shift) < shift
                half = len(cube) // 2
                cube = [jnp.where(low, cube[k], cube[k + half]) + jnp.where(low, pltpu.roll(cube[k], SUB - shift, 0), pltpu.roll(cube[k + half], shift, 0)) for k in range(half)]
            dact_ref[act_row(b, ti), cols] += cube[0]

    wide_rows = WIDE * rows_g
    n_wide = lax.div(total + WIDE - 1, WIDE)

    def clear(i, carry):
        h_ref[pl.ds(pl.multiple_of(i * rows_t, rows_t), rows_t), :] = jnp.zeros((rows_t, joint), BF16)
        return carry

    lax.fori_loop(n_tiles, n_wide * (WIDE // GROUPS), clear, 0)

    def backward(i, carry):
        groups = [(i * WIDE + g, g, *decode(i * WIDE + g)) for g in range(WIDE)]
        for group in groups:
            make_dz(*group)
        dh_ref[...] = jnp.dot(dz_ref[...], wt_ref[...], preferred_element_type=F32)
        h = h_ref[pl.ds(pl.multiple_of(i * wide_rows, wide_rows), wide_rows), :]
        for v in range(0, n_vt, 2):
            part = lax.dot_general(h, dz_ref[:, v * LANES:(v + 2) * LANES], (((0,), (0,)), ((), ())), preferred_element_type=F32)
            gw_ref[v] += part[:, :LANES]
            gw_ref[v + 1] += part[:, LANES:]
        for group in groups:
            make_sums(*group[1:])
        return carry

    lax.fori_loop(0, n_wide, backward, 0)
    da_ref[...] = dact_ref[...].astype(BF16)
    dc_ref[...] = dpred_ref[...].astype(BF16)


def lattice(n_seq, seq_idx, order, frame_len, label_len, labels, act, pred, w_out, w_out_t, n_upos, t_loc):
    n_own = frame_len.shape[0] // n_seq
    n_frames = n_seq * t_loc
    joint, vocab = w_out.shape
    cells = n_own * n_frames * n_upos
    n_diag = n_frames + n_upos - 1
    lat_rows = (n_diag + n_upos - 1) * n_upos
    return pl.pallas_call(
        functools.partial(lattice_kernel, n_own, n_frames, n_upos),
        out_shape=(
            VMEM(act.shape, BF16),
            VMEM(pred.shape, BF16),
            VMEM((vocab // LANES, joint, LANES), F32),
            VMEM((SUB, LANES), F32),
        ),
        in_specs=[sspec()] * 4 + [vspec()] * 5,
        out_specs=(vspec(),) * 4,
        scratch_shapes=[
            VMEM((cells, vocab), F32),
            VMEM((cells, joint), BF16),
            VMEM((lat_rows, LANES), F32),
            VMEM((lat_rows, LANES), F32),
            VMEM((n_diag + 1, n_upos, LANES), F32),
            VMEM((n_diag + 1, n_upos, LANES), F32),
            VMEM((n_own * n_upos, LANES), jnp.int32),
            VMEM(act.shape, F32),
            VMEM(pred.shape, F32),
            VMEM((GROUPS * SUB * SUB, vocab), F32),
            VMEM((GROUPS * SUB * SUB, vocab), F32),
            VMEM((WIDE * SUB * SUB, vocab), BF16),
            VMEM((WIDE * SUB * SUB, joint), F32),
        ],
        compiler_params=pltpu.CompilerParams(vmem_limit_bytes=60_400_000),
        name="lattice",
    )(seq_idx, order, frame_len, label_len, labels, in_vmem(act), in_vmem(pred), w_out, in_vmem(w_out_t))


class Copies:
    def __init__(self, send_sem, recv_sem):
        self.sems = (send_sem, recv_sem)
        self.all = []

    def start(self, src, dst, device):
        k = len(self.all)
        copy = pltpu.make_async_remote_copy(src_ref=src, dst_ref=dst, send_sem=self.sems[0].at[k], recv_sem=self.sems[1].at[k], device_id=device, device_id_type=MESH)
        copy.start()
        self.all.append(copy)
        return copy

    def drain(self):
        for copy in self.all:
            copy.wait_send()


class Ring:
    def __init__(self, me, device):
        self.me = me
        self.right, self.left, self.across = [device(lax.rem(me + hop, RING)) for hop in (1, RING - 1, 2)]
        self.nxt, self.prv, self.opp = lax.rem(me + 1, RING), lax.rem(me + RING - 1, RING), lax.rem(me + 2, RING)


class Reduce:
    def __init__(self, copies, ring, acc, bufs):
        self.copies, self.ring, self.acc = copies, ring, acc
        self.pair, self.from_left, self.from_right = bufs

    def begin(self):
        c, r, acc = self.copies, self.ring, self.acc
        self.a1 = c.start(acc(r.opp, 0), self.pair.at[0], r.right)
        self.b1 = c.start(acc(r.opp, 1), self.pair.at[1], r.left)
        self.b2 = c.start(acc(r.nxt, 1), self.from_left.at[1], r.right)
        self.a2 = c.start(acc(r.prv, 0), self.from_right.at[0], r.left)

    def middle(self):
        c, r, acc = self.copies, self.ring, self.acc
        self.a1.wait_recv()
        add = acc(r.nxt, 0)
        add[...] = add[...] + self.pair[0]
        self.a3 = c.start(add, self.from_left.at[0], r.right)
        self.b1.wait_recv()
        add = acc(r.prv, 1)
        add[...] = add[...] + self.pair[1]
        self.b3 = c.start(add, self.from_right.at[1], r.left)

    def end(self, target):
        for copy in (self.b2, self.a3, self.a2, self.b3):
            copy.wait_recv()
        for half in range(2):
            target(half)[...] = self.acc(self.ring.me, half)[...] + self.from_left[half] + self.from_right[half]


class Gather:
    def __init__(self, copies, ring, out):
        self.copies, self.ring, self.out = copies, ring, out

    def send(self, k, half, device):
        return self.copies.start(self.out(k, half), self.out(k, half), device)

    def begin(self):
        r = self.ring
        self.ra = self.send(r.me, 0, r.right)
        self.lb = self.send(r.me, 1, r.left)
        self.rb = self.send(r.me, 1, r.right)
        self.la = self.send(r.me, 0, r.left)

    def relay(self):
        r = self.ring
        self.ra.wait_recv()
        self.ra2 = self.send(r.prv, 0, r.right)
        self.lb.wait_recv()
        self.lb2 = self.send(r.nxt, 1, r.left)
        self.rb.wait_recv()
        self.la.wait_recv()

    def finish(self):
        self.ra2.wait_recv()
        self.lb2.wait_recv()


class Swap:
    def __init__(self, copies, ring, acc, bufs):
        self.copies, self.ring, self.acc, self.bufs = copies, ring, acc, bufs

    def begin(self):
        r = self.ring
        sends = ((r.nxt, r.right), (r.prv, r.left), (r.opp, r.across))
        self.sent = [self.copies.start(self.acc(k), buf, device) for (k, device), buf in zip(sends, self.bufs)]

    def end(self, target):
        for copy in self.sent:
            copy.wait_recv()
        target[...] = (self.acc(self.ring.me)[...] + self.bufs[0][...]) + (self.bufs[1][...] + self.bufs[2][...])


class Spread:
    def __init__(self, copies, ring, out):
        self.copies, self.ring, self.out = copies, ring, out

    def begin(self):
        r = self.ring
        self.sent = [self.copies.start(self.out(r.me), self.out(r.me), device) for device in (r.right, r.left, r.across)]

    def finish(self):
        for copy in self.sent:
            copy.wait_recv()


def rows_of(start, size):
    return pl.ds(pl.multiple_of(start, SUB), size)


def combine_kernel(n_seq, order_hbm, place_hbm, frames_hbm, pred_hbm, w_enc_hbm, w_pred_hbm, da_ref, dc_ref, gw_ref, loss_ref,
                   ge_out, gp_out, gwe_out, gwp_out, gwo_out, loss_out,
                   order_ref, place_ref, frames_ref, pred_ref, w_enc_ref, w_pred_ref, load_sem, dc_out, grad_rows_ref, *scratch):
    sources = (frames_hbm, order_hbm, pred_hbm, w_enc_hbm, place_hbm, w_pred_hbm)
    landed = (frames_ref, order_ref, pred_ref, w_enc_ref, place_ref, w_pred_ref)
    loads = [pltpu.make_async_copy(src, dst, load_sem.at[k]) for k, (src, dst) in enumerate(zip(sources, landed))]
    for copy in loads:
        copy.start()
    (enc_acc, enc_pair, enc_mid, enc_y, enc_x, outs_acc, outs_pair, outs_mid, outs_1, outs_2, pred_acc, pred_y, rows_ref, ge_ref, send_sem, recv_sem) = unflatten(scratch)
    seq = lax.axis_index("seq")
    y = lax.axis_index("data")
    x = lax.div(seq, CORES)
    core = lax.rem(seq, CORES)
    mate = {"seq": x * CORES + 1 - core}
    ring_x = Ring(x, lambda k: {"seq": k * CORES + core})
    ring_y = Ring(y, lambda k: {"data": k})
    barrier = pltpu.get_barrier_semaphore()
    for hop in range(1, n_seq):
        pl.semaphore_signal(barrier, inc=1, device_id={"seq": lax.rem(seq + hop, n_seq)}, device_id_type=MESH)
    for dev in (ring_y.right, ring_y.left, ring_y.across):
        pl.semaphore_signal(barrier, inc=1, device_id=dev, device_id_type=MESH)

    n_blk = gw_ref.shape[0] // 2
    n_utt = n_seq * frames_ref.shape[1]
    n_upos = pred_ref.shape[1]
    enc_half = enc_acc.shape[0] // CORES
    out_half = gw_ref.shape[1] // CORES
    enc_q, out_q = enc_half // RING, out_half // RING
    enc_s = enc_q // RING
    enc_row, out_row = core * enc_half, core * out_half
    contract_rows = (((0,), (0,)), ((), ()))

    n_own = frames_ref.shape[1]
    dc_out[pl.ds(seq * n_own, n_own)] = dc_ref[...].reshape(n_own, n_upos, -1)
    pl.semaphore_wait(barrier, n_seq - 1 + RING - 1)

    copies = Copies(send_sem, recv_sem)

    def swap_out(part):
        blocks = pl.ds(part * n_blk, n_blk)
        return copies.start(gw_ref.at[blocks, rows_of((1 - core) * out_half, out_half), :], outs_pair[part], mate)

    dc_gather = Gather(copies, ring_x, lambda k, half: dc_out.at[pl.ds((k * CORES + core) * n_own + half * (n_own // 2), n_own // 2)])
    swap_1 = swap_out(1)
    dc_gather.begin()
    dc_whole = lambda dev: dc_out.at[pl.ds(dev * n_own, n_own)]
    dc_mate = [copies.start(dc_whole(seq), dc_whole(seq), mate)]
    loads[0].wait()
    frames = frames_ref[...]
    enc_acc[...] = lax.dot_general(frames.reshape(-1, frames.shape[-1]), da_ref[...], contract_rows, preferred_element_type=F32)
    swap_enc = copies.start(enc_acc.at[rows_of((1 - core) * enc_half, enc_half), :], enc_pair, mate)
    swap_0 = swap_out(0)

    def dc_pass(k):
        dc_mate.append(copies.start(dc_whole(k * CORES + core), dc_whole(k * CORES + core), mate))

    def add_out(part):
        outs_acc[part][...] = gw_ref[pl.ds(part * n_blk, n_blk), rows_of(out_row, out_half), :] + outs_pair[part][...]

    def out_first(part):
        return lambda k, half: outs_acc[part].at[:, rows_of(k * out_q + half * (out_q // 2), out_q // 2), :]

    def out_second(part):
        return lambda k: outs_mid[part].at[k]

    rings = ((ring_x, ring_y), (ring_y, ring_x))
    first = [Reduce(copies, rings[part][0], out_first(part), outs_1[part]) for part in range(2)]
    second = [Swap(copies, rings[part][1], out_second(part), outs_2[part]) for part in range(2)]
    enc_first = Reduce(copies, ring_y, lambda k, half: enc_acc.at[rows_of(enc_row + k * enc_q + half * (enc_q // 2), enc_q // 2), :], enc_y)
    enc_second = Swap(copies, ring_x, lambda k: enc_mid.at[rows_of(k * enc_s, enc_s), :], enc_x)
    pred_first = Swap(copies, ring_y, lambda k: pred_acc.at[rows_of(k * enc_s, enc_s), :], pred_y)

    def out_place(part, k1, k2, half, whole=False):
        start, size = out_row + k1 * out_q, out_q
        if not whole:
            start, size = start + half * (out_q // 2), out_q // 2
        return gwo_out.at[part * n_blk + k2 if k2 is not None else pl.ds(part * n_blk, n_blk), rows_of(start, size), :]

    def pair_place(part):
        ring1, ring2 = rings[part]
        return (
            Spread(copies, ring2, lambda k: out_place(part, ring1.me, k, 0, True)),
            Gather(copies, ring1, lambda k, half: out_place(part, k, None, half)),
        )

    a_g1, a_g2 = pair_place(0)
    b_g1, b_g2 = pair_place(1)
    enc_at = lambda k: gwe_out.at[rows_of(enc_row + y * enc_q + k * enc_s, enc_s), :]
    enc_g1 = Spread(copies, ring_x, enc_at)
    enc_g2 = Gather(copies, ring_y, lambda k, half: gwe_out.at[rows_of(enc_row + k * enc_q + half * (enc_q // 2), enc_q // 2), :])
    pred_at = lambda k: gwp_out.at[x, core, rows_of(k * enc_s, enc_s), :]
    pred_g1 = Spread(copies, ring_y, pred_at)
    pred_g2 = Gather(copies, ring_x, lambda k, half: gwp_out.at[k, core, pl.ds(half * (enc_q // 2), enc_q // 2), :])

    last = []

    def pass_on(ref):
        last.append(copies.start(ref, ref, mate))

    a_whole = lambda k: out_place(0, k, None, 0, True)
    b_whole = lambda k: out_place(1, k, None, 0, True)
    enc_whole = lambda k: gwe_out.at[rows_of(enc_row + k * enc_q, enc_q), :]
    pred_whole = lambda k: gwp_out.at[k, core]

    def widen(g1, g2, whole):
        g1.finish()
        g2.begin()
        pass_on(whole(g2.ring.me))

    def relay(g2, whole):
        g2.relay()
        pass_on(whole(g2.ring.prv))
        pass_on(whole(g2.ring.nxt))

    def close(g2, whole):
        g2.finish()
        pass_on(whole(g2.ring.opp))

    swap_1.wait_recv()
    add_out(1)
    first[1].begin()
    swap_enc.wait_recv()
    enc_acc[rows_of(enc_row, enc_half), :] = enc_acc[rows_of(enc_row, enc_half), :] + enc_pair[...]
    dc_gather.relay()
    dc_pass(ring_x.prv)
    dc_pass(ring_x.nxt)
    swap_0.wait_recv()
    add_out(0)
    first[0].begin()
    first[1].middle()
    enc_first.begin()

    loads[3].wait()
    ge = lax.dot_general(da_ref[...], w_enc_ref[...], (((1,), (1,)), ((), ())), preferred_element_type=F32)
    ge_ref[...] = ge.astype(BF16).reshape(ge_ref.shape)
    ge_out[pl.ds(seq, 1)] = ge_ref[pl.ds(seq, 1)]
    loss_out[pl.ds(seq, 1)] = loss_ref[...][None]
    loads[1].wait()
    loads[2].wait()
    for k in range(n_utt):
        rows_ref[k * n_upos:(k + 1) * n_upos, :] = pred_ref[order_ref[k], :, pl.ds(pl.multiple_of(x * LANES, LANES), LANES)]
    dc_gather.finish()
    dc_pass(ring_x.opp)
    first[0].middle()
    first[1].end(lambda half: outs_mid[1].at[:, pl.ds(half * (out_q // 2), out_q // 2), :])
    second[1].begin()

    for copy in dc_mate:
        copy.wait_recv()
    pred_part = lax.dot_general(rows_ref[...], dc_out[...].reshape(n_utt * n_upos, -1), contract_rows, preferred_element_type=F32)
    pred_acc[...] = jnp.where(core == 0, pred_part[:enc_q], pred_part[enc_q:])
    pred_first.begin()
    enc_first.middle()
    small = []
    for hop in range(1, n_seq):
        peer = lax.rem(seq + hop, n_seq)
        small.append(copies.start(ge_ref.at[peer], ge_out.at[seq], {"seq": peer}))
        small.append(copies.start(loss_ref, loss_out.at[seq], {"seq": peer}))
    first[0].end(lambda half: outs_mid[0].at[:, pl.ds(half * (out_q // 2), out_q // 2), :])
    second[0].begin()
    second[1].end(out_place(1, y, x, 0, True))
    b_g1.begin()
    enc_first.end(lambda half: enc_mid.at[pl.ds(half * (enc_q // 2), enc_q // 2), :])
    enc_second.begin()
    pred_first.end(pred_at(y))
    pred_g1.begin()
    second[0].end(out_place(0, x, y, 0, True))
    a_g1.begin()

    loads[4].wait()
    loads[5].wait()
    for i in range(n_utt):
        grad_rows_ref[i] = dc_out[place_ref[i]]
    widen(b_g1, b_g2, b_whole)
    enc_second.end(enc_at(x))
    enc_g1.begin()
    widen(pred_g1, pred_g2, pred_whole)
    half_utt = n_utt // 2

    def grad_rows(part):
        rows = grad_rows_ref[part * half_utt:(part + 1) * half_utt].reshape(half_utt * n_upos, -1)
        grads = lax.dot_general(rows, w_pred_ref[...], (((1,), (1,)), ((), ())), preferred_element_type=F32)
        gp_out[part * half_utt:(part + 1) * half_utt] = grads.reshape(half_utt, n_upos, -1)

    grad_rows(0)
    relay(b_g2, b_whole)
    widen(enc_g1, enc_g2, enc_whole)
    grad_rows(1)
    relay(pred_g2, pred_whole)
    widen(a_g1, a_g2, a_whole)
    close(b_g2, b_whole)
    relay(enc_g2, enc_whole)
    relay(a_g2, a_whole)
    close(pred_g2, pred_whole)
    close(enc_g2, enc_whole)
    close(a_g2, a_whole)
    for copy in small + last:
        copy.wait_recv()
    copies.drain()


N_COPIES = 3 + 10 + 14 + 3 * 6 + 4 * 6 + 4 * 6 + 16


def unflatten(refs):
    refs = list(refs)
    take = lambda n: [refs.pop(0) for _ in range(n)]
    enc_acc, enc_pair, enc_mid = take(3)
    enc_y, enc_x = take(3), take(3)
    outs = [(take(1)[0], take(1)[0], take(1)[0], take(3), take(3)) for _ in range(2)]
    outs_acc, outs_pair, outs_mid, outs_1, outs_2 = zip(*outs)
    pred_acc = refs.pop(0)
    pred_y = take(3)
    return (enc_acc, enc_pair, enc_mid, enc_y, enc_x, outs_acc, outs_pair, outs_mid, outs_1, outs_2, pred_acc, pred_y, *refs)


def combine(n_seq, order, place, frames, pred_loc, w_enc, w_pred, da, dc, gw, loss):
    width = frames.shape[-1]
    n_utt, n_upos, _ = pred_loc.shape
    joint = da.shape[-1]
    n_blk = gw.shape[0] // 2
    enc_half, out_half = width // CORES, joint // CORES
    enc_q, out_q = enc_half // RING, out_half // RING
    enc_s = enc_q // RING
    ring = lambda *shape: [VMEM(shape, F32)] * 3
    outs = [VMEM((n_blk, out_half, LANES), F32)] * 2 + [VMEM((n_blk, out_q, LANES), F32)] + ring(2, n_blk, out_q // 2, LANES) + ring(out_q, LANES)
    return pl.pallas_call(
        functools.partial(combine_kernel, n_seq),
        out_shape=(
            VMEM(frames.shape, BF16),
            VMEM((n_utt, n_upos, width), F32),
            VMEM((width, joint), F32),
            VMEM((RING, CORES, enc_q, joint), F32),
            VMEM(gw.shape, F32),
            VMEM((n_seq,) + loss.shape, F32),
        ),
        in_specs=[pl.BlockSpec(memory_space=pltpu.HBM)] * 6 + [vspec()] * 4,
        out_specs=(vspec(),) * 6,
        scratch_shapes=[pltpu.SMEM(order.shape, jnp.int32)] * 2
        + [VMEM(v.shape, v.dtype) for v in (frames, pred_loc, w_enc, w_pred)]
        + [pltpu.SemaphoreType.DMA((6,)), VMEM((n_utt, n_upos, joint), BF16), VMEM((n_utt, n_upos, joint), BF16)]
        + [VMEM((width, joint), F32), VMEM((enc_half, joint), F32), VMEM((enc_q, joint), F32)]
        + ring(2, enc_q // 2, joint)
        + ring(enc_s, joint)
        + outs
        + outs
        + [VMEM((enc_q, joint), F32)]
        + ring(enc_s, joint)
        + [
            VMEM((n_utt * n_upos, LANES), BF16),
            VMEM(frames.shape, BF16),
            pltpu.SemaphoreType.DMA((N_COPIES,)),
            pltpu.SemaphoreType.DMA((N_COPIES,)),
        ],
        compiler_params=pltpu.CompilerParams(collective_id=1, has_side_effects=True, vmem_limit_bytes=48_000_000),
        name="combine",
    )(*(in_hbm(v) for v in (order, place, frames, pred_loc, w_enc, w_pred)), *(in_vmem(v) for v in (da, dc, gw, loss)))


def output_kernel(place_hbm, losses_ref, ge_ref, gp_ref, gwe_ref, gwp_ref, gw_ref,
                  loss_out, ge_out, gp_out, gwe_out, gwp_out, gwo_out, place_ref, rows_ref, loss_ref, load_sem, sem):
    n_utt = gp_out.shape[0]
    n_own = ge_ref.shape[1]
    n_cols, _, col = gw_ref.shape
    loads = [pltpu.make_async_copy(place_hbm, place_ref, load_sem.at[0]), pltpu.make_async_copy(losses_ref.at[:, 0, :], rows_ref, load_sem.at[1])]
    for copy in loads:
        copy.start()
    pairs = [(gp_ref, gp_out), (gwe_ref, gwe_out)]
    pairs += [(gw_ref.at[k], gwo_out.at[:, pl.ds(k * col, col)]) for k in range(n_cols)]
    blocks, cores, size, _ = gwp_ref.shape
    pairs += [(gwp_ref.at[k // cores, k % cores], gwp_out.at[pl.ds(k * size, size), :]) for k in range(blocks * cores)]
    copies = [pltpu.make_async_copy(src, dst, sem.at[k]) for k, (src, dst) in enumerate(pairs)]
    for copy in copies:
        copy.start()
    for copy in loads:
        copy.wait()
    for i in range(n_utt):
        place = place_ref[i]
        dev = place // n_own
        own = place - dev * n_own
        loss_ref[i] = rows_ref[dev, own]
        copy = pltpu.make_async_copy(ge_ref.at[dev, own], ge_out.at[i], sem.at[len(copies)])
        copy.start()
        copies.append(copy)
    copy = pltpu.make_async_copy(loss_ref, loss_out, sem.at[len(copies)])
    copy.start()
    copies.append(copy)
    for copy in copies:
        copy.wait()


def outputs(place, losses, ge, gp, gwe, gwp, gw):
    n_seq, n_own, t_loc, width = ge.shape
    n_cols, joint, col = gw.shape
    hbm = pl.BlockSpec(memory_space=pltpu.HBM)
    return pl.pallas_call(
        output_kernel,
        out_shape=(
            jax.ShapeDtypeStruct((n_seq * n_own,), F32),
            jax.ShapeDtypeStruct((n_seq * n_own, t_loc, width), BF16),
            jax.ShapeDtypeStruct(gp.shape, F32),
            jax.ShapeDtypeStruct((width, joint), F32),
            jax.ShapeDtypeStruct((width, joint), F32),
            jax.ShapeDtypeStruct((joint, n_cols * col), F32),
        ),
        in_specs=[hbm] + [vspec()] * 6,
        out_specs=(hbm,) * 6,
        scratch_shapes=[
            pltpu.SMEM(place.shape, jnp.int32),
            pltpu.SMEM((n_seq, losses.shape[-1]), F32),
            pltpu.SMEM(place.shape, F32),
            pltpu.SemaphoreType.DMA((2,)),
            pltpu.SemaphoreType.DMA((2 + n_cols + RING * CORES + n_seq * n_own + 1,)),
        ],
        compiler_params=pltpu.CompilerParams(vmem_limit_bytes=48_000_000),
        name="outputs",
    )(in_hbm(place), *(in_vmem(v) for v in (losses, ge, gp, gwe, gwp, gw)))


def solution(mesh):
    n_seq = mesh.shape["seq"]
    utt_rows = P(("part", "data"))
    utt_mats = P(("part", "data"), None)
    utt_cube = P(("part", "data"), None, None)
    enc_spec = P(("part", "data"), "seq", None)
    weight_in = P(None, None)
    weight_out = P("part", None)

    def body(enc_loc, pred_loc, w_enc, w_pred, w_out, labels, frame_len, label_len):
        t_loc = enc_loc.shape[1]
        n_upos = pred_loc.shape[1]
        seq_idx = lax.axis_index("seq").astype(jnp.int32).reshape(1)
        order, place, frames, act, pred, w_out_t = exchange(n_seq, frame_len, label_len, enc_loc, pred_loc, w_enc, w_pred, w_out)
        da, dc, gw, loss = lattice(n_seq, seq_idx, order, frame_len, label_len, labels, act, pred, w_out, w_out_t, n_upos, t_loc)
        ge, gp, gwe, gwp, gw, losses = combine(n_seq, order, place, frames, pred_loc, w_enc, w_pred, da, dc, gw, loss)
        loss, grad_enc, grad_pred, gw_enc, gw_pred, gw_out = outputs(place, losses, ge, gp, gwe, gwp, gw)
        return loss, grad_enc, grad_pred, gw_enc, gw_pred, gw_out

    return jax.shard_map(body, mesh=mesh, in_specs=(enc_spec, utt_cube, weight_in, weight_in, weight_in, utt_mats, utt_rows, utt_rows), out_specs=(utt_rows, enc_spec, utt_cube, weight_out, weight_out, weight_out), check_vma=False)
```

```python
import functools

import jax
import jax.numpy as jnp
from jax import lax
from jax.experimental import pallas as pl
from jax.experimental.pallas import tpu as pltpu
from jax.sharding import PartitionSpec as P

NEG = -1e30
MESH = pl.DeviceIdType.MESH
VMEM = pltpu.VMEM
F32 = jnp.float32
BF16 = jnp.bfloat16
VMEM_LIMIT = 67_000_000
SUB = 8
LANES = 128
GROUPS = 4
WIDE = 8
BLOCK = 32
CORES = 2
RING = 4


def vspec():
    return pl.BlockSpec(memory_space=pltpu.VMEM)


def in_hbm(x):
    return pltpu.with_memory_space_constraint(x, pltpu.HBM)


def in_vmem(x):
    return pltpu.with_memory_space_constraint(x, pltpu.VMEM)


def sspec():
    return pl.BlockSpec(memory_space=pltpu.SMEM)


def exchange_kernel(n_seq, flen_hbm, llen_hbm, enc_hbm, pred_hbm, w_enc_hbm, w_pred_hbm, w_out_hbm,
                    order_ref, place_ref, frames_ref, a_ref, c_ref, w_out_t_ref,
                    key_ref, cost_ref, rank_ref, by_rank_ref, sorted_ref, own_pred_ref, flen_ref, llen_ref, enc_ref, pred_ref, w_enc_ref, w_pred_ref, w_out_ref, load_sem, send_sem, recv_sem):
    sources = (flen_hbm, llen_hbm, enc_hbm, pred_hbm, w_pred_hbm, w_out_hbm, w_enc_hbm)
    landed = (flen_ref, llen_ref, enc_ref, pred_ref, w_pred_ref, w_out_ref, w_enc_ref)
    loads = [pltpu.make_async_copy(src, dst, load_sem.at[k]) for k, (src, dst) in enumerate(zip(sources, landed))]
    for copy in loads:
        copy.start()
    seq = lax.axis_index("seq")
    n_utt = enc_ref.shape[0]
    n_own = n_utt // n_seq
    barrier = pltpu.get_barrier_semaphore()
    for hop in range(1, n_seq):
        pl.semaphore_signal(barrier, inc=1, device_id={"seq": lax.rem(seq + hop, n_seq)}, device_id_type=MESH)

    def set_key(i, carry):
        cost = ((flen_ref[i] + SUB - 1) // SUB) * ((llen_ref[i] + SUB) // SUB)
        cost_ref[i] = cost
        key_ref[i] = cost * n_utt + i
        return carry

    def set_rank(i, carry):
        key = key_ref[i]
        rank = jnp.int32(0)
        for j in range(n_utt):
            rank = rank + jnp.where(key_ref[j] > key, 1, 0)
        rank_ref[i] = rank
        return carry

    def invert(src_ref, dst_ref):
        def body(k, carry):
            found = jnp.int32(0)
            for j in range(n_utt):
                found = found + jnp.where(src_ref[j] == k, j, 0)
            dst_ref[k] = found
            return carry

        lax.fori_loop(0, n_utt, body, 0)

    loads[0].wait()
    loads[1].wait()
    lax.fori_loop(0, n_utt, set_key, 0)
    lax.fori_loop(0, n_utt, set_rank, 0)
    invert(rank_ref, by_rank_ref)
    sums = [jnp.int32(0)] * n_seq
    for deal in range(n_own):
        spots = []
        for d in range(n_seq):
            spot = jnp.int32(0)
            for e in range(n_seq):
                if e != d:
                    before = sums[e] <= sums[d] if e < d else sums[e] < sums[d]
                    spot = spot + jnp.where(before, 1, 0)
            spots.append(spot)
        for d in range(n_seq):
            utt = by_rank_ref[deal * n_seq + spots[d]]
            order_ref[d * n_own + deal] = utt
            sums[d] = sums[d] + cost_ref[utt]
    loads[2].wait()
    for k in range(n_utt):
        sorted_ref[k] = enc_ref[order_ref[k]]
    pl.semaphore_wait(barrier, n_seq - 1)
    copies = []
    for hop in range(1, n_seq):
        peer = lax.rem(seq + hop, n_seq)
        copy = pltpu.make_async_remote_copy(
            src_ref=sorted_ref.at[pl.ds(peer * n_own, n_own)],
            dst_ref=frames_ref.at[seq],
            send_sem=send_sem.at[hop - 1],
            recv_sem=recv_sem.at[hop - 1],
            device_id={"seq": peer},
            device_id_type=MESH,
        )
        copy.start()
        copies.append(copy)
    frames_ref[pl.ds(seq, 1)] = sorted_ref[pl.ds(seq * n_own, n_own)][None]
    loads[3].wait()
    loads[4].wait()
    for j in range(n_own):
        own_pred_ref[j] = pred_ref[order_ref[seq * n_own + j]]
    own_pred = own_pred_ref[...]
    c_ref[...] = jnp.dot(own_pred.reshape(-1, own_pred.shape[-1]), w_pred_ref[...], preferred_element_type=F32).astype(BF16).astype(F32)
    loads[5].wait()
    w_out_t_ref[...] = w_out_ref[...].T
    invert(order_ref, place_ref)
    loads[6].wait()
    for copy in copies:
        copy.wait()
    frames = frames_ref[...]
    a_ref[...] = jnp.dot(frames.reshape(-1, frames.shape[-1]), w_enc_ref[...], preferred_element_type=F32).astype(BF16).astype(F32)


def exchange(n_seq, frame_len, label_len, enc_loc, pred_loc, w_enc, w_pred, w_out):
    n_utt, t_loc, width = enc_loc.shape
    n_own = n_utt // n_seq
    n_upos = pred_loc.shape[1]
    joint, vocab = w_out.shape
    return pl.pallas_call(
        functools.partial(exchange_kernel, n_seq),
        out_shape=(
            pltpu.HBM((n_utt,), jnp.int32),
            pltpu.HBM((n_utt,), jnp.int32),
            pltpu.HBM((n_seq, n_own, t_loc, width), BF16),
            VMEM((n_seq * n_own * t_loc, joint), F32),
            VMEM((n_own * n_upos, joint), F32),
            VMEM((vocab, joint), BF16),
        ),
        in_specs=[pl.BlockSpec(memory_space=pltpu.HBM)] * 7,
        out_specs=(sspec(),) * 2 + (vspec(),) * 4,
        scratch_shapes=[
            pltpu.SMEM((n_utt,), jnp.int32),
            pltpu.SMEM((n_utt,), jnp.int32),
            pltpu.SMEM((n_utt,), jnp.int32),
            pltpu.SMEM((n_utt,), jnp.int32),
            VMEM(enc_loc.shape, BF16),
            VMEM((n_own, n_upos, width), BF16),
            pltpu.SMEM((n_utt,), jnp.int32),
            pltpu.SMEM((n_utt,), jnp.int32),
        ]
        + [VMEM(v.shape, BF16) for v in (enc_loc, pred_loc, w_enc, w_pred, w_out)]
        + [
            pltpu.SemaphoreType.DMA((7,)),
            pltpu.SemaphoreType.DMA((n_seq - 1,)),
            pltpu.SemaphoreType.DMA((n_seq - 1,)),
        ],
        compiler_params=pltpu.CompilerParams(collective_id=0, has_side_effects=True, vmem_limit_bytes=40_000_000),
        name="exchange",
    )(*(in_hbm(v) for v in (frame_len, label_len, enc_loc, pred_loc, w_enc, w_pred, w_out)))


def logaddexp(x, y):
    top = jnp.maximum(x, y)
    return top + jnp.log(1.0 + jnp.exp(-jnp.abs(x - y)))


def lattice_kernel(n_own, n_frames, n_upos, seq_ref, order_ref, flen_ref, llen_ref, labels_ref, a_ref, c_ref, w_ref, wt_ref,
                   da_ref, dc_ref, gw_ref, loss_ref,
                   e_ref, h_ref, blank_ref, label_ref, alpha_ref, beta_ref, ids_ref, dact_ref, dpred_ref, work0, work1, dz_ref, dh_ref):
    vocab = w_ref.shape[1]
    joint = w_ref.shape[0]
    n_vt = vocab // LANES
    rows_g = SUB * SUB
    rows_t = GROUPS * rows_g
    n_diag = n_frames + n_upos - 1
    first = seq_ref[0] * n_own
    utts = [order_ref[first + b] for b in range(n_own)]
    lens_t = [flen_ref[utt] for utt in utts]
    lens_u = [llen_ref[utt] for utt in utts]
    blocks_t = [lax.div(n + SUB - 1, SUB) for n in lens_t]
    blocks_u = [lax.div(n + SUB, SUB) for n in lens_u]
    starts = [jnp.int32(0)]
    for b in range(n_own):
        starts.append(starts[-1] + blocks_t[b] * blocks_u[b])
    total = starts[-1]
    n_tiles = lax.div(total + GROUPS - 1, GROUPS)

    def decode(n):
        n = jnp.minimum(n, total - 1)
        b = jnp.int32(0)
        base, width = starts[0], blocks_u[0]
        for k in range(1, n_own):
            past = n >= starts[k]
            b = jnp.where(past, k, b)
            base = jnp.where(past, starts[k], base)
            width = jnp.where(past, blocks_u[k], width)
        ti = lax.div(n - base, width)
        return n, b, ti, n - base - ti * width

    pos_col = lax.broadcasted_iota(jnp.int32, (n_upos, n_upos - 1), 0)
    pos_row = lax.broadcasted_iota(jnp.int32, (n_upos, n_upos - 1), 1)
    for b in range(n_own):
        row = labels_ref[pl.ds(utts[b], 1), :].astype(F32)
        col = jnp.sum(jnp.where(pos_col == pos_row, row, 0.0), axis=1, keepdims=True)
        ids_ref[pl.ds(b * n_upos, n_upos), :] = jnp.broadcast_to(col, (n_upos, LANES)).astype(jnp.int32)

    blank_ref[...] = jnp.zeros_like(blank_ref)
    label_ref[...] = jnp.zeros_like(label_ref)
    gw_ref[...] = jnp.zeros_like(gw_ref)
    dact_ref[...] = jnp.zeros_like(dact_ref)
    dpred_ref[...] = jnp.zeros_like(dpred_ref)

    lane = lax.broadcasted_iota(jnp.int32, (SUB, LANES), 1)
    block_lane = lax.broadcasted_iota(jnp.int32, (BLOCK, LANES), 1)
    t_block = BLOCK // SUB
    works = (work0, work1)

    def tile_rows(i):
        return pl.ds(pl.multiple_of(jnp.clip(i, 0, n_tiles - 1) * rows_t, rows_t), rows_t)

    def tile_groups(i):
        return [decode(jnp.clip(i, 0, n_tiles - 1) * GROUPS + g) for g in range(GROUPS)]

    def pred_row(b, ui):
        return pl.ds(pl.multiple_of(b * n_upos + ui * SUB, SUB), SUB)

    def act_row(b, ti):
        return pl.ds(pl.multiple_of((ti * n_own + b) * SUB, SUB), SUB)

    def block_ids(b, ui):
        ids = ids_ref[pred_row(b, ui), :]
        return jnp.broadcast_to(ids[None], (t_block, SUB, LANES)).reshape(BLOCK, LANES)

    def cell_rows(ti, k, ui):
        return pl.ds(pl.multiple_of((n_diag - 1 - ti * SUB - k) * n_upos + ui * SUB, SUB), SUB)

    def make_hidden(i):
        first_row = jnp.clip(i, 0, n_tiles - 1) * rows_t
        for g, (n, b, ti, ui) in enumerate(tile_groups(i)):
            a8 = a_ref[act_row(b, ti), :]
            c8 = c_ref[pred_row(b, ui), :]
            h = jnp.tanh(a8[:, None, :] + c8[None, :, :]).reshape(rows_g, joint).astype(BF16)
            h_ref[pl.ds(pl.multiple_of(first_row + g * rows_g, rows_g), rows_g), :] = h

    def make_logits(i, z_ref):
        z_ref[...] = jnp.dot(h_ref[tile_rows(i), :], w_ref[...], preferred_element_type=F32)

    def make_softmax(i, z_ref):
        first_row = jnp.clip(i, 0, n_tiles - 1) * rows_t
        for g, (n, b, ti, ui) in enumerate(tile_groups(i)):
            ids = block_ids(b, ui)
            for r in range(0, rows_g, BLOCK):
                z = z_ref[g * rows_g + r:g * rows_g + r + BLOCK, :]
                top = jnp.max(z, axis=1, keepdims=True)
                e = jnp.exp(z - top)
                norm = jnp.sum(e, axis=1, keepdims=True)
                e_ref[pl.ds(pl.multiple_of(first_row + g * rows_g + r, BLOCK), BLOCK), :] = e
                log_norm = top + jnp.log(norm)
                picked = jnp.zeros((BLOCK, LANES), F32)
                for v in range(n_vt):
                    picked = picked + jnp.where(block_lane + v * LANES == ids, z[:, v * LANES:(v + 1) * LANES], 0.0)
                label = jnp.sum(picked, axis=1, keepdims=True) - log_norm
                blank = z[:, 0:1] - log_norm
                scale = 1.0 / norm
                rows = [cell_rows(ti, r // SUB + k, ui) for k in range(t_block)]
                old_blank = [blank_ref[at, :] for at in rows]
                old_label = [label_ref[at, :] for at in rows]
                for k, at in enumerate(rows):
                    sl = slice(k * SUB, (k + 1) * SUB)
                    blank_ref[at, :] = jnp.where(lane == b, blank[sl], jnp.where(lane == b + n_own, scale[sl], old_blank[k]))
                    label_ref[at, :] = jnp.where(lane == b, label[sl], old_label[k])

    make_hidden(0)
    make_logits(0, work0)
    make_hidden(1)

    def forward(j, carry):
        for half in range(2):
            i = 2 * j + half
            make_logits(i + 1, works[1 - half])
            make_softmax(i, works[half])
            make_hidden(i + 2)
        return carry

    def forward_tail(_, carry):
        make_softmax(n_tiles - 1, work0)
        return carry

    lax.fori_loop(0, lax.div(n_tiles, 2), forward, 0)
    lax.fori_loop(0, lax.rem(n_tiles, 2), forward_tail, 0)

    upos = lax.broadcasted_iota(jnp.int32, (n_upos, LANES), 0)
    utt = lax.broadcasted_iota(jnp.int32, (n_upos, LANES), 1)
    t_end = jnp.ones((n_upos, LANES), jnp.int32)
    u_end = jnp.zeros((n_upos, LANES), jnp.int32)
    for b in range(n_own):
        t_end = jnp.where(utt == b, lens_t[b], t_end)
        u_end = jnp.where(utt == b, lens_u[b], u_end)

    def diagonal(d):
        return pl.ds((n_diag - 1 - d) * n_upos, n_upos, stride=n_upos + 1)

    def down(x):
        return jnp.where(upos == 0, NEG, pltpu.roll(x, 1, 0))

    def up(x):
        return jnp.where(upos == n_upos - 1, NEG, pltpu.roll(x, n_upos - 1, 0))

    def edge(d):
        return jnp.where((d - upos == t_end) & (upos == u_end), 0.0, NEG)

    last = functools.reduce(jnp.maximum, [t + u for t, u in zip(lens_t, lens_u)])
    reach = functools.reduce(jnp.maximum, [(t + u) * SUB - 1 for t, u in zip(blocks_t, blocks_u)])
    alpha0 = jnp.where(upos == 0, 0.0, NEG).astype(F32)
    beta0 = edge(last)
    alpha_ref[0] = alpha0
    beta_ref[last] = beta0

    def sweep(k, carry):
        alpha, beta = carry
        d = k + 1
        alpha = logaddexp(alpha + blank_ref[diagonal(k), :], down(alpha + label_ref[diagonal(k), :]))
        alpha = jnp.where(upos <= d, alpha, NEG)
        alpha_ref[d] = alpha
        d = last - 1 - k
        inside = (d - upos < t_end) & (upos <= u_end)
        beta = logaddexp(beta + blank_ref[diagonal(d), :], up(beta) + label_ref[diagonal(d), :])
        beta = jnp.where(inside, beta, edge(d))
        beta_ref[d] = beta
        return alpha, beta

    lax.fori_loop(0, last, sweep, (alpha0, beta0))
    log_prob = beta_ref[0][0:1, :]
    loss_ref[...] = jnp.broadcast_to(-log_prob, (SUB, LANES))

    def occupancy(d, carry):
        t = d - upos
        alpha = alpha_ref[d]
        after = beta_ref[d + 1]
        cell_ok = (t >= 0) & (t < t_end) & (upos <= u_end)
        blank = blank_ref[diagonal(d), :]
        q0 = jnp.where(cell_ok, jnp.exp(alpha + blank + after - log_prob), 0.0)
        q1 = jnp.where(cell_ok & (upos < u_end), jnp.exp(alpha + label_ref[diagonal(d), :] + up(after) - log_prob), 0.0)
        blank_ref[diagonal(d), :] = jnp.where(utt < n_own, q0, blank)
        label_ref[diagonal(d), :] = q1
        return carry

    lax.fori_loop(0, jnp.minimum(reach, n_diag), occupancy, 0)

    sub_row = lax.broadcasted_iota(jnp.int32, (SUB, LANES), 0)

    def group_rows(n, r, size):
        return pl.ds(pl.multiple_of(n * rows_g + r, size), size)

    def make_dz(index, g, n, b, ti, ui):
        keep = (lane == b) & (index < total)
        ids = block_ids(b, ui)
        for r in range(0, rows_g, BLOCK):
            q0s, q1s, scales = [], [], []
            for k in range(t_block):
                at = cell_rows(ti, r // SUB + k, ui)
                blank = blank_ref[at, :]
                q0s.append(jnp.where(keep, blank, 0.0))
                scales.append(jnp.where(lane == b + n_own, blank, 0.0))
                q1s.append(jnp.where(keep, label_ref[at, :], 0.0))
            q0 = jnp.sum(jnp.concatenate(q0s, axis=0), axis=1, keepdims=True)
            q1 = jnp.sum(jnp.concatenate(q1s, axis=0), axis=1, keepdims=True)
            scale = jnp.sum(jnp.concatenate(scales, axis=0), axis=1, keepdims=True) * (q0 + q1)
            for v in range(n_vt):
                cols = slice(v * LANES, (v + 1) * LANES)
                dz = e_ref[group_rows(n, r, BLOCK), cols] * scale
                if v == 0:
                    dz = dz - jnp.where(block_lane == 0, q0, 0.0)
                dz = dz - jnp.where(block_lane + v * LANES == ids, q1, 0.0)
                dz_ref[g * rows_g + r:g * rows_g + r + BLOCK, cols] = dz.astype(BF16)

    def make_sums(g, n, b, ti, ui):
        for v in range(joint // LANES):
            cols = slice(v * LANES, (v + 1) * LANES)
            h = h_ref[group_rows(n, 0, rows_g), cols].astype(F32)
            ds = dh_ref[g * rows_g:(g + 1) * rows_g, cols] * (1.0 - h * h)
            cube = [ds[k * SUB:(k + 1) * SUB] for k in range(SUB)]
            dpred_ref[pred_row(b, ui), cols] += ((cube[0] + cube[1]) + (cube[2] + cube[3])) + ((cube[4] + cube[5]) + (cube[6] + cube[7]))
            for shift in (4, 2, 1):
                low = sub_row % (2 * shift) < shift
                half = len(cube) // 2
                cube = [jnp.where(low, cube[k], cube[k + half]) + jnp.where(low, pltpu.roll(cube[k], SUB - shift, 0), pltpu.roll(cube[k + half], shift, 0)) for k in range(half)]
            dact_ref[act_row(b, ti), cols] += cube[0]

    def backward_tile(start, width):
        groups = [(start + g, g, *decode(start + g)) for g in range(width)]
        rows = width * rows_g
        for group in groups:
            make_dz(*group)
        dh_ref[:rows] = jnp.dot(dz_ref[:rows], wt_ref[...], preferred_element_type=F32)
        h = h_ref[pl.ds(pl.multiple_of(start * rows_g, GROUPS * rows_g), rows), :]
        for v in range(0, n_vt, 2):
            part = lax.dot_general(h, dz_ref[:rows, v * LANES:(v + 2) * LANES], (((0,), (0,)), ((), ())), preferred_element_type=F32)
            gw_ref[v] += part[:, :LANES]
            gw_ref[v + 1] += part[:, LANES:]
        for group in groups:
            make_sums(*group[1:])

    def backward(i, carry):
        backward_tile(i * WIDE, WIDE)
        return carry

    n_wide = lax.div(total + WIDE - GROUPS - 1, WIDE)

    def backward_tail(_, carry):
        backward_tile(n_wide * WIDE, GROUPS)
        return carry

    lax.fori_loop(0, n_wide, backward, 0)
    lax.fori_loop(0, jnp.where(total > n_wide * WIDE, 1, 0), backward_tail, 0)
    da_ref[...] = dact_ref[...].astype(BF16)
    dc_ref[...] = dpred_ref[...].astype(BF16)


def lattice(n_seq, seq_idx, order, frame_len, label_len, labels, act, pred, w_out, w_out_t, n_upos, t_loc):
    n_own = frame_len.shape[0] // n_seq
    n_frames = n_seq * t_loc
    joint, vocab = w_out.shape
    cells = n_own * n_frames * n_upos
    n_diag = n_frames + n_upos - 1
    lat_rows = (n_diag + n_upos - 1) * n_upos
    return pl.pallas_call(
        functools.partial(lattice_kernel, n_own, n_frames, n_upos),
        out_shape=(
            VMEM(act.shape, BF16),
            VMEM(pred.shape, BF16),
            VMEM((vocab // LANES, joint, LANES), F32),
            VMEM((SUB, LANES), F32),
        ),
        in_specs=[sspec()] * 4 + [vspec()] * 5,
        out_specs=(vspec(),) * 4,
        scratch_shapes=[
            VMEM((cells, vocab), F32),
            VMEM((cells, joint), BF16),
            VMEM((lat_rows, LANES), F32),
            VMEM((lat_rows, LANES), F32),
            VMEM((n_diag + 1, n_upos, LANES), F32),
            VMEM((n_diag + 1, n_upos, LANES), F32),
            VMEM((n_own * n_upos, LANES), jnp.int32),
            VMEM(act.shape, F32),
            VMEM(pred.shape, F32),
            VMEM((GROUPS * SUB * SUB, vocab), F32),
            VMEM((GROUPS * SUB * SUB, vocab), F32),
            VMEM((WIDE * SUB * SUB, vocab), BF16),
            VMEM((WIDE * SUB * SUB, joint), F32),
        ],
        compiler_params=pltpu.CompilerParams(vmem_limit_bytes=60_400_000),
        name="lattice",
    )(seq_idx, order, frame_len, label_len, labels, in_vmem(act), in_vmem(pred), w_out, in_vmem(w_out_t))


class Copies:
    def __init__(self, send_sem, recv_sem):
        self.sems = (send_sem, recv_sem)
        self.all = []

    def start(self, src, dst, device):
        k = len(self.all)
        copy = pltpu.make_async_remote_copy(src_ref=src, dst_ref=dst, send_sem=self.sems[0].at[k], recv_sem=self.sems[1].at[k], device_id=device, device_id_type=MESH)
        copy.start()
        self.all.append(copy)
        return copy

    def drain(self):
        for copy in self.all:
            copy.wait_send()


class Ring:
    def __init__(self, me, device):
        self.me = me
        self.right, self.left, self.across = [device(lax.rem(me + hop, RING)) for hop in (1, RING - 1, 2)]
        self.nxt, self.prv, self.opp = lax.rem(me + 1, RING), lax.rem(me + RING - 1, RING), lax.rem(me + 2, RING)


class Reduce:
    def __init__(self, copies, ring, acc, bufs):
        self.copies, self.ring, self.acc = copies, ring, acc
        self.pair, self.from_left, self.from_right = bufs

    def begin(self):
        c, r, acc = self.copies, self.ring, self.acc
        self.a1 = c.start(acc(r.opp, 0), self.pair.at[0], r.right)
        self.b1 = c.start(acc(r.opp, 1), self.pair.at[1], r.left)
        self.b2 = c.start(acc(r.nxt, 1), self.from_left.at[1], r.right)
        self.a2 = c.start(acc(r.prv, 0), self.from_right.at[0], r.left)

    def middle(self):
        c, r, acc = self.copies, self.ring, self.acc
        self.a1.wait_recv()
        add = acc(r.nxt, 0)
        add[...] = add[...] + self.pair[0]
        self.a3 = c.start(add, self.from_left.at[0], r.right)
        self.b1.wait_recv()
        add = acc(r.prv, 1)
        add[...] = add[...] + self.pair[1]
        self.b3 = c.start(add, self.from_right.at[1], r.left)

    def end(self, target):
        for copy in (self.b2, self.a3, self.a2, self.b3):
            copy.wait_recv()
        for half in range(2):
            target(half)[...] = self.acc(self.ring.me, half)[...] + self.from_left[half] + self.from_right[half]


class Gather:
    def __init__(self, copies, ring, out):
        self.copies, self.ring, self.out = copies, ring, out

    def send(self, k, half, device):
        return self.copies.start(self.out(k, half), self.out(k, half), device)

    def begin(self):
        r = self.ring
        self.ra = self.send(r.me, 0, r.right)
        self.lb = self.send(r.me, 1, r.left)
        self.rb = self.send(r.me, 1, r.right)
        self.la = self.send(r.me, 0, r.left)

    def relay(self):
        r = self.ring
        self.ra.wait_recv()
        self.ra2 = self.send(r.prv, 0, r.right)
        self.lb.wait_recv()
        self.lb2 = self.send(r.nxt, 1, r.left)
        self.rb.wait_recv()
        self.la.wait_recv()

    def finish(self):
        self.ra2.wait_recv()
        self.lb2.wait_recv()


class Swap:
    def __init__(self, copies, ring, acc, bufs):
        self.copies, self.ring, self.acc, self.bufs = copies, ring, acc, bufs

    def begin(self):
        r = self.ring
        sends = ((r.nxt, r.right), (r.prv, r.left), (r.opp, r.across))
        self.sent = [self.copies.start(self.acc(k), buf, device) for (k, device), buf in zip(sends, self.bufs)]

    def end(self, target):
        for copy in self.sent:
            copy.wait_recv()
        target[...] = (self.acc(self.ring.me)[...] + self.bufs[0][...]) + (self.bufs[1][...] + self.bufs[2][...])


class Spread:
    def __init__(self, copies, ring, out):
        self.copies, self.ring, self.out = copies, ring, out

    def begin(self):
        r = self.ring
        self.sent = [self.copies.start(self.out(r.me), self.out(r.me), device) for device in (r.right, r.left, r.across)]

    def finish(self):
        for copy in self.sent:
            copy.wait_recv()


def rows_of(start, size):
    return pl.ds(pl.multiple_of(start, SUB), size)


def combine_kernel(n_seq, order_hbm, place_hbm, frames_hbm, pred_hbm, w_enc_hbm, w_pred_hbm, da_ref, dc_ref, gw_ref, loss_ref,
                   ge_out, gp_out, gwe_out, gwp_out, gwo_out, loss_out,
                   order_ref, place_ref, frames_ref, pred_ref, w_enc_ref, w_pred_ref, load_sem, dc_out, grad_rows_ref, *scratch):
    sources = (frames_hbm, order_hbm, pred_hbm, w_enc_hbm, place_hbm, w_pred_hbm)
    landed = (frames_ref, order_ref, pred_ref, w_enc_ref, place_ref, w_pred_ref)
    loads = [pltpu.make_async_copy(src, dst, load_sem.at[k]) for k, (src, dst) in enumerate(zip(sources, landed))]
    for copy in loads:
        copy.start()
    (enc_acc, enc_pair, enc_mid, enc_y, enc_x, outs_acc, outs_pair, outs_mid, outs_1, outs_2, pred_acc, pred_y, rows_ref, ge_ref, send_sem, recv_sem) = unflatten(scratch)
    seq = lax.axis_index("seq")
    y = lax.axis_index("data")
    x = lax.div(seq, CORES)
    core = lax.rem(seq, CORES)
    mate = {"seq": x * CORES + 1 - core}
    ring_x = Ring(x, lambda k: {"seq": k * CORES + core})
    ring_y = Ring(y, lambda k: {"data": k})
    barrier = pltpu.get_barrier_semaphore()
    for hop in range(1, n_seq):
        pl.semaphore_signal(barrier, inc=1, device_id={"seq": lax.rem(seq + hop, n_seq)}, device_id_type=MESH)
    for dev in (ring_y.right, ring_y.left, ring_y.across):
        pl.semaphore_signal(barrier, inc=1, device_id=dev, device_id_type=MESH)

    n_blk = gw_ref.shape[0] // 2
    n_utt = n_seq * frames_ref.shape[1]
    n_upos = pred_ref.shape[1]
    enc_half = enc_acc.shape[0] // CORES
    out_half = gw_ref.shape[1] // CORES
    enc_q, out_q = enc_half // RING, out_half // RING
    enc_s = enc_q // RING
    enc_row, out_row = core * enc_half, core * out_half
    contract_rows = (((0,), (0,)), ((), ()))

    n_own = frames_ref.shape[1]
    dc_out[pl.ds(seq * n_own, n_own)] = dc_ref[...].reshape(n_own, n_upos, -1)
    pl.semaphore_wait(barrier, n_seq - 1 + RING - 1)

    copies = Copies(send_sem, recv_sem)

    def swap_out(part):
        blocks = pl.ds(part * n_blk, n_blk)
        return copies.start(gw_ref.at[blocks, rows_of((1 - core) * out_half, out_half), :], outs_pair[part], mate)

    dc_gather = Gather(copies, ring_x, lambda k, half: dc_out.at[pl.ds((k * CORES + core) * n_own + half * (n_own // 2), n_own // 2)])
    swap_1 = swap_out(1)
    dc_gather.begin()
    dc_whole = lambda dev: dc_out.at[pl.ds(dev * n_own, n_own)]
    dc_mate = [copies.start(dc_whole(seq), dc_whole(seq), mate)]
    loads[0].wait()
    frames = frames_ref[...]
    enc_acc[...] = lax.dot_general(frames.reshape(-1, frames.shape[-1]), da_ref[...], contract_rows, preferred_element_type=F32)
    swap_enc = copies.start(enc_acc.at[rows_of((1 - core) * enc_half, enc_half), :], enc_pair, mate)
    swap_0 = swap_out(0)

    def dc_pass(k):
        dc_mate.append(copies.start(dc_whole(k * CORES + core), dc_whole(k * CORES + core), mate))

    def add_out(part):
        outs_acc[part][...] = gw_ref[pl.ds(part * n_blk, n_blk), rows_of(out_row, out_half), :] + outs_pair[part][...]

    def out_first(part):
        return lambda k, half: outs_acc[part].at[:, rows_of(k * out_q + half * (out_q // 2), out_q // 2), :]

    def out_second(part):
        return lambda k: outs_mid[part].at[k]

    rings = ((ring_x, ring_y), (ring_y, ring_x))
    first = [Reduce(copies, rings[part][0], out_first(part), outs_1[part]) for part in range(2)]
    second = [Swap(copies, rings[part][1], out_second(part), outs_2[part]) for part in range(2)]
    enc_first = Reduce(copies, ring_y, lambda k, half: enc_acc.at[rows_of(enc_row + k * enc_q + half * (enc_q // 2), enc_q // 2), :], enc_y)
    enc_second = Swap(copies, ring_x, lambda k: enc_mid.at[rows_of(k * enc_s, enc_s), :], enc_x)
    pred_first = Swap(copies, ring_y, lambda k: pred_acc.at[rows_of(k * enc_s, enc_s), :], pred_y)

    def out_place(part, k1, k2, half, whole=False):
        start, size = out_row + k1 * out_q, out_q
        if not whole:
            start, size = start + half * (out_q // 2), out_q // 2
        return gwo_out.at[part * n_blk + k2 if k2 is not None else pl.ds(part * n_blk, n_blk), rows_of(start, size), :]

    def pair_place(part):
        ring1, ring2 = rings[part]
        return (
            Spread(copies, ring2, lambda k: out_place(part, ring1.me, k, 0, True)),
            Gather(copies, ring1, lambda k, half: out_place(part, k, None, half)),
        )

    a_g1, a_g2 = pair_place(0)
    b_g1, b_g2 = pair_place(1)
    enc_at = lambda k: gwe_out.at[rows_of(enc_row + y * enc_q + k * enc_s, enc_s), :]
    enc_g1 = Spread(copies, ring_x, enc_at)
    enc_g2 = Gather(copies, ring_y, lambda k, half: gwe_out.at[rows_of(enc_row + k * enc_q + half * (enc_q // 2), enc_q // 2), :])
    pred_at = lambda k: gwp_out.at[x, core, rows_of(k * enc_s, enc_s), :]
    pred_g1 = Spread(copies, ring_y, pred_at)
    pred_g2 = Gather(copies, ring_x, lambda k, half: gwp_out.at[k, core, pl.ds(half * (enc_q // 2), enc_q // 2), :])

    last = []

    def pass_on(ref):
        last.append(copies.start(ref, ref, mate))

    a_whole = lambda k: out_place(0, k, None, 0, True)
    b_whole = lambda k: out_place(1, k, None, 0, True)
    enc_whole = lambda k: gwe_out.at[rows_of(enc_row + k * enc_q, enc_q), :]
    pred_whole = lambda k: gwp_out.at[k, core]

    def widen(g1, g2, whole):
        g1.finish()
        g2.begin()
        pass_on(whole(g2.ring.me))

    def relay(g2, whole):
        g2.relay()
        pass_on(whole(g2.ring.prv))
        pass_on(whole(g2.ring.nxt))

    def close(g2, whole):
        g2.finish()
        pass_on(whole(g2.ring.opp))

    swap_1.wait_recv()
    add_out(1)
    first[1].begin()
    swap_enc.wait_recv()
    enc_acc[rows_of(enc_row, enc_half), :] = enc_acc[rows_of(enc_row, enc_half), :] + enc_pair[...]
    dc_gather.relay()
    dc_pass(ring_x.prv)
    dc_pass(ring_x.nxt)
    swap_0.wait_recv()
    add_out(0)
    first[0].begin()
    first[1].middle()
    enc_first.begin()

    loads[3].wait()
    ge = lax.dot_general(da_ref[...], w_enc_ref[...], (((1,), (1,)), ((), ())), preferred_element_type=F32)
    ge_ref[...] = ge.astype(BF16).reshape(ge_ref.shape)
    ge_out[pl.ds(seq, 1)] = ge_ref[pl.ds(seq, 1)]
    loss_out[pl.ds(seq, 1)] = loss_ref[...][None]
    loads[1].wait()
    loads[2].wait()
    for k in range(n_utt):
        rows_ref[k * n_upos:(k + 1) * n_upos, :] = pred_ref[order_ref[k], :, pl.ds(pl.multiple_of(x * LANES, LANES), LANES)]
    dc_gather.finish()
    dc_pass(ring_x.opp)
    first[0].middle()
    first[1].end(lambda half: outs_mid[1].at[:, pl.ds(half * (out_q // 2), out_q // 2), :])
    second[1].begin()

    for copy in dc_mate:
        copy.wait_recv()
    pred_part = lax.dot_general(rows_ref[...], dc_out[...].reshape(n_utt * n_upos, -1), contract_rows, preferred_element_type=F32)
    pred_acc[...] = jnp.where(core == 0, pred_part[:enc_q], pred_part[enc_q:])
    pred_first.begin()
    enc_first.middle()
    small = []
    for hop in range(1, n_seq):
        peer = lax.rem(seq + hop, n_seq)
        small.append(copies.start(ge_ref.at[peer], ge_out.at[seq], {"seq": peer}))
        small.append(copies.start(loss_ref, loss_out.at[seq], {"seq": peer}))
    first[0].end(lambda half: outs_mid[0].at[:, pl.ds(half * (out_q // 2), out_q // 2), :])
    second[0].begin()
    second[1].end(out_place(1, y, x, 0, True))
    b_g1.begin()
    enc_first.end(lambda half: enc_mid.at[pl.ds(half * (enc_q // 2), enc_q // 2), :])
    enc_second.begin()
    pred_first.end(pred_at(y))
    pred_g1.begin()
    second[0].end(out_place(0, x, y, 0, True))
    a_g1.begin()

    loads[4].wait()
    loads[5].wait()
    for i in range(n_utt):
        grad_rows_ref[i] = dc_out[place_ref[i]]
    widen(b_g1, b_g2, b_whole)
    enc_second.end(enc_at(x))
    enc_g1.begin()
    widen(pred_g1, pred_g2, pred_whole)
    half_utt = n_utt // 2

    def grad_rows(part):
        rows = grad_rows_ref[part * half_utt:(part + 1) * half_utt].reshape(half_utt * n_upos, -1)
        grads = lax.dot_general(rows, w_pred_ref[...], (((1,), (1,)), ((), ())), preferred_element_type=F32)
        gp_out[part * half_utt:(part + 1) * half_utt] = grads.reshape(half_utt, n_upos, -1)

    grad_rows(0)
    relay(b_g2, b_whole)
    widen(enc_g1, enc_g2, enc_whole)
    grad_rows(1)
    relay(pred_g2, pred_whole)
    widen(a_g1, a_g2, a_whole)
    close(b_g2, b_whole)
    relay(enc_g2, enc_whole)
    relay(a_g2, a_whole)
    close(pred_g2, pred_whole)
    close(enc_g2, enc_whole)
    close(a_g2, a_whole)
    for copy in small + last:
        copy.wait_recv()
    copies.drain()


N_COPIES = 3 + 10 + 14 + 3 * 6 + 4 * 6 + 4 * 6 + 16


def unflatten(refs):
    refs = list(refs)
    take = lambda n: [refs.pop(0) for _ in range(n)]
    enc_acc, enc_pair, enc_mid = take(3)
    enc_y, enc_x = take(3), take(3)
    outs = [(take(1)[0], take(1)[0], take(1)[0], take(3), take(3)) for _ in range(2)]
    outs_acc, outs_pair, outs_mid, outs_1, outs_2 = zip(*outs)
    pred_acc = refs.pop(0)
    pred_y = take(3)
    return (enc_acc, enc_pair, enc_mid, enc_y, enc_x, outs_acc, outs_pair, outs_mid, outs_1, outs_2, pred_acc, pred_y, *refs)


def combine(n_seq, order, place, frames, pred_loc, w_enc, w_pred, da, dc, gw, loss):
    width = frames.shape[-1]
    n_utt, n_upos, _ = pred_loc.shape
    joint = da.shape[-1]
    n_blk = gw.shape[0] // 2
    enc_half, out_half = width // CORES, joint // CORES
    enc_q, out_q = enc_half // RING, out_half // RING
    enc_s = enc_q // RING
    ring = lambda *shape: [VMEM(shape, F32)] * 3
    outs = [VMEM((n_blk, out_half, LANES), F32)] * 2 + [VMEM((n_blk, out_q, LANES), F32)] + ring(2, n_blk, out_q // 2, LANES) + ring(out_q, LANES)
    return pl.pallas_call(
        functools.partial(combine_kernel, n_seq),
        out_shape=(
            VMEM(frames.shape, BF16),
            VMEM((n_utt, n_upos, width), F32),
            VMEM((width, joint), F32),
            VMEM((RING, CORES, enc_q, joint), F32),
            VMEM(gw.shape, F32),
            VMEM((n_seq,) + loss.shape, F32),
        ),
        in_specs=[pl.BlockSpec(memory_space=pltpu.HBM)] * 6 + [vspec()] * 4,
        out_specs=(vspec(),) * 6,
        scratch_shapes=[pltpu.SMEM(order.shape, jnp.int32)] * 2
        + [VMEM(v.shape, v.dtype) for v in (frames, pred_loc, w_enc, w_pred)]
        + [pltpu.SemaphoreType.DMA((6,)), VMEM((n_utt, n_upos, joint), BF16), VMEM((n_utt, n_upos, joint), BF16)]
        + [VMEM((width, joint), F32), VMEM((enc_half, joint), F32), VMEM((enc_q, joint), F32)]
        + ring(2, enc_q // 2, joint)
        + ring(enc_s, joint)
        + outs
        + outs
        + [VMEM((enc_q, joint), F32)]
        + ring(enc_s, joint)
        + [
            VMEM((n_utt * n_upos, LANES), BF16),
            VMEM(frames.shape, BF16),
            pltpu.SemaphoreType.DMA((N_COPIES,)),
            pltpu.SemaphoreType.DMA((N_COPIES,)),
        ],
        compiler_params=pltpu.CompilerParams(collective_id=1, has_side_effects=True, vmem_limit_bytes=48_000_000),
        name="combine",
    )(*(in_hbm(v) for v in (order, place, frames, pred_loc, w_enc, w_pred)), *(in_vmem(v) for v in (da, dc, gw, loss)))


def output_kernel(place_hbm, losses_ref, ge_ref, gp_ref, gwe_ref, gwp_ref, gw_ref,
                  loss_out, ge_out, gp_out, gwe_out, gwp_out, gwo_out, place_ref, rows_ref, loss_ref, load_sem, sem):
    n_utt = gp_out.shape[0]
    n_own = ge_ref.shape[1]
    n_cols, _, col = gw_ref.shape
    loads = [pltpu.make_async_copy(place_hbm, place_ref, load_sem.at[0]), pltpu.make_async_copy(losses_ref.at[:, 0, :], rows_ref, load_sem.at[1])]
    for copy in loads:
        copy.start()
    pairs = [(gp_ref, gp_out), (gwe_ref, gwe_out)]
    pairs += [(gw_ref.at[k], gwo_out.at[:, pl.ds(k * col, col)]) for k in range(n_cols)]
    blocks, cores, size, _ = gwp_ref.shape
    pairs += [(gwp_ref.at[k // cores, k % cores], gwp_out.at[pl.ds(k * size, size), :]) for k in range(blocks * cores)]
    copies = [pltpu.make_async_copy(src, dst, sem.at[k]) for k, (src, dst) in enumerate(pairs)]
    for copy in copies:
        copy.start()
    for copy in loads:
        copy.wait()
    for i in range(n_utt):
        place = place_ref[i]
        dev = place // n_own
        own = place - dev * n_own
        loss_ref[i] = rows_ref[dev, own]
        copy = pltpu.make_async_copy(ge_ref.at[dev, own], ge_out.at[i], sem.at[len(copies)])
        copy.start()
        copies.append(copy)
    copy = pltpu.make_async_copy(loss_ref, loss_out, sem.at[len(copies)])
    copy.start()
    copies.append(copy)
    for copy in copies:
        copy.wait()


def outputs(place, losses, ge, gp, gwe, gwp, gw):
    n_seq, n_own, t_loc, width = ge.shape
    n_cols, joint, col = gw.shape
    hbm = pl.BlockSpec(memory_space=pltpu.HBM)
    return pl.pallas_call(
        output_kernel,
        out_shape=(
            jax.ShapeDtypeStruct((n_seq * n_own,), F32),
            jax.ShapeDtypeStruct((n_seq * n_own, t_loc, width), BF16),
            jax.ShapeDtypeStruct(gp.shape, F32),
            jax.ShapeDtypeStruct((width, joint), F32),
            jax.ShapeDtypeStruct((width, joint), F32),
            jax.ShapeDtypeStruct((joint, n_cols * col), F32),
        ),
        in_specs=[hbm] + [vspec()] * 6,
        out_specs=(hbm,) * 6,
        scratch_shapes=[
            pltpu.SMEM(place.shape, jnp.int32),
            pltpu.SMEM((n_seq, losses.shape[-1]), F32),
            pltpu.SMEM(place.shape, F32),
            pltpu.SemaphoreType.DMA((2,)),
            pltpu.SemaphoreType.DMA((2 + n_cols + RING * CORES + n_seq * n_own + 1,)),
        ],
        compiler_params=pltpu.CompilerParams(vmem_limit_bytes=48_000_000),
        name="outputs",
    )(in_hbm(place), *(in_vmem(v) for v in (losses, ge, gp, gwe, gwp, gw)))


def solution(mesh):
    n_seq = mesh.shape["seq"]
    utt_rows = P(("part", "data"))
    utt_mats = P(("part", "data"), None)
    utt_cube = P(("part", "data"), None, None)
    enc_spec = P(("part", "data"), "seq", None)
    weight_in = P(None, None)
    weight_out = P("part", None)

    def body(enc_loc, pred_loc, w_enc, w_pred, w_out, labels, frame_len, label_len):
        t_loc = enc_loc.shape[1]
        n_upos = pred_loc.shape[1]
        seq_idx = lax.axis_index("seq").astype(jnp.int32).reshape(1)
        order, place, frames, act, pred, w_out_t = exchange(n_seq, frame_len, label_len, enc_loc, pred_loc, w_enc, w_pred, w_out)
        da, dc, gw, loss = lattice(n_seq, seq_idx, order, frame_len, label_len, labels, act, pred, w_out, w_out_t, n_upos, t_loc)
        ge, gp, gwe, gwp, gw, losses = combine(n_seq, order, place, frames, pred_loc, w_enc, w_pred, da, dc, gw, loss)
        loss, grad_enc, grad_pred, gw_enc, gw_pred, gw_out = outputs(place, losses, ge, gp, gwe, gwp, gw)
        return loss, grad_enc, grad_pred, gw_enc, gw_pred, gw_out

    return jax.shard_map(body, mesh=mesh, in_specs=(enc_spec, utt_cube, weight_in, weight_in, weight_in, utt_mats, utt_rows, utt_rows), out_specs=(utt_rows, enc_spec, utt_cube, weight_out, weight_out, weight_out), check_vma=False)
```

```python
import functools

import jax
import jax.numpy as jnp
from jax import lax
from jax.experimental import pallas as pl
from jax.experimental.pallas import tpu as pltpu
from jax.sharding import PartitionSpec as P

NEG = -1e30
MESH = pl.DeviceIdType.MESH
VMEM = pltpu.VMEM
F32 = jnp.float32
BF16 = jnp.bfloat16
VMEM_LIMIT = 67_000_000
SUB = 8
LANES = 128
GROUPS = 4
WIDE = 8
BLOCK = 64
CORES = 2
RING = 4


def vspec():
    return pl.BlockSpec(memory_space=pltpu.VMEM)


def in_hbm(x):
    return pltpu.with_memory_space_constraint(x, pltpu.HBM)


def in_vmem(x):
    return pltpu.with_memory_space_constraint(x, pltpu.VMEM)


def sspec():
    return pl.BlockSpec(memory_space=pltpu.SMEM)


def exchange_kernel(n_seq, flen_hbm, llen_hbm, enc_hbm, pred_hbm, w_enc_hbm, w_pred_hbm, w_out_hbm,
                    order_ref, place_ref, frames_ref, a_ref, c_ref, w_out_t_ref,
                    key_ref, cost_ref, rank_ref, by_rank_ref, sorted_ref, own_pred_ref, flen_ref, llen_ref, enc_ref, pred_ref, w_enc_ref, w_pred_ref, w_out_ref, load_sem, send_sem, recv_sem):
    sources = (flen_hbm, llen_hbm, enc_hbm, pred_hbm, w_pred_hbm, w_out_hbm, w_enc_hbm)
    landed = (flen_ref, llen_ref, enc_ref, pred_ref, w_pred_ref, w_out_ref, w_enc_ref)
    loads = [pltpu.make_async_copy(src, dst, load_sem.at[k]) for k, (src, dst) in enumerate(zip(sources, landed))]
    for copy in loads:
        copy.start()
    seq = lax.axis_index("seq")
    n_utt = enc_ref.shape[0]
    n_own = n_utt // n_seq
    barrier = pltpu.get_barrier_semaphore()
    for hop in range(1, n_seq):
        pl.semaphore_signal(barrier, inc=1, device_id={"seq": lax.rem(seq + hop, n_seq)}, device_id_type=MESH)

    def set_key(i, carry):
        cost = ((flen_ref[i] + SUB - 1) // SUB) * ((llen_ref[i] + SUB) // SUB)
        cost_ref[i] = cost
        key_ref[i] = cost * n_utt + i
        return carry

    def set_rank(i, carry):
        key = key_ref[i]
        rank = jnp.int32(0)
        for j in range(n_utt):
            rank = rank + jnp.where(key_ref[j] > key, 1, 0)
        rank_ref[i] = rank
        return carry

    def invert(src_ref, dst_ref):
        def body(k, carry):
            found = jnp.int32(0)
            for j in range(n_utt):
                found = found + jnp.where(src_ref[j] == k, j, 0)
            dst_ref[k] = found
            return carry

        lax.fori_loop(0, n_utt, body, 0)

    loads[0].wait()
    loads[1].wait()
    lax.fori_loop(0, n_utt, set_key, 0)
    lax.fori_loop(0, n_utt, set_rank, 0)
    invert(rank_ref, by_rank_ref)
    sums = [jnp.int32(0)] * n_seq
    for deal in range(n_own):
        spots = []
        for d in range(n_seq):
            spot = jnp.int32(0)
            for e in range(n_seq):
                if e != d:
                    before = sums[e] <= sums[d] if e < d else sums[e] < sums[d]
                    spot = spot + jnp.where(before, 1, 0)
            spots.append(spot)
        for d in range(n_seq):
            utt = by_rank_ref[deal * n_seq + spots[d]]
            order_ref[d * n_own + deal] = utt
            sums[d] = sums[d] + cost_ref[utt]
    loads[2].wait()
    for k in range(n_utt):
        sorted_ref[k] = enc_ref[order_ref[k]]
    pl.semaphore_wait(barrier, n_seq - 1)
    copies = []
    for hop in range(1, n_seq):
        peer = lax.rem(seq + hop, n_seq)
        copy = pltpu.make_async_remote_copy(
            src_ref=sorted_ref.at[pl.ds(peer * n_own, n_own)],
            dst_ref=frames_ref.at[seq],
            send_sem=send_sem.at[hop - 1],
            recv_sem=recv_sem.at[hop - 1],
            device_id={"seq": peer},
            device_id_type=MESH,
        )
        copy.start()
        copies.append(copy)
    frames_ref[pl.ds(seq, 1)] = sorted_ref[pl.ds(seq * n_own, n_own)][None]
    loads[3].wait()
    loads[4].wait()
    for j in range(n_own):
        own_pred_ref[j] = pred_ref[order_ref[seq * n_own + j]]
    own_pred = own_pred_ref[...]
    c_ref[...] = jnp.dot(own_pred.reshape(-1, own_pred.shape[-1]), w_pred_ref[...], preferred_element_type=F32).astype(BF16).astype(F32)
    loads[5].wait()
    w_out_t_ref[...] = w_out_ref[...].T
    invert(order_ref, place_ref)
    loads[6].wait()
    for copy in copies:
        copy.wait()
    frames = frames_ref[...]
    a_ref[...] = jnp.dot(frames.reshape(-1, frames.shape[-1]), w_enc_ref[...], preferred_element_type=F32).astype(BF16).astype(F32)


def exchange(n_seq, frame_len, label_len, enc_loc, pred_loc, w_enc, w_pred, w_out):
    n_utt, t_loc, width = enc_loc.shape
    n_own = n_utt // n_seq
    n_upos = pred_loc.shape[1]
    joint, vocab = w_out.shape
    return pl.pallas_call(
        functools.partial(exchange_kernel, n_seq),
        out_shape=(
            pltpu.HBM((n_utt,), jnp.int32),
            pltpu.HBM((n_utt,), jnp.int32),
            pltpu.HBM((n_seq, n_own, t_loc, width), BF16),
            VMEM((n_seq * n_own * t_loc, joint), F32),
            VMEM((n_own * n_upos, joint), F32),
            VMEM((vocab, joint), BF16),
        ),
        in_specs=[pl.BlockSpec(memory_space=pltpu.HBM)] * 7,
        out_specs=(sspec(),) * 2 + (vspec(),) * 4,
        scratch_shapes=[
            pltpu.SMEM((n_utt,), jnp.int32),
            pltpu.SMEM((n_utt,), jnp.int32),
            pltpu.SMEM((n_utt,), jnp.int32),
            pltpu.SMEM((n_utt,), jnp.int32),
            VMEM(enc_loc.shape, BF16),
            VMEM((n_own, n_upos, width), BF16),
            pltpu.SMEM((n_utt,), jnp.int32),
            pltpu.SMEM((n_utt,), jnp.int32),
        ]
        + [VMEM(v.shape, BF16) for v in (enc_loc, pred_loc, w_enc, w_pred, w_out)]
        + [
            pltpu.SemaphoreType.DMA((7,)),
            pltpu.SemaphoreType.DMA((n_seq - 1,)),
            pltpu.SemaphoreType.DMA((n_seq - 1,)),
        ],
        compiler_params=pltpu.CompilerParams(collective_id=0, has_side_effects=True, vmem_limit_bytes=40_000_000),
        name="exchange",
    )(*(in_hbm(v) for v in (frame_len, label_len, enc_loc, pred_loc, w_enc, w_pred, w_out)))


def logaddexp(x, y):
    top = jnp.maximum(x, y)
    return top + jnp.log(1.0 + jnp.exp(-jnp.abs(x - y)))


def lattice_kernel(n_own, n_frames, n_upos, seq_ref, order_ref, flen_ref, llen_ref, labels_ref, a_ref, c_ref, w_ref, wt_ref,
                   da_ref, dc_ref, gw_ref, loss_ref,
                   e_ref, h_ref, blank_ref, label_ref, alpha_ref, beta_ref, ids_ref, dact_ref, dpred_ref, work0, work1, dz_ref, dh_ref):
    vocab = w_ref.shape[1]
    joint = w_ref.shape[0]
    n_vt = vocab // LANES
    rows_g = SUB * SUB
    rows_t = GROUPS * rows_g
    n_diag = n_frames + n_upos - 1
    first = seq_ref[0] * n_own
    utts = [order_ref[first + b] for b in range(n_own)]
    lens_t = [flen_ref[utt] for utt in utts]
    lens_u = [llen_ref[utt] for utt in utts]
    blocks_t = [lax.div(n + SUB - 1, SUB) for n in lens_t]
    blocks_u = [lax.div(n + SUB, SUB) for n in lens_u]
    starts = [jnp.int32(0)]
    for b in range(n_own):
        starts.append(starts[-1] + blocks_t[b] * blocks_u[b])
    total = starts[-1]
    n_tiles = lax.div(total + GROUPS - 1, GROUPS)

    def decode(n):
        n = jnp.minimum(n, total - 1)
        b = jnp.int32(0)
        base, width = starts[0], blocks_u[0]
        for k in range(1, n_own):
            past = n >= starts[k]
            b = jnp.where(past, k, b)
            base = jnp.where(past, starts[k], base)
            width = jnp.where(past, blocks_u[k], width)
        ti = lax.div(n - base, width)
        return n, b, ti, n - base - ti * width

    pos_col = lax.broadcasted_iota(jnp.int32, (n_upos, n_upos - 1), 0)
    pos_row = lax.broadcasted_iota(jnp.int32, (n_upos, n_upos - 1), 1)
    for b in range(n_own):
        row = labels_ref[pl.ds(utts[b], 1), :].astype(F32)
        col = jnp.sum(jnp.where(pos_col == pos_row, row, 0.0), axis=1, keepdims=True)
        ids_ref[pl.ds(b * n_upos, n_upos), :] = jnp.broadcast_to(col, (n_upos, LANES)).astype(jnp.int32)

    blank_ref[...] = jnp.zeros_like(blank_ref)
    label_ref[...] = jnp.zeros_like(label_ref)
    gw_ref[...] = jnp.zeros_like(gw_ref)
    dact_ref[...] = jnp.zeros_like(dact_ref)
    dpred_ref[...] = jnp.zeros_like(dpred_ref)

    lane = lax.broadcasted_iota(jnp.int32, (SUB, LANES), 1)
    block_lane = lax.broadcasted_iota(jnp.int32, (BLOCK, LANES), 1)
    t_block = BLOCK // SUB
    works = (work0, work1)

    def tile_rows(i):
        return pl.ds(pl.multiple_of(jnp.clip(i, 0, n_tiles - 1) * rows_t, rows_t), rows_t)

    def tile_groups(i):
        return [decode(jnp.clip(i, 0, n_tiles - 1) * GROUPS + g) for g in range(GROUPS)]

    def pred_row(b, ui):
        return pl.ds(pl.multiple_of(b * n_upos + ui * SUB, SUB), SUB)

    def act_row(b, ti):
        return pl.ds(pl.multiple_of((ti * n_own + b) * SUB, SUB), SUB)

    def block_ids(b, ui):
        ids = ids_ref[pred_row(b, ui), :]
        return jnp.broadcast_to(ids[None], (t_block, SUB, LANES)).reshape(BLOCK, LANES)

    def cell_rows(ti, k, ui):
        return pl.ds(pl.multiple_of((n_diag - 1 - ti * SUB - k) * n_upos + ui * SUB, SUB), SUB)

    def make_hidden(i):
        first_row = jnp.clip(i, 0, n_tiles - 1) * rows_t
        for g, (n, b, ti, ui) in enumerate(tile_groups(i)):
            a_rows = a_ref.at[act_row(b, ti), :]
            c8 = c_ref[pred_row(b, ui), :]
            h = jnp.concatenate([jnp.tanh(a_rows[pl.ds(k, SUB, stride=0), :] + c8) for k in range(SUB)], axis=0).astype(BF16)
            h_ref[pl.ds(pl.multiple_of(first_row + g * rows_g, rows_g), rows_g), :] = h

    def make_logits(i, z_ref):
        z_ref[...] = jnp.dot(h_ref[tile_rows(i), :], w_ref[...], preferred_element_type=F32)

    def make_softmax(i, z_ref):
        first_row = jnp.clip(i, 0, n_tiles - 1) * rows_t
        for g, (n, b, ti, ui) in enumerate(tile_groups(i)):
            ids = block_ids(b, ui)
            for r in range(0, rows_g, BLOCK):
                z = z_ref[g * rows_g + r:g * rows_g + r + BLOCK, :]
                top = jnp.max(z, axis=1, keepdims=True)
                e = jnp.exp(z - top)
                norm = jnp.sum(e, axis=1, keepdims=True)
                e_ref[pl.ds(pl.multiple_of(first_row + g * rows_g + r, BLOCK), BLOCK), :] = e
                log_norm = top + jnp.log(norm)
                picked = jnp.zeros((BLOCK, LANES), F32)
                for v in range(n_vt):
                    picked = picked + jnp.where(block_lane + v * LANES == ids, z[:, v * LANES:(v + 1) * LANES], 0.0)
                label = jnp.sum(picked, axis=1, keepdims=True) - log_norm
                blank = z[:, 0:1] - log_norm
                scale = 1.0 / norm
                rows = [cell_rows(ti, r // SUB + k, ui) for k in range(t_block)]
                old_blank = [blank_ref[at, :] for at in rows]
                old_label = [label_ref[at, :] for at in rows]
                for k, at in enumerate(rows):
                    sl = slice(k * SUB, (k + 1) * SUB)
                    blank_ref[at, :] = jnp.where(lane == b, blank[sl], jnp.where(lane == b + n_own, scale[sl], old_blank[k]))
                    label_ref[at, :] = jnp.where(lane == b, label[sl], old_label[k])

    make_hidden(0)
    make_logits(0, work0)
    make_hidden(1)

    def forward(j, carry):
        for half in range(2):
            i = 2 * j + half
            make_logits(i + 1, works[1 - half])
            make_softmax(i, works[half])
            make_hidden(i + 2)
        return carry

    def forward_tail(_, carry):
        make_softmax(n_tiles - 1, work0)
        return carry

    lax.fori_loop(0, lax.div(n_tiles, 2), forward, 0)
    lax.fori_loop(0, lax.rem(n_tiles, 2), forward_tail, 0)

    upos = lax.broadcasted_iota(jnp.int32, (n_upos, LANES), 0)
    utt = lax.broadcasted_iota(jnp.int32, (n_upos, LANES), 1)
    t_end = jnp.ones((n_upos, LANES), jnp.int32)
    u_end = jnp.zeros((n_upos, LANES), jnp.int32)
    for b in range(n_own):
        t_end = jnp.where(utt == b, lens_t[b], t_end)
        u_end = jnp.where(utt == b, lens_u[b], u_end)

    def diagonal(d):
        return pl.ds((n_diag - 1 - d) * n_upos, n_upos, stride=n_upos + 1)

    def down(x):
        return jnp.where(upos == 0, NEG, pltpu.roll(x, 1, 0))

    def up(x):
        return jnp.where(upos == n_upos - 1, NEG, pltpu.roll(x, n_upos - 1, 0))

    def edge(d):
        return jnp.where((d - upos == t_end) & (upos == u_end), 0.0, NEG)

    last = functools.reduce(jnp.maximum, [t + u for t, u in zip(lens_t, lens_u)])
    reach = functools.reduce(jnp.maximum, [(t + u) * SUB - 1 for t, u in zip(blocks_t, blocks_u)])
    alpha0 = jnp.where(upos == 0, 0.0, NEG).astype(F32)
    beta0 = edge(last)
    alpha_ref[0] = alpha0
    beta_ref[last] = beta0

    def sweep(k, carry):
        alpha, beta = carry
        d = k + 1
        alpha = logaddexp(alpha + blank_ref[diagonal(k), :], down(alpha + label_ref[diagonal(k), :]))
        alpha = jnp.where(upos <= d, alpha, NEG)
        alpha_ref[d] = alpha
        d = last - 1 - k
        inside = (d - upos < t_end) & (upos <= u_end)
        beta = logaddexp(beta + blank_ref[diagonal(d), :], up(beta) + label_ref[diagonal(d), :])
        beta = jnp.where(inside, beta, edge(d))
        beta_ref[d] = beta
        return alpha, beta

    lax.fori_loop(0, last, sweep, (alpha0, beta0))
    log_prob = beta_ref[0][0:1, :]
    loss_ref[...] = jnp.broadcast_to(-log_prob, (SUB, LANES))

    def occupancy(d, carry):
        t = d - upos
        alpha = alpha_ref[d]
        after = beta_ref[d + 1]
        cell_ok = (t >= 0) & (t < t_end) & (upos <= u_end)
        blank = blank_ref[diagonal(d), :]
        q0 = jnp.where(cell_ok, jnp.exp(alpha + blank + after - log_prob), 0.0)
        q1 = jnp.where(cell_ok & (upos < u_end), jnp.exp(alpha + label_ref[diagonal(d), :] + up(after) - log_prob), 0.0)
        blank_ref[diagonal(d), :] = jnp.where(utt < n_own, q0, blank)
        label_ref[diagonal(d), :] = q1
        return carry

    lax.fori_loop(0, jnp.minimum(reach, n_diag), occupancy, 0)

    sub_row = lax.broadcasted_iota(jnp.int32, (SUB, LANES), 0)

    def group_rows(n, r, size):
        return pl.ds(pl.multiple_of(n * rows_g + r, size), size)

    def make_dz(index, g, n, b, ti, ui):
        keep = (lane == b) & (index < total)
        ids = block_ids(b, ui)
        for r in range(0, rows_g, BLOCK):
            q0s, q1s, scales = [], [], []
            for k in range(t_block):
                at = cell_rows(ti, r // SUB + k, ui)
                blank = blank_ref[at, :]
                q0s.append(jnp.where(keep, blank, 0.0))
                scales.append(jnp.where(lane == b + n_own, blank, 0.0))
                q1s.append(jnp.where(keep, label_ref[at, :], 0.0))
            q0 = jnp.sum(jnp.concatenate(q0s, axis=0), axis=1, keepdims=True)
            q1 = jnp.sum(jnp.concatenate(q1s, axis=0), axis=1, keepdims=True)
            scale = jnp.sum(jnp.concatenate(scales, axis=0), axis=1, keepdims=True) * (q0 + q1)
            for v in range(n_vt):
                cols = slice(v * LANES, (v + 1) * LANES)
                dz = e_ref[group_rows(n, r, BLOCK), cols] * scale
                if v == 0:
                    dz = dz - jnp.where(block_lane == 0, q0, 0.0)
                dz = dz - jnp.where(block_lane + v * LANES == ids, q1, 0.0)
                dz_ref[g * rows_g + r:g * rows_g + r + BLOCK, cols] = dz.astype(BF16)

    def make_sums(g, n, b, ti, ui):
        for v in range(joint // LANES):
            cols = slice(v * LANES, (v + 1) * LANES)
            h = h_ref[group_rows(n, 0, rows_g), cols].astype(F32)
            ds = dh_ref[g * rows_g:(g + 1) * rows_g, cols] * (1.0 - h * h)
            cube = [ds[k * SUB:(k + 1) * SUB] for k in range(SUB)]
            dpred_ref[pred_row(b, ui), cols] += ((cube[0] + cube[1]) + (cube[2] + cube[3])) + ((cube[4] + cube[5]) + (cube[6] + cube[7]))
            for shift in (4, 2, 1):
                low = sub_row % (2 * shift) < shift
                half = len(cube) // 2
                cube = [jnp.where(low, cube[k], cube[k + half]) + jnp.where(low, pltpu.roll(cube[k], SUB - shift, 0), pltpu.roll(cube[k + half], shift, 0)) for k in range(half)]
            dact_ref[act_row(b, ti), cols] += cube[0]

    def backward_tile(start, width):
        groups = [(start + g, g, *decode(start + g)) for g in range(width)]
        rows = width * rows_g
        for group in groups:
            make_dz(*group)
        dh_ref[:rows] = jnp.dot(dz_ref[:rows], wt_ref[...], preferred_element_type=F32)
        h = h_ref[pl.ds(pl.multiple_of(start * rows_g, GROUPS * rows_g), rows), :]
        for v in range(0, n_vt, 2):
            part = lax.dot_general(h, dz_ref[:rows, v * LANES:(v + 2) * LANES], (((0,), (0,)), ((), ())), preferred_element_type=F32)
            gw_ref[v] += part[:, :LANES]
            gw_ref[v + 1] += part[:, LANES:]
        for group in groups:
            make_sums(*group[1:])

    def backward(i, carry):
        backward_tile(i * WIDE, WIDE)
        return carry

    n_wide = lax.div(total + WIDE - GROUPS - 1, WIDE)

    def backward_tail(_, carry):
        backward_tile(n_wide * WIDE, GROUPS)
        return carry

    lax.fori_loop(0, n_wide, backward, 0)
    lax.fori_loop(0, jnp.where(total > n_wide * WIDE, 1, 0), backward_tail, 0)
    da_ref[...] = dact_ref[...].astype(BF16)
    dc_ref[...] = dpred_ref[...].astype(BF16)


def lattice(n_seq, seq_idx, order, frame_len, label_len, labels, act, pred, w_out, w_out_t, n_upos, t_loc):
    n_own = frame_len.shape[0] // n_seq
    n_frames = n_seq * t_loc
    joint, vocab = w_out.shape
    cells = n_own * n_frames * n_upos
    n_diag = n_frames + n_upos - 1
    lat_rows = (n_diag + n_upos - 1) * n_upos
    return pl.pallas_call(
        functools.partial(lattice_kernel, n_own, n_frames, n_upos),
        out_shape=(
            VMEM(act.shape, BF16),
            VMEM(pred.shape, BF16),
            VMEM((vocab // LANES, joint, LANES), F32),
            VMEM((SUB, LANES), F32),
        ),
        in_specs=[sspec()] * 4 + [vspec()] * 5,
        out_specs=(vspec(),) * 4,
        scratch_shapes=[
            VMEM((cells, vocab), F32),
            VMEM((cells, joint), BF16),
            VMEM((lat_rows, LANES), F32),
            VMEM((lat_rows, LANES), F32),
            VMEM((n_diag + 1, n_upos, LANES), F32),
            VMEM((n_diag + 1, n_upos, LANES), F32),
            VMEM((n_own * n_upos, LANES), jnp.int32),
            VMEM(act.shape, F32),
            VMEM(pred.shape, F32),
            VMEM((GROUPS * SUB * SUB, vocab), F32),
            VMEM((GROUPS * SUB * SUB, vocab), F32),
            VMEM((WIDE * SUB * SUB, vocab), BF16),
            VMEM((WIDE * SUB * SUB, joint), F32),
        ],
        compiler_params=pltpu.CompilerParams(vmem_limit_bytes=60_400_000),
        name="lattice",
    )(seq_idx, order, frame_len, label_len, labels, in_vmem(act), in_vmem(pred), w_out, in_vmem(w_out_t))


class Copies:
    def __init__(self, send_sem, recv_sem):
        self.sems = (send_sem, recv_sem)
        self.all = []

    def start(self, src, dst, device):
        k = len(self.all)
        copy = pltpu.make_async_remote_copy(src_ref=src, dst_ref=dst, send_sem=self.sems[0].at[k], recv_sem=self.sems[1].at[k], device_id=device, device_id_type=MESH)
        copy.start()
        self.all.append(copy)
        return copy

    def drain(self):
        for copy in self.all:
            copy.wait_send()


class Ring:
    def __init__(self, me, device):
        self.me = me
        self.right, self.left, self.across = [device(lax.rem(me + hop, RING)) for hop in (1, RING - 1, 2)]
        self.nxt, self.prv, self.opp = lax.rem(me + 1, RING), lax.rem(me + RING - 1, RING), lax.rem(me + 2, RING)


class Reduce:
    def __init__(self, copies, ring, acc, bufs):
        self.copies, self.ring, self.acc = copies, ring, acc
        self.pair, self.from_left, self.from_right = bufs

    def begin(self):
        c, r, acc = self.copies, self.ring, self.acc
        self.a1 = c.start(acc(r.opp, 0), self.pair.at[0], r.right)
        self.b1 = c.start(acc(r.opp, 1), self.pair.at[1], r.left)
        self.b2 = c.start(acc(r.nxt, 1), self.from_left.at[1], r.right)
        self.a2 = c.start(acc(r.prv, 0), self.from_right.at[0], r.left)

    def middle(self):
        c, r, acc = self.copies, self.ring, self.acc
        self.a1.wait_recv()
        add = acc(r.nxt, 0)
        add[...] = add[...] + self.pair[0]
        self.a3 = c.start(add, self.from_left.at[0], r.right)
        self.b1.wait_recv()
        add = acc(r.prv, 1)
        add[...] = add[...] + self.pair[1]
        self.b3 = c.start(add, self.from_right.at[1], r.left)

    def end(self, target):
        for copy in (self.b2, self.a3, self.a2, self.b3):
            copy.wait_recv()
        for half in range(2):
            target(half)[...] = self.acc(self.ring.me, half)[...] + self.from_left[half] + self.from_right[half]


class Gather:
    def __init__(self, copies, ring, out):
        self.copies, self.ring, self.out = copies, ring, out

    def send(self, k, half, device):
        return self.copies.start(self.out(k, half), self.out(k, half), device)

    def begin(self):
        r = self.ring
        self.ra = self.send(r.me, 0, r.right)
        self.lb = self.send(r.me, 1, r.left)
        self.rb = self.send(r.me, 1, r.right)
        self.la = self.send(r.me, 0, r.left)

    def relay(self):
        r = self.ring
        self.ra.wait_recv()
        self.ra2 = self.send(r.prv, 0, r.right)
        self.lb.wait_recv()
        self.lb2 = self.send(r.nxt, 1, r.left)
        self.rb.wait_recv()
        self.la.wait_recv()

    def finish(self):
        self.ra2.wait_recv()
        self.lb2.wait_recv()


class Swap:
    def __init__(self, copies, ring, acc, bufs):
        self.copies, self.ring, self.acc, self.bufs = copies, ring, acc, bufs

    def begin(self):
        r = self.ring
        sends = ((r.nxt, r.right), (r.prv, r.left), (r.opp, r.across))
        self.sent = [self.copies.start(self.acc(k), buf, device) for (k, device), buf in zip(sends, self.bufs)]

    def end(self, target):
        for copy in self.sent:
            copy.wait_recv()
        target[...] = (self.acc(self.ring.me)[...] + self.bufs[0][...]) + (self.bufs[1][...] + self.bufs[2][...])


class Spread:
    def __init__(self, copies, ring, out):
        self.copies, self.ring, self.out = copies, ring, out

    def begin(self):
        r = self.ring
        self.sent = [self.copies.start(self.out(r.me), self.out(r.me), device) for device in (r.right, r.left, r.across)]

    def finish(self):
        for copy in self.sent:
            copy.wait_recv()


def rows_of(start, size):
    return pl.ds(pl.multiple_of(start, SUB), size)


def combine_kernel(n_seq, order_hbm, place_hbm, frames_hbm, pred_hbm, w_enc_hbm, w_pred_hbm, da_ref, dc_ref, gw_ref, loss_ref,
                   ge_out, gp_out, gwe_out, gwp_out, gwo_out, loss_out,
                   order_ref, place_ref, frames_ref, pred_ref, w_enc_ref, w_pred_ref, load_sem, dc_out, grad_rows_ref, *scratch):
    sources = (frames_hbm, order_hbm, pred_hbm, w_enc_hbm, place_hbm, w_pred_hbm)
    landed = (frames_ref, order_ref, pred_ref, w_enc_ref, place_ref, w_pred_ref)
    loads = [pltpu.make_async_copy(src, dst, load_sem.at[k]) for k, (src, dst) in enumerate(zip(sources, landed))]
    for copy in loads:
        copy.start()
    (enc_acc, enc_pair, enc_mid, enc_y, enc_x, outs_acc, outs_pair, outs_mid, outs_1, outs_2, pred_acc, pred_y, rows_ref, ge_ref, send_sem, recv_sem) = unflatten(scratch)
    seq = lax.axis_index("seq")
    y = lax.axis_index("data")
    x = lax.div(seq, CORES)
    core = lax.rem(seq, CORES)
    mate = {"seq": x * CORES + 1 - core}
    ring_x = Ring(x, lambda k: {"seq": k * CORES + core})
    ring_y = Ring(y, lambda k: {"data": k})
    barrier = pltpu.get_barrier_semaphore()
    for hop in range(1, n_seq):
        pl.semaphore_signal(barrier, inc=1, device_id={"seq": lax.rem(seq + hop, n_seq)}, device_id_type=MESH)
    for dev in (ring_y.right, ring_y.left, ring_y.across):
        pl.semaphore_signal(barrier, inc=1, device_id=dev, device_id_type=MESH)

    n_blk = gw_ref.shape[0] // 2
    n_utt = n_seq * frames_ref.shape[1]
    n_upos = pred_ref.shape[1]
    enc_half = enc_acc.shape[0] // CORES
    out_half = gw_ref.shape[1] // CORES
    enc_q, out_q = enc_half // RING, out_half // RING
    enc_s = enc_q // RING
    enc_row, out_row = core * enc_half, core * out_half
    contract_rows = (((0,), (0,)), ((), ()))

    n_own = frames_ref.shape[1]
    dc_out[pl.ds(seq * n_own, n_own)] = dc_ref[...].reshape(n_own, n_upos, -1)
    pl.semaphore_wait(barrier, n_seq - 1 + RING - 1)

    copies = Copies(send_sem, recv_sem)

    def swap_out(part):
        blocks = pl.ds(part * n_blk, n_blk)
        return copies.start(gw_ref.at[blocks, rows_of((1 - core) * out_half, out_half), :], outs_pair[part], mate)

    dc_gather = Gather(copies, ring_x, lambda k, half: dc_out.at[pl.ds((k * CORES + core) * n_own + half * (n_own // 2), n_own // 2)])
    swap_1 = swap_out(1)
    dc_gather.begin()
    dc_whole = lambda dev: dc_out.at[pl.ds(dev * n_own, n_own)]
    dc_mate = [copies.start(dc_whole(seq), dc_whole(seq), mate)]
    loads[0].wait()
    frames = frames_ref[...]
    enc_acc[...] = lax.dot_general(frames.reshape(-1, frames.shape[-1]), da_ref[...], contract_rows, preferred_element_type=F32)
    swap_enc = copies.start(enc_acc.at[rows_of((1 - core) * enc_half, enc_half), :], enc_pair, mate)
    swap_0 = swap_out(0)

    def dc_pass(k):
        dc_mate.append(copies.start(dc_whole(k * CORES + core), dc_whole(k * CORES + core), mate))

    def add_out(part):
        outs_acc[part][...] = gw_ref[pl.ds(part * n_blk, n_blk), rows_of(out_row, out_half), :] + outs_pair[part][...]

    def out_first(part):
        return lambda k, half: outs_acc[part].at[:, rows_of(k * out_q + half * (out_q // 2), out_q // 2), :]

    def out_second(part):
        return lambda k: outs_mid[part].at[k]

    rings = ((ring_x, ring_y), (ring_y, ring_x))
    first = [Reduce(copies, rings[part][0], out_first(part), outs_1[part]) for part in range(2)]
    second = [Swap(copies, rings[part][1], out_second(part), outs_2[part]) for part in range(2)]
    enc_first = Reduce(copies, ring_y, lambda k, half: enc_acc.at[rows_of(enc_row + k * enc_q + half * (enc_q // 2), enc_q // 2), :], enc_y)
    enc_second = Swap(copies, ring_x, lambda k: enc_mid.at[rows_of(k * enc_s, enc_s), :], enc_x)
    pred_first = Swap(copies, ring_y, lambda k: pred_acc.at[rows_of(k * enc_s, enc_s), :], pred_y)

    def out_place(part, k1, k2, half, whole=False):
        start, size = out_row + k1 * out_q, out_q
        if not whole:
            start, size = start + half * (out_q // 2), out_q // 2
        return gwo_out.at[part * n_blk + k2 if k2 is not None else pl.ds(part * n_blk, n_blk), rows_of(start, size), :]

    def pair_place(part):
        ring1, ring2 = rings[part]
        return (
            Spread(copies, ring2, lambda k: out_place(part, ring1.me, k, 0, True)),
            Gather(copies, ring1, lambda k, half: out_place(part, k, None, half)),
        )

    a_g1, a_g2 = pair_place(0)
    b_g1, b_g2 = pair_place(1)
    enc_at = lambda k: gwe_out.at[rows_of(enc_row + y * enc_q + k * enc_s, enc_s), :]
    enc_g1 = Spread(copies, ring_x, enc_at)
    enc_g2 = Gather(copies, ring_y, lambda k, half: gwe_out.at[rows_of(enc_row + k * enc_q + half * (enc_q // 2), enc_q // 2), :])
    pred_at = lambda k: gwp_out.at[x, core, rows_of(k * enc_s, enc_s), :]
    pred_g1 = Spread(copies, ring_y, pred_at)
    pred_g2 = Gather(copies, ring_x, lambda k, half: gwp_out.at[k, core, pl.ds(half * (enc_q // 2), enc_q // 2), :])

    last = []

    def pass_on(ref):
        last.append(copies.start(ref, ref, mate))

    a_whole = lambda k: out_place(0, k, None, 0, True)
    b_whole = lambda k: out_place(1, k, None, 0, True)
    enc_whole = lambda k: gwe_out.at[rows_of(enc_row + k * enc_q, enc_q), :]
    pred_whole = lambda k: gwp_out.at[k, core]

    def widen(g1, g2, whole):
        g1.finish()
        g2.begin()
        pass_on(whole(g2.ring.me))

    def relay(g2, whole):
        g2.relay()
        pass_on(whole(g2.ring.prv))
        pass_on(whole(g2.ring.nxt))

    def close(g2, whole):
        g2.finish()
        pass_on(whole(g2.ring.opp))

    swap_1.wait_recv()
    add_out(1)
    first[1].begin()
    swap_enc.wait_recv()
    enc_acc[rows_of(enc_row, enc_half), :] = enc_acc[rows_of(enc_row, enc_half), :] + enc_pair[...]
    dc_gather.relay()
    dc_pass(ring_x.prv)
    dc_pass(ring_x.nxt)
    swap_0.wait_recv()
    add_out(0)
    first[0].begin()
    first[1].middle()
    enc_first.begin()

    loads[3].wait()
    ge = lax.dot_general(da_ref[...], w_enc_ref[...], (((1,), (1,)), ((), ())), preferred_element_type=F32)
    ge_ref[...] = ge.astype(BF16).reshape(ge_ref.shape)
    ge_out[pl.ds(seq, 1)] = ge_ref[pl.ds(seq, 1)]
    loss_out[pl.ds(seq, 1)] = loss_ref[...][None]
    loads[1].wait()
    loads[2].wait()
    for k in range(n_utt):
        rows_ref[k * n_upos:(k + 1) * n_upos, :] = pred_ref[order_ref[k], :, pl.ds(pl.multiple_of(x * LANES, LANES), LANES)]
    dc_gather.finish()
    dc_pass(ring_x.opp)
    first[0].middle()
    first[1].end(lambda half: outs_mid[1].at[:, pl.ds(half * (out_q // 2), out_q // 2), :])
    second[1].begin()

    for copy in dc_mate:
        copy.wait_recv()
    pred_part = lax.dot_general(rows_ref[...], dc_out[...].reshape(n_utt * n_upos, -1), contract_rows, preferred_element_type=F32)
    pred_acc[...] = jnp.where(core == 0, pred_part[:enc_q], pred_part[enc_q:])
    pred_first.begin()
    enc_first.middle()
    small = []
    for hop in range(1, n_seq):
        peer = lax.rem(seq + hop, n_seq)
        small.append(copies.start(ge_ref.at[peer], ge_out.at[seq], {"seq": peer}))
        small.append(copies.start(loss_ref, loss_out.at[seq], {"seq": peer}))
    first[0].end(lambda half: outs_mid[0].at[:, pl.ds(half * (out_q // 2), out_q // 2), :])
    second[0].begin()
    second[1].end(out_place(1, y, x, 0, True))
    b_g1.begin()
    enc_first.end(lambda half: enc_mid.at[pl.ds(half * (enc_q // 2), enc_q // 2), :])
    enc_second.begin()
    pred_first.end(pred_at(y))
    pred_g1.begin()
    second[0].end(out_place(0, x, y, 0, True))
    a_g1.begin()

    loads[4].wait()
    loads[5].wait()
    for i in range(n_utt):
        grad_rows_ref[i] = dc_out[place_ref[i]]
    widen(b_g1, b_g2, b_whole)
    enc_second.end(enc_at(x))
    enc_g1.begin()
    widen(pred_g1, pred_g2, pred_whole)
    half_utt = n_utt // 2

    def grad_rows(part):
        rows = grad_rows_ref[part * half_utt:(part + 1) * half_utt].reshape(half_utt * n_upos, -1)
        grads = lax.dot_general(rows, w_pred_ref[...], (((1,), (1,)), ((), ())), preferred_element_type=F32)
        gp_out[part * half_utt:(part + 1) * half_utt] = grads.reshape(half_utt, n_upos, -1)

    grad_rows(0)
    relay(b_g2, b_whole)
    widen(enc_g1, enc_g2, enc_whole)
    grad_rows(1)
    relay(pred_g2, pred_whole)
    widen(a_g1, a_g2, a_whole)
    close(b_g2, b_whole)
    relay(enc_g2, enc_whole)
    relay(a_g2, a_whole)
    close(pred_g2, pred_whole)
    close(enc_g2, enc_whole)
    close(a_g2, a_whole)
    for copy in small + last:
        copy.wait_recv()
    copies.drain()


N_COPIES = 3 + 10 + 14 + 3 * 6 + 4 * 6 + 4 * 6 + 16


def unflatten(refs):
    refs = list(refs)
    take = lambda n: [refs.pop(0) for _ in range(n)]
    enc_acc, enc_pair, enc_mid = take(3)
    enc_y, enc_x = take(3), take(3)
    outs = [(take(1)[0], take(1)[0], take(1)[0], take(3), take(3)) for _ in range(2)]
    outs_acc, outs_pair, outs_mid, outs_1, outs_2 = zip(*outs)
    pred_acc = refs.pop(0)
    pred_y = take(3)
    return (enc_acc, enc_pair, enc_mid, enc_y, enc_x, outs_acc, outs_pair, outs_mid, outs_1, outs_2, pred_acc, pred_y, *refs)


def combine(n_seq, order, place, frames, pred_loc, w_enc, w_pred, da, dc, gw, loss):
    width = frames.shape[-1]
    n_utt, n_upos, _ = pred_loc.shape
    joint = da.shape[-1]
    n_blk = gw.shape[0] // 2
    enc_half, out_half = width // CORES, joint // CORES
    enc_q, out_q = enc_half // RING, out_half // RING
    enc_s = enc_q // RING
    ring = lambda *shape: [VMEM(shape, F32)] * 3
    outs = [VMEM((n_blk, out_half, LANES), F32)] * 2 + [VMEM((n_blk, out_q, LANES), F32)] + ring(2, n_blk, out_q // 2, LANES) + ring(out_q, LANES)
    return pl.pallas_call(
        functools.partial(combine_kernel, n_seq),
        out_shape=(
            VMEM(frames.shape, BF16),
            VMEM((n_utt, n_upos, width), F32),
            VMEM((width, joint), F32),
            VMEM((RING, CORES, enc_q, joint), F32),
            VMEM(gw.shape, F32),
            VMEM((n_seq,) + loss.shape, F32),
        ),
        in_specs=[pl.BlockSpec(memory_space=pltpu.HBM)] * 6 + [vspec()] * 4,
        out_specs=(vspec(),) * 6,
        scratch_shapes=[pltpu.SMEM(order.shape, jnp.int32)] * 2
        + [VMEM(v.shape, v.dtype) for v in (frames, pred_loc, w_enc, w_pred)]
        + [pltpu.SemaphoreType.DMA((6,)), VMEM((n_utt, n_upos, joint), BF16), VMEM((n_utt, n_upos, joint), BF16)]
        + [VMEM((width, joint), F32), VMEM((enc_half, joint), F32), VMEM((enc_q, joint), F32)]
        + ring(2, enc_q // 2, joint)
        + ring(enc_s, joint)
        + outs
        + outs
        + [VMEM((enc_q, joint), F32)]
        + ring(enc_s, joint)
        + [
            VMEM((n_utt * n_upos, LANES), BF16),
            VMEM(frames.shape, BF16),
            pltpu.SemaphoreType.DMA((N_COPIES,)),
            pltpu.SemaphoreType.DMA((N_COPIES,)),
        ],
        compiler_params=pltpu.CompilerParams(collective_id=1, has_side_effects=True, vmem_limit_bytes=48_000_000),
        name="combine",
    )(*(in_hbm(v) for v in (order, place, frames, pred_loc, w_enc, w_pred)), *(in_vmem(v) for v in (da, dc, gw, loss)))


def output_kernel(place_hbm, losses_ref, ge_ref, gp_ref, gwe_ref, gwp_ref, gw_ref,
                  loss_out, ge_out, gp_out, gwe_out, gwp_out, gwo_out, place_ref, rows_ref, loss_ref, load_sem, sem):
    n_utt = gp_out.shape[0]
    n_own = ge_ref.shape[1]
    n_cols, _, col = gw_ref.shape
    loads = [pltpu.make_async_copy(place_hbm, place_ref, load_sem.at[0]), pltpu.make_async_copy(losses_ref.at[:, 0, :], rows_ref, load_sem.at[1])]
    for copy in loads:
        copy.start()
    pairs = [(gp_ref, gp_out), (gwe_ref, gwe_out)]
    pairs += [(gw_ref.at[k], gwo_out.at[:, pl.ds(k * col, col)]) for k in range(n_cols)]
    blocks, cores, size, _ = gwp_ref.shape
    pairs += [(gwp_ref.at[k // cores, k % cores], gwp_out.at[pl.ds(k * size, size), :]) for k in range(blocks * cores)]
    copies = [pltpu.make_async_copy(src, dst, sem.at[k]) for k, (src, dst) in enumerate(pairs)]
    for copy in copies:
        copy.start()
    for copy in loads:
        copy.wait()
    for i in range(n_utt):
        place = place_ref[i]
        dev = place // n_own
        own = place - dev * n_own
        loss_ref[i] = rows_ref[dev, own]
        copy = pltpu.make_async_copy(ge_ref.at[dev, own], ge_out.at[i], sem.at[len(copies)])
        copy.start()
        copies.append(copy)
    copy = pltpu.make_async_copy(loss_ref, loss_out, sem.at[len(copies)])
    copy.start()
    copies.append(copy)
    for copy in copies:
        copy.wait()


def outputs(place, losses, ge, gp, gwe, gwp, gw):
    n_seq, n_own, t_loc, width = ge.shape
    n_cols, joint, col = gw.shape
    hbm = pl.BlockSpec(memory_space=pltpu.HBM)
    return pl.pallas_call(
        output_kernel,
        out_shape=(
            jax.ShapeDtypeStruct((n_seq * n_own,), F32),
            jax.ShapeDtypeStruct((n_seq * n_own, t_loc, width), BF16),
            jax.ShapeDtypeStruct(gp.shape, F32),
            jax.ShapeDtypeStruct((width, joint), F32),
            jax.ShapeDtypeStruct((width, joint), F32),
            jax.ShapeDtypeStruct((joint, n_cols * col), F32),
        ),
        in_specs=[hbm] + [vspec()] * 6,
        out_specs=(hbm,) * 6,
        scratch_shapes=[
            pltpu.SMEM(place.shape, jnp.int32),
            pltpu.SMEM((n_seq, losses.shape[-1]), F32),
            pltpu.SMEM(place.shape, F32),
            pltpu.SemaphoreType.DMA((2,)),
            pltpu.SemaphoreType.DMA((2 + n_cols + RING * CORES + n_seq * n_own + 1,)),
        ],
        compiler_params=pltpu.CompilerParams(vmem_limit_bytes=48_000_000),
        name="outputs",
    )(in_hbm(place), *(in_vmem(v) for v in (losses, ge, gp, gwe, gwp, gw)))


def solution(mesh):
    n_seq = mesh.shape["seq"]
    utt_rows = P(("part", "data"))
    utt_mats = P(("part", "data"), None)
    utt_cube = P(("part", "data"), None, None)
    enc_spec = P(("part", "data"), "seq", None)
    weight_in = P(None, None)
    weight_out = P("part", None)

    def body(enc_loc, pred_loc, w_enc, w_pred, w_out, labels, frame_len, label_len):
        t_loc = enc_loc.shape[1]
        n_upos = pred_loc.shape[1]
        seq_idx = lax.axis_index("seq").astype(jnp.int32).reshape(1)
        order, place, frames, act, pred, w_out_t = exchange(n_seq, frame_len, label_len, enc_loc, pred_loc, w_enc, w_pred, w_out)
        da, dc, gw, loss = lattice(n_seq, seq_idx, order, frame_len, label_len, labels, act, pred, w_out, w_out_t, n_upos, t_loc)
        ge, gp, gwe, gwp, gw, losses = combine(n_seq, order, place, frames, pred_loc, w_enc, w_pred, da, dc, gw, loss)
        loss, grad_enc, grad_pred, gw_enc, gw_pred, gw_out = outputs(place, losses, ge, gp, gwe, gwp, gw)
        return loss, grad_enc, grad_pred, gw_enc, gw_pred, gw_out

    return jax.shard_map(body, mesh=mesh, in_specs=(enc_spec, utt_cube, weight_in, weight_in, weight_in, utt_mats, utt_rows, utt_rows), out_specs=(utt_rows, enc_spec, utt_cube, weight_out, weight_out, weight_out), check_vma=False)
```

```python
import functools

import jax
import jax.numpy as jnp
from jax import lax
from jax.experimental import pallas as pl
from jax.experimental.pallas import tpu as pltpu
from jax.sharding import PartitionSpec as P

NEG = -1e30
MESH = pl.DeviceIdType.MESH
VMEM = pltpu.VMEM
F32 = jnp.float32
BF16 = jnp.bfloat16
VMEM_LIMIT = 67_000_000
SUB = 8
LANES = 128
GROUPS = 4
WIDE = 8
BLOCK = 64
CORES = 2
RING = 4


def vspec():
    return pl.BlockSpec(memory_space=pltpu.VMEM)


def in_hbm(x):
    return pltpu.with_memory_space_constraint(x, pltpu.HBM)


def in_vmem(x):
    return pltpu.with_memory_space_constraint(x, pltpu.VMEM)


def sspec():
    return pl.BlockSpec(memory_space=pltpu.SMEM)


def exchange_kernel(n_seq, flen_hbm, llen_hbm, enc_hbm, pred_hbm, w_enc_hbm, w_pred_hbm, w_out_hbm,
                    order_ref, place_ref, frames_ref, a_ref, c_ref, w_out_t_ref,
                    key_ref, cost_ref, rank_ref, by_rank_ref, sorted_ref, own_pred_ref, flen_ref, llen_ref, enc_ref, pred_ref, w_enc_ref, w_pred_ref, w_out_ref, load_sem, send_sem, recv_sem):
    sources = (flen_hbm, llen_hbm, enc_hbm, pred_hbm, w_pred_hbm, w_out_hbm, w_enc_hbm)
    landed = (flen_ref, llen_ref, enc_ref, pred_ref, w_pred_ref, w_out_ref, w_enc_ref)
    loads = [pltpu.make_async_copy(src, dst, load_sem.at[k]) for k, (src, dst) in enumerate(zip(sources, landed))]
    for copy in loads:
        copy.start()
    seq = lax.axis_index("seq")
    n_utt = enc_ref.shape[0]
    n_own = n_utt // n_seq
    barrier = pltpu.get_barrier_semaphore()
    for hop in range(1, n_seq):
        pl.semaphore_signal(barrier, inc=1, device_id={"seq": lax.rem(seq + hop, n_seq)}, device_id_type=MESH)

    def set_key(i, carry):
        cost = ((flen_ref[i] + SUB - 1) // SUB) * ((llen_ref[i] + SUB) // SUB)
        cost_ref[i] = cost
        key_ref[i] = cost * n_utt + i
        return carry

    def set_rank(i, carry):
        key = key_ref[i]
        rank = jnp.int32(0)
        for j in range(n_utt):
            rank = rank + jnp.where(key_ref[j] > key, 1, 0)
        rank_ref[i] = rank
        return carry

    def invert(src_ref, dst_ref):
        def body(k, carry):
            found = jnp.int32(0)
            for j in range(n_utt):
                found = found + jnp.where(src_ref[j] == k, j, 0)
            dst_ref[k] = found
            return carry

        lax.fori_loop(0, n_utt, body, 0)

    loads[0].wait()
    loads[1].wait()
    lax.fori_loop(0, n_utt, set_key, 0)
    lax.fori_loop(0, n_utt, set_rank, 0)
    invert(rank_ref, by_rank_ref)
    sums = [jnp.int32(0)] * n_seq
    for deal in range(n_own):
        spots = []
        for d in range(n_seq):
            spot = jnp.int32(0)
            for e in range(n_seq):
                if e != d:
                    before = sums[e] <= sums[d] if e < d else sums[e] < sums[d]
                    spot = spot + jnp.where(before, 1, 0)
            spots.append(spot)
        for d in range(n_seq):
            utt = by_rank_ref[deal * n_seq + spots[d]]
            order_ref[d * n_own + deal] = utt
            sums[d] = sums[d] + cost_ref[utt]
    loads[2].wait()
    for k in range(n_utt):
        sorted_ref[k] = enc_ref[order_ref[k]]
    pl.semaphore_wait(barrier, n_seq - 1)
    copies = []
    for hop in range(1, n_seq):
        peer = lax.rem(seq + hop, n_seq)
        copy = pltpu.make_async_remote_copy(
            src_ref=sorted_ref.at[pl.ds(peer * n_own, n_own)],
            dst_ref=frames_ref.at[seq],
            send_sem=send_sem.at[hop - 1],
            recv_sem=recv_sem.at[hop - 1],
            device_id={"seq": peer},
            device_id_type=MESH,
        )
        copy.start()
        copies.append(copy)
    frames_ref[pl.ds(seq, 1)] = sorted_ref[pl.ds(seq * n_own, n_own)][None]
    loads[3].wait()
    loads[4].wait()
    for j in range(n_own):
        own_pred_ref[j] = pred_ref[order_ref[seq * n_own + j]]
    own_pred = own_pred_ref[...]
    c_ref[...] = jnp.dot(own_pred.reshape(-1, own_pred.shape[-1]), w_pred_ref[...], preferred_element_type=F32).astype(BF16).astype(F32)
    loads[5].wait()
    w_out_t_ref[...] = w_out_ref[...].T
    invert(order_ref, place_ref)
    loads[6].wait()
    for copy in copies:
        copy.wait()
    frames = frames_ref[...]
    a_ref[...] = jnp.dot(frames.reshape(-1, frames.shape[-1]), w_enc_ref[...], preferred_element_type=F32).astype(BF16).astype(F32)


def exchange(n_seq, frame_len, label_len, enc_loc, pred_loc, w_enc, w_pred, w_out):
    n_utt, t_loc, width = enc_loc.shape
    n_own = n_utt // n_seq
    n_upos = pred_loc.shape[1]
    joint, vocab = w_out.shape
    return pl.pallas_call(
        functools.partial(exchange_kernel, n_seq),
        out_shape=(
            pltpu.HBM((n_utt,), jnp.int32),
            pltpu.HBM((n_utt,), jnp.int32),
            pltpu.HBM((n_seq, n_own, t_loc, width), BF16),
            VMEM((n_seq * n_own * t_loc, joint), F32),
            VMEM((n_own * n_upos, joint), F32),
            VMEM((vocab, joint), BF16),
        ),
        in_specs=[pl.BlockSpec(memory_space=pltpu.HBM)] * 7,
        out_specs=(sspec(),) * 2 + (vspec(),) * 4,
        scratch_shapes=[
            pltpu.SMEM((n_utt,), jnp.int32),
            pltpu.SMEM((n_utt,), jnp.int32),
            pltpu.SMEM((n_utt,), jnp.int32),
            pltpu.SMEM((n_utt,), jnp.int32),
            VMEM(enc_loc.shape, BF16),
            VMEM((n_own, n_upos, width), BF16),
            pltpu.SMEM((n_utt,), jnp.int32),
            pltpu.SMEM((n_utt,), jnp.int32),
        ]
        + [VMEM(v.shape, BF16) for v in (enc_loc, pred_loc, w_enc, w_pred, w_out)]
        + [
            pltpu.SemaphoreType.DMA((7,)),
            pltpu.SemaphoreType.DMA((n_seq - 1,)),
            pltpu.SemaphoreType.DMA((n_seq - 1,)),
        ],
        compiler_params=pltpu.CompilerParams(collective_id=0, has_side_effects=True, vmem_limit_bytes=40_000_000),
        name="exchange",
    )(*(in_hbm(v) for v in (frame_len, label_len, enc_loc, pred_loc, w_enc, w_pred, w_out)))


def logaddexp(x, y):
    top = jnp.maximum(x, y)
    return top + jnp.log(1.0 + jnp.exp(-jnp.abs(x - y)))


def lattice_kernel(n_own, n_frames, n_upos, seq_ref, order_ref, flen_ref, llen_ref, labels_ref, a_ref, c_ref, w_ref, wt_ref,
                   da_ref, dc_ref, gw_ref, loss_ref,
                   e_ref, h_ref, blank_ref, label_ref, alpha_ref, beta_ref, ids_ref, dact_ref, dpred_ref, work0, work1, dz_ref, dh_ref):
    vocab = w_ref.shape[1]
    joint = w_ref.shape[0]
    n_vt = vocab // LANES
    rows_g = SUB * SUB
    rows_t = GROUPS * rows_g
    n_diag = n_frames + n_upos - 1
    first = seq_ref[0] * n_own
    utts = [order_ref[first + b] for b in range(n_own)]
    lens_t = [flen_ref[utt] for utt in utts]
    lens_u = [llen_ref[utt] for utt in utts]
    blocks_t = [lax.div(n + SUB - 1, SUB) for n in lens_t]
    blocks_u = [lax.div(n + SUB, SUB) for n in lens_u]
    starts = [jnp.int32(0)]
    for b in range(n_own):
        starts.append(starts[-1] + blocks_t[b] * blocks_u[b])
    total = starts[-1]
    n_tiles = lax.div(total + GROUPS - 1, GROUPS)

    def decode(n):
        n = jnp.minimum(n, total - 1)
        b = jnp.int32(0)
        base, width = starts[0], blocks_u[0]
        for k in range(1, n_own):
            past = n >= starts[k]
            b = jnp.where(past, k, b)
            base = jnp.where(past, starts[k], base)
            width = jnp.where(past, blocks_u[k], width)
        ti = lax.div(n - base, width)
        return n, b, ti, n - base - ti * width

    pos_col = lax.broadcasted_iota(jnp.int32, (n_upos, n_upos - 1), 0)
    pos_row = lax.broadcasted_iota(jnp.int32, (n_upos, n_upos - 1), 1)
    for b in range(n_own):
        row = labels_ref[pl.ds(utts[b], 1), :].astype(F32)
        col = jnp.sum(jnp.where(pos_col == pos_row, row, 0.0), axis=1, keepdims=True)
        ids_ref[pl.ds(b * n_upos, n_upos), :] = jnp.broadcast_to(col, (n_upos, LANES)).astype(jnp.int32)

    blank_ref[...] = jnp.zeros_like(blank_ref)
    label_ref[...] = jnp.zeros_like(label_ref)
    gw_ref[...] = jnp.zeros_like(gw_ref)
    dact_ref[...] = jnp.zeros_like(dact_ref)
    dpred_ref[...] = jnp.zeros_like(dpred_ref)

    lane = lax.broadcasted_iota(jnp.int32, (SUB, LANES), 1)
    block_lane = lax.broadcasted_iota(jnp.int32, (BLOCK, LANES), 1)
    t_block = BLOCK // SUB
    works = (work0, work1)

    def tile_rows(i):
        return pl.ds(pl.multiple_of(jnp.clip(i, 0, n_tiles - 1) * rows_t, rows_t), rows_t)

    def tile_groups(i):
        return [decode(jnp.clip(i, 0, n_tiles - 1) * GROUPS + g) for g in range(GROUPS)]

    def pred_row(b, ui):
        return pl.ds(pl.multiple_of(b * n_upos + ui * SUB, SUB), SUB)

    def act_row(b, ti):
        return pl.ds(pl.multiple_of((ti * n_own + b) * SUB, SUB), SUB)

    def block_ids(b, ui):
        ids = ids_ref[pred_row(b, ui), :]
        return jnp.broadcast_to(ids[None], (t_block, SUB, LANES)).reshape(BLOCK, LANES)

    def cell_rows(ti, k, ui):
        return pl.ds(pl.multiple_of((n_diag - 1 - ti * SUB - k) * n_upos + ui * SUB, SUB), SUB)

    def make_hidden(i):
        first_row = jnp.clip(i, 0, n_tiles - 1) * rows_t
        for g, (n, b, ti, ui) in enumerate(tile_groups(i)):
            a_rows = a_ref.at[act_row(b, ti), :]
            c8 = c_ref[pred_row(b, ui), :]
            h = jnp.concatenate([jnp.tanh(a_rows[pl.ds(k, SUB, stride=0), :] + c8) for k in range(SUB)], axis=0).astype(BF16)
            h_ref[pl.ds(pl.multiple_of(first_row + g * rows_g, rows_g), rows_g), :] = h

    def make_logits(i, z_ref):
        z_ref[...] = jnp.dot(h_ref[tile_rows(i), :], w_ref[...], preferred_element_type=F32)

    def make_softmax(i, z_ref):
        first_row = jnp.clip(i, 0, n_tiles - 1) * rows_t
        for g, (n, b, ti, ui) in enumerate(tile_groups(i)):
            ids = block_ids(b, ui)
            for r in range(0, rows_g, BLOCK):
                z = z_ref[g * rows_g + r:g * rows_g + r + BLOCK, :]
                top = jnp.max(z, axis=1, keepdims=True)
                e = jnp.exp(z - top)
                norm = jnp.sum(e, axis=1, keepdims=True)
                e_ref[pl.ds(pl.multiple_of(first_row + g * rows_g + r, BLOCK), BLOCK), :] = e
                log_norm = top + jnp.log(norm)
                picked = jnp.zeros((BLOCK, LANES), F32)
                for v in range(n_vt):
                    picked = picked + jnp.where(block_lane + v * LANES == ids, z[:, v * LANES:(v + 1) * LANES], 0.0)
                label = jnp.sum(picked, axis=1, keepdims=True) - log_norm
                blank = z[:, 0:1] - log_norm
                scale = 1.0 / norm
                rows = [cell_rows(ti, r // SUB + k, ui) for k in range(t_block)]
                old_blank = [blank_ref[at, :] for at in rows]
                old_label = [label_ref[at, :] for at in rows]
                for k, at in enumerate(rows):
                    sl = slice(k * SUB, (k + 1) * SUB)
                    blank_ref[at, :] = jnp.where(lane == b, blank[sl], jnp.where(lane == b + n_own, scale[sl], old_blank[k]))
                    label_ref[at, :] = jnp.where(lane == b, label[sl], old_label[k])

    make_hidden(0)
    make_logits(0, work0)
    make_hidden(1)

    def forward(j, carry):
        for half in range(2):
            i = 2 * j + half
            make_logits(i + 1, works[1 - half])
            make_softmax(i, works[half])
            make_hidden(i + 2)
        return carry

    def forward_tail(_, carry):
        make_softmax(n_tiles - 1, work0)
        return carry

    lax.fori_loop(0, lax.div(n_tiles, 2), forward, 0)
    lax.fori_loop(0, lax.rem(n_tiles, 2), forward_tail, 0)

    upos = lax.broadcasted_iota(jnp.int32, (n_upos, LANES), 0)
    utt = lax.broadcasted_iota(jnp.int32, (n_upos, LANES), 1)
    t_end = jnp.ones((n_upos, LANES), jnp.int32)
    u_end = jnp.zeros((n_upos, LANES), jnp.int32)
    for b in range(n_own):
        t_end = jnp.where(utt == b, lens_t[b], t_end)
        u_end = jnp.where(utt == b, lens_u[b], u_end)

    def diagonal(d):
        return pl.ds((n_diag - 1 - d) * n_upos, n_upos, stride=n_upos + 1)

    def down(x):
        return jnp.where(upos == 0, NEG, pltpu.roll(x, 1, 0))

    def up(x):
        return jnp.where(upos == n_upos - 1, NEG, pltpu.roll(x, n_upos - 1, 0))

    def edge(d):
        return jnp.where((d - upos == t_end) & (upos == u_end), 0.0, NEG)

    last = functools.reduce(jnp.maximum, [t + u for t, u in zip(lens_t, lens_u)])
    reach = functools.reduce(jnp.maximum, [(t + u) * SUB - 1 for t, u in zip(blocks_t, blocks_u)])
    alpha0 = jnp.where(upos == 0, 0.0, NEG).astype(F32)
    beta0 = edge(last)
    alpha_ref[0] = alpha0
    beta_ref[last] = beta0

    def sweep(k, carry):
        alpha, beta = carry
        d = k + 1
        alpha = logaddexp(alpha + blank_ref[diagonal(k), :], down(alpha + label_ref[diagonal(k), :]))
        alpha = jnp.where(upos <= d, alpha, NEG)
        alpha_ref[d] = alpha
        d = last - 1 - k
        inside = (d - upos < t_end) & (upos <= u_end)
        beta = logaddexp(beta + blank_ref[diagonal(d), :], up(beta) + label_ref[diagonal(d), :])
        beta = jnp.where(inside, beta, edge(d))
        beta_ref[d] = beta
        return alpha, beta

    lax.fori_loop(0, last, sweep, (alpha0, beta0))
    log_prob = beta_ref[0][0:1, :]
    loss_ref[...] = jnp.broadcast_to(-log_prob, (SUB, LANES))

    def occupancy(d, carry):
        t = d - upos
        alpha = alpha_ref[d]
        after = beta_ref[d + 1]
        cell_ok = (t >= 0) & (t < t_end) & (upos <= u_end)
        blank = blank_ref[diagonal(d), :]
        q0 = jnp.where(cell_ok, jnp.exp(alpha + blank + after - log_prob), 0.0)
        q1 = jnp.where(cell_ok & (upos < u_end), jnp.exp(alpha + label_ref[diagonal(d), :] + up(after) - log_prob), 0.0)
        blank_ref[diagonal(d), :] = jnp.where(utt < n_own, q0, blank)
        label_ref[diagonal(d), :] = q1
        return carry

    lax.fori_loop(0, jnp.minimum(reach, n_diag), occupancy, 0)

    sub_row = lax.broadcasted_iota(jnp.int32, (SUB, LANES), 0)

    def group_rows(n, r, size):
        return pl.ds(pl.multiple_of(n * rows_g + r, size), size)

    def make_dz(index, g, n, b, ti, ui):
        keep = (lane == b) & (index < total)
        ids = block_ids(b, ui)
        for r in range(0, rows_g, BLOCK):
            q0s, q1s, scales = [], [], []
            for k in range(t_block):
                at = cell_rows(ti, r // SUB + k, ui)
                blank = blank_ref[at, :]
                q0s.append(jnp.where(keep, blank, 0.0))
                scales.append(jnp.where(lane == b + n_own, blank, 0.0))
                q1s.append(jnp.where(keep, label_ref[at, :], 0.0))
            q0 = jnp.sum(jnp.concatenate(q0s, axis=0), axis=1, keepdims=True)
            q1 = jnp.sum(jnp.concatenate(q1s, axis=0), axis=1, keepdims=True)
            scale = jnp.sum(jnp.concatenate(scales, axis=0), axis=1, keepdims=True) * (q0 + q1)
            for v in range(n_vt):
                cols = slice(v * LANES, (v + 1) * LANES)
                dz = e_ref[group_rows(n, r, BLOCK), cols] * scale
                if v == 0:
                    dz = dz - jnp.where(block_lane == 0, q0, 0.0)
                dz = dz - jnp.where(block_lane + v * LANES == ids, q1, 0.0)
                dz_ref[g * rows_g + r:g * rows_g + r + BLOCK, cols] = dz.astype(BF16)

    def make_sums(g, n, b, ti, ui):
        for v in range(joint // LANES):
            cols = slice(v * LANES, (v + 1) * LANES)
            h = h_ref[group_rows(n, 0, rows_g), cols].astype(F32)
            ds = dh_ref[g * rows_g:(g + 1) * rows_g, cols] * (1.0 - h * h)
            cube = [ds[k * SUB:(k + 1) * SUB] for k in range(SUB)]
            dpred_ref[pred_row(b, ui), cols] += ((cube[0] + cube[1]) + (cube[2] + cube[3])) + ((cube[4] + cube[5]) + (cube[6] + cube[7]))
            for shift in (4, 2, 1):
                low = sub_row % (2 * shift) < shift
                half = len(cube) // 2
                cube = [jnp.where(low, cube[k], cube[k + half]) + jnp.where(low, pltpu.roll(cube[k], SUB - shift, 0), pltpu.roll(cube[k + half], shift, 0)) for k in range(half)]
            dact_ref[act_row(b, ti), cols] += cube[0]

    def backward_tile(start, width):
        groups = [(start + g, g, *decode(start + g)) for g in range(width)]
        rows = width * rows_g
        for group in groups:
            make_dz(*group)
        dh_ref[:rows] = jnp.dot(dz_ref[:rows], wt_ref[...], preferred_element_type=F32)
        h = h_ref[pl.ds(pl.multiple_of(start * rows_g, GROUPS * rows_g), rows), :]
        for v in range(0, n_vt, 2):
            part = lax.dot_general(h, dz_ref[:rows, v * LANES:(v + 2) * LANES], (((0,), (0,)), ((), ())), preferred_element_type=F32)
            gw_ref[v] += part[:, :LANES]
            gw_ref[v + 1] += part[:, LANES:]
        for group in groups:
            make_sums(*group[1:])

    def backward(i, carry):
        backward_tile(i * WIDE, WIDE)
        return carry

    n_wide = lax.div(total + WIDE - GROUPS - 1, WIDE)

    def backward_tail(_, carry):
        backward_tile(n_wide * WIDE, GROUPS)
        return carry

    lax.fori_loop(0, n_wide, backward, 0)
    lax.fori_loop(0, jnp.where(total > n_wide * WIDE, 1, 0), backward_tail, 0)
    da_ref[...] = dact_ref[...].astype(BF16)
    dc_ref[...] = dpred_ref[...].astype(BF16)


def lattice(n_seq, seq_idx, order, frame_len, label_len, labels, act, pred, w_out, w_out_t, n_upos, t_loc):
    n_own = frame_len.shape[0] // n_seq
    n_frames = n_seq * t_loc
    joint, vocab = w_out.shape
    cells = n_own * n_frames * n_upos
    n_diag = n_frames + n_upos - 1
    lat_rows = (n_diag + n_upos - 1) * n_upos
    return pl.pallas_call(
        functools.partial(lattice_kernel, n_own, n_frames, n_upos),
        out_shape=(
            VMEM(act.shape, BF16),
            VMEM(pred.shape, BF16),
            VMEM((vocab // LANES, joint, LANES), F32),
            VMEM((SUB, LANES), F32),
        ),
        in_specs=[sspec()] * 4 + [vspec()] * 5,
        out_specs=(vspec(),) * 4,
        scratch_shapes=[
            VMEM((cells, vocab), F32),
            VMEM((cells, joint), BF16),
            VMEM((lat_rows, LANES), F32),
            VMEM((lat_rows, LANES), F32),
            VMEM((n_diag + 1, n_upos, LANES), F32),
            VMEM((n_diag + 1, n_upos, LANES), F32),
            VMEM((n_own * n_upos, LANES), jnp.int32),
            VMEM(act.shape, F32),
            VMEM(pred.shape, F32),
            VMEM((GROUPS * SUB * SUB, vocab), F32),
            VMEM((GROUPS * SUB * SUB, vocab), F32),
            VMEM((WIDE * SUB * SUB, vocab), BF16),
            VMEM((WIDE * SUB * SUB, joint), F32),
        ],
        compiler_params=pltpu.CompilerParams(vmem_limit_bytes=60_400_000),
        name="lattice",
    )(seq_idx, order, frame_len, label_len, labels, in_vmem(act), in_vmem(pred), w_out, in_vmem(w_out_t))


class Copies:
    def __init__(self, send_sem, recv_sem):
        self.sems = (send_sem, recv_sem)
        self.all = []

    def start(self, src, dst, device):
        k = len(self.all)
        copy = pltpu.make_async_remote_copy(src_ref=src, dst_ref=dst, send_sem=self.sems[0].at[k], recv_sem=self.sems[1].at[k], device_id=device, device_id_type=MESH)
        copy.start()
        self.all.append(copy)
        return copy

    def drain(self):
        for copy in self.all:
            copy.wait_send()


class Ring:
    def __init__(self, me, device):
        self.me = me
        self.right, self.left, self.across = [device(lax.rem(me + hop, RING)) for hop in (1, RING - 1, 2)]
        self.nxt, self.prv, self.opp = lax.rem(me + 1, RING), lax.rem(me + RING - 1, RING), lax.rem(me + 2, RING)


class Reduce:
    def __init__(self, copies, ring, acc, bufs):
        self.copies, self.ring, self.acc = copies, ring, acc
        self.pair, self.from_left, self.from_right = bufs

    def begin(self):
        c, r, acc = self.copies, self.ring, self.acc
        self.a1 = c.start(acc(r.opp, 0), self.pair.at[0], r.right)
        self.b1 = c.start(acc(r.opp, 1), self.pair.at[1], r.left)
        self.b2 = c.start(acc(r.nxt, 1), self.from_left.at[1], r.right)
        self.a2 = c.start(acc(r.prv, 0), self.from_right.at[0], r.left)

    def middle(self):
        c, r, acc = self.copies, self.ring, self.acc
        self.a1.wait_recv()
        add = acc(r.nxt, 0)
        add[...] = add[...] + self.pair[0]
        self.a3 = c.start(add, self.from_left.at[0], r.right)
        self.b1.wait_recv()
        add = acc(r.prv, 1)
        add[...] = add[...] + self.pair[1]
        self.b3 = c.start(add, self.from_right.at[1], r.left)

    def end(self, target):
        for copy in (self.b2, self.a3, self.a2, self.b3):
            copy.wait_recv()
        for half in range(2):
            target(half)[...] = self.acc(self.ring.me, half)[...] + self.from_left[half] + self.from_right[half]


class Gather:
    def __init__(self, copies, ring, out):
        self.copies, self.ring, self.out = copies, ring, out

    def send(self, k, half, device):
        return self.copies.start(self.out(k, half), self.out(k, half), device)

    def begin(self):
        r = self.ring
        self.ra = self.send(r.me, 0, r.right)
        self.lb = self.send(r.me, 1, r.left)
        self.rb = self.send(r.me, 1, r.right)
        self.la = self.send(r.me, 0, r.left)

    def relay(self):
        r = self.ring
        self.ra.wait_recv()
        self.ra2 = self.send(r.prv, 0, r.right)
        self.lb.wait_recv()
        self.lb2 = self.send(r.nxt, 1, r.left)
        self.rb.wait_recv()
        self.la.wait_recv()

    def finish(self):
        self.ra2.wait_recv()
        self.lb2.wait_recv()


class Swap:
    def __init__(self, copies, ring, acc, bufs):
        self.copies, self.ring, self.acc, self.bufs = copies, ring, acc, bufs

    def begin(self):
        r = self.ring
        sends = ((r.nxt, r.right), (r.prv, r.left), (r.opp, r.across))
        self.sent = [self.copies.start(self.acc(k), buf, device) for (k, device), buf in zip(sends, self.bufs)]

    def end(self, target):
        for copy in self.sent:
            copy.wait_recv()
        target[...] = (self.acc(self.ring.me)[...] + self.bufs[0][...]) + (self.bufs[1][...] + self.bufs[2][...])


class Spread:
    def __init__(self, copies, ring, out):
        self.copies, self.ring, self.out = copies, ring, out

    def begin(self):
        r = self.ring
        self.sent = [self.copies.start(self.out(r.me), self.out(r.me), device) for device in (r.right, r.left, r.across)]

    def finish(self):
        for copy in self.sent:
            copy.wait_recv()


def rows_of(start, size):
    return pl.ds(pl.multiple_of(start, SUB), size)


def combine_kernel(n_seq, order_hbm, place_hbm, frames_hbm, pred_hbm, w_enc_hbm, w_pred_hbm, da_ref, dc_ref, gw_ref, loss_ref,
                   ge_out, gp_out, gwe_out, gwp_out, gwo_out, loss_out,
                   order_ref, place_ref, frames_ref, pred_ref, w_enc_ref, w_pred_ref, load_sem, dc_out, grad_rows_ref, *scratch):
    sources = (frames_hbm, order_hbm, pred_hbm, w_enc_hbm, place_hbm, w_pred_hbm)
    landed = (frames_ref, order_ref, pred_ref, w_enc_ref, place_ref, w_pred_ref)
    loads = [pltpu.make_async_copy(src, dst, load_sem.at[k]) for k, (src, dst) in enumerate(zip(sources, landed))]
    for copy in loads:
        copy.start()
    (enc_acc, enc_pair, enc_mid, enc_y, enc_x, outs_acc, outs_pair, outs_mid, outs_1, outs_2, pred_acc, pred_y, rows_ref, ge_ref, send_sem, recv_sem) = unflatten(scratch)
    seq = lax.axis_index("seq")
    y = lax.axis_index("data")
    x = lax.div(seq, CORES)
    core = lax.rem(seq, CORES)
    mate = {"seq": x * CORES + 1 - core}
    ring_x = Ring(x, lambda k: {"seq": k * CORES + core})
    ring_y = Ring(y, lambda k: {"data": k})
    barrier = pltpu.get_barrier_semaphore()
    for hop in range(1, n_seq):
        pl.semaphore_signal(barrier, inc=1, device_id={"seq": lax.rem(seq + hop, n_seq)}, device_id_type=MESH)
    for dev in (ring_y.right, ring_y.left, ring_y.across):
        pl.semaphore_signal(barrier, inc=1, device_id=dev, device_id_type=MESH)

    n_blk = gw_ref.shape[0] // 2
    n_utt = n_seq * frames_ref.shape[1]
    n_upos = pred_ref.shape[1]
    enc_half = enc_acc.shape[0] // CORES
    out_half = gw_ref.shape[1] // CORES
    enc_q, out_q = enc_half // RING, out_half // RING
    enc_s = enc_q // RING
    enc_row, out_row = core * enc_half, core * out_half
    contract_rows = (((0,), (0,)), ((), ()))

    n_own = frames_ref.shape[1]
    dc_out[pl.ds(seq * n_own, n_own)] = dc_ref[...].reshape(n_own, n_upos, -1)
    pl.semaphore_wait(barrier, n_seq - 1 + RING - 1)

    copies = Copies(send_sem, recv_sem)

    def swap_out(part):
        blocks = pl.ds(part * n_blk, n_blk)
        return copies.start(gw_ref.at[blocks, rows_of((1 - core) * out_half, out_half), :], outs_pair[part], mate)

    dc_gather = Gather(copies, ring_x, lambda k, half: dc_out.at[pl.ds((k * CORES + core) * n_own + half * (n_own // 2), n_own // 2)])
    swap_1 = swap_out(1)
    dc_gather.begin()
    dc_whole = lambda dev: dc_out.at[pl.ds(dev * n_own, n_own)]
    dc_mate = [copies.start(dc_whole(seq), dc_whole(seq), mate)]
    loads[0].wait()
    frames = frames_ref[...]
    enc_acc[...] = lax.dot_general(frames.reshape(-1, frames.shape[-1]), da_ref[...], contract_rows, preferred_element_type=F32)
    swap_enc = copies.start(enc_acc.at[rows_of((1 - core) * enc_half, enc_half), :], enc_pair, mate)
    swap_0 = swap_out(0)

    def dc_pass(k):
        dc_mate.append(copies.start(dc_whole(k * CORES + core), dc_whole(k * CORES + core), mate))

    def add_out(part):
        outs_acc[part][...] = gw_ref[pl.ds(part * n_blk, n_blk), rows_of(out_row, out_half), :] + outs_pair[part][...]

    def out_first(part):
        return lambda k, half: outs_acc[part].at[:, rows_of(k * out_q + half * (out_q // 2), out_q // 2), :]

    def out_second(part):
        return lambda k: outs_mid[part].at[k]

    rings = ((ring_x, ring_y), (ring_y, ring_x))
    first = [Reduce(copies, rings[part][0], out_first(part), outs_1[part]) for part in range(2)]
    second = [Swap(copies, rings[part][1], out_second(part), outs_2[part]) for part in range(2)]
    enc_first = Reduce(copies, ring_y, lambda k, half: enc_acc.at[rows_of(enc_row + k * enc_q + half * (enc_q // 2), enc_q // 2), :], enc_y)
    enc_second = Swap(copies, ring_x, lambda k: enc_mid.at[rows_of(k * enc_s, enc_s), :], enc_x)
    pred_first = Swap(copies, ring_y, lambda k: pred_acc.at[rows_of(k * enc_s, enc_s), :], pred_y)

    def out_place(part, k1, k2, half, whole=False):
        start, size = out_row + k1 * out_q, out_q
        if not whole:
            start, size = start + half * (out_q // 2), out_q // 2
        return gwo_out.at[part * n_blk + k2 if k2 is not None else pl.ds(part * n_blk, n_blk), rows_of(start, size), :]

    def pair_place(part):
        ring1, ring2 = rings[part]
        return (
            Spread(copies, ring2, lambda k: out_place(part, ring1.me, k, 0, True)),
            Gather(copies, ring1, lambda k, half: out_place(part, k, None, half)),
        )

    a_g1, a_g2 = pair_place(0)
    b_g1, b_g2 = pair_place(1)
    enc_at = lambda k: gwe_out.at[rows_of(enc_row + y * enc_q + k * enc_s, enc_s), :]
    enc_g1 = Spread(copies, ring_x, enc_at)
    enc_g2 = Gather(copies, ring_y, lambda k, half: gwe_out.at[rows_of(enc_row + k * enc_q + half * (enc_q // 2), enc_q // 2), :])
    pred_at = lambda k: gwp_out.at[x, core, rows_of(k * enc_s, enc_s), :]
    pred_g1 = Spread(copies, ring_y, pred_at)
    pred_g2 = Gather(copies, ring_x, lambda k, half: gwp_out.at[k, core, pl.ds(half * (enc_q // 2), enc_q // 2), :])

    last = []

    def pass_on(ref):
        last.append(copies.start(ref, ref, mate))

    a_whole = lambda k: out_place(0, k, None, 0, True)
    b_whole = lambda k: out_place(1, k, None, 0, True)
    enc_whole = lambda k: gwe_out.at[rows_of(enc_row + k * enc_q, enc_q), :]
    pred_whole = lambda k: gwp_out.at[k, core]

    def widen(g1, g2, whole):
        g1.finish()
        g2.begin()
        pass_on(whole(g2.ring.me))

    def relay(g2, whole):
        g2.relay()
        pass_on(whole(g2.ring.prv))
        pass_on(whole(g2.ring.nxt))

    def close(g2, whole):
        g2.finish()
        pass_on(whole(g2.ring.opp))

    swap_1.wait_recv()
    add_out(1)
    first[1].begin()
    swap_enc.wait_recv()
    enc_acc[rows_of(enc_row, enc_half), :] = enc_acc[rows_of(enc_row, enc_half), :] + enc_pair[...]
    dc_gather.relay()
    dc_pass(ring_x.prv)
    dc_pass(ring_x.nxt)
    swap_0.wait_recv()
    add_out(0)
    first[0].begin()
    first[1].middle()
    enc_first.begin()

    loads[3].wait()
    ge = lax.dot_general(da_ref[...], w_enc_ref[...], (((1,), (1,)), ((), ())), preferred_element_type=F32)
    ge_ref[...] = ge.astype(BF16).reshape(ge_ref.shape)
    ge_out[pl.ds(seq, 1)] = ge_ref[pl.ds(seq, 1)]
    loss_out[pl.ds(seq, 1)] = loss_ref[...][None]
    loads[1].wait()
    loads[2].wait()
    for k in range(n_utt):
        rows_ref[k * n_upos:(k + 1) * n_upos, :] = pred_ref[order_ref[k], :, pl.ds(pl.multiple_of(x * LANES, LANES), LANES)]
    dc_gather.finish()
    dc_pass(ring_x.opp)
    first[0].middle()
    first[1].end(lambda half: outs_mid[1].at[:, pl.ds(half * (out_q // 2), out_q // 2), :])
    second[1].begin()

    small = []
    for hop in range(1, n_seq):
        peer = lax.rem(seq + hop, n_seq)
        small.append(copies.start(ge_ref.at[peer], ge_out.at[seq], {"seq": peer}))
        small.append(copies.start(loss_ref, loss_out.at[seq], {"seq": peer}))

    for copy in dc_mate:
        copy.wait_recv()
    pred_part = lax.dot_general(rows_ref[...], dc_out[...].reshape(n_utt * n_upos, -1), contract_rows, preferred_element_type=F32)
    pred_acc[...] = jnp.where(core == 0, pred_part[:enc_q], pred_part[enc_q:])
    pred_first.begin()
    enc_first.middle()
    first[0].end(lambda half: outs_mid[0].at[:, pl.ds(half * (out_q // 2), out_q // 2), :])
    second[0].begin()
    second[1].end(out_place(1, y, x, 0, True))
    b_g1.begin()
    enc_first.end(lambda half: enc_mid.at[pl.ds(half * (enc_q // 2), enc_q // 2), :])
    enc_second.begin()
    pred_first.end(pred_at(y))
    pred_g1.begin()
    second[0].end(out_place(0, x, y, 0, True))
    a_g1.begin()

    loads[4].wait()
    loads[5].wait()
    for i in range(n_utt):
        grad_rows_ref[i] = dc_out[place_ref[i]]
    widen(b_g1, b_g2, b_whole)
    enc_second.end(enc_at(x))
    enc_g1.begin()
    widen(pred_g1, pred_g2, pred_whole)
    half_utt = n_utt // 2

    def grad_rows(part):
        rows = grad_rows_ref[part * half_utt:(part + 1) * half_utt].reshape(half_utt * n_upos, -1)
        grads = lax.dot_general(rows, w_pred_ref[...], (((1,), (1,)), ((), ())), preferred_element_type=F32)
        gp_out[part * half_utt:(part + 1) * half_utt] = grads.reshape(half_utt, n_upos, -1)

    relay(b_g2, b_whole)
    widen(enc_g1, enc_g2, enc_whole)
    relay(pred_g2, pred_whole)
    widen(a_g1, a_g2, a_whole)
    grad_rows(0)
    close(b_g2, b_whole)
    grad_rows(1)
    relay(enc_g2, enc_whole)
    relay(a_g2, a_whole)
    close(pred_g2, pred_whole)
    close(enc_g2, enc_whole)
    close(a_g2, a_whole)
    for copy in small + last:
        copy.wait_recv()
    copies.drain()


N_COPIES = 3 + 10 + 14 + 3 * 6 + 4 * 6 + 4 * 6 + 16


def unflatten(refs):
    refs = list(refs)
    take = lambda n: [refs.pop(0) for _ in range(n)]
    enc_acc, enc_pair, enc_mid = take(3)
    enc_y, enc_x = take(3), take(3)
    outs = [(take(1)[0], take(1)[0], take(1)[0], take(3), take(3)) for _ in range(2)]
    outs_acc, outs_pair, outs_mid, outs_1, outs_2 = zip(*outs)
    pred_acc = refs.pop(0)
    pred_y = take(3)
    return (enc_acc, enc_pair, enc_mid, enc_y, enc_x, outs_acc, outs_pair, outs_mid, outs_1, outs_2, pred_acc, pred_y, *refs)


def combine(n_seq, order, place, frames, pred_loc, w_enc, w_pred, da, dc, gw, loss):
    width = frames.shape[-1]
    n_utt, n_upos, _ = pred_loc.shape
    joint = da.shape[-1]
    n_blk = gw.shape[0] // 2
    enc_half, out_half = width // CORES, joint // CORES
    enc_q, out_q = enc_half // RING, out_half // RING
    enc_s = enc_q // RING
    ring = lambda *shape: [VMEM(shape, F32)] * 3
    outs = [VMEM((n_blk, out_half, LANES), F32)] * 2 + [VMEM((n_blk, out_q, LANES), F32)] + ring(2, n_blk, out_q // 2, LANES) + ring(out_q, LANES)
    return pl.pallas_call(
        functools.partial(combine_kernel, n_seq),
        out_shape=(
            VMEM(frames.shape, BF16),
            VMEM((n_utt, n_upos, width), F32),
            VMEM((width, joint), F32),
            VMEM((RING, CORES, enc_q, joint), F32),
            VMEM(gw.shape, F32),
            VMEM((n_seq,) + loss.shape, F32),
        ),
        in_specs=[pl.BlockSpec(memory_space=pltpu.HBM)] * 6 + [vspec()] * 4,
        out_specs=(vspec(),) * 6,
        scratch_shapes=[pltpu.SMEM(order.shape, jnp.int32)] * 2
        + [VMEM(v.shape, v.dtype) for v in (frames, pred_loc, w_enc, w_pred)]
        + [pltpu.SemaphoreType.DMA((6,)), VMEM((n_utt, n_upos, joint), BF16), VMEM((n_utt, n_upos, joint), BF16)]
        + [VMEM((width, joint), F32), VMEM((enc_half, joint), F32), VMEM((enc_q, joint), F32)]
        + ring(2, enc_q // 2, joint)
        + ring(enc_s, joint)
        + outs
        + outs
        + [VMEM((enc_q, joint), F32)]
        + ring(enc_s, joint)
        + [
            VMEM((n_utt * n_upos, LANES), BF16),
            VMEM(frames.shape, BF16),
            pltpu.SemaphoreType.DMA((N_COPIES,)),
            pltpu.SemaphoreType.DMA((N_COPIES,)),
        ],
        compiler_params=pltpu.CompilerParams(collective_id=1, has_side_effects=True, vmem_limit_bytes=48_000_000),
        name="combine",
    )(*(in_hbm(v) for v in (order, place, frames, pred_loc, w_enc, w_pred)), *(in_vmem(v) for v in (da, dc, gw, loss)))


def output_kernel(place_hbm, losses_ref, ge_ref, gp_ref, gwe_ref, gwp_ref, gw_ref,
                  loss_out, ge_out, gp_out, gwe_out, gwp_out, gwo_out, place_ref, rows_ref, loss_ref, load_sem, sem):
    n_utt = gp_out.shape[0]
    n_own = ge_ref.shape[1]
    n_cols, _, col = gw_ref.shape
    loads = [pltpu.make_async_copy(place_hbm, place_ref, load_sem.at[0]), pltpu.make_async_copy(losses_ref.at[:, 0, :], rows_ref, load_sem.at[1])]
    for copy in loads:
        copy.start()
    pairs = [(gp_ref, gp_out), (gwe_ref, gwe_out)]
    pairs += [(gw_ref.at[k], gwo_out.at[:, pl.ds(k * col, col)]) for k in range(n_cols)]
    blocks, cores, size, _ = gwp_ref.shape
    pairs += [(gwp_ref.at[k // cores, k % cores], gwp_out.at[pl.ds(k * size, size), :]) for k in range(blocks * cores)]
    copies = [pltpu.make_async_copy(src, dst, sem.at[k]) for k, (src, dst) in enumerate(pairs)]
    for copy in copies:
        copy.start()
    for copy in loads:
        copy.wait()
    for i in range(n_utt):
        place = place_ref[i]
        dev = place // n_own
        own = place - dev * n_own
        loss_ref[i] = rows_ref[dev, own]
        copy = pltpu.make_async_copy(ge_ref.at[dev, own], ge_out.at[i], sem.at[len(copies)])
        copy.start()
        copies.append(copy)
    copy = pltpu.make_async_copy(loss_ref, loss_out, sem.at[len(copies)])
    copy.start()
    copies.append(copy)
    for copy in copies:
        copy.wait()


def outputs(place, losses, ge, gp, gwe, gwp, gw):
    n_seq, n_own, t_loc, width = ge.shape
    n_cols, joint, col = gw.shape
    hbm = pl.BlockSpec(memory_space=pltpu.HBM)
    return pl.pallas_call(
        output_kernel,
        out_shape=(
            jax.ShapeDtypeStruct((n_seq * n_own,), F32),
            jax.ShapeDtypeStruct((n_seq * n_own, t_loc, width), BF16),
            jax.ShapeDtypeStruct(gp.shape, F32),
            jax.ShapeDtypeStruct((width, joint), F32),
            jax.ShapeDtypeStruct((width, joint), F32),
            jax.ShapeDtypeStruct((joint, n_cols * col), F32),
        ),
        in_specs=[hbm] + [vspec()] * 6,
        out_specs=(hbm,) * 6,
        scratch_shapes=[
            pltpu.SMEM(place.shape, jnp.int32),
            pltpu.SMEM((n_seq, losses.shape[-1]), F32),
            pltpu.SMEM(place.shape, F32),
            pltpu.SemaphoreType.DMA((2,)),
            pltpu.SemaphoreType.DMA((2 + n_cols + RING * CORES + n_seq * n_own + 1,)),
        ],
        compiler_params=pltpu.CompilerParams(vmem_limit_bytes=48_000_000),
        name="outputs",
    )(in_hbm(place), *(in_vmem(v) for v in (losses, ge, gp, gwe, gwp, gw)))


def solution(mesh):
    n_seq = mesh.shape["seq"]
    utt_rows = P(("part", "data"))
    utt_mats = P(("part", "data"), None)
    utt_cube = P(("part", "data"), None, None)
    enc_spec = P(("part", "data"), "seq", None)
    weight_in = P(None, None)
    weight_out = P("part", None)

    def body(enc_loc, pred_loc, w_enc, w_pred, w_out, labels, frame_len, label_len):
        t_loc = enc_loc.shape[1]
        n_upos = pred_loc.shape[1]
        seq_idx = lax.axis_index("seq").astype(jnp.int32).reshape(1)
        order, place, frames, act, pred, w_out_t = exchange(n_seq, frame_len, label_len, enc_loc, pred_loc, w_enc, w_pred, w_out)
        da, dc, gw, loss = lattice(n_seq, seq_idx, order, frame_len, label_len, labels, act, pred, w_out, w_out_t, n_upos, t_loc)
        ge, gp, gwe, gwp, gw, losses = combine(n_seq, order, place, frames, pred_loc, w_enc, w_pred, da, dc, gw, loss)
        loss, grad_enc, grad_pred, gw_enc, gw_pred, gw_out = outputs(place, losses, ge, gp, gwe, gwp, gw)
        return loss, grad_enc, grad_pred, gw_enc, gw_pred, gw_out

    return jax.shard_map(body, mesh=mesh, in_specs=(enc_spec, utt_cube, weight_in, weight_in, weight_in, utt_mats, utt_rows, utt_rows), out_specs=(utt_rows, enc_spec, utt_cube, weight_out, weight_out, weight_out), check_vma=False)
```
